32 devices in a mesh: dp: 8 (over z, y), tensor: 4 (over x, core).
Axes of the slice: x: 2, y: 2, z: 4, core: 2. Of those that a mesh axis runs over, the one named last changes fastest.
Arguments:
- inputs: bfloat16 [4096, 2048], P('dp'), may hold values from -18 to 18
- norm1_gain: float32 [2048], replicated, may hold values from 0.5 to 1.5
- query_weight: bfloat16 [2048, 2048], P(None, 'tensor'), may hold values from -1 to 1
- key_weight: bfloat16 [2048, 512], P(None, 'tensor'), may hold values from -1 to 1
- value_weight: bfloat16 [2048, 512], P(None, 'tensor'), may hold values from -0.125 to 0.125
- w_out: bfloat16 [2048, 2048], P('tensor'), may hold values from -0.5 to 0.5
- norm2_gain: float32 [2048], replicated, may hold values from 0.5 to 1.5
- w_gate: bfloat16 [2048, 8192], P(None, 'tensor'), may hold values from -0.125 to 0.125
- w_up: bfloat16 [2048, 8192], P(None, 'tensor'), may hold values from -0.125 to 0.125
- w_down: bfloat16 [8192, 2048], P('tensor'), may hold values from -0.0625 to 0.0625
- doc_ids: int32 [4096], P('dp'), may hold values from 0 to 31, never falling along the last dimension, each value on 1 to 512 neighbouring positions
- grad_output: bfloat16 [4096, 2048], P('dp'), may hold values from -6 to 6
Outputs:
- output: bfloat16 [4096, 2048], P('dp')
- grad_inputs: bfloat16 [4096, 2048], P('dp')
- grad_norm1: float32 [2048], P('dp')
- grad_query: float32 [2048, 2048], P('dp', 'tensor')
- grad_key: float32 [2048, 512], P('dp', 'tensor')
- grad_value: float32 [2048, 512], P('dp', 'tensor')
- grad_outproj: float32 [2048, 2048], P(('tensor', 'dp'))
- grad_norm2: float32 [2048], P('dp')
- grad_gate: float32 [2048, 8192], P('dp', 'tensor')
- grad_up: float32 [2048, 8192], P('dp', 'tensor')
- grad_down: float32 [8192, 2048], P(('tensor', 'dp'))
The draws below stay inside these ranges and needn't reach their ends.
Inputs may be any that keep to these rules, and one draw needn't show every extreme that they name: `doc_ids`: document numbers never fall along the tokens; each number covers 1 to 512 consecutive tokens and one document has exactly 512 tokens.
All inputs are finite; a program needn't handle non-finite values.
Results may differ from the reference program's by a relative error of at most 0.029.
Values may be sent and summed in bfloat16 or wider, within the bound.
A program may use at most 256 MiB of HBM per device.

```python
import math
import jax
import jax.numpy as jnp
import numpy as np
from jax import lax

D = 2048
H = 32
KEY_VALUE_HEADS = 8
HEAD_SIZE = 64
FF = 8192
DOC_MAX = 512
TOK_DEV = 512
TOTAL_TOKENS = 4096
N_DP = 8


def draw_weight(key, salt_value, head_count):
    base_rows = jnp.clip(jax.random.normal(jax.random.fold_in(key, salt_value), (D, head_count * HEAD_SIZE), jnp.float32), -6.0, 6.0) * D ** (-0.5)
    return base_rows


def draw_query_weight(key, part):
    return draw_weight(key, 101, H).astype(jnp.bfloat16)


def draw_key_weight(key, part):
    return draw_weight(key, 102, KEY_VALUE_HEADS).astype(jnp.bfloat16)


def draw_inputs(key, part):
    random_part = jnp.clip(jax.random.normal(jax.random.fold_in(key, 21), (TOTAL_TOKENS, D), jnp.float32), -6.0, 6.0)
    pairing = jax.random.permutation(jax.random.fold_in(key, 22), N_DP)
    row_block = jnp.arange(TOTAL_TOKENS, dtype=jnp.int32) // TOK_DEV
    col_block = jnp.arange(D, dtype=jnp.int32) // (D // N_DP)
    boosted = jnp.where(pairing[row_block][:, None] == col_block[None, :], 3.0, 1.0)
    base_rows = random_part * boosted
    return base_rows.astype(jnp.bfloat16)


def steps_of(rng, shape, shards, smallest, top_value):
    def one(dim, blocks):
        steps = jax.random.uniform(jax.random.fold_in(jax.random.fold_in(rng, 6), dim), (blocks,), jnp.float32, smallest / len(shards), top_value / len(shards))
        return jnp.repeat(jnp.exp(steps), shape[dim] // blocks).reshape((-1,) + (1,) * (len(shape) - dim - 1))

    gain = one(*shards[0])
    for cut in shards[1:]:
        gain = gain * one(*cut)
    return gain


def length_profile(amount, total, limit, slope):
    portions = [(1 << 20) // math.isqrt(standing ** slope) + 1 for standing in range(2, amount + 1)]
    rest, counts = total - limit - (amount - 1), [1] * (amount - 1)
    while rest > 0:
        candidates = [i for i in range(amount - 1) if counts[i] < limit]
        whole, left = sum([portions[i] for i in candidates]), rest
        for i in candidates:
            extra = min(limit - counts[i], max(1, left * portions[i] // whole), rest)
            counts[i] = counts[i] + extra
            rest = rest - extra
    return np.array([limit] + counts)


def uneven(own_key, amount, total, bound, slope):
    if amount == 2:
        one = jax.random.randint(own_key, (), max(1, total - bound), min(bound, total - 1) + 1)
        return jnp.stack([one, total - one])
    lengths = jnp.asarray(length_profile(amount, total, bound, slope), jnp.int32)
    couples = (amount - 1) // 2
    giver, taker = lengths[1:1 + 2 * couples:2], lengths[2:2 + 2 * couples:2]
    margin = jnp.minimum(giver - 1, bound - taker)
    shifted = jax.random.randint(jax.random.fold_in(own_key, 1), (couples,), 0, 1 << 20) % (margin + 1)
    lengths = lengths.at[1:1 + 2 * couples:2].set(giver - shifted).at[2:2 + 2 * couples:2].set(taker + shifted)
    return lengths[jax.random.permutation(jax.random.fold_in(own_key, 2), amount)]


def gaussian(own_key, shape, scale, limit, split=(), kind=jnp.bfloat16):
    gain = steps_of(own_key, shape, split, -0.22, 0.18) if split else 1.0
    entries = jax.random.normal(own_key, shape, jnp.float32) * scale * gain
    return jnp.minimum(jnp.maximum(entries, -limit), limit).astype(kind)


def setup_inputs(seed: int = 0) -> dict:
    key_list = jax.random.split(jax.random.key(seed), 13)
    return {
        "inputs": draw_inputs(jax.random.fold_in(key_list[12], 71), 0),
        "norm1_gain": jnp.clip(1.0 + 0.1 * jax.random.normal(key_list[1], (D,), jnp.float32), 0.5, 1.5),
        "query_weight": draw_query_weight(jax.random.fold_in(key_list[12], 71), 0),
        "key_weight": draw_key_weight(jax.random.fold_in(key_list[12], 71), 0),
        "value_weight": gaussian(key_list[4], (D, KEY_VALUE_HEADS * HEAD_SIZE), D ** -0.5, 0.125, ((1, 4),)),
        "w_out": gaussian(key_list[5], (H * HEAD_SIZE, D), (H * HEAD_SIZE // 16) ** -0.5, 0.5, ((0, 4),)),
        "norm2_gain": jnp.clip(1.0 + 0.1 * jax.random.normal(key_list[6], (D,), jnp.float32), 0.5, 1.5),
        "w_gate": gaussian(key_list[7], (D, FF), D ** -0.5, 0.125, ((1, 4),)),
        "w_up": gaussian(key_list[8], (D, FF), D ** -0.5, 0.125, ((1, 4),)),
        "w_down": gaussian(key_list[9], (FF, D), FF ** -0.5, 0.0625, ((0, 4),)),
        "doc_ids": jnp.searchsorted(jnp.cumsum(uneven(key_list[10], TOTAL_TOKENS * 4 // DOC_MAX, TOTAL_TOKENS, DOC_MAX, 1)), jnp.arange(TOTAL_TOKENS), side="right").astype(jnp.int32),
        "grad_output": gaussian(key_list[11], (TOTAL_TOKENS, D), 1.0, 6.0, ((0, 8),)),
    }


NORM_EPSILON = 1e-05

def rope_table(half_count):
    adjusted = []
    for index in range(half_count):
        base_value = 500000.0 ** (-index / half_count)
        wave_length = 2.0 * math.pi / base_value
        smooth = (8192.0 / wave_length - 1.0) / 3.0
        if wave_length > 8192.0:
            adjusted.append(base_value / 32.0)
        elif wave_length >= 2048.0:
            adjusted.append((1.0 - smooth) * base_value / 32.0 + smooth * base_value)
        else:
            adjusted.append(base_value)
    return jnp.asarray(adjusted, dtype=jnp.float32)

def rope_angles(start_row, count_rows, half_count):
    positions = (start_row + jnp.arange(count_rows, dtype=jnp.int32)).astype(jnp.float32)
    phase_angle = positions[:, None] * rope_table(half_count)[None, :]
    return (jnp.cos(phase_angle)[:, None, :], jnp.sin(phase_angle)[:, None, :])

def rotate_halves(values, cosine_table, sine_values):
    half_size = values.shape[-1] // 2
    first_half = values[..., :half_size]
    second_half = values[..., half_size:]
    return jnp.concatenate([first_half * cosine_table - second_half * sine_values, second_half * cosine_table + first_half * sine_values], axis=-1)

def norm_rows(values, gain_row):
    inverse_root = lax.rsqrt(lax.optimization_barrier(jnp.mean(values * values, axis=-1, keepdims=True)) + NORM_EPSILON)
    return (inverse_root, values * inverse_root * gain_row)

def norm_back(values, inverse_root, gain_row, upstream):
    scaled = gain_row * upstream
    gain_grad = lax.optimization_barrier(jnp.sum(upstream * values * inverse_root, axis=0))
    input_grad = inverse_root * scaled - values * inverse_root ** 3 * lax.optimization_barrier(jnp.mean(scaled * values, axis=-1, keepdims=True))
    return (gain_grad, input_grad)

def wide_einsum(form, left_side, right_side):
    return jnp.einsum(form, left_side.astype(jnp.float32), right_side.astype(jnp.float32))

def block_scores(query_rows, key_rows, query_ids, key_ids, query_pos, key_pos):
    scores = wide_einsum('qgrd,kgd->grqk', query_rows, key_rows) * HEAD_SIZE ** (-0.5)
    allowed = (query_ids[:, None] == key_ids[None, :]) & (key_pos[None, :] <= query_pos[:, None])
    return jnp.where(allowed, scores, -1e+30)

def block_forward(query_rows, key_rows, value_rows, query_ids, key_ids, query_pos, key_pos):
    scores = block_scores(query_rows, key_rows, query_ids, key_ids, query_pos, key_pos)
    row_peak = lax.optimization_barrier(jnp.max(scores, axis=-1, keepdims=True))
    logsum = row_peak + jnp.log(lax.optimization_barrier(jnp.sum(jnp.exp(scores - row_peak), axis=-1, keepdims=True)))
    prob_low = jnp.exp(scores - logsum).astype(jnp.bfloat16)
    mixed_rows = wide_einsum('grqk,kgd->qgrd', prob_low, value_rows)
    return (mixed_rows.astype(jnp.bfloat16), logsum)

def block_backward(query_rows, key_rows, value_rows, out_rows, grad_rows, logsum, query_ids, key_ids, query_pos, key_pos):
    scores = block_scores(query_rows, key_rows, query_ids, key_ids, query_pos, key_pos)
    prob_rows = jnp.exp(scores - logsum)
    grad_vals = wide_einsum('grqk,qgrd->kgd', prob_rows.astype(jnp.bfloat16), grad_rows)
    delta_rows = lax.optimization_barrier(jnp.sum(out_rows.astype(jnp.float32) * grad_rows.astype(jnp.float32), axis=-1))
    grad_probs = wide_einsum('qgrd,kgd->grqk', grad_rows, value_rows)
    grad_scores = (prob_rows * (grad_probs - jnp.transpose(delta_rows, (1, 2, 0))[..., None])).astype(jnp.bfloat16)
    grad_query_rows = wide_einsum('grqk,kgd->qgrd', grad_scores, key_rows) * HEAD_SIZE ** (-0.5)
    grad_key_rows = wide_einsum('grqk,qgrd->kgd', grad_scores, query_rows) * HEAD_SIZE ** (-0.5)
    return (grad_query_rows, grad_key_rows, grad_vals)

def reference(inputs, norm1_gain, query_weight, key_weight, value_weight, w_out, norm2_gain, w_gate, w_up, w_down, doc_ids, grad_output):
    group_size = H // KEY_VALUE_HEADS
    blocks = TOTAL_TOKENS // DOC_MAX
    cosine_table, sine_values = rope_angles(0, TOTAL_TOKENS, HEAD_SIZE // 2)
    inputs_wide = inputs.astype(jnp.float32)
    root_one, normed = norm_rows(inputs_wide, norm1_gain)
    normed_narrow_input = normed.astype(jnp.bfloat16)
    query_raw = jnp.dot(normed_narrow_input, query_weight, preferred_element_type=jnp.float32).reshape(TOTAL_TOKENS, H, HEAD_SIZE)
    key_raw = jnp.dot(normed_narrow_input, key_weight, preferred_element_type=jnp.float32).reshape(TOTAL_TOKENS, KEY_VALUE_HEADS, HEAD_SIZE)
    value_low = jnp.dot(normed_narrow_input, value_weight, preferred_element_type=jnp.float32).astype(jnp.bfloat16).reshape(TOTAL_TOKENS, KEY_VALUE_HEADS, HEAD_SIZE)
    query_low = rotate_halves(query_raw, cosine_table, sine_values).astype(jnp.bfloat16).reshape(TOTAL_TOKENS, KEY_VALUE_HEADS, group_size, HEAD_SIZE)
    key_low = rotate_halves(key_raw, cosine_table, sine_values).astype(jnp.bfloat16)
    pad_keys = jnp.concatenate([jnp.zeros((DOC_MAX, KEY_VALUE_HEADS, HEAD_SIZE), jnp.bfloat16), key_low], axis=0)
    pad_values = jnp.concatenate([jnp.zeros((DOC_MAX, KEY_VALUE_HEADS, HEAD_SIZE), jnp.bfloat16), value_low], axis=0)
    query_ids = doc_ids + 1
    pad_ids = jnp.concatenate([jnp.zeros((DOC_MAX,), jnp.int32), query_ids])
    pad_pos = jnp.arange(TOTAL_TOKENS + DOC_MAX, dtype=jnp.int32) - DOC_MAX
    query_pos = jnp.arange(TOTAL_TOKENS, dtype=jnp.int32)

    def block_inputs(number):
        start_row = number * DOC_MAX
        return (lax.dynamic_slice_in_dim(query_low, start_row, DOC_MAX), lax.dynamic_slice_in_dim(pad_keys, start_row, 2 * DOC_MAX), lax.dynamic_slice_in_dim(pad_values, start_row, 2 * DOC_MAX), lax.dynamic_slice_in_dim(query_ids, start_row, DOC_MAX), lax.dynamic_slice_in_dim(pad_ids, start_row, 2 * DOC_MAX), lax.dynamic_slice_in_dim(query_pos, start_row, DOC_MAX), lax.dynamic_slice_in_dim(pad_pos, start_row, 2 * DOC_MAX))

    def forward_block(number):
        pieces = block_inputs(number)
        return block_forward(*pieces)
    numbers = jnp.arange(blocks, dtype=jnp.int32)
    mixed_blocks, logsum_blocks = lax.map(forward_block, numbers)
    mixed_low = mixed_blocks.reshape(TOTAL_TOKENS, H * HEAD_SIZE)
    residual = inputs_wide + jnp.dot(mixed_low, w_out, preferred_element_type=jnp.float32)
    step_rows = math.gcd(TOTAL_TOKENS, 4096)

    def mlp_step(totals, pieces):
        residual_rows, grad_rows = pieces
        root_two, normed_two = norm_rows(residual_rows, norm2_gain)
        normed_two_low = normed_two.astype(jnp.bfloat16)
        gate_value = jnp.dot(normed_two_low, w_gate, preferred_element_type=jnp.float32)
        up_value = jnp.dot(normed_two_low, w_up, preferred_element_type=jnp.float32)
        hidden_low = (jax.nn.silu(gate_value) * up_value).astype(jnp.bfloat16)
        output_rows = (residual_rows + jnp.dot(hidden_low, w_down, preferred_element_type=jnp.float32)).astype(jnp.bfloat16)
        grad_wdown = jnp.dot(hidden_low.T, grad_rows, preferred_element_type=jnp.float32)
        grad_hidden = jnp.dot(grad_rows, w_down.T, preferred_element_type=jnp.float32)
        sigmoid_gate = jax.nn.sigmoid(gate_value)
        grad_gate_low = (grad_hidden * up_value * sigmoid_gate * (1.0 + gate_value * (1.0 - sigmoid_gate))).astype(jnp.bfloat16)
        grad_up_low = (grad_hidden * jax.nn.silu(gate_value)).astype(jnp.bfloat16)
        grad_wgate = jnp.dot(normed_two_low.T, grad_gate_low, preferred_element_type=jnp.float32)
        grad_wup = jnp.dot(normed_two_low.T, grad_up_low, preferred_element_type=jnp.float32)
        grad_normed_two = jnp.dot(grad_gate_low, w_gate.T, preferred_element_type=jnp.float32) + jnp.dot(grad_up_low, w_up.T, preferred_element_type=jnp.float32)
        gain_grad, input_grad = norm_back(residual_rows, root_two, norm2_gain, grad_normed_two)
        new_totals = (totals[0] + grad_wgate, totals[1] + grad_wup, totals[2] + grad_wdown, totals[3] + gain_grad)
        return (new_totals, (output_rows, grad_rows.astype(jnp.float32) + input_grad))
    start_totals = (jnp.zeros((D, FF), jnp.float32), jnp.zeros((D, FF), jnp.float32), jnp.zeros((FF, D), jnp.float32), jnp.zeros((D,), jnp.float32))
    mlp_totals, mlp_rows = lax.scan(mlp_step, start_totals, (residual.reshape(TOTAL_TOKENS // step_rows, step_rows, D), grad_output.reshape(TOTAL_TOKENS // step_rows, step_rows, D)))
    grad_wgate, grad_wup, grad_wdown, grad_gain_two = mlp_totals
    output = mlp_rows[0].reshape(TOTAL_TOKENS, D)
    grad_residual = mlp_rows[1].reshape(TOTAL_TOKENS, D)
    grad_res_low = grad_residual.astype(jnp.bfloat16)
    grad_wout = jnp.dot(mixed_low.T, grad_res_low, preferred_element_type=jnp.float32)
    grad_mixed = jnp.dot(grad_res_low, w_out.T, preferred_element_type=jnp.float32).astype(jnp.bfloat16).reshape(TOTAL_TOKENS, KEY_VALUE_HEADS, group_size, HEAD_SIZE)
    mixed_view = mixed_low.reshape(TOTAL_TOKENS, KEY_VALUE_HEADS, group_size, HEAD_SIZE)

    def backward_block(number):
        pieces = block_inputs(number)
        start_row = number * DOC_MAX
        return block_backward(pieces[0], pieces[1], pieces[2], lax.dynamic_slice_in_dim(mixed_view, start_row, DOC_MAX), lax.dynamic_slice_in_dim(grad_mixed, start_row, DOC_MAX), logsum_blocks[number], pieces[3], pieces[4], pieces[5], pieces[6])
    grad_q_blocks, grad_k_blocks, grad_v_blocks = lax.map(backward_block, numbers)
    zero_block = jnp.zeros((1, DOC_MAX, KEY_VALUE_HEADS, HEAD_SIZE), jnp.float32)
    key_raw_gradient = (grad_k_blocks[:, DOC_MAX:] + jnp.concatenate([grad_k_blocks[1:, :DOC_MAX], zero_block], axis=0)).reshape(TOTAL_TOKENS, KEY_VALUE_HEADS, HEAD_SIZE)
    grad_vals = (grad_v_blocks[:, DOC_MAX:] + jnp.concatenate([grad_v_blocks[1:, :DOC_MAX], zero_block], axis=0)).reshape(TOTAL_TOKENS, KEY_VALUE_HEADS * HEAD_SIZE)
    grad_qraw = grad_q_blocks.reshape(TOTAL_TOKENS, H, HEAD_SIZE)
    query_low_gradient = rotate_halves(grad_qraw, cosine_table, -sine_values).astype(jnp.bfloat16).reshape(TOTAL_TOKENS, H * HEAD_SIZE)
    key_low_gradient = rotate_halves(key_raw_gradient, cosine_table, -sine_values).astype(jnp.bfloat16).reshape(TOTAL_TOKENS, KEY_VALUE_HEADS * HEAD_SIZE)
    value_low_gradient = grad_vals.astype(jnp.bfloat16)
    grad_wquery = jnp.dot(normed_narrow_input.T, query_low_gradient, preferred_element_type=jnp.float32)
    key_weight_gradient = jnp.dot(normed_narrow_input.T, key_low_gradient, preferred_element_type=jnp.float32)
    grad_wvalue = jnp.dot(normed_narrow_input.T, value_low_gradient, preferred_element_type=jnp.float32)
    normed_input_gradient = jnp.dot(query_low_gradient, query_weight.T, preferred_element_type=jnp.float32) + jnp.dot(key_low_gradient, key_weight.T, preferred_element_type=jnp.float32) + jnp.dot(value_low_gradient, value_weight.T, preferred_element_type=jnp.float32)
    grad_gain_one, input_grad = norm_back(inputs_wide, root_one, norm1_gain, normed_input_gradient)
    grad_inputs = (grad_residual + input_grad).astype(jnp.bfloat16)
    return (output, grad_inputs, grad_gain_one, grad_wquery, key_weight_gradient, grad_wvalue, grad_wout, grad_gain_two, grad_wgate, grad_wup, grad_wdown)
```

```python
import math

import jax
import jax.numpy as jnp
from jax import lax
from jax.sharding import PartitionSpec as P

HEAD_SIZE = 64
DOC_MAX = 512
NORM_EPSILON = 1e-05

PAIR = 2


def rope_table(half_count):
    adjusted = []
    for index in range(half_count):
        base_value = 500000.0 ** (-index / half_count)
        wave_length = 2.0 * math.pi / base_value
        smooth = (8192.0 / wave_length - 1.0) / 3.0
        if wave_length > 8192.0:
            adjusted.append(base_value / 32.0)
        elif wave_length >= 2048.0:
            adjusted.append((1.0 - smooth) * base_value / 32.0 + smooth * base_value)
        else:
            adjusted.append(base_value)
    return jnp.asarray(adjusted, dtype=jnp.float32)


def rope_angles(start_row, count_rows, half_count):
    positions = (start_row + jnp.arange(count_rows, dtype=jnp.int32)).astype(jnp.float32)
    phase_angle = positions[:, None] * rope_table(half_count)[None, :]
    return (jnp.cos(phase_angle)[:, None, :], jnp.sin(phase_angle)[:, None, :])


def rotate_halves(values, cosine_table, sine_values):
    half_size = values.shape[-1] // 2
    first_half = values[..., :half_size]
    second_half = values[..., half_size:]
    return jnp.concatenate(
        [
            first_half * cosine_table - second_half * sine_values,
            second_half * cosine_table + first_half * sine_values,
        ],
        axis=-1,
    )


def norm_rows(values, gain_row):
    inverse_root = lax.rsqrt(jnp.mean(values * values, axis=-1, keepdims=True) + NORM_EPSILON)
    return (inverse_root, values * inverse_root * gain_row)


def norm_back(values, inverse_root, gain_row, upstream):
    scaled = gain_row * upstream
    return inverse_root * scaled - values * inverse_root**3 * jnp.mean(
        scaled * values, axis=-1, keepdims=True
    )


def passed_along(block, axis, distance):
    devices = range(lax.axis_size(axis))
    route = [(i - distance, i) for i in devices if i - distance in devices]
    return lax.ppermute(block, axis, route)


def tensor_swap(block, bit):
    return lax.ppermute(block, "tensor", [(i, i ^ bit) for i in range(lax.axis_size("tensor"))])


def pair_swap(block):
    return lax.ppermute(block, "dp", [(i, i ^ 1) for i in range(lax.axis_size("dp"))])


def group_shift(block, distance):
    count = lax.axis_size("dp")
    groups = count // PAIR
    return lax.ppermute(
        block,
        "dp",
        [(i, ((i // PAIR + distance) % groups) * PAIR + i % PAIR) for i in range(count)],
    )


def tensor_sum(part):
    half = part.shape[1] // 2
    low = lax.axis_index("tensor") % 2
    first, second = part[:, :half], part[:, half:]
    mine = jnp.where(low == 0, first, second)
    other = jnp.where(low == 0, second, first).astype(jnp.bfloat16)
    mine = mine + tensor_swap(other, 1).astype(jnp.float32)
    bit = 2
    while bit < lax.axis_size("tensor"):
        rounded = mine.astype(jnp.bfloat16)
        mine = rounded.astype(jnp.float32) + tensor_swap(rounded, bit).astype(jnp.float32)
        bit *= 2
    mine = mine.astype(jnp.bfloat16)
    other = tensor_swap(mine, 1)
    return jnp.concatenate(
        [jnp.where(low == 0, mine, other), jnp.where(low == 0, other, mine)], axis=1
    ).astype(jnp.float32)


def gather_groups(block):
    half = block.shape[1] // 2
    low = lax.axis_index("tensor") % 2
    piece = lax.dynamic_slice_in_dim(block, low * half, half, axis=1)
    rows = [block]
    for _ in range(lax.axis_size("dp") // PAIR - 1):
        piece = group_shift(piece, 1)
        other = tensor_swap(piece, 1)
        rows.append(
            jnp.concatenate(
                [jnp.where(low == 0, piece, other), jnp.where(low == 0, other, piece)], axis=1
            )
        )
    return jnp.concatenate(rows, axis=0)


def pair_sum(part):
    member = lax.axis_index("dp") % PAIR
    mine = lax.dynamic_index_in_dim(part, member, 1, keepdims=False)
    other = lax.dynamic_index_in_dim(part, 1 - member, 1, keepdims=False)
    return mine + pair_swap(other.astype(jnp.bfloat16)).astype(jnp.float32)


def group_exchange(blocks):
    groups = blocks.shape[0]
    group = lax.axis_index("dp") // PAIR
    received = []
    for distance in range(groups):
        block = lax.dynamic_index_in_dim(blocks, (group + distance) % groups, 0, keepdims=False)
        received.append(block if distance == 0 else group_shift(block, distance))
    return received


def scatter_sum(part):
    summed = pair_sum(part)
    groups = summed.shape[0]
    group = lax.axis_index("dp") // PAIR
    total = lax.dynamic_index_in_dim(summed, group, 0, keepdims=False)
    rounded = summed.astype(jnp.bfloat16)
    for block in group_exchange(rounded)[1:]:
        total = total + block.astype(jnp.float32)
    return total


def block_scores(query_rows, key_rows, query_ids, key_ids, query_pos, key_pos):
    scores = jnp.einsum(
        "qgrd,kgd->grqk", query_rows, key_rows, preferred_element_type=jnp.float32
    ) * HEAD_SIZE ** (-0.5)
    allowed = (query_ids[:, None] == key_ids[None, :]) & (key_pos[None, :] <= query_pos[:, None])
    return jnp.where(allowed, scores, -1e30)


def block_forward(query_rows, key_rows, value_rows, query_ids, key_ids, query_pos, key_pos):
    scores = block_scores(query_rows, key_rows, query_ids, key_ids, query_pos, key_pos)
    row_peak = jnp.max(scores, axis=-1, keepdims=True)
    logsum = row_peak + jnp.log(jnp.sum(jnp.exp(scores - row_peak), axis=-1, keepdims=True))
    prob_low = jnp.exp(scores - logsum).astype(jnp.bfloat16)
    mixed_rows = jnp.einsum(
        "grqk,kgd->qgrd", prob_low, value_rows, preferred_element_type=jnp.float32
    )
    return (mixed_rows.astype(jnp.bfloat16), logsum)


def block_backward(
    query_rows,
    key_rows,
    value_rows,
    out_rows,
    grad_rows,
    logsum,
    query_ids,
    key_ids,
    query_pos,
    key_pos,
):
    scores = block_scores(query_rows, key_rows, query_ids, key_ids, query_pos, key_pos)
    prob_rows = jnp.exp(scores - logsum)
    grad_vals = jnp.einsum(
        "grqk,qgrd->kgd",
        prob_rows.astype(jnp.bfloat16),
        grad_rows,
        preferred_element_type=jnp.float32,
    )
    delta_rows = jnp.sum(out_rows.astype(jnp.float32) * grad_rows.astype(jnp.float32), axis=-1)
    grad_probs = jnp.einsum(
        "qgrd,kgd->grqk", grad_rows, value_rows, preferred_element_type=jnp.float32
    )
    grad_scores = (
        prob_rows * (grad_probs - jnp.transpose(delta_rows, (1, 2, 0))[..., None])
    ).astype(jnp.bfloat16)
    grad_query_rows = jnp.einsum(
        "grqk,kgd->qgrd", grad_scores, key_rows, preferred_element_type=jnp.float32
    ) * HEAD_SIZE ** (-0.5)
    grad_key_rows = jnp.einsum(
        "grqk,qgrd->kgd", grad_scores, query_rows, preferred_element_type=jnp.float32
    ) * HEAD_SIZE ** (-0.5)
    return (grad_query_rows, grad_key_rows, grad_vals)


def dot(form, left, right):
    return jnp.einsum(form, left, right, preferred_element_type=jnp.float32)


def gated(gate_value, up_value):
    return (jax.nn.silu(gate_value) * up_value).astype(jnp.bfloat16)


def gated_back(grad_hidden, gate_value, up_value):
    sigmoid_gate = jax.nn.sigmoid(gate_value)
    grad_gate_low = (
        grad_hidden * up_value * sigmoid_gate * (1.0 + gate_value * (1.0 - sigmoid_gate))
    ).astype(jnp.bfloat16)
    return grad_gate_low, (grad_hidden * jax.nn.silu(gate_value)).astype(jnp.bfloat16)


def shards(
    inputs,
    norm1_gain,
    query_weight,
    key_weight,
    value_weight,
    w_out,
    norm2_gain,
    w_gate,
    w_up,
    w_down,
    doc_ids,
    grad_output,
):
    tok_rows, width = inputs.shape
    heads_here = query_weight.shape[1] // HEAD_SIZE
    kv_here = key_weight.shape[1] // HEAD_SIZE
    group_size = heads_here // kv_here
    n_dp = lax.axis_size("dp")
    groups = n_dp // PAIR
    group = lax.axis_index("dp") // PAIR
    offset = lax.axis_index("dp") * tok_rows
    grad_all = gather_groups(grad_output)

    cosine_table, sine_values = rope_angles(offset, tok_rows, HEAD_SIZE // 2)
    inputs_wide = inputs.astype(jnp.float32)
    root_one, normed = norm_rows(inputs_wide, norm1_gain)
    normed_low = normed.astype(jnp.bfloat16)
    query_raw = dot("td,dh->th", normed_low, query_weight).reshape(tok_rows, heads_here, HEAD_SIZE)
    key_raw = dot("td,dh->th", normed_low, key_weight).reshape(tok_rows, kv_here, HEAD_SIZE)
    value_low = dot("td,dh->th", normed_low, value_weight).astype(jnp.bfloat16)
    query_low = (
        rotate_halves(query_raw, cosine_table, sine_values)
        .astype(jnp.bfloat16)
        .reshape(tok_rows, kv_here, group_size, HEAD_SIZE)
    )
    key_low = (
        rotate_halves(key_raw, cosine_table, sine_values)
        .astype(jnp.bfloat16)
        .reshape(tok_rows, kv_here * HEAD_SIZE)
    )
    query_ids = doc_ids + 1
    tail = jnp.concatenate([key_low, value_low], axis=1)
    prev_tail = passed_along(tail, "dp", 1)
    prev_ids = passed_along(query_ids, "dp", 1)
    both = jnp.concatenate([prev_tail, tail], axis=0)
    keys_all = both[:, : kv_here * HEAD_SIZE].reshape(2 * DOC_MAX, kv_here, HEAD_SIZE)
    values_all = both[:, kv_here * HEAD_SIZE :].reshape(2 * DOC_MAX, kv_here, HEAD_SIZE)
    ids_all = jnp.concatenate([prev_ids, query_ids])
    pos_all = offset - DOC_MAX + jnp.arange(tok_rows + DOC_MAX, dtype=jnp.int32)
    query_pos = pos_all[DOC_MAX:]
    mixed_block, logsum_block = block_forward(
        query_low, keys_all, values_all, query_ids, ids_all, query_pos, pos_all
    )
    mixed_low = mixed_block.reshape(tok_rows, heads_here * HEAD_SIZE)
    residual = inputs_wide + tensor_sum(dot("te,ed->td", mixed_low, w_out))

    root_two, normed_two = norm_rows(residual, norm2_gain)
    normed_two_low = normed_two.astype(jnp.bfloat16)
    normed_all = gather_groups(normed_two_low)
    gate_value = dot("td,df->tf", normed_two_low, w_gate)
    up_value = dot("td,df->tf", normed_two_low, w_up)
    grad_hidden = dot("td,fd->tf", grad_output, w_down)
    hidden_low = gated(gate_value, up_value)
    grad_gate_low, grad_up_low = gated_back(grad_hidden, gate_value, up_value)
    normed_two_part = dot("tf,df->td", grad_gate_low, w_gate) + dot("tf,df->td", grad_up_low, w_up)
    grad_normed_two = tensor_sum(normed_two_part)
    gain_two_part = jnp.sum(normed_two_part * residual * root_two, axis=0)
    output = (residual + tensor_sum(dot("tf,fd->td", hidden_low, w_down))).astype(jnp.bfloat16)

    share = w_gate.shape[1] // groups
    gate_share = lax.dynamic_slice_in_dim(w_gate, group * share, share, axis=1)
    up_share = lax.dynamic_slice_in_dim(w_up, group * share, share, axis=1)
    down_share = lax.dynamic_slice_in_dim(w_down, group * share, share, axis=0)
    gate_all = dot("td,df->tf", normed_all, gate_share)
    up_all = dot("td,df->tf", normed_all, up_share)
    grad_hidden_all = dot("td,fd->tf", grad_all, down_share)
    hidden_all = gated(gate_all, up_all)
    gate_low_all, up_low_all = gated_back(grad_hidden_all, gate_all, up_all)
    down_part = dot("tf,td->fd", hidden_all, grad_all)
    grad_wdown = pair_sum(down_part.reshape(1, PAIR, share // PAIR, width))[0]
    rows_here = width // n_dp

    def column_grad(low_all):
        part = dot("td,tf->df", normed_all, low_all)
        summed = pair_sum(part.reshape(groups, PAIR, rows_here, share)).astype(jnp.bfloat16)
        full = jnp.zeros((rows_here, groups * share), jnp.float32)
        for distance, block in enumerate(group_exchange(summed)):
            full = lax.dynamic_update_slice_in_dim(
                full, block.astype(jnp.float32), ((group - distance) % groups) * share, axis=1
            )
        return full

    grad_wgate = column_grad(gate_low_all)
    grad_wup = column_grad(up_low_all)

    grad_residual = grad_output.astype(jnp.float32) + norm_back(
        residual, root_two, norm2_gain, grad_normed_two
    )
    grad_res_low = grad_residual.astype(jnp.bfloat16)
    wout_part = dot("te,td->ed", mixed_low, grad_res_low)
    grad_wout = scatter_sum(wout_part.reshape(groups, PAIR, -1, width))
    grad_mixed = (
        dot("td,ed->te", grad_res_low, w_out)
        .astype(jnp.bfloat16)
        .reshape(tok_rows, kv_here, group_size, HEAD_SIZE)
    )
    mixed_view = mixed_low.reshape(tok_rows, kv_here, group_size, HEAD_SIZE)
    grad_query_rows, grad_key_rows, grad_value_rows = block_backward(
        query_low,
        keys_all,
        values_all,
        mixed_view,
        grad_mixed,
        logsum_block,
        query_ids,
        ids_all,
        query_pos,
        pos_all,
    )
    sent = jnp.concatenate(
        [
            grad_key_rows.reshape(2 * DOC_MAX, kv_here * HEAD_SIZE),
            grad_value_rows.reshape(2 * DOC_MAX, kv_here * HEAD_SIZE),
        ],
        axis=1,
    )
    back = passed_along(sent[:DOC_MAX].astype(jnp.bfloat16), "dp", -1).astype(jnp.float32)
    own = sent[DOC_MAX:] + back
    grad_qraw = grad_query_rows.reshape(tok_rows, heads_here, HEAD_SIZE)
    query_low_gradient = (
        rotate_halves(grad_qraw, cosine_table, -sine_values)
        .astype(jnp.bfloat16)
        .reshape(tok_rows, heads_here * HEAD_SIZE)
    )
    key_low_gradient = (
        rotate_halves(
            own[:, : kv_here * HEAD_SIZE].reshape(tok_rows, kv_here, HEAD_SIZE),
            cosine_table,
            -sine_values,
        )
        .astype(jnp.bfloat16)
        .reshape(tok_rows, kv_here * HEAD_SIZE)
    )
    value_low_gradient = own[:, kv_here * HEAD_SIZE :].astype(jnp.bfloat16)
    low_gradient = jnp.concatenate(
        [query_low_gradient, key_low_gradient, value_low_gradient], axis=1
    )
    normed_one_part = (
        dot("kl,ql->kq", query_low_gradient, query_weight)
        + dot("kl,ql->kq", key_low_gradient, key_weight)
        + dot("kl,ql->kq", value_low_gradient, value_weight)
    )
    grad_normed_one = tensor_sum(normed_one_part)
    gain_one_part = jnp.sum(normed_one_part * inputs_wide * root_one, axis=0)
    qkv_part = dot("wj,wq->jq", normed_low, low_gradient)
    columns = qkv_part.shape[1]
    gains = jnp.stack(
        [gain_one_part.reshape(n_dp, rows_here), gain_two_part.reshape(n_dp, rows_here)], axis=1
    )
    gains = jnp.pad(gains, ((0, 0), (0, 14), (0, columns - rows_here)))
    qkv_part = jnp.concatenate([qkv_part.reshape(n_dp, rows_here, columns), gains], axis=1)
    qkv_sum = scatter_sum(qkv_part.reshape(groups, PAIR, rows_here + 16, columns))
    grad_qkv = qkv_sum[:rows_here]
    gain_sums = qkv_sum[rows_here : rows_here + 16, :rows_here]
    bit = 1
    while bit < lax.axis_size("tensor"):
        gain_sums = gain_sums + tensor_swap(gain_sums, bit)
        bit *= 2
    grad_input_norm = norm_back(inputs_wide, root_one, norm1_gain, grad_normed_one)
    grad_inputs = (grad_residual + grad_input_norm).astype(jnp.bfloat16)
    q_columns = query_weight.shape[1]
    k_columns = key_weight.shape[1]
    return (
        output,
        grad_inputs,
        gain_sums[0],
        grad_qkv[:, :q_columns],
        grad_qkv[:, q_columns : q_columns + k_columns],
        grad_qkv[:, q_columns + k_columns :],
        grad_wout,
        gain_sums[1],
        grad_wgate,
        grad_wup,
        grad_wdown,
    )


def solution(mesh):
    return jax.shard_map(
        shards,
        mesh=mesh,
        in_specs=(
            P("dp", None),
            P(),
            P(None, "tensor"),
            P(None, "tensor"),
            P(None, "tensor"),
            P("tensor", None),
            P(),
            P(None, "tensor"),
            P(None, "tensor"),
            P("tensor", None),
            P("dp"),
            P("dp", None),
        ),
        out_specs=(
            P("dp", None),
            P("dp", None),
            P("dp"),
            P("dp", "tensor"),
            P("dp", "tensor"),
            P("dp", "tensor"),
            P(("tensor", "dp"), None),
            P("dp"),
            P("dp", "tensor"),
            P("dp", "tensor"),
            P(("tensor", "dp"), None),
        ),
        check_vma=False,
    )
```

```python
import functools
import math

import jax
import jax.numpy as jnp
from jax import lax
from jax.experimental import pallas as pl
from jax.experimental.pallas import tpu as pltpu
from jax.sharding import PartitionSpec as P

HEAD_SIZE = 64
DOC_MAX = 512
NORM_EPSILON = 1e-05

PAIR = 2
MESH = pl.DeviceIdType.MESH
EPS = NORM_EPSILON


def nn(a, b):
    return lax.dot_general(a, b, (((1,), (0,)), ((), ())), preferred_element_type=jnp.float32)
def nt(a, b):
    return lax.dot_general(a, b, (((1,), (1,)), ((), ())), preferred_element_type=jnp.float32)

def flip(index, bit):
    return index + bit - 2 * bit * ((index // bit) % 2)

def meet(*partners):
    barrier = pltpu.get_barrier_semaphore()
    for axis, index in partners:
        pl.semaphore_signal(barrier, inc=1, device_id={axis: index}, device_id_type=MESH)
    pl.semaphore_wait(barrier, len(partners))

def send(src, dst, sems, slot, axis, index):
    copy = pltpu.make_async_remote_copy(
        src_ref=src, dst_ref=dst, send_sem=sems.at[0, slot], recv_sem=sems.at[1, slot],
        device_id={axis: index}, device_id_type=MESH)
    copy.start()
    return copy

def swiglu(gate, up, grad):
    sig = 0.5 * (1.0 + jnp.tanh(0.5 * gate))
    silu = gate * sig
    hidden = (silu * up).astype(jnp.bfloat16)
    grad_gate = (grad * up * sig * (1.0 + gate * (1.0 - sig))).astype(jnp.bfloat16)
    grad_up = (grad * silu).astype(jnp.bfloat16)
    return hidden, grad_gate, grad_up

def mlp_kernel(n_dp, n_tensor, normed_hbm, grad_hbm, part_g, gate_hbm, up_hbm, down_hbm,
               out_ref, back_ref, all_hbm, rest_g,
               normed, grad, gate_w, up_w, down_w, hid, low_gate, low_up, load, far):
    rows, width = normed.shape
    cols = gate_w.shape[1]
    groups = n_dp // PAIR
    me_dp, me_t = lax.axis_index("dp"), lax.axis_index("tensor")
    right = lax.rem(me_dp + PAIR, n_dp)
    left = lax.rem(me_dp + n_dp - PAIR, n_dp)
    core, across = flip(me_t, 1), flip(me_t, 2)
    tile = 256
    tiles = cols // tile
    def cp(s, d, i):
        return pltpu.make_async_copy(s, d, load.at[i])
    def gate_tile(c, f):
        return cp(gate_hbm.at[:, c], gate_w.at[:, c], 2 + 3 * f)
    def up_tile(c, f):
        return cp(up_hbm.at[:, c], up_w.at[:, c], 3 + 3 * f)
    def down_tile(c, f):
        return cp(down_hbm.at[c, :], down_w.at[c, :], 4 + 3 * f)
    cp(normed_hbm, normed, 0).start()
    cp(grad_hbm, grad, 1).start()
    for f in range(tiles):
        c = pl.ds(f * tile, tile)
        gate_tile(c, f).start(); up_tile(c, f).start(); down_tile(c, f).start()

    meet(("dp", right), ("dp", left), ("tensor", core), ("tensor", across))
    piece = rows // n_tensor
    def part(t):
        return pl.ds(pl.multiple_of(t * piece, piece), piece)
    steps = groups - 1
    per = 4
    def ring(s):
        src = (normed_hbm if s == 1 else all_hbm.at[s - 2]).at[part(me_t), :]
        return send(src, all_hbm.at[s - 1].at[part(me_t), :], far, (s - 1) * per, "dp", right)
    def spread(s, level):
        held = [me_t, across][:level + 1]
        other = [across, core][level]
        block = all_hbm.at[s - 1]
        return [send(block.at[part(h), :], block.at[part(h), :], far, (s - 1) * per + 1 + level + i, "tensor", other)
                for i, h in enumerate(held)]
    def spread_g(b, level):
        base = (steps + b) * per
        if level == 0:
            return [send(part_g.at[b], rest_g.at[b].at[part(me_t), :], far, base, "tensor", across)]
        return [send(part_g.at[b], rest_g.at[b].at[part(me_t), :], far, base + 1, "tensor", core),
                send(rest_g.at[b].at[part(across), :], rest_g.at[b].at[part(across), :], far, base + 2, "tensor", core)]
    def wait(copies):
        for c in copies:
            c.wait()

    flying = {}
    if steps:
        flying["ring"] = [ring(1)]
    if steps > 1:
        flying["g"] = spread_g(0, 0)
    def advance(s):
        if s <= steps:
            wait(flying.pop("ring"))
            if s < steps:
                flying["ring"] = [ring(s + 1)]
                flying["spread", s, 0] = spread(s, 0)
    def finish(s, level):
        if ("spread", s, level) in flying:
            wait(flying.pop(("spread", s, level)))
            if level == 0:
                flying["spread", s, 1] = spread(s, 1)
    def advance_g(b):
        if "g" in flying:
            wait(flying.pop("g"))
            flying["gc", b] = spread_g(b, 1)
            if b + 1 < groups - 2:
                flying["g"] = spread_g(b + 1, 0)

    cp(normed_hbm, normed, 0).wait()
    cp(grad_hbm, grad, 1).wait()
    def first(f, _):
        c = pl.ds(pl.multiple_of(f * tile, tile), tile)
        gate_tile(c, f).wait()
        g = nn(normed[...], gate_w[:, c])
        up_tile(c, f).wait()
        u = nn(normed[...], up_w[:, c])
        down_tile(c, f).wait()
        h = nt(grad[...], down_w[c, :])
        a, b, d = swiglu(g, u, h)
        hid[:, c] = a
        low_gate[:, c] = b
        low_up[:, c] = d
        return 0
    early = min(5, tiles)
    lax.fori_loop(0, early, first, 0)
    advance(1)
    advance_g(0)
    lax.fori_loop(early, tiles, first, 0)
    wtile = 256
    wtiles = width // wtile
    def second(j, _):
        c = pl.ds(pl.multiple_of(j * wtile, wtile), wtile)
        back_ref[:, c] = (nt(low_gate[...], gate_w[c, :]) + nt(low_up[...], up_w[c, :])).astype(back_ref.dtype)
        return 0
    def third(j, _):
        c = pl.ds(pl.multiple_of(j * wtile, wtile), wtile)
        out_ref[:, c] = nn(hid[...], down_w[:, c]).astype(out_ref.dtype)
        return 0
    lax.fori_loop(0, wtiles, third, 0)
    advance(2)
    advance_g(1)
    finish(1, 0)
    lax.fori_loop(0, wtiles, second, 0)
    for s in range(3, steps + 1):
        finish(s - 1, 0)
        advance(s)
    for b in range(2, groups - 2):
        advance_g(b)
    for s in range(1, steps):
        finish(s, 0)
    for key in sorted(k for k in flying if k not in ("ring", "g")):
        wait(flying[key])

def mlp(normed, grad_output, part_g, w_gate, w_up, w_down, n_dp, n_tensor):
    rows, width = normed.shape
    cols = w_gate.shape[1]
    groups = n_dp // PAIR
    tiles = cols // 256
    anyspec = pl.BlockSpec(memory_space=pl.ANY)
    vm = pl.BlockSpec(memory_space=pltpu.VMEM)
    bf = jnp.bfloat16
    return pl.pallas_call(
        functools.partial(mlp_kernel, n_dp, n_tensor),
        out_shape=(jax.ShapeDtypeStruct((rows, width), bf), jax.ShapeDtypeStruct((rows, width), bf),
                   jax.ShapeDtypeStruct((groups - 1, rows, width), bf), jax.ShapeDtypeStruct((max(groups - 2, 1), rows, width), bf)),
        in_specs=[anyspec] * 6, out_specs=(vm, vm, anyspec, anyspec),
        scratch_shapes=[pltpu.VMEM((rows, width), bf), pltpu.VMEM((rows, width), bf),
                        pltpu.VMEM((width, cols), bf), pltpu.VMEM((width, cols), bf), pltpu.VMEM((cols, width), bf),
                        pltpu.VMEM((rows, cols), bf), pltpu.VMEM((rows, cols), bf), pltpu.VMEM((rows, cols), bf),
                        pltpu.SemaphoreType.DMA((2 + 3 * tiles,)),
                        pltpu.SemaphoreType.DMA((2, 8 * groups)),
                        ],
        compiler_params=pltpu.CompilerParams(collective_id=2, has_side_effects=True, vmem_limit_bytes=60 << 20),
        cost_estimate=pl.CostEstimate(flops=12 * rows * width * cols, bytes_accessed=2 * (3 * width * cols + 8 * rows * width), transcendentals=rows * cols),
        name="feed_forward",
    )(normed, grad_output, part_g, w_gate, w_up, w_down)

def wgrad_kernel(n_dp, n_tensor, own_n, all_n, own_g, one_g, part_g, rest_g, gate_t, up_t, down, back_hbm,
                 d_own, d_send, g_own, g_send, u_own, u_send, sum_ref,
                 n_all, g_all, wg, wu, wd, hid, lowg, lowu, mine, in1, mid, in2, load, far, ar):
    rows, width = own_n.shape
    share = gate_t.shape[0]
    groups = n_dp // PAIR
    me_dp, me_t = lax.axis_index("dp"), lax.axis_index("tensor")
    member = lax.rem(me_dp, PAIR)
    bits = []
    bit = n_tensor // 2
    while bit:
        bits.append(bit); bit //= 2
    piece = rows // n_tensor
    def part(t):
        return pl.ds(pl.multiple_of(t * piece, piece), piece)
    def at(r, t):
        return pl.ds(pl.multiple_of(r * rows + t * piece, piece), piece)
    count = [0]
    def cp(s, d):
        c = pltpu.make_async_copy(s, d, load.at[count[0]]); count[0] += 1
        c.start(); return c
    half = rows // 2
    low = lax.rem(me_t, 2)
    def half_rows(c):
        return pl.ds(pl.multiple_of(c * half, half), half)
    w1 = [cp(gate_t, wg), cp(own_n, n_all.at[pl.ds(0, rows), :])]
    w2 = [cp(up_t, wu)]
    w3 = [cp(down, wd), cp(own_g, g_all.at[pl.ds(0, rows), :])]
    w4 = [cp(back_hbm.at[half_rows(low), :], mine)]
    blocks = {}
    for r in range(1, groups):
        if r < groups - 1:
            wn = [cp(all_n.at[r - 1], n_all.at[pl.ds(r * rows, rows), :])]
        else:
            wn = [cp(all_n.at[r - 1].at[part(me_t), :], n_all.at[at(r, me_t), :])]
        if r == 1:
            wgr = [cp(one_g, g_all.at[pl.ds(r * rows, rows), :])]
        else:
            wgr = [cp(part_g.at[r - 2], g_all.at[at(r, me_t), :])]
            held = [me_t]
            for b in bits:
                held = held + [flip(h, b) for h in held]
            for h in held[1:]:
                wgr.append(cp(rest_g.at[r - 2].at[part(h), :], g_all.at[at(r, h), :]))
        blocks[r] = (wn, wgr)
    meet(*[("tensor", flip(me_t, b)) for b in bits])
    core = flip(me_t, 1)
    ar1 = send(back_hbm.at[half_rows(1 - low), :], in1, ar, 0, "tensor", core)
    last = groups - 1
    def wait(cs):
        for c in cs: c.wait()
    spread = {}
    if last >= 1:
        wait(blocks[last][0])
        spread[0] = [send(n_all.at[at(last, me_t), :], n_all.at[at(last, me_t), :], far, 0, "tensor", flip(me_t, bits[0]))]

    def pass_a(r):
        rs = pl.ds(r * rows, rows)
        g = nt(wg[...], n_all[rs, :])
        u = nt(wu[...], n_all[rs, :])
        h = nt(wd[...], g_all[rs, :])
        a, b, d = swiglu(g, u, h)
        hid[:, rs] = a; lowg[:, rs] = b; lowu[:, rs] = d
    wait(w1); wait(w2); wait(w3)
    pass_a(0)
    wait(w4); ar1.wait()
    mid[...] = (mine[...].astype(jnp.float32) + in1[...].astype(jnp.float32)).astype(jnp.bfloat16)
    if last > 1:
        wait(blocks[1][0]); wait(blocks[1][1])
        pass_a(1)
    if last >= 1 and len(bits) > 1:
        wait(spread[0])
        held = [me_t, flip(me_t, bits[0])]
        spread[1] = [send(n_all.at[at(last, h), :], n_all.at[at(last, h), :], far, 1 + i, "tensor", flip(me_t, bits[1])) for i, h in enumerate(held)]
    ar2 = send(mid, in2, ar, 1, "tensor", flip(me_t, 2))
    for r in range(2, last):
        wait(blocks[r][0]); wait(blocks[r][1])
        pass_a(r)
    if last >= 1:
        wait(blocks[last][1]); wait(spread[len(bits) - 1])
        pass_a(last)
    def down_tile(j, _):
        c = pl.ds(pl.multiple_of(j * 512, 512), 512)
        hrows = share // PAIR
        own = nn(hid[pl.ds(pl.multiple_of(member * hrows, hrows), hrows), :], g_all[:, c])
        oth = nn(hid[pl.ds(pl.multiple_of((1 - member) * hrows, hrows), hrows), :], g_all[:, c])
        d_own[:, c] = own; d_send[:, c] = oth.astype(jnp.bfloat16)
        return 0
    lax.fori_loop(0, width // 512, down_tile, 0)
    dcols = width // n_dp
    def col_tile(low_ref, own_ref, send_ref):
        def body(q, _):
            a = pl.ds(pl.multiple_of((q * PAIR + member) * dcols, dcols), dcols)
            b = pl.ds(pl.multiple_of((q * PAIR + 1 - member) * dcols, dcols), dcols)
            send_ref[q] = nn(low_ref[...], n_all[:, b]).astype(jnp.bfloat16)
            own_ref[q] = nn(low_ref[...], n_all[:, a])
            return 0
        return body
    lax.fori_loop(0, groups, col_tile(lowg, g_own, g_send), 0)
    ar2.wait()
    sum_ref[half_rows(low), :] = (mid[...].astype(jnp.float32) + in2[...].astype(jnp.float32)).astype(jnp.bfloat16)
    lax.fori_loop(0, groups - 1, col_tile(lowu, u_own, u_send), 0)
    ar3 = send(sum_ref.at[half_rows(low), :], sum_ref.at[half_rows(low), :], ar, 2, "tensor", core)
    lax.fori_loop(groups - 1, groups, col_tile(lowu, u_own, u_send), 0)
    ar3.wait()

def wgrad(own_n, all_n, own_g, one_g, part_g, rest_g, gate_t, up_t, down, back, n_dp, n_tensor):
    rows, width = own_n.shape
    share = gate_t.shape[0]
    groups = n_dp // PAIR
    anyspec = pl.BlockSpec(memory_space=pl.ANY)
    vm = pl.BlockSpec(memory_space=pltpu.VMEM)
    bf, f32 = jnp.bfloat16, jnp.float32
    sd = jax.ShapeDtypeStruct
    dcols = width // n_dp
    V = pltpu.VMEM
    tall = groups * rows
    return pl.pallas_call(
        functools.partial(wgrad_kernel, n_dp, n_tensor),
        out_shape=(sd((share // PAIR, width), f32), sd((share // PAIR, width), bf),
                   sd((groups, share, dcols), f32), sd((groups, share, dcols), bf),
                   sd((groups, share, dcols), f32), sd((groups, share, dcols), bf), sd((rows, width), bf)),
        in_specs=[anyspec] * 10, out_specs=(vm,) * 7,
        scratch_shapes=[V((tall, width), bf), V((tall, width), bf), V((share, width), bf), V((share, width), bf), V((share, width), bf),
                        V((share, tall), bf), V((share, tall), bf), V((share, tall), bf),
                        V((rows // 2, width), bf), V((rows // 2, width), bf), V((rows // 2, width), bf), V((rows // 2, width), bf),
                        pltpu.SemaphoreType.DMA((6 + (groups - 1) * (1 + n_tensor),)),
                        pltpu.SemaphoreType.DMA((2, n_tensor)), pltpu.SemaphoreType.DMA((2, 3))],
        compiler_params=pltpu.CompilerParams(collective_id=3, has_side_effects=True, vmem_limit_bytes=62 << 20),
        cost_estimate=pl.CostEstimate(flops=12 * tall * width * share, bytes_accessed=2 * (3 * width * share + 4 * tall * width), transcendentals=tall * share),
        name="weight_gradients",
    )(own_n, all_n, own_g, one_g, part_g, rest_g, gate_t, up_t, down, back)
TILE = 128
CHUNK = 256

def turn(values, cosine, sine):
    lane = lax.broadcasted_iota(jnp.int32, values.shape, 1)
    swapped = jnp.where(lane % HEAD_SIZE < HEAD_SIZE // 2,
                        pltpu.roll(values, 128 - HEAD_SIZE // 2, 1), pltpu.roll(values, HEAD_SIZE // 2, 1))
    return values * cosine + swapped * sine

def place(values, head, side):
    v = values if head == side else pltpu.roll(values, HEAD_SIZE, 1)
    lane = lax.broadcasted_iota(jnp.int32, values.shape, 1)
    return jnp.where(lane // HEAD_SIZE == side, v, jnp.zeros_like(v))

def bias_of(ids_col, ids_row, row0, col0, shape, window):
    q = lax.broadcasted_iota(jnp.int32, shape, 0) + row0
    k = lax.broadcasted_iota(jnp.int32, shape, 1) + col0
    return jnp.where((ids_col == ids_row) & (k <= q), 0.0, -1e30)

def attention_kernel(n_dp, n_tensor, x_hbm, gain1, wq_hbm, wk_hbm, wv_hbm, wo_hbm, gain2, cos_ref, sin_ref, ids_col, ids_row, g_hbm,
                     normed_ref, q_ref, kv_ref, idrow_ref, lse_ref, mixed_ref, res_ref, normed2_ref, one_g, part_g,
                     x, wq, wk, wv, wo, kvar, vvar, partial, out1, in1, mid, in2, total, load, far, halo, ar):
    rows, width = x.shape
    groups = n_dp // PAIR
    me_dp, me_t = lax.axis_index("dp"), lax.axis_index("tensor")
    right = lax.rem(me_dp + PAIR, n_dp)
    left = lax.rem(me_dp + n_dp - PAIR, n_dp)
    after = lax.rem(me_dp + 1, n_dp)
    before = lax.rem(me_dp + n_dp - 1, n_dp)
    core, across = flip(me_t, 1), flip(me_t, 2)
    piece = rows // n_tensor
    def part(t):
        return pl.ds(pl.multiple_of(t * piece, piece), piece)
    count = [0]
    def cp(s, d):
        c = pltpu.make_async_copy(s, d, load.at[count[0]]); count[0] += 1
        c.start(); return c
    w_x = cp(x_hbm, x); w_k = cp(wk_hbm, wk); w_v = cp(wv_hbm, wv); w_q = cp(wq_hbm, wq); w_o = cp(wo_hbm, wo)
    meet(("dp", after), ("dp", before), ("dp", right), ("dp", left), ("tensor", core), ("tensor", across))
    ring = send(g_hbm.at[part(me_t), :], one_g.at[part(me_t), :], far, 0, "dp", right)
    ids_go = send(ids_row, idrow_ref.at[0], halo, 0, "dp", after)
    idrow_ref[1] = ids_row[...]

    w_x.wait()
    def norm_one(i, _):
        r = pl.ds(pl.multiple_of(i * TILE, TILE), TILE)
        v = x[r, :].astype(jnp.float32)
        root = lax.rsqrt(jnp.mean(v * v, axis=1, keepdims=True) + EPS)
        normed_ref[r, :] = (v * root * gain1[...]).astype(jnp.bfloat16)
        return 0
    lax.fori_loop(0, rows // TILE, norm_one, 0)
    w_k.wait(); w_v.wait()
    own = pl.ds(rows, rows)
    kv_ref[1, :, 0:128] = turn(nn(normed_ref[...], wk[...]), cos_ref[...], sin_ref[...]).astype(jnp.bfloat16)
    kv_ref[1, :, 128:256] = nn(normed_ref[...], wv[...]).astype(jnp.bfloat16)
    w_q.wait()
    pairs = wq.shape[1] // 128
    def q_pair(p, _):
        c = pl.ds(pl.multiple_of(p * 256, 256), 256)
        raw = nn(normed_ref[...], wq[:, c])
        for s in range(2):
            d = pl.ds(pl.multiple_of(p * 256 + s * 128, 128), 128)
            q_ref[:, d] = (turn(raw[:, s * 128:(s + 1) * 128], cos_ref[...], sin_ref[...]).astype(jnp.bfloat16) * HEAD_SIZE ** -0.5).astype(jnp.bfloat16)
        return 0
    kv_go = send(kv_ref.at[1], kv_ref.at[0], halo, 1, "dp", after)
    lax.fori_loop(0, pairs // 2, q_pair, 0)
    ring.wait()
    if groups > 2:
        ring = send(one_g.at[part(me_t), :], part_g.at[0], far, 1, "dp", right)
    across_g = send(one_g.at[part(me_t), :], one_g.at[part(me_t), :], far, groups - 1, "tensor", across)
    def variants(side_rows, b):
        for g in range(2):
            for s in range(2):
                kvar[g, s, side_rows, :] = place(kv_ref[b, :, 0:128], g, s)
                vvar[g, s, side_rows, :] = place(kv_ref[b, :, 128:256], g, s)
    variants(own, 1)
    ids_go.wait(); kv_go.wait()
    variants(pl.ds(0, rows), 0)
    w_o.wait()

    window = rows + TILE
    def attend(i):
        r = pl.ds(i * TILE, TILE)
        k = pl.ds(i * TILE, window)
        ids_k = jnp.concatenate([idrow_ref[0], idrow_ref[1]], axis=1)[:, i * TILE:i * TILE + window]
        bias = bias_of(ids_col[r, :], ids_k, rows, 0, (TILE, window), window)
        bias = jnp.concatenate([bias, bias], axis=0)
        lane = lax.broadcasted_iota(jnp.int32, (TILE, 128), 1)
        logs = jnp.zeros((TILE, 128), jnp.float32)
        for g in range(2):
            q2 = jnp.concatenate([q_ref[r, (2 * g) * 128:(2 * g + 1) * 128], q_ref[r, (2 * g + 1) * 128:(2 * g + 2) * 128]], axis=0)
            mixed = None
            for s in range(2):
                score = nt(q2, kvar[g, s, k, :]) + bias
                peak = jnp.max(score, axis=1, keepdims=True)
                e = jnp.exp(score - peak)
                l = jnp.sum(e, axis=1, keepdims=True)
                prob = (e * (1.0 / l)).astype(jnp.bfloat16)
                m = nn(prob, vvar[g, s, k, :])
                mixed = m if mixed is None else mixed + m
                lse = peak + jnp.log(l)
                for b in range(2):
                    head = 4 * g + 2 * b + s
                    logs = jnp.where(lane == head, lse[b * TILE:(b + 1) * TILE, :], logs)
            for b in range(2):
                mixed_ref[r, (2 * g + b) * 128:(2 * g + b + 1) * 128] = mixed[b * TILE:(b + 1) * TILE, :].astype(jnp.bfloat16)
        lse_ref[r, :] = logs

    hrow = CHUNK // 2
    low = lax.rem(me_t, 2)
    def own_rows(c):
        return pl.ds(pl.multiple_of(c * CHUNK + low * hrow, hrow), hrow)
    def oth_rows(c):
        return pl.ds(pl.multiple_of(c * CHUNK + (1 - low) * hrow, hrow), hrow)
    def project(c):
        def body(j, _):
            d = pl.ds(pl.multiple_of(j * 512, 512), 512)
            out1[c, :, d] = nn(mixed_ref[oth_rows(c), :], wo[:, d]).astype(jnp.bfloat16)
            partial[c, :, d] = nn(mixed_ref[own_rows(c), :], wo[:, d])
            return 0
        lax.fori_loop(0, width // 512, body, 0)
    def step1(c):
        return send(out1.at[c], in1.at[c], ar, 3 * c, "tensor", core)
    def step2(c):
        mid[c] = (partial[c] + in1[c].astype(jnp.float32)).astype(jnp.bfloat16)
        return send(mid.at[c], in2.at[c], ar, 3 * c + 1, "tensor", across)
    def step3(c):
        total[own_rows(c), :] = (mid[c].astype(jnp.float32) + in2[c].astype(jnp.float32)).astype(jnp.bfloat16)
        return send(total.at[own_rows(c), :], total.at[own_rows(c), :], ar, 3 * c + 2, "tensor", core)
    def finish(r):
        v = x[r, :].astype(jnp.float32) + total[r, :].astype(jnp.float32)
        res_ref[r, :] = v
        root = lax.rsqrt(jnp.mean(v * v, axis=1, keepdims=True) + EPS)
        normed2_ref[r, :] = (v * root * gain2[...]).astype(jnp.bfloat16)

    chunks = rows // CHUNK
    per = CHUNK // TILE
    flights = {}
    def go_round(i):
        nonlocal ring
        if i == 2:
            ring.wait()
            if groups > 3: ring = send(part_g.at[0], part_g.at[1], far, 2, "dp", right)
    for i in range(rows // TILE):
        attend(i)
        c = i // per
        if i % per == per - 1:
            project(c)
            flights[1, c] = step1(c)
        elif c > 0:
            flights[1, c - 1].wait(); flights[2, c - 1] = step2(c - 1)
        if i == 1:
            across_g.wait()
            core_g = [send(one_g.at[part(t), :], one_g.at[part(t), :], far, groups + j, "tensor", core) for j, t in enumerate((me_t, across))]
    c = chunks - 1
    flights[1, c].wait(); flights[2, c] = step2(c)
    if groups > 2:
        go_round(2)
    for s in range(4, groups):
        ring.wait(); ring = send(part_g.at[s - 3], part_g.at[s - 2], far, groups + 2 + s, "dp", right)
    for c in range(chunks):
        flights[2, c].wait(); flights[3, c] = step3(c)
        finish(own_rows(c))
        flights[3, c].wait()
        finish(oth_rows(c))
    for q in core_g: q.wait()
    if groups > 2: ring.wait()

def attend_forward(x, gain1, wq, wk, wv, wo, gain2, cosine, sine, ids, grad_output, n_dp, n_tensor):
    rows, width = x.shape
    groups = n_dp // PAIR
    anyspec = pl.BlockSpec(memory_space=pl.ANY)
    vm = pl.BlockSpec(memory_space=pltpu.VMEM)
    bf, f32 = jnp.bfloat16, jnp.float32
    sd = jax.ShapeDtypeStruct
    V = pltpu.VMEM
    piece = rows // n_tensor
    chunks = rows // CHUNK
    qc = wq.shape[1]
    D = pltpu.SemaphoreType.DMA
    return pl.pallas_call(
        functools.partial(attention_kernel, n_dp, n_tensor),
        out_shape=(sd((rows, width), bf), sd((rows, qc), bf), sd((2, rows, 256), bf), sd((2, 1, rows), jnp.int32), sd((rows, 128), f32),
                   sd((rows, qc), bf), sd((rows, width), f32), sd((rows, width), bf),
                   sd((rows, width), bf), sd((max(groups - 2, 1), piece, width), bf)),
        in_specs=[anyspec, vm, anyspec, anyspec, anyspec, anyspec, vm, vm, vm, vm, vm, anyspec],
        out_specs=(vm,) * 8 + (anyspec,) * 2,
        scratch_shapes=[V((rows, width), bf), V((width, qc), bf), V((width, 128), bf), V((width, 128), bf), V((qc, width), bf),
                        V((2, 2, 2 * rows, 128), bf), V((2, 2, 2 * rows, 128), bf),
                        V((chunks, CHUNK // 2, width), f32), V((chunks, CHUNK // 2, width), bf), V((chunks, CHUNK // 2, width), bf),
                        V((chunks, CHUNK // 2, width), bf), V((chunks, CHUNK // 2, width), bf), V((rows, width), bf),
                        D((5,)), D((2, 2 * groups + 8)), D((2, 2)), D((2, 3 * chunks))],
        compiler_params=pltpu.CompilerParams(collective_id=1, has_side_effects=True, vmem_limit_bytes=56 << 20),
        cost_estimate=pl.CostEstimate(flops=2 * rows * width * (2 * qc + 256) + 16 * rows * rows * 5 * 128, bytes_accessed=2 * (width * (2 * qc + 256) + 6 * rows * width), transcendentals=8 * rows * rows),
        name="attention_forward",
    )(x, gain1.reshape(1, width), wq, wk, wv, wo, gain2.reshape(1, width), cosine, sine, ids.reshape(rows, 1), ids.reshape(1, rows), grad_output)


def rope_table(half_count):
    adjusted = []
    for index in range(half_count):
        base_value = 500000.0 ** (-index / half_count)
        wave_length = 2.0 * math.pi / base_value
        smooth = (8192.0 / wave_length - 1.0) / 3.0
        if wave_length > 8192.0:
            adjusted.append(base_value / 32.0)
        elif wave_length >= 2048.0:
            adjusted.append((1.0 - smooth) * base_value / 32.0 + smooth * base_value)
        else:
            adjusted.append(base_value)
    return jnp.asarray(adjusted, dtype=jnp.float32)


def rope_angles(start_row, count_rows, half_count):
    positions = (start_row + jnp.arange(count_rows, dtype=jnp.int32)).astype(jnp.float32)
    phase_angle = positions[:, None] * rope_table(half_count)[None, :]
    return (jnp.cos(phase_angle)[:, None, :], jnp.sin(phase_angle)[:, None, :])


def rotate_halves(values, cosine_table, sine_values):
    half_size = values.shape[-1] // 2
    first_half = values[..., :half_size]
    second_half = values[..., half_size:]
    return jnp.concatenate(
        [
            first_half * cosine_table - second_half * sine_values,
            second_half * cosine_table + first_half * sine_values,
        ],
        axis=-1,
    )


def norm_rows(values, gain_row):
    inverse_root = lax.rsqrt(jnp.mean(values * values, axis=-1, keepdims=True) + NORM_EPSILON)
    return (inverse_root, values * inverse_root * gain_row)


def norm_back(values, inverse_root, gain_row, upstream):
    scaled = gain_row * upstream
    return inverse_root * scaled - values * inverse_root**3 * jnp.mean(
        scaled * values, axis=-1, keepdims=True
    )


def passed_along(block, axis, distance):
    devices = range(lax.axis_size(axis))
    route = [(i - distance, i) for i in devices if i - distance in devices]
    return lax.ppermute(block, axis, route)


def tensor_swap(block, bit):
    return lax.ppermute(block, "tensor", [(i, i ^ bit) for i in range(lax.axis_size("tensor"))])


def pair_swap(block):
    return lax.ppermute(block, "dp", [(i, i ^ 1) for i in range(lax.axis_size("dp"))])


def group_shift(block, distance):
    count = lax.axis_size("dp")
    groups = count // PAIR
    return lax.ppermute(
        block,
        "dp",
        [(i, ((i // PAIR + distance) % groups) * PAIR + i % PAIR) for i in range(count)],
    )


def tensor_sum(part):
    half = part.shape[1] // 2
    low = lax.axis_index("tensor") % 2
    first, second = part[:, :half], part[:, half:]
    mine = jnp.where(low == 0, first, second)
    other = jnp.where(low == 0, second, first).astype(jnp.bfloat16)
    mine = mine + tensor_swap(other, 1).astype(jnp.float32)
    bit = 2
    while bit < lax.axis_size("tensor"):
        rounded = mine.astype(jnp.bfloat16)
        mine = rounded.astype(jnp.float32) + tensor_swap(rounded, bit).astype(jnp.float32)
        bit *= 2
    mine = mine.astype(jnp.bfloat16)
    other = tensor_swap(mine, 1)
    return jnp.concatenate(
        [jnp.where(low == 0, mine, other), jnp.where(low == 0, other, mine)], axis=1
    ).astype(jnp.float32)


def gather_groups(block):
    half = block.shape[1] // 2
    low = lax.axis_index("tensor") % 2
    piece = lax.dynamic_slice_in_dim(block, low * half, half, axis=1)
    rows = [block]
    for _ in range(lax.axis_size("dp") // PAIR - 1):
        piece = group_shift(piece, 1)
        other = tensor_swap(piece, 1)
        rows.append(
            jnp.concatenate(
                [jnp.where(low == 0, piece, other), jnp.where(low == 0, other, piece)], axis=1
            )
        )
    return jnp.concatenate(rows, axis=0)


def pair_sum(part):
    member = lax.axis_index("dp") % PAIR
    mine = lax.dynamic_index_in_dim(part, member, 1, keepdims=False)
    other = lax.dynamic_index_in_dim(part, 1 - member, 1, keepdims=False)
    return mine + pair_swap(other.astype(jnp.bfloat16)).astype(jnp.float32)


def group_exchange(blocks):
    groups = blocks.shape[0]
    group = lax.axis_index("dp") // PAIR
    received = []
    for distance in range(groups):
        block = lax.dynamic_index_in_dim(blocks, (group + distance) % groups, 0, keepdims=False)
        received.append(block if distance == 0 else group_shift(block, distance))
    return received


def scatter_sum(part):
    summed = pair_sum(part)
    groups = summed.shape[0]
    group = lax.axis_index("dp") // PAIR
    total = lax.dynamic_index_in_dim(summed, group, 0, keepdims=False)
    rounded = summed.astype(jnp.bfloat16)
    for block in group_exchange(rounded)[1:]:
        total = total + block.astype(jnp.float32)
    return total


def block_scores(query_rows, key_rows, query_ids, key_ids, query_pos, key_pos):
    scores = jnp.einsum(
        "qgrd,kgd->grqk", query_rows, key_rows, preferred_element_type=jnp.float32
    ) * HEAD_SIZE ** (-0.5)
    allowed = (query_ids[:, None] == key_ids[None, :]) & (key_pos[None, :] <= query_pos[:, None])
    return jnp.where(allowed, scores, -1e30)


def block_forward(query_rows, key_rows, value_rows, query_ids, key_ids, query_pos, key_pos):
    scores = block_scores(query_rows, key_rows, query_ids, key_ids, query_pos, key_pos)
    row_peak = jnp.max(scores, axis=-1, keepdims=True)
    logsum = row_peak + jnp.log(jnp.sum(jnp.exp(scores - row_peak), axis=-1, keepdims=True))
    prob_low = jnp.exp(scores - logsum).astype(jnp.bfloat16)
    mixed_rows = jnp.einsum(
        "grqk,kgd->qgrd", prob_low, value_rows, preferred_element_type=jnp.float32
    )
    return (mixed_rows.astype(jnp.bfloat16), logsum)


def block_backward(
    query_rows,
    key_rows,
    value_rows,
    out_rows,
    grad_rows,
    logsum,
    query_ids,
    key_ids,
    query_pos,
    key_pos,
):
    scores = block_scores(query_rows, key_rows, query_ids, key_ids, query_pos, key_pos)
    prob_rows = jnp.exp(scores - logsum)
    grad_vals = jnp.einsum(
        "grqk,qgrd->kgd",
        prob_rows.astype(jnp.bfloat16),
        grad_rows,
        preferred_element_type=jnp.float32,
    )
    delta_rows = jnp.sum(out_rows.astype(jnp.float32) * grad_rows.astype(jnp.float32), axis=-1)
    grad_probs = jnp.einsum(
        "qgrd,kgd->grqk", grad_rows, value_rows, preferred_element_type=jnp.float32
    )
    grad_scores = (
        prob_rows * (grad_probs - jnp.transpose(delta_rows, (1, 2, 0))[..., None])
    ).astype(jnp.bfloat16)
    grad_query_rows = jnp.einsum(
        "grqk,kgd->qgrd", grad_scores, key_rows, preferred_element_type=jnp.float32
    ) * HEAD_SIZE ** (-0.5)
    grad_key_rows = jnp.einsum(
        "grqk,qgrd->kgd", grad_scores, query_rows, preferred_element_type=jnp.float32
    ) * HEAD_SIZE ** (-0.5)
    return (grad_query_rows, grad_key_rows, grad_vals)


def dot(form, left, right):
    return jnp.einsum(form, left, right, preferred_element_type=jnp.float32)


def gated(gate_value, up_value):
    return (jax.nn.silu(gate_value) * up_value).astype(jnp.bfloat16)


def gated_back(grad_hidden, gate_value, up_value):
    sigmoid_gate = jax.nn.sigmoid(gate_value)
    grad_gate_low = (
        grad_hidden * up_value * sigmoid_gate * (1.0 + gate_value * (1.0 - sigmoid_gate))
    ).astype(jnp.bfloat16)
    return grad_gate_low, (grad_hidden * jax.nn.silu(gate_value)).astype(jnp.bfloat16)


def shards_plain(
    inputs,
    norm1_gain,
    query_weight,
    key_weight,
    value_weight,
    w_out,
    norm2_gain,
    w_gate,
    w_up,
    w_down,
    doc_ids,
    grad_output,
):
    tok_rows, width = inputs.shape
    heads_here = query_weight.shape[1] // HEAD_SIZE
    kv_here = key_weight.shape[1] // HEAD_SIZE
    group_size = heads_here // kv_here
    n_dp = lax.axis_size("dp")
    groups = n_dp // PAIR
    group = lax.axis_index("dp") // PAIR
    offset = lax.axis_index("dp") * tok_rows
    grad_all = gather_groups(grad_output)

    cosine_table, sine_values = rope_angles(offset, tok_rows, HEAD_SIZE // 2)
    inputs_wide = inputs.astype(jnp.float32)
    root_one, normed = norm_rows(inputs_wide, norm1_gain)
    normed_low = normed.astype(jnp.bfloat16)
    query_raw = dot("td,dh->th", normed_low, query_weight).reshape(tok_rows, heads_here, HEAD_SIZE)
    key_raw = dot("td,dh->th", normed_low, key_weight).reshape(tok_rows, kv_here, HEAD_SIZE)
    value_low = dot("td,dh->th", normed_low, value_weight).astype(jnp.bfloat16)
    query_low = (
        rotate_halves(query_raw, cosine_table, sine_values)
        .astype(jnp.bfloat16)
        .reshape(tok_rows, kv_here, group_size, HEAD_SIZE)
    )
    key_low = (
        rotate_halves(key_raw, cosine_table, sine_values)
        .astype(jnp.bfloat16)
        .reshape(tok_rows, kv_here * HEAD_SIZE)
    )
    query_ids = doc_ids + 1
    tail = jnp.concatenate([key_low, value_low], axis=1)
    prev_tail = passed_along(tail, "dp", 1)
    prev_ids = passed_along(query_ids, "dp", 1)
    both = jnp.concatenate([prev_tail, tail], axis=0)
    keys_all = both[:, : kv_here * HEAD_SIZE].reshape(2 * DOC_MAX, kv_here, HEAD_SIZE)
    values_all = both[:, kv_here * HEAD_SIZE :].reshape(2 * DOC_MAX, kv_here, HEAD_SIZE)
    ids_all = jnp.concatenate([prev_ids, query_ids])
    pos_all = offset - DOC_MAX + jnp.arange(tok_rows + DOC_MAX, dtype=jnp.int32)
    query_pos = pos_all[DOC_MAX:]
    mixed_block, logsum_block = block_forward(
        query_low, keys_all, values_all, query_ids, ids_all, query_pos, pos_all
    )
    mixed_low = mixed_block.reshape(tok_rows, heads_here * HEAD_SIZE)
    residual = inputs_wide + tensor_sum(dot("te,ed->td", mixed_low, w_out))

    root_two, normed_two = norm_rows(residual, norm2_gain)
    normed_two_low = normed_two.astype(jnp.bfloat16)
    normed_all = gather_groups(normed_two_low)
    gate_value = dot("td,df->tf", normed_two_low, w_gate)
    up_value = dot("td,df->tf", normed_two_low, w_up)
    grad_hidden = dot("td,fd->tf", grad_output, w_down)
    hidden_low = gated(gate_value, up_value)
    grad_gate_low, grad_up_low = gated_back(grad_hidden, gate_value, up_value)
    normed_two_part = dot("tf,df->td", grad_gate_low, w_gate) + dot("tf,df->td", grad_up_low, w_up)
    grad_normed_two = tensor_sum(normed_two_part)
    gain_two_part = jnp.sum(normed_two_part * residual * root_two, axis=0)
    output = (residual + tensor_sum(dot("tf,fd->td", hidden_low, w_down))).astype(jnp.bfloat16)

    share = w_gate.shape[1] // groups
    gate_share = lax.dynamic_slice_in_dim(w_gate, group * share, share, axis=1)
    up_share = lax.dynamic_slice_in_dim(w_up, group * share, share, axis=1)
    down_share = lax.dynamic_slice_in_dim(w_down, group * share, share, axis=0)
    gate_all = dot("td,df->tf", normed_all, gate_share)
    up_all = dot("td,df->tf", normed_all, up_share)
    grad_hidden_all = dot("td,fd->tf", grad_all, down_share)
    hidden_all = gated(gate_all, up_all)
    gate_low_all, up_low_all = gated_back(grad_hidden_all, gate_all, up_all)
    down_part = dot("tf,td->fd", hidden_all, grad_all)
    grad_wdown = pair_sum(down_part.reshape(1, PAIR, share // PAIR, width))[0]
    rows_here = width // n_dp

    def column_grad(low_all):
        part = dot("td,tf->df", normed_all, low_all)
        summed = pair_sum(part.reshape(groups, PAIR, rows_here, share)).astype(jnp.bfloat16)
        full = jnp.zeros((rows_here, groups * share), jnp.float32)
        for distance, block in enumerate(group_exchange(summed)):
            full = lax.dynamic_update_slice_in_dim(
                full, block.astype(jnp.float32), ((group - distance) % groups) * share, axis=1
            )
        return full

    grad_wgate = column_grad(gate_low_all)
    grad_wup = column_grad(up_low_all)

    grad_residual = grad_output.astype(jnp.float32) + norm_back(
        residual, root_two, norm2_gain, grad_normed_two
    )
    grad_res_low = grad_residual.astype(jnp.bfloat16)
    wout_part = dot("te,td->ed", mixed_low, grad_res_low)
    grad_wout = scatter_sum(wout_part.reshape(groups, PAIR, -1, width))
    grad_mixed = (
        dot("td,ed->te", grad_res_low, w_out)
        .astype(jnp.bfloat16)
        .reshape(tok_rows, kv_here, group_size, HEAD_SIZE)
    )
    mixed_view = mixed_low.reshape(tok_rows, kv_here, group_size, HEAD_SIZE)
    grad_query_rows, grad_key_rows, grad_value_rows = block_backward(
        query_low,
        keys_all,
        values_all,
        mixed_view,
        grad_mixed,
        logsum_block,
        query_ids,
        ids_all,
        query_pos,
        pos_all,
    )
    sent = jnp.concatenate(
        [
            grad_key_rows.reshape(2 * DOC_MAX, kv_here * HEAD_SIZE),
            grad_value_rows.reshape(2 * DOC_MAX, kv_here * HEAD_SIZE),
        ],
        axis=1,
    )
    back = passed_along(sent[:DOC_MAX].astype(jnp.bfloat16), "dp", -1).astype(jnp.float32)
    own = sent[DOC_MAX:] + back
    grad_qraw = grad_query_rows.reshape(tok_rows, heads_here, HEAD_SIZE)
    query_low_gradient = (
        rotate_halves(grad_qraw, cosine_table, -sine_values)
        .astype(jnp.bfloat16)
        .reshape(tok_rows, heads_here * HEAD_SIZE)
    )
    key_low_gradient = (
        rotate_halves(
            own[:, : kv_here * HEAD_SIZE].reshape(tok_rows, kv_here, HEAD_SIZE),
            cosine_table,
            -sine_values,
        )
        .astype(jnp.bfloat16)
        .reshape(tok_rows, kv_here * HEAD_SIZE)
    )
    value_low_gradient = own[:, kv_here * HEAD_SIZE :].astype(jnp.bfloat16)
    low_gradient = jnp.concatenate(
        [query_low_gradient, key_low_gradient, value_low_gradient], axis=1
    )
    normed_one_part = (
        dot("kl,ql->kq", query_low_gradient, query_weight)
        + dot("kl,ql->kq", key_low_gradient, key_weight)
        + dot("kl,ql->kq", value_low_gradient, value_weight)
    )
    grad_normed_one = tensor_sum(normed_one_part)
    gain_one_part = jnp.sum(normed_one_part * inputs_wide * root_one, axis=0)
    qkv_part = dot("wj,wq->jq", normed_low, low_gradient)
    columns = qkv_part.shape[1]
    gains = jnp.stack(
        [gain_one_part.reshape(n_dp, rows_here), gain_two_part.reshape(n_dp, rows_here)], axis=1
    )
    gains = jnp.pad(gains, ((0, 0), (0, 14), (0, columns - rows_here)))
    qkv_part = jnp.concatenate([qkv_part.reshape(n_dp, rows_here, columns), gains], axis=1)
    qkv_sum = scatter_sum(qkv_part.reshape(groups, PAIR, rows_here + 16, columns))
    grad_qkv = qkv_sum[:rows_here]
    gain_sums = qkv_sum[rows_here : rows_here + 16, :rows_here]
    bit = 1
    while bit < lax.axis_size("tensor"):
        gain_sums = gain_sums + tensor_swap(gain_sums, bit)
        bit *= 2
    grad_input_norm = norm_back(inputs_wide, root_one, norm1_gain, grad_normed_one)
    grad_inputs = (grad_residual + grad_input_norm).astype(jnp.bfloat16)
    q_columns = query_weight.shape[1]
    k_columns = key_weight.shape[1]
    return (
        output,
        grad_inputs,
        gain_sums[0],
        grad_qkv[:, :q_columns],
        grad_qkv[:, q_columns : q_columns + k_columns],
        grad_qkv[:, q_columns + k_columns :],
        grad_wout,
        gain_sums[1],
        grad_wgate,
        grad_wup,
        grad_wdown,
    )


def shards(
    inputs,
    norm1_gain,
    query_weight,
    key_weight,
    value_weight,
    w_out,
    norm2_gain,
    w_gate,
    w_up,
    w_down,
    doc_ids,
    grad_output,
):
    tok_rows, width = inputs.shape
    heads_here = query_weight.shape[1] // HEAD_SIZE
    kv_here = key_weight.shape[1] // HEAD_SIZE
    group_size = heads_here // kv_here
    n_dp = lax.axis_size("dp")
    groups = n_dp // PAIR
    group = lax.axis_index("dp") // PAIR
    offset = lax.axis_index("dp") * tok_rows
    share = w_gate.shape[1] // groups
    gate_t = lax.dynamic_slice_in_dim(w_gate, group * share, share, axis=1).T
    up_t = lax.dynamic_slice_in_dim(w_up, group * share, share, axis=1).T
    down_share = lax.dynamic_slice_in_dim(w_down, group * share, share, axis=0)
    cosine_table, sine_values = rope_angles(offset, tok_rows, HEAD_SIZE // 2)
    cosine = jnp.tile(cosine_table[:, 0, :], (1, 4))
    sine = jnp.tile(jnp.concatenate([-sine_values[:, 0, :], sine_values[:, 0, :]], axis=1), (1, 2))
    n_tensor = lax.axis_size("tensor")
    normed_low, query_scaled, kv, id_rows, _, mixed_low, residual, normed_two_low, one_g, part_g = attend_forward(
        inputs, norm1_gain, query_weight, key_weight, value_weight, w_out, norm2_gain, cosine, sine, doc_ids, grad_output, n_dp, n_tensor)
    mlp_part, back_part, normed_rest, rest_g = mlp(normed_two_low, grad_output, part_g, w_gate, w_up, w_down, n_dp, n_tensor)
    d_own, d_send, g_own, g_send, u_own, u_send, grad_normed_two = wgrad(
        normed_two_low, normed_rest, grad_output, one_g, part_g, rest_g, gate_t, up_t, down_share, back_part, n_dp, n_tensor)
    grad_normed_two = grad_normed_two.astype(jnp.float32)
    rows_here = width // n_dp
    inputs_wide = inputs.astype(jnp.float32)
    root_one = lax.rsqrt(jnp.mean(inputs_wide * inputs_wide, axis=-1, keepdims=True) + NORM_EPSILON)
    root_two = lax.rsqrt(jnp.mean(residual * residual, axis=-1, keepdims=True) + NORM_EPSILON)
    gain_two_part = jnp.sum(back_part.astype(jnp.float32) * residual * root_two, axis=0)
    output = (residual + tensor_sum(mlp_part.astype(jnp.float32))).astype(jnp.bfloat16)
    grad_wdown = d_own + pair_swap(d_send).astype(jnp.float32)

    def column_grad(own, sent):
        summed = (own + pair_swap(sent).astype(jnp.float32)).astype(jnp.bfloat16)
        blocks = group_exchange(summed)[::-1]
        ring = jnp.stack(blocks + blocks)
        full = lax.dynamic_slice_in_dim(ring, groups - 1 - group, groups, axis=0)
        return full.reshape(groups * share, rows_here).T.astype(jnp.float32)

    grad_wgate = column_grad(g_own, g_send)
    grad_wup = column_grad(u_own, u_send)
    query_low = (query_scaled.astype(jnp.float32) * HEAD_SIZE ** 0.5).astype(jnp.bfloat16).reshape(tok_rows, kv_here, group_size, HEAD_SIZE)
    keys_all = kv[:, :, : kv_here * HEAD_SIZE].reshape(2 * DOC_MAX, kv_here, HEAD_SIZE)
    values_all = kv[:, :, kv_here * HEAD_SIZE :].reshape(2 * DOC_MAX, kv_here, HEAD_SIZE)
    query_ids = doc_ids
    ids_all = id_rows.reshape(2 * DOC_MAX)
    pos_all = offset - DOC_MAX + jnp.arange(tok_rows + DOC_MAX, dtype=jnp.int32)
    query_pos = pos_all[DOC_MAX:]
    scores = block_scores(query_low, keys_all, query_ids, ids_all, query_pos, pos_all)
    row_peak = jnp.max(scores, axis=-1, keepdims=True)
    logsum_block = row_peak + jnp.log(jnp.sum(jnp.exp(scores - row_peak), axis=-1, keepdims=True))

    grad_residual = grad_output.astype(jnp.float32) + norm_back(
        residual, root_two, norm2_gain, grad_normed_two
    )
    grad_res_low = grad_residual.astype(jnp.bfloat16)
    wout_part = dot("te,td->ed", mixed_low, grad_res_low)
    grad_wout = scatter_sum(wout_part.reshape(groups, PAIR, -1, width))
    grad_mixed = (
        dot("td,ed->te", grad_res_low, w_out)
        .astype(jnp.bfloat16)
        .reshape(tok_rows, kv_here, group_size, HEAD_SIZE)
    )
    mixed_view = mixed_low.reshape(tok_rows, kv_here, group_size, HEAD_SIZE)
    grad_query_rows, grad_key_rows, grad_value_rows = block_backward(
        query_low,
        keys_all,
        values_all,
        mixed_view,
        grad_mixed,
        logsum_block,
        query_ids,
        ids_all,
        query_pos,
        pos_all,
    )
    sent = jnp.concatenate(
        [
            grad_key_rows.reshape(2 * DOC_MAX, kv_here * HEAD_SIZE),
            grad_value_rows.reshape(2 * DOC_MAX, kv_here * HEAD_SIZE),
        ],
        axis=1,
    )
    back = passed_along(sent[:DOC_MAX].astype(jnp.bfloat16), "dp", -1).astype(jnp.float32)
    own = sent[DOC_MAX:] + back
    grad_qraw = grad_query_rows.reshape(tok_rows, heads_here, HEAD_SIZE)
    query_low_gradient = (
        rotate_halves(grad_qraw, cosine_table, -sine_values)
        .astype(jnp.bfloat16)
        .reshape(tok_rows, heads_here * HEAD_SIZE)
    )
    key_low_gradient = (
        rotate_halves(
            own[:, : kv_here * HEAD_SIZE].reshape(tok_rows, kv_here, HEAD_SIZE),
            cosine_table,
            -sine_values,
        )
        .astype(jnp.bfloat16)
        .reshape(tok_rows, kv_here * HEAD_SIZE)
    )
    value_low_gradient = own[:, kv_here * HEAD_SIZE :].astype(jnp.bfloat16)
    low_gradient = jnp.concatenate(
        [query_low_gradient, key_low_gradient, value_low_gradient], axis=1
    )
    normed_one_part = (
        dot("kl,ql->kq", query_low_gradient, query_weight)
        + dot("kl,ql->kq", key_low_gradient, key_weight)
        + dot("kl,ql->kq", value_low_gradient, value_weight)
    )
    grad_normed_one = tensor_sum(normed_one_part)
    gain_one_part = jnp.sum(normed_one_part * inputs_wide * root_one, axis=0)
    qkv_part = dot("wj,wq->jq", normed_low, low_gradient)
    columns = qkv_part.shape[1]
    gains = jnp.stack(
        [gain_one_part.reshape(n_dp, rows_here), gain_two_part.reshape(n_dp, rows_here)], axis=1
    )
    gains = jnp.pad(gains, ((0, 0), (0, 14), (0, columns - rows_here)))
    qkv_part = jnp.concatenate([qkv_part.reshape(n_dp, rows_here, columns), gains], axis=1)
    qkv_sum = scatter_sum(qkv_part.reshape(groups, PAIR, rows_here + 16, columns))
    grad_qkv = qkv_sum[:rows_here]
    gain_sums = qkv_sum[rows_here : rows_here + 16, :rows_here]
    bit = 1
    while bit < lax.axis_size("tensor"):
        gain_sums = gain_sums + tensor_swap(gain_sums, bit)
        bit *= 2
    grad_input_norm = norm_back(inputs_wide, root_one, norm1_gain, grad_normed_one)
    grad_inputs = (grad_residual + grad_input_norm).astype(jnp.bfloat16)
    q_columns = query_weight.shape[1]
    k_columns = key_weight.shape[1]
    return (
        output,
        grad_inputs,
        gain_sums[0],
        grad_qkv[:, :q_columns],
        grad_qkv[:, q_columns : q_columns + k_columns],
        grad_qkv[:, q_columns + k_columns :],
        grad_wout,
        gain_sums[1],
        grad_wgate,
        grad_wup,
        grad_wdown,
    )


def kernels_fit(mesh, *args):
    n_dp, n_tensor = mesh.shape["dp"], mesh.shape["tensor"]
    width = args[0].shape[1]
    return (
        n_dp % PAIR == 0
        and n_dp // PAIR <= 4
        and n_tensor == 4
        and width // n_dp % 128 == 0
        and args[3].shape[1] // n_tensor == 2 * HEAD_SIZE
        and args[2].shape[1] == 4 * args[3].shape[1]
    )


def solution(mesh):
    def step(*args):
        return mapped(mesh, shards if kernels_fit(mesh, *args) else shards_plain)(*args)

    return step


def mapped(mesh, function):
    return jax.shard_map(
        function,
        mesh=mesh,
        in_specs=(
            P("dp", None),
            P(),
            P(None, "tensor"),
            P(None, "tensor"),
            P(None, "tensor"),
            P("tensor", None),
            P(),
            P(None, "tensor"),
            P(None, "tensor"),
            P("tensor", None),
            P("dp"),
            P("dp", None),
        ),
        out_specs=(
            P("dp", None),
            P("dp", None),
            P("dp"),
            P("dp", "tensor"),
            P("dp", "tensor"),
            P("dp", "tensor"),
            P(("tensor", "dp"), None),
            P("dp"),
            P("dp", "tensor"),
            P("dp", "tensor"),
            P(("tensor", "dp"), None),
        ),
        check_vma=False,
    )
```

```python
import functools
import math

import jax
import jax.numpy as jnp
from jax import lax
from jax.experimental import pallas as pl
from jax.experimental.pallas import tpu as pltpu
from jax.sharding import PartitionSpec as P

HEAD_SIZE = 64
DOC_MAX = 512
NORM_EPSILON = 1e-05

PAIR = 2
MESH = pl.DeviceIdType.MESH
EPS = NORM_EPSILON


def nn(a, b):
    return lax.dot_general(a, b, (((1,), (0,)), ((), ())), preferred_element_type=jnp.float32)
def nt(a, b):
    return lax.dot_general(a, b, (((1,), (1,)), ((), ())), preferred_element_type=jnp.float32)

def flip(index, bit):
    return index + bit - 2 * bit * ((index // bit) % 2)

def meet(*partners):
    barrier = pltpu.get_barrier_semaphore()
    for axis, index in partners:
        pl.semaphore_signal(barrier, inc=1, device_id={axis: index}, device_id_type=MESH)
    pl.semaphore_wait(barrier, len(partners))

def send(src, dst, sems, slot, axis, index):
    copy = pltpu.make_async_remote_copy(
        src_ref=src, dst_ref=dst, send_sem=sems.at[0, slot], recv_sem=sems.at[1, slot],
        device_id={axis: index}, device_id_type=MESH)
    copy.start()
    return copy

def swiglu(gate, up, grad):
    sig = 0.5 * (1.0 + jnp.tanh(0.5 * gate))
    silu = gate * sig
    hidden = (silu * up).astype(jnp.bfloat16)
    grad_gate = (grad * up * sig * (1.0 + gate * (1.0 - sig))).astype(jnp.bfloat16)
    grad_up = (grad * silu).astype(jnp.bfloat16)
    return hidden, grad_gate, grad_up

def mlp_kernel(n_dp, n_tensor, normed_hbm, grad_hbm, part_g, gate_hbm, up_hbm, down_hbm,
               out_ref, back_ref, all_hbm, rest_g, gain_ref,
               normed, grad, gate_w, up_w, down_w, hid, low_gate, low_up, load, far):
    rows, width = normed.shape
    cols = gate_w.shape[1]
    groups = n_dp // PAIR
    me_dp, me_t = lax.axis_index("dp"), lax.axis_index("tensor")
    right = lax.rem(me_dp + PAIR, n_dp)
    left = lax.rem(me_dp + n_dp - PAIR, n_dp)
    core, across = flip(me_t, 1), flip(me_t, 2)
    tile = 256
    tiles = cols // tile
    def cp(s, d, i):
        return pltpu.make_async_copy(s, d, load.at[i])
    def gate_tile(c, f):
        return cp(gate_hbm.at[:, c], gate_w.at[:, c], 2 + 3 * f)
    def up_tile(c, f):
        return cp(up_hbm.at[:, c], up_w.at[:, c], 3 + 3 * f)
    def down_tile(c, f):
        return cp(down_hbm.at[c, :], down_w.at[c, :], 4 + 3 * f)
    cp(normed_hbm, normed, 0).start()
    cp(grad_hbm, grad, 1).start()
    for f in range(tiles):
        c = pl.ds(f * tile, tile)
        gate_tile(c, f).start(); up_tile(c, f).start(); down_tile(c, f).start()

    meet(("dp", right), ("dp", left), ("tensor", core), ("tensor", across))
    piece = rows // n_tensor
    def part(t):
        return pl.ds(pl.multiple_of(t * piece, piece), piece)
    steps = groups - 1
    per = 4
    def ring(s):
        src = (normed_hbm if s == 1 else all_hbm.at[s - 2]).at[part(me_t), :]
        return send(src, all_hbm.at[s - 1].at[part(me_t), :], far, (s - 1) * per, "dp", right)
    def spread(s, level):
        held = [me_t, across][:level + 1]
        other = [across, core][level]
        block = all_hbm.at[s - 1]
        return [send(block.at[part(h), :], block.at[part(h), :], far, (s - 1) * per + 1 + level + i, "tensor", other)
                for i, h in enumerate(held)]
    def spread_g(b, level):
        base = (steps + b) * per
        if level == 0:
            return [send(part_g.at[b], rest_g.at[b].at[part(me_t), :], far, base, "tensor", across)]
        return [send(part_g.at[b], rest_g.at[b].at[part(me_t), :], far, base + 1, "tensor", core),
                send(rest_g.at[b].at[part(across), :], rest_g.at[b].at[part(across), :], far, base + 2, "tensor", core)]
    def wait(copies):
        for c in copies:
            c.wait()

    flying = {}
    if steps:
        flying["ring"] = [ring(1)]
    if steps > 1:
        flying["g"] = spread_g(0, 0)
    def advance(s):
        if s <= steps:
            wait(flying.pop("ring"))
            if s < steps:
                flying["ring"] = [ring(s + 1)]
                flying["spread", s, 0] = spread(s, 0)
    def finish(s, level):
        if ("spread", s, level) in flying:
            wait(flying.pop(("spread", s, level)))
            if level == 0:
                flying["spread", s, 1] = spread(s, 1)
    def advance_g(b):
        if "g" in flying:
            wait(flying.pop("g"))
            flying["gc", b] = spread_g(b, 1)
            if b + 1 < groups - 2:
                flying["g"] = spread_g(b + 1, 0)

    cp(normed_hbm, normed, 0).wait()
    cp(grad_hbm, grad, 1).wait()
    def first(f, _):
        c = pl.ds(pl.multiple_of(f * tile, tile), tile)
        gate_tile(c, f).wait()
        g = nn(normed[...], gate_w[:, c])
        up_tile(c, f).wait()
        u = nn(normed[...], up_w[:, c])
        down_tile(c, f).wait()
        h = nt(grad[...], down_w[c, :])
        a, b, d = swiglu(g, u, h)
        hid[:, c] = a
        low_gate[:, c] = b
        low_up[:, c] = d
        return 0
    early = min(5, tiles)
    lax.fori_loop(0, early, first, 0)
    advance(1)
    advance_g(0)
    lax.fori_loop(early, tiles, first, 0)
    wtile = 256
    wtiles = width // wtile
    def second(j, _):
        c = pl.ds(pl.multiple_of(j * wtile, wtile), wtile)
        b = nt(low_gate[...], gate_w[c, :]) + nt(low_up[...], up_w[c, :])
        back_ref[:, c] = b.astype(back_ref.dtype)
        gain_ref[0:1, c] = jnp.sum(b * normed[:, c].astype(jnp.float32), axis=0, keepdims=True)
        return 0
    def third(j, _):
        c = pl.ds(pl.multiple_of(j * wtile, wtile), wtile)
        out_ref[:, c] = nn(hid[...], down_w[:, c]).astype(out_ref.dtype)
        return 0
    lax.fori_loop(0, wtiles, third, 0)
    advance(2)
    advance_g(1)
    finish(1, 0)
    lax.fori_loop(0, wtiles, second, 0)
    for s in range(3, steps + 1):
        finish(s - 1, 0)
        advance(s)
    for b in range(2, groups - 2):
        advance_g(b)
    for s in range(1, steps):
        finish(s, 0)
    for key in sorted(k for k in flying if k not in ("ring", "g")):
        wait(flying[key])

def mlp(normed, grad_output, part_g, w_gate, w_up, w_down, n_dp, n_tensor):
    rows, width = normed.shape
    cols = w_gate.shape[1]
    groups = n_dp // PAIR
    tiles = cols // 256
    anyspec = pl.BlockSpec(memory_space=pl.ANY)
    vm = pl.BlockSpec(memory_space=pltpu.VMEM)
    bf = jnp.bfloat16
    return pl.pallas_call(
        functools.partial(mlp_kernel, n_dp, n_tensor),
        out_shape=(jax.ShapeDtypeStruct((rows, width), bf), jax.ShapeDtypeStruct((rows, width), bf),
                   jax.ShapeDtypeStruct((groups - 1, rows, width), bf), jax.ShapeDtypeStruct((max(groups - 2, 1), rows, width), bf), jax.ShapeDtypeStruct((1, width), jnp.float32)),
        in_specs=[anyspec] * 6, out_specs=(vm, vm, anyspec, anyspec, vm),
        scratch_shapes=[pltpu.VMEM((rows, width), bf), pltpu.VMEM((rows, width), bf),
                        pltpu.VMEM((width, cols), bf), pltpu.VMEM((width, cols), bf), pltpu.VMEM((cols, width), bf),
                        pltpu.VMEM((rows, cols), bf), pltpu.VMEM((rows, cols), bf), pltpu.VMEM((rows, cols), bf),
                        pltpu.SemaphoreType.DMA((2 + 3 * tiles,)),
                        pltpu.SemaphoreType.DMA((2, 8 * groups)),
                        ],
        compiler_params=pltpu.CompilerParams(collective_id=2, has_side_effects=True, vmem_limit_bytes=60 << 20),
        cost_estimate=pl.CostEstimate(flops=12 * rows * width * cols, bytes_accessed=2 * (3 * width * cols + 8 * rows * width), transcendentals=rows * cols),
        name="feed_forward",
    )(normed, grad_output, part_g, w_gate, w_up, w_down)

def wgrad_kernel(n_dp, n_tensor, own_n, all_n, own_g, one_g, part_g, rest_g, gate_t, up_t, down, back_hbm,
                 d_own, g_own, g_send, u_own, u_send, sum_ref,
                 d_send, d_in, n_all, g_all, wg, wu, wd, hid, lowg, lowu, mine, in1, mid, in2, load, far, ar, sy):
    rows, width = own_n.shape
    share = gate_t.shape[0]
    groups = n_dp // PAIR
    me_dp, me_t = lax.axis_index("dp"), lax.axis_index("tensor")
    member = lax.rem(me_dp, PAIR)
    bits = []
    bit = n_tensor // 2
    while bit:
        bits.append(bit); bit //= 2
    piece = rows // n_tensor
    def part(t):
        return pl.ds(pl.multiple_of(t * piece, piece), piece)
    def at(r, t):
        return pl.ds(pl.multiple_of(r * rows + t * piece, piece), piece)
    count = [0]
    def cp(s, d):
        c = pltpu.make_async_copy(s, d, load.at[count[0]]); count[0] += 1
        c.start(); return c
    half = rows // 2
    low = lax.rem(me_t, 2)
    def half_rows(c):
        return pl.ds(pl.multiple_of(c * half, half), half)
    w1 = [cp(gate_t, wg), cp(own_n, n_all.at[pl.ds(0, rows), :])]
    w2 = [cp(up_t, wu)]
    w3 = [cp(down, wd), cp(own_g, g_all.at[pl.ds(0, rows), :])]
    w4 = [cp(back_hbm.at[half_rows(low), :], mine)]
    blocks = {}
    for r in range(1, groups):
        if r < groups - 1:
            wn = [cp(all_n.at[r - 1], n_all.at[pl.ds(r * rows, rows), :])]
        else:
            wn = [cp(all_n.at[r - 1].at[part(me_t), :], n_all.at[at(r, me_t), :])]
        if r == 1:
            wgr = [cp(one_g, g_all.at[pl.ds(r * rows, rows), :])]
        else:
            wgr = [cp(part_g.at[r - 2], g_all.at[at(r, me_t), :])]
            held = [me_t]
            for b in bits:
                held = held + [flip(h, b) for h in held]
            for h in held[1:]:
                wgr.append(cp(rest_g.at[r - 2].at[part(h), :], g_all.at[at(r, h), :]))
        blocks[r] = (wn, wgr)
    pair = flip(me_dp, 1)
    meet(("dp", pair), *[("tensor", flip(me_t, b)) for b in bits])
    core = flip(me_t, 1)
    ar1 = send(back_hbm.at[half_rows(1 - low), :], in1, ar, 0, "tensor", core)
    last = groups - 1
    def wait(cs):
        for c in cs: c.wait()
    spread = {}
    if last >= 1:
        wait(blocks[last][0])
        spread[0] = [send(n_all.at[at(last, me_t), :], n_all.at[at(last, me_t), :], far, 0, "tensor", flip(me_t, bits[0]))]

    def pass_a(r):
        rs = pl.ds(r * rows, rows)
        g = nt(wg[...], n_all[rs, :])
        u = nt(wu[...], n_all[rs, :])
        h = nt(wd[...], g_all[rs, :])
        a, b, d = swiglu(g, u, h)
        hid[:, rs] = a; lowg[:, rs] = b; lowu[:, rs] = d
    wait(w1); wait(w2); wait(w3)
    pass_a(0)
    wait(w4); ar1.wait()
    mid[...] = (mine[...].astype(jnp.float32) + in1[...].astype(jnp.float32)).astype(jnp.bfloat16)
    if last > 1:
        wait(blocks[1][0]); wait(blocks[1][1])
        pass_a(1)
    if last >= 1 and len(bits) > 1:
        wait(spread[0])
        held = [me_t, flip(me_t, bits[0])]
        spread[1] = [send(n_all.at[at(last, h), :], n_all.at[at(last, h), :], far, 1 + i, "tensor", flip(me_t, bits[1])) for i, h in enumerate(held)]
    ar2 = send(mid, in2, ar, 1, "tensor", flip(me_t, 2))
    for r in range(2, last):
        wait(blocks[r][0]); wait(blocks[r][1])
        pass_a(r)
    if last >= 1:
        wait(blocks[last][1]); wait(spread[len(bits) - 1])
        pass_a(last)
    hrows = share // PAIR
    to_pair = []
    for j in range(width // 512):
        c = pl.ds(j * 512, 512)
        d_send[j] = nn(hid[pl.ds(pl.multiple_of((1 - member) * hrows, hrows), hrows), :], g_all[:, c]).astype(jnp.bfloat16)
        d_own[:, c] = nn(hid[pl.ds(pl.multiple_of(member * hrows, hrows), hrows), :], g_all[:, c])
        to_pair.append(send(d_send.at[j], d_in.at[j], sy, j, "dp", pair))
    dcols = width // n_dp
    def col_tile(low_ref, own_ref, send_ref):
        def body(q, _):
            a = pl.ds(pl.multiple_of((q * PAIR + member) * dcols, dcols), dcols)
            b = pl.ds(pl.multiple_of((q * PAIR + 1 - member) * dcols, dcols), dcols)
            send_ref[q] = nn(low_ref[...], n_all[:, b]).astype(jnp.bfloat16)
            own_ref[q] = nn(low_ref[...], n_all[:, a])
            return 0
        return body
    lax.fori_loop(0, groups, col_tile(lowg, g_own, g_send), 0)
    ar2.wait()
    sum_ref[half_rows(low), :] = (mid[...].astype(jnp.float32) + in2[...].astype(jnp.float32)).astype(jnp.bfloat16)
    lax.fori_loop(0, groups - 1, col_tile(lowu, u_own, u_send), 0)
    ar3 = send(sum_ref.at[half_rows(low), :], sum_ref.at[half_rows(low), :], ar, 2, "tensor", core)
    lax.fori_loop(groups - 1, groups, col_tile(lowu, u_own, u_send), 0)
    for j, q in enumerate(to_pair):
        q.wait()
        d_own[:, j * 512:(j + 1) * 512] += d_in[j].astype(jnp.float32)
    ar3.wait()

def wgrad(own_n, all_n, own_g, one_g, part_g, rest_g, gate_t, up_t, down, back, n_dp, n_tensor):
    rows, width = own_n.shape
    share = gate_t.shape[0]
    groups = n_dp // PAIR
    anyspec = pl.BlockSpec(memory_space=pl.ANY)
    vm = pl.BlockSpec(memory_space=pltpu.VMEM)
    bf, f32 = jnp.bfloat16, jnp.float32
    sd = jax.ShapeDtypeStruct
    dcols = width // n_dp
    V = pltpu.VMEM
    tall = groups * rows
    return pl.pallas_call(
        functools.partial(wgrad_kernel, n_dp, n_tensor),
        out_shape=(sd((share // PAIR, width), f32),
                   sd((groups, share, dcols), f32), sd((groups, share, dcols), bf),
                   sd((groups, share, dcols), f32), sd((groups, share, dcols), bf), sd((rows, width), bf)),
        in_specs=[anyspec] * 10, out_specs=(vm,) * 6,
        scratch_shapes=[V((width // 512, share // PAIR, 512), bf), V((width // 512, share // PAIR, 512), bf), V((tall, width), bf), V((tall, width), bf), V((share, width), bf), V((share, width), bf), V((share, width), bf),
                        V((share, tall), bf), V((share, tall), bf), V((share, tall), bf),
                        V((rows // 2, width), bf), V((rows // 2, width), bf), V((rows // 2, width), bf), V((rows // 2, width), bf),
                        pltpu.SemaphoreType.DMA((6 + (groups - 1) * (1 + n_tensor),)),
                        pltpu.SemaphoreType.DMA((2, n_tensor)), pltpu.SemaphoreType.DMA((2, 3)), pltpu.SemaphoreType.DMA((2, width // 512))],
        compiler_params=pltpu.CompilerParams(collective_id=3, has_side_effects=True, vmem_limit_bytes=62 << 20),
        cost_estimate=pl.CostEstimate(flops=12 * tall * width * share, bytes_accessed=2 * (3 * width * share + 4 * tall * width), transcendentals=tall * share),
        name="weight_gradients",
    )(own_n, all_n, own_g, one_g, part_g, rest_g, gate_t, up_t, down, back)
TILE = 128
CHUNK = 256

def turn(values, cosine, sine):
    lane = lax.broadcasted_iota(jnp.int32, values.shape, 1)
    swapped = jnp.where(lane % HEAD_SIZE < HEAD_SIZE // 2,
                        pltpu.roll(values, 128 - HEAD_SIZE // 2, 1), pltpu.roll(values, HEAD_SIZE // 2, 1))
    return values * cosine + swapped * sine

def place(values, head, side):
    v = values if head == side else pltpu.roll(values, HEAD_SIZE, 1)
    lane = lax.broadcasted_iota(jnp.int32, values.shape, 1)
    return jnp.where(lane // HEAD_SIZE == side, v, jnp.zeros_like(v))

def bias_of(ids_col, ids_row, row0, col0, shape, window):
    q = lax.broadcasted_iota(jnp.int32, shape, 0) + row0
    k = lax.broadcasted_iota(jnp.int32, shape, 1) + col0
    return jnp.where((ids_col == ids_row) & (k <= q), 0.0, -1e30)

def attention_kernel(n_dp, n_tensor, x_hbm, gain1, wq_hbm, wk_hbm, wv_hbm, wo_hbm, gain2, cos_ref, sin_ref, ids_col, ids_row, g_hbm,
                     normed_ref, q_ref, kv_ref, idrow_ref, lse_ref, mixed_ref, res_ref, normed2_ref, one_g, part_g,
                     x, wq, wk, wv, wo, kvar, vvar, partial, out1, in1, mid, in2, total, load, far, halo, ar):
    rows, width = x.shape
    groups = n_dp // PAIR
    me_dp, me_t = lax.axis_index("dp"), lax.axis_index("tensor")
    right = lax.rem(me_dp + PAIR, n_dp)
    left = lax.rem(me_dp + n_dp - PAIR, n_dp)
    after = lax.rem(me_dp + 1, n_dp)
    before = lax.rem(me_dp + n_dp - 1, n_dp)
    core, across = flip(me_t, 1), flip(me_t, 2)
    piece = rows // n_tensor
    def part(t):
        return pl.ds(pl.multiple_of(t * piece, piece), piece)
    count = [0]
    def cp(s, d):
        c = pltpu.make_async_copy(s, d, load.at[count[0]]); count[0] += 1
        c.start(); return c
    w_x = cp(x_hbm, x); w_k = cp(wk_hbm, wk); w_v = cp(wv_hbm, wv); w_q = cp(wq_hbm, wq); w_o = cp(wo_hbm, wo)
    meet(("dp", after), ("dp", before), ("dp", right), ("dp", left), ("tensor", core), ("tensor", across))
    ring = send(g_hbm.at[part(me_t), :], one_g.at[part(me_t), :], far, 0, "dp", right)
    ids_go = send(ids_row, idrow_ref.at[0], halo, 0, "dp", after)
    idrow_ref[1] = ids_row[...]

    w_x.wait()
    def norm_one(i, _):
        r = pl.ds(pl.multiple_of(i * TILE, TILE), TILE)
        v = x[r, :].astype(jnp.float32)
        root = lax.rsqrt(jnp.mean(v * v, axis=1, keepdims=True) + EPS)
        normed_ref[r, :] = (v * root * gain1[...]).astype(jnp.bfloat16)
        return 0
    lax.fori_loop(0, rows // TILE, norm_one, 0)
    w_k.wait(); w_v.wait()
    own = pl.ds(rows, rows)
    kv_ref[1, :, 0:128] = turn(nn(normed_ref[...], wk[...]), cos_ref[...], sin_ref[...]).astype(jnp.bfloat16)
    kv_ref[1, :, 128:256] = nn(normed_ref[...], wv[...]).astype(jnp.bfloat16)
    w_q.wait()
    pairs = wq.shape[1] // 128
    def q_pair(p, _):
        c = pl.ds(pl.multiple_of(p * 256, 256), 256)
        raw = nn(normed_ref[...], wq[:, c])
        for s in range(2):
            d = pl.ds(pl.multiple_of(p * 256 + s * 128, 128), 128)
            q_ref[:, d] = (turn(raw[:, s * 128:(s + 1) * 128], cos_ref[...], sin_ref[...]).astype(jnp.bfloat16) * HEAD_SIZE ** -0.5).astype(jnp.bfloat16)
        return 0
    kv_go = send(kv_ref.at[1], kv_ref.at[0], halo, 1, "dp", after)
    lax.fori_loop(0, pairs // 2, q_pair, 0)
    ring.wait()
    if groups > 2:
        ring = send(one_g.at[part(me_t), :], part_g.at[0], far, 1, "dp", right)
    across_g = send(one_g.at[part(me_t), :], one_g.at[part(me_t), :], far, groups - 1, "tensor", across)
    def variants(side_rows, b):
        for g in range(2):
            for s in range(2):
                kvar[g, s, side_rows, :] = place(kv_ref[b, :, 0:128], g, s)
                vvar[g, s, side_rows, :] = place(kv_ref[b, :, 128:256], g, s)
    variants(own, 1)
    ids_go.wait(); kv_go.wait()
    variants(pl.ds(0, rows), 0)
    w_o.wait()

    window = rows + TILE
    def attend(i):
        r = pl.ds(i * TILE, TILE)
        k = pl.ds(i * TILE, window)
        ids_k = jnp.concatenate([idrow_ref[0], idrow_ref[1]], axis=1)[:, i * TILE:i * TILE + window]
        bias = bias_of(ids_col[r, :], ids_k, rows, 0, (TILE, window), window)
        bias = jnp.concatenate([bias, bias], axis=0)
        lane = lax.broadcasted_iota(jnp.int32, (TILE, 128), 1)
        logs = jnp.zeros((TILE, 128), jnp.float32)
        for g in range(2):
            q2 = jnp.concatenate([q_ref[r, (2 * g) * 128:(2 * g + 1) * 128], q_ref[r, (2 * g + 1) * 128:(2 * g + 2) * 128]], axis=0)
            mixed = None
            for s in range(2):
                score = nt(q2, kvar[g, s, k, :]) + bias
                peak = jnp.max(score, axis=1, keepdims=True)
                e = jnp.exp(score - peak)
                l = jnp.sum(e, axis=1, keepdims=True)
                prob = (e * (1.0 / l)).astype(jnp.bfloat16)
                m = nn(prob, vvar[g, s, k, :])
                mixed = m if mixed is None else mixed + m
                lse = peak + jnp.log(l)
                for b in range(2):
                    head = 4 * g + 2 * b + s
                    logs = jnp.where(lane == head, lse[b * TILE:(b + 1) * TILE, :], logs)
            for b in range(2):
                mixed_ref[r, (2 * g + b) * 128:(2 * g + b + 1) * 128] = mixed[b * TILE:(b + 1) * TILE, :].astype(jnp.bfloat16)
        lse_ref[r, :] = logs

    hrow = CHUNK // 2
    low = lax.rem(me_t, 2)
    def own_rows(c):
        return pl.ds(pl.multiple_of(c * CHUNK + low * hrow, hrow), hrow)
    def oth_rows(c):
        return pl.ds(pl.multiple_of(c * CHUNK + (1 - low) * hrow, hrow), hrow)
    def project(c):
        def body(j, _):
            d = pl.ds(pl.multiple_of(j * 512, 512), 512)
            out1[c, :, d] = nn(mixed_ref[oth_rows(c), :], wo[:, d]).astype(jnp.bfloat16)
            partial[c, :, d] = nn(mixed_ref[own_rows(c), :], wo[:, d])
            return 0
        lax.fori_loop(0, width // 512, body, 0)
    def step1(c):
        return send(out1.at[c], in1.at[c], ar, 3 * c, "tensor", core)
    def step2(c):
        mid[c] = (partial[c] + in1[c].astype(jnp.float32)).astype(jnp.bfloat16)
        return send(mid.at[c], in2.at[c], ar, 3 * c + 1, "tensor", across)
    def step3(c):
        total[own_rows(c), :] = (mid[c].astype(jnp.float32) + in2[c].astype(jnp.float32)).astype(jnp.bfloat16)
        return send(total.at[own_rows(c), :], total.at[own_rows(c), :], ar, 3 * c + 2, "tensor", core)
    def finish(r):
        v = x[r, :].astype(jnp.float32) + total[r, :].astype(jnp.float32)
        res_ref[r, :] = v
        root = lax.rsqrt(jnp.mean(v * v, axis=1, keepdims=True) + EPS)
        normed2_ref[r, :] = (v * root * gain2[...]).astype(jnp.bfloat16)

    chunks = rows // CHUNK
    per = CHUNK // TILE
    flights = {}
    def go_round(i):
        nonlocal ring
        if i == 2:
            ring.wait()
            if groups > 3: ring = send(part_g.at[0], part_g.at[1], far, 2, "dp", right)
    for i in range(rows // TILE):
        attend(i)
        c = i // per
        if i % per == per - 1:
            project(c)
            flights[1, c] = step1(c)
        elif c > 0:
            flights[1, c - 1].wait(); flights[2, c - 1] = step2(c - 1)
        if i == 1:
            across_g.wait()
            core_g = [send(one_g.at[part(t), :], one_g.at[part(t), :], far, groups + j, "tensor", core) for j, t in enumerate((me_t, across))]
    c = chunks - 1
    flights[1, c].wait(); flights[2, c] = step2(c)
    if groups > 2:
        go_round(2)
    for s in range(4, groups):
        ring.wait(); ring = send(part_g.at[s - 3], part_g.at[s - 2], far, groups + 2 + s, "dp", right)
    for c in range(chunks):
        flights[2, c].wait(); flights[3, c] = step3(c)
        finish(own_rows(c))
        flights[3, c].wait()
        finish(oth_rows(c))
    for q in core_g: q.wait()
    if groups > 2: ring.wait()

def attend_forward(x, gain1, wq, wk, wv, wo, gain2, cosine, sine, ids, grad_output, n_dp, n_tensor):
    rows, width = x.shape
    groups = n_dp // PAIR
    anyspec = pl.BlockSpec(memory_space=pl.ANY)
    vm = pl.BlockSpec(memory_space=pltpu.VMEM)
    bf, f32 = jnp.bfloat16, jnp.float32
    sd = jax.ShapeDtypeStruct
    V = pltpu.VMEM
    piece = rows // n_tensor
    chunks = rows // CHUNK
    qc = wq.shape[1]
    D = pltpu.SemaphoreType.DMA
    return pl.pallas_call(
        functools.partial(attention_kernel, n_dp, n_tensor),
        out_shape=(sd((rows, width), bf), sd((rows, qc), bf), sd((2, rows, 256), bf), sd((2, 1, rows), jnp.int32), sd((rows, 128), f32),
                   sd((rows, qc), bf), sd((rows, width), f32), sd((rows, width), bf),
                   sd((rows, width), bf), sd((max(groups - 2, 1), piece, width), bf)),
        in_specs=[anyspec, vm, anyspec, anyspec, anyspec, anyspec, vm, vm, vm, vm, vm, anyspec],
        out_specs=(vm,) * 8 + (anyspec,) * 2,
        scratch_shapes=[V((rows, width), bf), V((width, qc), bf), V((width, 128), bf), V((width, 128), bf), V((qc, width), bf),
                        V((2, 2, 2 * rows, 128), bf), V((2, 2, 2 * rows, 128), bf),
                        V((chunks, CHUNK // 2, width), f32), V((chunks, CHUNK // 2, width), bf), V((chunks, CHUNK // 2, width), bf),
                        V((chunks, CHUNK // 2, width), bf), V((chunks, CHUNK // 2, width), bf), V((rows, width), bf),
                        D((5,)), D((2, 2 * groups + 8)), D((2, 2)), D((2, 3 * chunks))],
        compiler_params=pltpu.CompilerParams(collective_id=1, has_side_effects=True, vmem_limit_bytes=56 << 20),
        cost_estimate=pl.CostEstimate(flops=2 * rows * width * (2 * qc + 256) + 16 * rows * rows * 5 * 128, bytes_accessed=2 * (width * (2 * qc + 256) + 6 * rows * width), transcendentals=8 * rows * rows),
        name="attention_forward",
    )(x, gain1.reshape(1, width), wq, wk, wv, wo, gain2.reshape(1, width), cosine, sine, ids.reshape(rows, 1), ids.reshape(1, rows), grad_output)

def backward_kernel(n_dp, n_tensor, gn_hbm, res_hbm, x_hbm, go_hbm, mlp_hbm, normed_hbm, wo_hbm, wq_hbm, wk_hbm, wv_hbm,
                    g_own, g_send, u_own, u_send, mixed_hbm, q_hbm, kv_hbm, gain1, gain2, gain2_part, ids_col, ids_row, cos_ref, sin_ref,
                    out_hbm, gin_hbm, gate_hbm, up_hbm, gains_ref, qkv_ref, wout_ref,
                    gn, res, go, normed, wo, wq, wk, wv, mixed, q_ref, kv_ref, own32, resid, low_res, gm, kvar, vvar, kvart, dk, dv,
                    low, lowt, tile32, wsend, wown, win, wz, gyin, gsum, gz, uyin, usum, uz, qsend, qown, qin, qz,
                    amine, amid, min1, min2, ain1, ain2, hprev, hin, gacc, gs, gown, gyi, gzi, gt, gti,
                    load, sy, sz, sx, sh, sg):
    rows, width = go.shape
    groups = n_dp // PAIR
    me_dp, me_t = lax.axis_index("dp"), lax.axis_index("tensor")
    group, member = me_dp // PAIR, lax.rem(me_dp, PAIR)
    pair = flip(me_dp, 1)
    after = lax.rem(me_dp + 1, n_dp)
    before = lax.rem(me_dp + n_dp - 1, n_dp)
    core, across = flip(me_t, 1), flip(me_t, 2)
    low_t = lax.rem(me_t, 2)
    def at_group(s):
        return lax.rem(group + s, groups)
    def from_group(s):
        return lax.rem(group + groups - s, groups)
    f32, bf = jnp.float32, jnp.bfloat16
    qc = wq.shape[1]
    dcols = width // n_dp
    half = rows // 2
    def rows_of(start, size):
        return pl.ds(pl.multiple_of(start, size), size)
    def half_rows(c):
        return rows_of(c * half, half)
    def cp(s, d, i):
        c = pltpu.make_async_copy(s, d, load.at[i])
        c.start()
        return c
    w_gn = cp(gn_hbm, gn, 0); w_res = cp(res_hbm, res, 1); w_go = cp(go_hbm, go, 2)
    w_wo = cp(wo_hbm, wo, 3); w_mlp = cp(mlp_hbm.at[half_rows(low_t), :], amine, 4)
    w_kv = cp(kv_hbm, kv_ref, 5); w_mx = cp(mixed_hbm, mixed, 6); w_qr = cp(q_hbm, q_ref, 7)
    w_own = cp(g_own, own32, 8); w_nm = cp(normed_hbm, normed, 9)
    w_q = cp(wq_hbm, wq, 10); w_k = cp(wk_hbm, wk, 11); w_v = cp(wv_hbm, wv, 12)
    meet(("dp", pair), ("dp", after), ("dp", before), ("tensor", core), ("tensor", across),
         *[("dp", at_group(s) * PAIR + member) for s in range(1, groups)])
    y_g = send(g_send, gyin, sy, 0, "dp", pair)
    m1 = send(mlp_hbm.at[half_rows(1 - low_t), :], min1, sx, 0, "tensor", core)

    w_gn.wait(); w_res.wait(); w_go.wait()
    NR = 64
    def norm_two(i, _):
        r = rows_of(i * NR, NR)
        v = res[r, :]
        root = lax.rsqrt(jnp.mean(v * v, axis=1, keepdims=True) + EPS)
        up = gn[r, :].astype(f32) * gain2[...]
        mean = jnp.mean(up * v, axis=1, keepdims=True)
        d = go[r, :].astype(f32) + root * up - v * (root * root * root * mean)
        resid[r, :] = d
        low_res[r, :] = d.astype(bf)
        return 0
    lax.fori_loop(0, rows // NR, norm_two, 0)
    w_wo.wait()
    def mix_tile(i, _):
        r = rows_of(i * half, half)
        gm[r, :] = nt(low_res[r, :], wo[...]).astype(bf)
        return 0
    lax.fori_loop(0, 2, mix_tile, 0)
    w_mlp.wait(); m1.wait()
    amid[...] = (amine[...].astype(f32) + min1[...].astype(f32)).astype(bf)
    w_kv.wait()
    for g in range(2):
        for s in range(2):
            for b in range(2):
                kvar[g, s, pl.ds(b * rows, rows), :] = place(kv_ref[b, :, 0:128], g, s)
                vvar[g, s, pl.ds(b * rows, rows), :] = place(kv_ref[b, :, 128:256], g, s)
            kvart[g, s] = kvar[g, s].T
    dk[...] = jnp.zeros_like(dk)
    dv[...] = jnp.zeros_like(dv)
    m2 = send(amid, min2, sx, 1, "tensor", across)
    w_mx.wait()
    lowt[0:qc, :] = mixed[...].T
    hrow = qc // n_dp
    def wout_tile(j, _):
        c = rows_of(j * 256, 256)
        tile32[...] = nn(lowt[0:qc, :], low_res[:, c])
        for z in range(groups):
            wown[z, :, c] = tile32[rows_of((z * PAIR + member) * hrow, hrow), :].astype(bf)
            wsend[z, :, c] = tile32[rows_of((z * PAIR + 1 - member) * hrow, hrow), :].astype(bf)
        return 0
    lax.fori_loop(0, width // 256, wout_tile, 0)
    w_qr.wait()

    window = rows + TILE
    def attend(i, _):
        r = rows_of(i * TILE, TILE)
        k = pl.ds(pl.multiple_of(i * TILE, TILE), window)
        kpos = lax.broadcasted_iota(jnp.int32, (window, TILE), 0)
        qpos = lax.broadcasted_iota(jnp.int32, (window, TILE), 1) + rows
        bias = jnp.where((ids_col[k, :] == ids_row[:, r]) & (kpos <= qpos), 0.0, -1e30)
        bias = jnp.concatenate([bias, bias], axis=1)
        for g in range(2):
            q2 = jnp.concatenate([q_ref[r, (2 * g) * 128:(2 * g + 1) * 128], q_ref[r, (2 * g + 1) * 128:(2 * g + 2) * 128]], axis=0)
            do2 = jnp.concatenate([gm[r, (2 * g) * 128:(2 * g + 1) * 128], gm[r, (2 * g + 1) * 128:(2 * g + 2) * 128]], axis=0)
            dqt = None
            for s in range(2):
                st = nt(kvar[g, s, k, :], q2) + bias
                peak = jnp.max(st, axis=0, keepdims=True)
                e = jnp.exp(st - peak)
                pt = e * (1.0 / jnp.sum(e, axis=0, keepdims=True))
                dpt = nt(vvar[g, s, k, :], do2)
                delta = jnp.sum(pt * dpt, axis=0, keepdims=True)
                dst = (pt * (dpt - delta)).astype(bf)
                dv[g, s, k, :] += nn(pt.astype(bf), do2)
                dk[g, s, k, :] += nn(dst, q2)
                part = nn(kvart[g, s, :, k], dst)
                dqt = part if dqt is None else dqt + part
            d = dqt.T * HEAD_SIZE ** -0.5
            for b in range(2):
                low[r, (2 * g + b) * 128:(2 * g + b + 1) * 128] = turn(d[b * TILE:(b + 1) * TILE, :], cos_ref[r, :], -sin_ref[r, :]).astype(bf)
        return 0
    lax.fori_loop(0, rows // TILE, attend, 0)

    def exchange(src, dst, base):
        return [send(src.at[at_group(s)], dst.at[s - 1], sz, base + s - 1, "dp", at_group(s) * PAIR + member) for s in range(1, groups)]
    w_own.wait(); y_g.wait()
    y_u = send(u_send, uyin, sy, 1, "dp", pair)
    def pair_add(total_ref, got):
        for z in range(groups):
            total_ref[z] = (own32[z] + got[z].astype(f32)).astype(bf)
    pair_add(gsum, gyin)
    def gathered(acc, b):
        r = pl.ds(b * rows, rows)
        lane = lax.broadcasted_iota(jnp.int32, (rows, 128), 1)
        first = acc[0, 0, r, :] + pltpu.roll(acc[0, 1, r, :], HEAD_SIZE, 1)
        second = pltpu.roll(acc[1, 0, r, :], HEAD_SIZE, 1) + acc[1, 1, r, :]
        return jnp.where(lane < HEAD_SIZE, first, second)
    hprev[:, 0:128] = gathered(dk, 0).astype(bf)
    hprev[:, 128:256] = gathered(dv, 0).astype(bf)
    halo = send(hprev, hin, sh, 0, "dp", before)
    z_g = exchange(gsum, gz, 0)
    w_own = cp(u_own, own32, 8)
    m2.wait()
    def out_rows(i, _):
        r = rows_of(low_t * half + i * NR, NR)
        m = rows_of(i * NR, NR)
        summed = (amid[m, :].astype(f32) + min2[m, :].astype(f32)).astype(bf)
        go[r, :] = (res[r, :] + summed.astype(f32)).astype(bf)
        return 0
    lax.fori_loop(0, half // NR, out_rows, 0)
    w_out = cp(go.at[half_rows(low_t), :], out_hbm.at[half_rows(low_t), :], 2)
    m3 = send(go.at[half_rows(low_t), :], out_hbm.at[half_rows(low_t), :], sx, 2, "tensor", core)
    lowt[0:qc, :] = low[:, 0:qc].T
    w_nm.wait()
    def grad_cols(row0, count):
        def body(z, _):
            a = rows_of((z * PAIR + member) * dcols, dcols)
            b = rows_of((z * PAIR + 1 - member) * dcols, dcols)
            t = lowt[row0:row0 + count, :]
            qsend[z, row0:row0 + count, :] = nn(t, normed[:, b]).astype(bf)
            qown[z, row0:row0 + count, :] = nn(t, normed[:, a]).astype(bf)
            return 0
        lax.fori_loop(0, groups, body, 0)
    grad_cols(0, qc)
    halo.wait()
    kraw = gathered(dk, 1) + hin[:, 0:128].astype(f32)
    low[:, qc:qc + 128] = turn(kraw, cos_ref[...], -sin_ref[...]).astype(bf)
    low[:, qc + 128:qc + 256] = (gathered(dv, 1) + hin[:, 128:256].astype(f32)).astype(bf)
    w_q.wait(); w_k.wait(); w_v.wait()
    def normed_part(j, _):
        c = rows_of(j * 256, 256)
        p = (nt(low[:, 0:qc], wq[c, :]) + nt(low[:, qc:qc + 128], wk[c, :]) + nt(low[:, qc + 128:qc + 256], wv[c, :]))
        res[:, c] = p
        gacc[0:1, c] = jnp.sum(p * normed[:, c].astype(f32), axis=0, keepdims=True) / gain1[0:1, c]
        gacc[1:2, c] = gain2_part[0:1, c] / gain2[0:1, c]
        return 0
    lax.fori_loop(0, width // 256, normed_part, 0)
    hchunk = CHUNK // 2
    chunks = rows // CHUNK
    def own_rows(c):
        return rows_of(c * CHUNK + low_t * hchunk, hchunk)
    def oth_rows(c):
        return rows_of(c * CHUNK + (1 - low_t) * hchunk, hchunk)
    def buf(c):
        return pl.ds(c * hchunk, hchunk)
    flights = {}
    for c in range(chunks):
        amine[buf(c), :] = res[oth_rows(c), :].astype(bf)
        flights[1, c] = send(amine.at[buf(c), :], ain1.at[buf(c), :], sx, 3 + 3 * c, "tensor", core)
    for z in range(groups):
        for m in range(PAIR):
            d0 = (z * PAIR + m) * dcols
            gs[m, z, 0:2, :] = gacc[0:2, d0:d0 + dcols]
    gown[...] = gs[member]
    y_gain = send(gs.at[1 - member], gyi, sg, 0, "dp", pair)
    lowt[qc:qc + 256, :] = low[:, qc:qc + 256].T
    grad_cols(qc, 256)
    for c in range(chunks):
        flights[1, c].wait()
        amid[buf(c), :] = (res[own_rows(c), :] + ain1[buf(c), :].astype(f32)).astype(bf)
        flights[2, c] = send(amid.at[buf(c), :], ain2.at[buf(c), :], sx, 4 + 3 * c, "tensor", across)
    y_gain.wait()
    gown[...] = gown[...] + gyi[...]
    w_x = cp(x_hbm, normed, 9)
    z_gain = [send(gown.at[at_group(s)], gzi.at[s - 1], sg, s, "dp", at_group(s) * PAIR + member) for s in range(1, groups)]
    y_u.wait()
    y_w = send(wsend, win, sy, 2, "dp", pair)
    w_own.wait()
    pair_add(usum, uyin)
    for q in z_g:
        q.wait()
    z_u = exchange(usum, uz, groups)
    def transposed(sum_ref, got, hbm):
        out = []
        share = sum_ref.shape[1]
        for s in range(groups):
            block = sum_ref[group] if s == 0 else got[s - 1]
            for h in range(share // 256):
                own32[s, h * 256:h * 256 + dcols, :] = block[h * 256:(h + 1) * 256, :].astype(f32).T
                out.append(cp(own32.at[s, h * 256:h * 256 + dcols, :], hbm.at[:, rows_of(from_group(s) * share + h * 256, 256)], 13 + 2 * s + h))
        return out
    w_gate = transposed(gsum, gz, gate_hbm)
    w_x.wait()
    def norm_one(r):
        v = normed[r, :].astype(f32)
        root = lax.rsqrt(jnp.mean(v * v, axis=1, keepdims=True) + EPS)
        up = gn[r, :].astype(f32) * gain1[...]
        mean = jnp.mean(up * v, axis=1, keepdims=True)
        low_res[r, :] = (resid[r, :] + root * up - v * (root * root * root * mean)).astype(bf)
    for c in range(chunks):
        flights[2, c].wait()
        gn[own_rows(c), :] = (amid[buf(c), :].astype(f32) + ain2[buf(c), :].astype(f32)).astype(bf)
        flights[3, c] = send(gn.at[own_rows(c), :], gn.at[own_rows(c), :], sx, 5 + 3 * c, "tensor", core)
        norm_one(own_rows(c))
        flights[3, c].wait()
        norm_one(oth_rows(c))
    w_gin = cp(low_res, gin_hbm, 1)
    for q in z_gain:
        q.wait()
    total = gown[group]
    for s in range(1, groups):
        total = total + gzi[s - 1]
    gt[0] = total
    t1 = send(gt.at[0], gti.at[0], sg, groups, "tensor", core)
    t1.wait()
    gt[1] = gt[0] + gti[0]
    t2 = send(gt.at[1], gti.at[1], sg, groups + 1, "tensor", across)
    t2.wait()
    gains_ref[...] = gt[1] + gti[1]
    y_w.wait()
    y_q = send(qsend, qin, sy, 3, "dp", pair)
    for z in range(groups):
        wown[z] = (wown[z].astype(f32) + win[z].astype(f32)).astype(bf)
    for q in z_u:
        q.wait()
    z_w = exchange(wown, wz, 2 * groups)
    for q in w_gate:
        q.wait()
    w_up = transposed(usum, uz, up_hbm)
    for q in z_w:
        q.wait()
    acc = wown[group].astype(f32)
    for s in range(1, groups):
        acc = acc + wz[s - 1].astype(f32)
    wout_ref[...] = acc
    y_q.wait()
    for z in range(groups):
        qown[z] = (qown[z].astype(f32) + qin[z].astype(f32)).astype(bf)
    z_q = exchange(qown, qz, 3 * groups)
    for q in z_q:
        q.wait()
    acc = qown[group].astype(f32)
    for s in range(1, groups):
        acc = acc + qz[s - 1].astype(f32)
    qkv_ref[...] = acc.T
    for q in w_up:
        q.wait()
    w_gin.wait()
    w_out.wait()
    m3.wait()

def backward(gn, residual, x, grad_output, mlp_part, normed, wo, wq, wk, wv, g_own, g_send, u_own, u_send, mixed, q, kv, gain1, gain2, gain2_part,
             ids_col, ids_row, cosine, sine, n_dp, n_tensor):
    rows, width = x.shape
    groups = n_dp // PAIR
    share = g_own.shape[1]
    dcols = width // n_dp
    qc = wq.shape[1]
    cols = qc + 256
    A = pl.BlockSpec(memory_space=pl.ANY)
    vm = pl.BlockSpec(memory_space=pltpu.VMEM)
    bf, f32 = jnp.bfloat16, jnp.float32
    sd = jax.ShapeDtypeStruct
    V = pltpu.VMEM
    D = pltpu.SemaphoreType.DMA
    half = rows // 2
    hrow = qc // n_dp
    act = V((rows, width), bf)
    return pl.pallas_call(
        functools.partial(backward_kernel, n_dp, n_tensor),
        out_shape=(sd((rows, width), bf), sd((rows, width), bf), sd((dcols, groups * share), f32), sd((dcols, groups * share), f32),
                   sd((8, dcols), f32), sd((dcols, cols), f32), sd((hrow, width), f32)),
        in_specs=[A] * 17 + [vm] * 7,
        out_specs=(A,) * 4 + (vm,) * 3,
        scratch_shapes=[act, V((rows, width), f32), act, act, V((qc, width), bf), V((width, qc), bf), V((width, 128), bf), V((width, 128), bf),
                        V((rows, qc), bf), V((rows, qc), bf), V((2, rows, 256), bf), V((groups, share, dcols), f32), V((rows, width), f32), act, V((rows, qc), bf),
                        V((2, 2, 2 * rows, 128), bf), V((2, 2, 2 * rows, 128), bf), V((2, 2, 128, 2 * rows), bf),
                        V((2, 2, 2 * rows, 128), f32), V((2, 2, 2 * rows, 128), f32),
                        V((rows, cols), bf), V((cols, rows), bf), V((qc, 256), f32),
                        V((groups, hrow, width), bf), V((groups, hrow, width), bf), V((groups, hrow, width), bf), V((groups - 1, hrow, width), bf),
                        *[V((groups, share, dcols), bf), V((groups, share, dcols), bf), V((groups - 1, share, dcols), bf)] * 2,
                        V((groups, cols, dcols), bf), V((groups, cols, dcols), bf), V((groups, cols, dcols), bf), V((groups - 1, cols, dcols), bf),
                        *[V((half, width), bf)] * 6,
                        V((rows, 256), bf), V((rows, 256), bf), V((8, width), f32), V((PAIR, groups, 8, dcols), f32), V((groups, 8, dcols), f32),
                        V((groups, 8, dcols), f32), V((groups - 1, 8, dcols), f32), V((2, 8, dcols), f32), V((2, 8, dcols), f32),
                        D((13 + 2 * groups,)), D((2, 4)), D((2, 4 * groups)), D((2, 3 + 3 * (rows // CHUNK))), D((2, 1)), D((2, groups + 2))],
        compiler_params=pltpu.CompilerParams(collective_id=4, has_side_effects=True, vmem_limit_bytes=67043328),
        cost_estimate=pl.CostEstimate(flops=4 * rows * width * (2 * qc + 256) + 40 * rows * rows * 5 * 128, bytes_accessed=40 * rows * width, transcendentals=8 * rows * rows),
        name="attention_backward",
    )(gn, residual, x, grad_output, mlp_part, normed, wo, wq, wk, wv, g_own, g_send, u_own, u_send, mixed, q, kv,
      gain1.reshape(1, width), gain2.reshape(1, width), gain2_part, ids_col, ids_row, cosine, sine)


def rope_table(half_count):
    adjusted = []
    for index in range(half_count):
        base_value = 500000.0 ** (-index / half_count)
        wave_length = 2.0 * math.pi / base_value
        smooth = (8192.0 / wave_length - 1.0) / 3.0
        if wave_length > 8192.0:
            adjusted.append(base_value / 32.0)
        elif wave_length >= 2048.0:
            adjusted.append((1.0 - smooth) * base_value / 32.0 + smooth * base_value)
        else:
            adjusted.append(base_value)
    return jnp.asarray(adjusted, dtype=jnp.float32)


def rope_angles(start_row, count_rows, half_count):
    positions = (start_row + jnp.arange(count_rows, dtype=jnp.int32)).astype(jnp.float32)
    phase_angle = positions[:, None] * rope_table(half_count)[None, :]
    return (jnp.cos(phase_angle)[:, None, :], jnp.sin(phase_angle)[:, None, :])


def rotate_halves(values, cosine_table, sine_values):
    half_size = values.shape[-1] // 2
    first_half = values[..., :half_size]
    second_half = values[..., half_size:]
    return jnp.concatenate(
        [
            first_half * cosine_table - second_half * sine_values,
            second_half * cosine_table + first_half * sine_values,
        ],
        axis=-1,
    )


def norm_rows(values, gain_row):
    inverse_root = lax.rsqrt(jnp.mean(values * values, axis=-1, keepdims=True) + NORM_EPSILON)
    return (inverse_root, values * inverse_root * gain_row)


def norm_back(values, inverse_root, gain_row, upstream):
    scaled = gain_row * upstream
    return inverse_root * scaled - values * inverse_root**3 * jnp.mean(
        scaled * values, axis=-1, keepdims=True
    )


def passed_along(block, axis, distance):
    devices = range(lax.axis_size(axis))
    route = [(i - distance, i) for i in devices if i - distance in devices]
    return lax.ppermute(block, axis, route)


def tensor_swap(block, bit):
    return lax.ppermute(block, "tensor", [(i, i ^ bit) for i in range(lax.axis_size("tensor"))])


def pair_swap(block):
    return lax.ppermute(block, "dp", [(i, i ^ 1) for i in range(lax.axis_size("dp"))])


def group_shift(block, distance):
    count = lax.axis_size("dp")
    groups = count // PAIR
    return lax.ppermute(
        block,
        "dp",
        [(i, ((i // PAIR + distance) % groups) * PAIR + i % PAIR) for i in range(count)],
    )


def tensor_sum(part):
    half = part.shape[1] // 2
    low = lax.axis_index("tensor") % 2
    first, second = part[:, :half], part[:, half:]
    mine = jnp.where(low == 0, first, second)
    other = jnp.where(low == 0, second, first).astype(jnp.bfloat16)
    mine = mine + tensor_swap(other, 1).astype(jnp.float32)
    bit = 2
    while bit < lax.axis_size("tensor"):
        rounded = mine.astype(jnp.bfloat16)
        mine = rounded.astype(jnp.float32) + tensor_swap(rounded, bit).astype(jnp.float32)
        bit *= 2
    mine = mine.astype(jnp.bfloat16)
    other = tensor_swap(mine, 1)
    return jnp.concatenate(
        [jnp.where(low == 0, mine, other), jnp.where(low == 0, other, mine)], axis=1
    ).astype(jnp.float32)


def gather_groups(block):
    half = block.shape[1] // 2
    low = lax.axis_index("tensor") % 2
    piece = lax.dynamic_slice_in_dim(block, low * half, half, axis=1)
    rows = [block]
    for _ in range(lax.axis_size("dp") // PAIR - 1):
        piece = group_shift(piece, 1)
        other = tensor_swap(piece, 1)
        rows.append(
            jnp.concatenate(
                [jnp.where(low == 0, piece, other), jnp.where(low == 0, other, piece)], axis=1
            )
        )
    return jnp.concatenate(rows, axis=0)


def pair_sum(part):
    member = lax.axis_index("dp") % PAIR
    mine = lax.dynamic_index_in_dim(part, member, 1, keepdims=False)
    other = lax.dynamic_index_in_dim(part, 1 - member, 1, keepdims=False)
    return mine + pair_swap(other.astype(jnp.bfloat16)).astype(jnp.float32)


def group_exchange(blocks):
    groups = blocks.shape[0]
    group = lax.axis_index("dp") // PAIR
    received = []
    for distance in range(groups):
        block = lax.dynamic_index_in_dim(blocks, (group + distance) % groups, 0, keepdims=False)
        received.append(block if distance == 0 else group_shift(block, distance))
    return received


def scatter_sum(part):
    summed = pair_sum(part)
    groups = summed.shape[0]
    group = lax.axis_index("dp") // PAIR
    total = lax.dynamic_index_in_dim(summed, group, 0, keepdims=False)
    rounded = summed.astype(jnp.bfloat16)
    for block in group_exchange(rounded)[1:]:
        total = total + block.astype(jnp.float32)
    return total


def block_scores(query_rows, key_rows, query_ids, key_ids, query_pos, key_pos):
    scores = jnp.einsum(
        "qgrd,kgd->grqk", query_rows, key_rows, preferred_element_type=jnp.float32
    ) * HEAD_SIZE ** (-0.5)
    allowed = (query_ids[:, None] == key_ids[None, :]) & (key_pos[None, :] <= query_pos[:, None])
    return jnp.where(allowed, scores, -1e30)


def block_forward(query_rows, key_rows, value_rows, query_ids, key_ids, query_pos, key_pos):
    scores = block_scores(query_rows, key_rows, query_ids, key_ids, query_pos, key_pos)
    row_peak = jnp.max(scores, axis=-1, keepdims=True)
    logsum = row_peak + jnp.log(jnp.sum(jnp.exp(scores - row_peak), axis=-1, keepdims=True))
    prob_low = jnp.exp(scores - logsum).astype(jnp.bfloat16)
    mixed_rows = jnp.einsum(
        "grqk,kgd->qgrd", prob_low, value_rows, preferred_element_type=jnp.float32
    )
    return (mixed_rows.astype(jnp.bfloat16), logsum)


def block_backward(
    query_rows,
    key_rows,
    value_rows,
    out_rows,
    grad_rows,
    logsum,
    query_ids,
    key_ids,
    query_pos,
    key_pos,
):
    scores = block_scores(query_rows, key_rows, query_ids, key_ids, query_pos, key_pos)
    prob_rows = jnp.exp(scores - logsum)
    grad_vals = jnp.einsum(
        "grqk,qgrd->kgd",
        prob_rows.astype(jnp.bfloat16),
        grad_rows,
        preferred_element_type=jnp.float32,
    )
    delta_rows = jnp.sum(out_rows.astype(jnp.float32) * grad_rows.astype(jnp.float32), axis=-1)
    grad_probs = jnp.einsum(
        "qgrd,kgd->grqk", grad_rows, value_rows, preferred_element_type=jnp.float32
    )
    grad_scores = (
        prob_rows * (grad_probs - jnp.transpose(delta_rows, (1, 2, 0))[..., None])
    ).astype(jnp.bfloat16)
    grad_query_rows = jnp.einsum(
        "grqk,kgd->qgrd", grad_scores, key_rows, preferred_element_type=jnp.float32
    ) * HEAD_SIZE ** (-0.5)
    grad_key_rows = jnp.einsum(
        "grqk,qgrd->kgd", grad_scores, query_rows, preferred_element_type=jnp.float32
    ) * HEAD_SIZE ** (-0.5)
    return (grad_query_rows, grad_key_rows, grad_vals)


def dot(form, left, right):
    return jnp.einsum(form, left, right, preferred_element_type=jnp.float32)


def gated(gate_value, up_value):
    return (jax.nn.silu(gate_value) * up_value).astype(jnp.bfloat16)


def gated_back(grad_hidden, gate_value, up_value):
    sigmoid_gate = jax.nn.sigmoid(gate_value)
    grad_gate_low = (
        grad_hidden * up_value * sigmoid_gate * (1.0 + gate_value * (1.0 - sigmoid_gate))
    ).astype(jnp.bfloat16)
    return grad_gate_low, (grad_hidden * jax.nn.silu(gate_value)).astype(jnp.bfloat16)


def shards_plain(
    inputs,
    norm1_gain,
    query_weight,
    key_weight,
    value_weight,
    w_out,
    norm2_gain,
    w_gate,
    w_up,
    w_down,
    doc_ids,
    grad_output,
):
    tok_rows, width = inputs.shape
    heads_here = query_weight.shape[1] // HEAD_SIZE
    kv_here = key_weight.shape[1] // HEAD_SIZE
    group_size = heads_here // kv_here
    n_dp = lax.axis_size("dp")
    groups = n_dp // PAIR
    group = lax.axis_index("dp") // PAIR
    offset = lax.axis_index("dp") * tok_rows
    grad_all = gather_groups(grad_output)

    cosine_table, sine_values = rope_angles(offset, tok_rows, HEAD_SIZE // 2)
    inputs_wide = inputs.astype(jnp.float32)
    root_one, normed = norm_rows(inputs_wide, norm1_gain)
    normed_low = normed.astype(jnp.bfloat16)
    query_raw = dot("td,dh->th", normed_low, query_weight).reshape(tok_rows, heads_here, HEAD_SIZE)
    key_raw = dot("td,dh->th", normed_low, key_weight).reshape(tok_rows, kv_here, HEAD_SIZE)
    value_low = dot("td,dh->th", normed_low, value_weight).astype(jnp.bfloat16)
    query_low = (
        rotate_halves(query_raw, cosine_table, sine_values)
        .astype(jnp.bfloat16)
        .reshape(tok_rows, kv_here, group_size, HEAD_SIZE)
    )
    key_low = (
        rotate_halves(key_raw, cosine_table, sine_values)
        .astype(jnp.bfloat16)
        .reshape(tok_rows, kv_here * HEAD_SIZE)
    )
    query_ids = doc_ids + 1
    tail = jnp.concatenate([key_low, value_low], axis=1)
    prev_tail = passed_along(tail, "dp", 1)
    prev_ids = passed_along(query_ids, "dp", 1)
    both = jnp.concatenate([prev_tail, tail], axis=0)
    keys_all = both[:, : kv_here * HEAD_SIZE].reshape(2 * DOC_MAX, kv_here, HEAD_SIZE)
    values_all = both[:, kv_here * HEAD_SIZE :].reshape(2 * DOC_MAX, kv_here, HEAD_SIZE)
    ids_all = jnp.concatenate([prev_ids, query_ids])
    pos_all = offset - DOC_MAX + jnp.arange(tok_rows + DOC_MAX, dtype=jnp.int32)
    query_pos = pos_all[DOC_MAX:]
    mixed_block, logsum_block = block_forward(
        query_low, keys_all, values_all, query_ids, ids_all, query_pos, pos_all
    )
    mixed_low = mixed_block.reshape(tok_rows, heads_here * HEAD_SIZE)
    residual = inputs_wide + tensor_sum(dot("te,ed->td", mixed_low, w_out))

    root_two, normed_two = norm_rows(residual, norm2_gain)
    normed_two_low = normed_two.astype(jnp.bfloat16)
    normed_all = gather_groups(normed_two_low)
    gate_value = dot("td,df->tf", normed_two_low, w_gate)
    up_value = dot("td,df->tf", normed_two_low, w_up)
    grad_hidden = dot("td,fd->tf", grad_output, w_down)
    hidden_low = gated(gate_value, up_value)
    grad_gate_low, grad_up_low = gated_back(grad_hidden, gate_value, up_value)
    normed_two_part = dot("tf,df->td", grad_gate_low, w_gate) + dot("tf,df->td", grad_up_low, w_up)
    grad_normed_two = tensor_sum(normed_two_part)
    gain_two_part = jnp.sum(normed_two_part * residual * root_two, axis=0)
    output = (residual + tensor_sum(dot("tf,fd->td", hidden_low, w_down))).astype(jnp.bfloat16)

    share = w_gate.shape[1] // groups
    gate_share = lax.dynamic_slice_in_dim(w_gate, group * share, share, axis=1)
    up_share = lax.dynamic_slice_in_dim(w_up, group * share, share, axis=1)
    down_share = lax.dynamic_slice_in_dim(w_down, group * share, share, axis=0)
    gate_all = dot("td,df->tf", normed_all, gate_share)
    up_all = dot("td,df->tf", normed_all, up_share)
    grad_hidden_all = dot("td,fd->tf", grad_all, down_share)
    hidden_all = gated(gate_all, up_all)
    gate_low_all, up_low_all = gated_back(grad_hidden_all, gate_all, up_all)
    down_part = dot("tf,td->fd", hidden_all, grad_all)
    grad_wdown = pair_sum(down_part.reshape(1, PAIR, share // PAIR, width))[0]
    rows_here = width // n_dp

    def column_grad(low_all):
        part = dot("td,tf->df", normed_all, low_all)
        summed = pair_sum(part.reshape(groups, PAIR, rows_here, share)).astype(jnp.bfloat16)
        full = jnp.zeros((rows_here, groups * share), jnp.float32)
        for distance, block in enumerate(group_exchange(summed)):
            full = lax.dynamic_update_slice_in_dim(
                full, block.astype(jnp.float32), ((group - distance) % groups) * share, axis=1
            )
        return full

    grad_wgate = column_grad(gate_low_all)
    grad_wup = column_grad(up_low_all)

    grad_residual = grad_output.astype(jnp.float32) + norm_back(
        residual, root_two, norm2_gain, grad_normed_two
    )
    grad_res_low = grad_residual.astype(jnp.bfloat16)
    wout_part = dot("te,td->ed", mixed_low, grad_res_low)
    grad_wout = scatter_sum(wout_part.reshape(groups, PAIR, -1, width))
    grad_mixed = (
        dot("td,ed->te", grad_res_low, w_out)
        .astype(jnp.bfloat16)
        .reshape(tok_rows, kv_here, group_size, HEAD_SIZE)
    )
    mixed_view = mixed_low.reshape(tok_rows, kv_here, group_size, HEAD_SIZE)
    grad_query_rows, grad_key_rows, grad_value_rows = block_backward(
        query_low,
        keys_all,
        values_all,
        mixed_view,
        grad_mixed,
        logsum_block,
        query_ids,
        ids_all,
        query_pos,
        pos_all,
    )
    sent = jnp.concatenate(
        [
            grad_key_rows.reshape(2 * DOC_MAX, kv_here * HEAD_SIZE),
            grad_value_rows.reshape(2 * DOC_MAX, kv_here * HEAD_SIZE),
        ],
        axis=1,
    )
    back = passed_along(sent[:DOC_MAX].astype(jnp.bfloat16), "dp", -1).astype(jnp.float32)
    own = sent[DOC_MAX:] + back
    grad_qraw = grad_query_rows.reshape(tok_rows, heads_here, HEAD_SIZE)
    query_low_gradient = (
        rotate_halves(grad_qraw, cosine_table, -sine_values)
        .astype(jnp.bfloat16)
        .reshape(tok_rows, heads_here * HEAD_SIZE)
    )
    key_low_gradient = (
        rotate_halves(
            own[:, : kv_here * HEAD_SIZE].reshape(tok_rows, kv_here, HEAD_SIZE),
            cosine_table,
            -sine_values,
        )
        .astype(jnp.bfloat16)
        .reshape(tok_rows, kv_here * HEAD_SIZE)
    )
    value_low_gradient = own[:, kv_here * HEAD_SIZE :].astype(jnp.bfloat16)
    low_gradient = jnp.concatenate(
        [query_low_gradient, key_low_gradient, value_low_gradient], axis=1
    )
    normed_one_part = (
        dot("kl,ql->kq", query_low_gradient, query_weight)
        + dot("kl,ql->kq", key_low_gradient, key_weight)
        + dot("kl,ql->kq", value_low_gradient, value_weight)
    )
    grad_normed_one = tensor_sum(normed_one_part)
    gain_one_part = jnp.sum(normed_one_part * inputs_wide * root_one, axis=0)
    qkv_part = dot("wj,wq->jq", normed_low, low_gradient)
    columns = qkv_part.shape[1]
    gains = jnp.stack(
        [gain_one_part.reshape(n_dp, rows_here), gain_two_part.reshape(n_dp, rows_here)], axis=1
    )
    gains = jnp.pad(gains, ((0, 0), (0, 14), (0, columns - rows_here)))
    qkv_part = jnp.concatenate([qkv_part.reshape(n_dp, rows_here, columns), gains], axis=1)
    qkv_sum = scatter_sum(qkv_part.reshape(groups, PAIR, rows_here + 16, columns))
    grad_qkv = qkv_sum[:rows_here]
    gain_sums = qkv_sum[rows_here : rows_here + 16, :rows_here]
    bit = 1
    while bit < lax.axis_size("tensor"):
        gain_sums = gain_sums + tensor_swap(gain_sums, bit)
        bit *= 2
    grad_input_norm = norm_back(inputs_wide, root_one, norm1_gain, grad_normed_one)
    grad_inputs = (grad_residual + grad_input_norm).astype(jnp.bfloat16)
    q_columns = query_weight.shape[1]
    k_columns = key_weight.shape[1]
    return (
        output,
        grad_inputs,
        gain_sums[0],
        grad_qkv[:, :q_columns],
        grad_qkv[:, q_columns : q_columns + k_columns],
        grad_qkv[:, q_columns + k_columns :],
        grad_wout,
        gain_sums[1],
        grad_wgate,
        grad_wup,
        grad_wdown,
    )


def shards(
    inputs,
    norm1_gain,
    query_weight,
    key_weight,
    value_weight,
    w_out,
    norm2_gain,
    w_gate,
    w_up,
    w_down,
    doc_ids,
    grad_output,
):
    tok_rows, width = inputs.shape
    heads_here = query_weight.shape[1] // HEAD_SIZE
    kv_here = key_weight.shape[1] // HEAD_SIZE
    group_size = heads_here // kv_here
    n_dp = lax.axis_size("dp")
    groups = n_dp // PAIR
    group = lax.axis_index("dp") // PAIR
    offset = lax.axis_index("dp") * tok_rows
    share = w_gate.shape[1] // groups
    gate_t = lax.dynamic_slice_in_dim(w_gate, group * share, share, axis=1).T
    up_t = lax.dynamic_slice_in_dim(w_up, group * share, share, axis=1).T
    down_share = lax.dynamic_slice_in_dim(w_down, group * share, share, axis=0)
    cosine_table, sine_values = rope_angles(offset, tok_rows, HEAD_SIZE // 2)
    cosine = jnp.tile(cosine_table[:, 0, :], (1, 4))
    sine = jnp.tile(jnp.concatenate([-sine_values[:, 0, :], sine_values[:, 0, :]], axis=1), (1, 2))
    n_tensor = lax.axis_size("tensor")
    normed_low, query_scaled, kv, id_rows, _, mixed_low, residual, normed_two_low, one_g, part_g = attend_forward(
        inputs, norm1_gain, query_weight, key_weight, value_weight, w_out, norm2_gain, cosine, sine, doc_ids, grad_output, n_dp, n_tensor)
    mlp_part, back_part, normed_rest, rest_g, gain_two_part = mlp(normed_two_low, grad_output, part_g, w_gate, w_up, w_down, n_dp, n_tensor)
    grad_wdown, g_own, g_send, u_own, u_send, grad_normed_two = wgrad(
        normed_two_low, normed_rest, grad_output, one_g, part_g, rest_g, gate_t, up_t, down_share, back_part, n_dp, n_tensor)
    output, grad_inputs, grad_wgate, grad_wup, gain_sums, grad_qkv, grad_wout = backward(
        grad_normed_two, residual, inputs, grad_output, mlp_part, normed_low, w_out, query_weight, key_weight, value_weight,
        g_own, g_send, u_own, u_send, mixed_low, query_scaled, kv, norm1_gain, norm2_gain, gain_two_part,
        id_rows.reshape(2 * tok_rows, 1), doc_ids.reshape(1, tok_rows), cosine, sine, n_dp, n_tensor)
    q_columns = query_weight.shape[1]
    k_columns = key_weight.shape[1]
    return (
        output,
        grad_inputs,
        gain_sums[0],
        grad_qkv[:, :q_columns],
        grad_qkv[:, q_columns : q_columns + k_columns],
        grad_qkv[:, q_columns + k_columns :],
        grad_wout,
        gain_sums[1],
        grad_wgate,
        grad_wup,
        grad_wdown,
    )


def kernels_fit(mesh, *args):
    n_dp, n_tensor = mesh.shape["dp"], mesh.shape["tensor"]
    width = args[0].shape[1]
    return (
        n_dp % PAIR == 0
        and n_dp // PAIR <= 4
        and n_tensor == 4
        and width // n_dp in (128, 256)
        and args[7].shape[1] // n_tensor // (n_dp // PAIR) % 256 == 0
        and args[0].shape[0] // n_dp == DOC_MAX
        and args[3].shape[1] // n_tensor == 2 * HEAD_SIZE
        and args[2].shape[1] == 4 * args[3].shape[1]
    )


def solution(mesh):
    def step(*args):
        return mapped(mesh, shards if kernels_fit(mesh, *args) else shards_plain)(*args)

    return step


def mapped(mesh, function):
    return jax.shard_map(
        function,
        mesh=mesh,
        in_specs=(
            P("dp", None),
            P(),
            P(None, "tensor"),
            P(None, "tensor"),
            P(None, "tensor"),
            P("tensor", None),
            P(),
            P(None, "tensor"),
            P(None, "tensor"),
            P("tensor", None),
            P("dp"),
            P("dp", None),
        ),
        out_specs=(
            P("dp", None),
            P("dp", None),
            P("dp"),
            P("dp", "tensor"),
            P("dp", "tensor"),
            P("dp", "tensor"),
            P(("tensor", "dp"), None),
            P("dp"),
            P("dp", "tensor"),
            P("dp", "tensor"),
            P(("tensor", "dp"), None),
        ),
        check_vma=False,
    )
```

```python
import functools
import math

import jax
import jax.numpy as jnp
from jax import lax
from jax.experimental import pallas as pl
from jax.experimental.pallas import tpu as pltpu
from jax.sharding import PartitionSpec as P

HEAD_SIZE = 64
DOC_MAX = 512
NORM_EPSILON = 1e-05

PAIR = 2
MESH = pl.DeviceIdType.MESH
EPS = NORM_EPSILON


def nn(a, b):
    return lax.dot_general(a, b, (((1,), (0,)), ((), ())), preferred_element_type=jnp.float32)
def nt(a, b):
    return lax.dot_general(a, b, (((1,), (1,)), ((), ())), preferred_element_type=jnp.float32)

def flip(index, bit):
    return index + bit - 2 * bit * ((index // bit) % 2)

def meet(*partners):
    barrier = pltpu.get_barrier_semaphore()
    for axis, index in partners:
        pl.semaphore_signal(barrier, inc=1, device_id={axis: index}, device_id_type=MESH)
    pl.semaphore_wait(barrier, len(partners))

def send(src, dst, sems, slot, axis, index):
    copy = pltpu.make_async_remote_copy(
        src_ref=src, dst_ref=dst, send_sem=sems.at[0, slot], recv_sem=sems.at[1, slot],
        device_id={axis: index}, device_id_type=MESH)
    copy.start()
    return copy

def swiglu(gate, up, grad):
    sig = 0.5 * (1.0 + jnp.tanh(0.5 * gate))
    silu = gate * sig
    hidden = (silu * up).astype(jnp.bfloat16)
    grad_gate = (grad * up * sig * (1.0 + gate * (1.0 - sig))).astype(jnp.bfloat16)
    grad_up = (grad * silu).astype(jnp.bfloat16)
    return hidden, grad_gate, grad_up

def mlp_kernel(n_dp, n_tensor, normed_hbm, grad_hbm, part_g, gate_hbm, up_hbm, down_hbm,
               out_ref, back_ref, all_hbm, rest_g, gain_ref,
               normed, grad, gate_w, up_w, down_w, hid, low_gate, low_up, load, far):
    rows, width = normed.shape
    cols = gate_w.shape[1]
    groups = n_dp // PAIR
    me_dp, me_t = lax.axis_index("dp"), lax.axis_index("tensor")
    right = lax.rem(me_dp + PAIR, n_dp)
    left = lax.rem(me_dp + n_dp - PAIR, n_dp)
    core, across = flip(me_t, 1), flip(me_t, 2)
    tile = 256
    tiles = cols // tile
    def cp(s, d, i):
        return pltpu.make_async_copy(s, d, load.at[i])
    def gate_tile(c, f):
        return cp(gate_hbm.at[:, c], gate_w.at[:, c], 2 + 3 * f)
    def up_tile(c, f):
        return cp(up_hbm.at[:, c], up_w.at[:, c], 3 + 3 * f)
    def down_tile(c, f):
        return cp(down_hbm.at[c, :], down_w.at[c, :], 4 + 3 * f)
    cp(normed_hbm, normed, 0).start()
    def load_tile(f):
        c = pl.ds(pl.multiple_of(f * tile, tile), tile)
        gate_tile(c, f).start()
        up_tile(c, f).start()
        down_tile(c, f).start()
    load_tile(0)
    cp(grad_hbm, grad, 1).start()
    ahead = 3
    for f in range(1, ahead):
        load_tile(f)
    meet(("dp", right), ("dp", left), ("tensor", core), ("tensor", across))
    piece = rows // n_tensor
    def part(t):
        return pl.ds(pl.multiple_of(t * piece, piece), piece)
    steps = groups - 1
    per = 4
    def ring(s):
        src = (normed_hbm if s == 1 else all_hbm.at[s - 2]).at[part(me_t), :]
        return send(src, all_hbm.at[s - 1].at[part(me_t), :], far, s * per, "dp", right)
    def spread_n(level):
        block = all_hbm.at[0]
        held, other = [me_t, across][:level + 1], [across, core][level]
        return [send(block.at[part(h), :], block.at[part(h), :], far, 1 + level + i, "tensor", other) for i, h in enumerate(held)]
    def spread_g(b, level):
        base = (steps + 1 + b) * per
        if level == 0:
            return [send(part_g.at[b], rest_g.at[b].at[part(me_t), :], far, base, "tensor", across)]
        return [send(part_g.at[b], rest_g.at[b].at[part(me_t), :], far, base + 1, "tensor", core),
                send(rest_g.at[b].at[part(across), :], rest_g.at[b].at[part(across), :], far, base + 2, "tensor", core)]
    def wait(copies):
        for c in copies:
            c.wait()

    ring_n = ring(1)
    g_x = {b: spread_g(b, 0) for b in range(min(2, steps))}

    cp(normed_hbm, normed, 0).wait()
    cp(grad_hbm, grad, 1).wait()
    def first(f, _):
        c = pl.ds(pl.multiple_of(f * tile, tile), tile)
        @pl.when(f + ahead < tiles)
        def _():
            load_tile(f + ahead)
        gate_tile(c, f).wait()
        g = nn(normed[...], gate_w[:, c])
        up_tile(c, f).wait()
        u = nn(normed[...], up_w[:, c])
        down_tile(c, f).wait()
        h = nt(grad[...], down_w[c, :])
        a, b, d = swiglu(g, u, h)
        hid[:, c] = a
        low_gate[:, c] = b
        low_up[:, c] = d
        return 0
    early = min(5, tiles)
    lax.fori_loop(0, early, first, 0)
    ring_n.wait()
    if steps > 1:
        ring_n = ring(2)
    n_x = spread_n(0)
    lax.fori_loop(early, tiles, first, 0)
    g_core = []
    for b in list(g_x):
        wait(g_x.pop(b))
        g_core = g_core + spread_g(b, 1)
    for b in range(2, steps):
        g_x[b] = spread_g(b, 0)
    wtile = 256
    wtiles = width // wtile
    def second(j, _):
        c = pl.ds(pl.multiple_of(j * wtile, wtile), wtile)
        b = nt(low_gate[...], gate_w[c, :]) + nt(low_up[...], up_w[c, :])
        back_ref[:, c] = b.astype(back_ref.dtype)
        gain_ref[0:1, c] = jnp.sum(b * normed[:, c].astype(jnp.float32), axis=0, keepdims=True)
        return 0
    def third(j, _):
        c = pl.ds(pl.multiple_of(j * wtile, wtile), wtile)
        out_ref[:, c] = nn(hid[...], down_w[:, c]).astype(out_ref.dtype)
        return 0
    lax.fori_loop(0, wtiles, third, 0)
    for s in range(2, steps):
        ring_n.wait()
        ring_n = ring(s + 1)
    wait(n_x)
    n_core = spread_n(1)
    lax.fori_loop(0, wtiles // 2, second, 0)
    for b in list(g_x):
        wait(g_x.pop(b))
        g_core = g_core + spread_g(b, 1)
    lax.fori_loop(wtiles // 2, wtiles, second, 0)
    if steps > 1:
        ring_n.wait()
    wait(n_core)
    wait(g_core)

def mlp(normed, grad_output, part_g, w_gate, w_up, w_down, n_dp, n_tensor):
    rows, width = normed.shape
    cols = w_gate.shape[1]
    groups = n_dp // PAIR
    tiles = cols // 256
    anyspec = pl.BlockSpec(memory_space=pl.ANY)
    vm = pl.BlockSpec(memory_space=pltpu.VMEM)
    bf = jnp.bfloat16
    return pl.pallas_call(
        functools.partial(mlp_kernel, n_dp, n_tensor),
        out_shape=(jax.ShapeDtypeStruct((rows, width), bf), jax.ShapeDtypeStruct((rows, width), bf),
                   jax.ShapeDtypeStruct((groups - 1, rows, width), bf), jax.ShapeDtypeStruct((groups - 1, rows, width), bf), jax.ShapeDtypeStruct((1, width), jnp.float32)),
        in_specs=[anyspec] * 6, out_specs=(vm, vm, anyspec, anyspec, vm),
        scratch_shapes=[pltpu.VMEM((rows, width), bf), pltpu.VMEM((rows, width), bf),
                        pltpu.VMEM((width, cols), bf), pltpu.VMEM((width, cols), bf), pltpu.VMEM((cols, width), bf),
                        pltpu.VMEM((rows, cols), bf), pltpu.VMEM((rows, cols), bf), pltpu.VMEM((rows, cols), bf),
                        pltpu.SemaphoreType.DMA((2 + 3 * tiles,)),
                        pltpu.SemaphoreType.DMA((2, 8 * groups)),
                        ],
        compiler_params=pltpu.CompilerParams(collective_id=2, has_side_effects=True, vmem_limit_bytes=60 << 20),
        cost_estimate=pl.CostEstimate(flops=12 * rows * width * cols, bytes_accessed=2 * (3 * width * cols + 8 * rows * width), transcendentals=rows * cols),
        name="feed_forward",
    )(normed, grad_output, part_g, w_gate, w_up, w_down)

def wgrad_kernel(n_dp, n_tensor, own_n, all_n, own_g, part_g, rest_g, gate_t, up_t, down_hbm, back_hbm,
                 d_own, d_send, g_sum, u_own, u_send, sum_ref,
                 g_own, g_send, g_in, n_all, g_all, wg, wu, wd, hid, lowg, lowu, mine, in1, mid, in2, load, far, ar, sy):
    rows, width = own_n.shape
    share = gate_t.shape[0]
    groups = n_dp // PAIR
    me_dp, me_t = lax.axis_index("dp"), lax.axis_index("tensor")
    member = lax.rem(me_dp, PAIR)
    bits = []
    bit = n_tensor // 2
    while bit:
        bits.append(bit); bit //= 2
    piece = rows // n_tensor
    def part(t):
        return pl.ds(pl.multiple_of(t * piece, piece), piece)
    def at(r, t):
        return pl.ds(pl.multiple_of(r * rows + t * piece, piece), piece)
    count = [0]
    def cp(s, d):
        c = pltpu.make_async_copy(s, d, load.at[count[0]]); count[0] += 1
        c.start(); return c
    half = rows // 2
    low = lax.rem(me_t, 2)
    def half_rows(c):
        return pl.ds(pl.multiple_of(c * half, half), half)
    w1 = [cp(gate_t, wg), cp(own_n, n_all.at[pl.ds(0, rows), :])]
    w2 = [cp(up_t, wu)]
    w3 = [cp(down_hbm.at[pl.ds(pl.multiple_of(me_dp // PAIR * share, share), share), :], wd), cp(own_g, g_all.at[pl.ds(0, rows), :])]
    w4 = [cp(back_hbm.at[half_rows(low), :], mine)]
    last = groups - 1
    others = [flip(me_t, 1), flip(me_t, 2), flip(flip(me_t, 1), 2)]
    blocks = {}
    for r in range(1, groups):
        if r == 1:
            wn = [cp(all_n.at[0], n_all.at[pl.ds(rows, rows), :])]
        else:
            wn = [cp(all_n.at[r - 1].at[part(me_t), :], n_all.at[at(r, me_t), :])]
        wgr = [cp(part_g.at[r - 1], g_all.at[at(r, me_t), :])]
        for h in others:
            wgr.append(cp(rest_g.at[r - 1].at[part(h), :], g_all.at[at(r, h), :]))
        blocks[r] = (wn, wgr)
    pair = flip(me_dp, 1)
    core, across = flip(me_t, 1), flip(me_t, 2)
    meet(("dp", pair), ("tensor", core), ("tensor", across))
    ar1 = send(back_hbm.at[half_rows(1 - low), :], in1, ar, 0, "tensor", core)
    def wait(cs):
        for c in cs:
            c.wait()
    def spread(r, level):
        held, other = [me_t, across][:level + 1], [across, core][level]
        return [send(n_all.at[at(r, h), :], n_all.at[at(r, h), :], far, 3 * (r - 2) + level + i, "tensor", other) for i, h in enumerate(held)]
    spreads = {}
    if last > 1:
        wait(blocks[2][0])
        spreads[2, 0] = spread(2, 0)

    def pass_a(r):
        rs = pl.ds(r * rows, rows)
        g = nt(wg[...], n_all[rs, :])
        u = nt(wu[...], n_all[rs, :])
        h = nt(wd[...], g_all[rs, :])
        a, b, d = swiglu(g, u, h)
        hid[:, rs] = a; lowg[:, rs] = b; lowu[:, rs] = d
    wait(w1)
    wait(w2)
    wait(w3)
    pass_a(0)
    for r in range(3, groups):
        wait(blocks[r][0])
        spreads[r, 0] = spread(r, 0)
    wait(w4)
    ar1.wait()
    mid[...] = (mine[...].astype(jnp.float32) + in1[...].astype(jnp.float32)).astype(jnp.bfloat16)
    if last > 0:
        wait(blocks[1][0])
        wait(blocks[1][1])
        pass_a(1)
    for r in range(2, groups):
        wait(spreads[r, 0])
        spreads[r, 1] = spread(r, 1)
        if r == last:
            ar2 = send(mid, in2, ar, 1, "tensor", across)
        wait(blocks[r][1])
        wait(spreads[r, 1])
        pass_a(r)
    if last < 2:
        ar2 = send(mid, in2, ar, 1, "tensor", across)
    dcols = width // n_dp
    def col_tile(low_ref, own_ref, send_ref):
        def body(q, _):
            a = pl.ds(pl.multiple_of((q * PAIR + member) * dcols, dcols), dcols)
            b = pl.ds(pl.multiple_of((q * PAIR + 1 - member) * dcols, dcols), dcols)
            send_ref[q] = nn(low_ref[...], n_all[:, b]).astype(jnp.bfloat16)
            own_ref[q] = nn(low_ref[...], n_all[:, a]).astype(jnp.bfloat16)
            return 0
        return body
    to_pair = []
    for q in range(groups):
        col_tile(lowg, g_own, g_send)(q, 0)
        to_pair.append(send(g_send.at[q], g_in.at[q], sy, q, "dp", pair))
    hrows = share // PAIR
    def down_tile(j, _):
        c = pl.ds(pl.multiple_of(j * 512, 512), 512)
        d_send[:, c] = nn(hid[pl.ds(pl.multiple_of((1 - member) * hrows, hrows), hrows), :], g_all[:, c]).astype(jnp.bfloat16)
        d_own[:, c] = nn(hid[pl.ds(pl.multiple_of(member * hrows, hrows), hrows), :], g_all[:, c]).astype(jnp.bfloat16)
        return 0
    lax.fori_loop(0, width // 512, down_tile, 0)
    lax.fori_loop(0, groups - 1, col_tile(lowu, u_own, u_send), 0)
    ar2.wait()
    sum_ref[half_rows(low), :] = (mid[...].astype(jnp.float32) + in2[...].astype(jnp.float32)).astype(jnp.bfloat16)
    lax.fori_loop(groups - 1, groups, col_tile(lowu, u_own, u_send), 0)
    ar3 = send(sum_ref.at[half_rows(low), :], sum_ref.at[half_rows(low), :], ar, 2, "tensor", core)
    for q in range(groups):
        to_pair[q].wait()
        g_sum[q] = (g_own[q].astype(jnp.float32) + g_in[q].astype(jnp.float32)).astype(jnp.bfloat16)
    ar3.wait()

def wgrad(own_n, all_n, own_g, part_g, rest_g, gate_t, up_t, down, back, n_dp, n_tensor):
    rows, width = own_n.shape
    share = gate_t.shape[0]
    groups = n_dp // PAIR
    anyspec = pl.BlockSpec(memory_space=pl.ANY)
    vm = pl.BlockSpec(memory_space=pltpu.VMEM)
    bf, f32 = jnp.bfloat16, jnp.float32
    sd = jax.ShapeDtypeStruct
    dcols = width // n_dp
    V = pltpu.VMEM
    tall = groups * rows
    return pl.pallas_call(
        functools.partial(wgrad_kernel, n_dp, n_tensor),
        out_shape=(sd((share // PAIR, width), bf), sd((share // PAIR, width), bf), sd((groups, share, dcols), bf),
                   sd((groups, share, dcols), bf), sd((groups, share, dcols), bf), sd((rows, width), bf)),
        in_specs=[anyspec] * 9, out_specs=(vm,) * 6,
        scratch_shapes=[*[V((groups, share, dcols), bf)] * 3, V((tall, width), bf), V((tall, width), bf),
                        V((share, width), bf), V((share, width), bf), V((share, width), bf),
                        V((share, tall), bf), V((share, tall), bf), V((share, tall), bf),
                        *[V((rows // 2, width), bf)] * 4,
                        pltpu.SemaphoreType.DMA((6 + (groups - 1) * (1 + n_tensor),)),
                        pltpu.SemaphoreType.DMA((2, 3 * groups)), pltpu.SemaphoreType.DMA((2, 3)), pltpu.SemaphoreType.DMA((2, groups))],
        compiler_params=pltpu.CompilerParams(collective_id=3, has_side_effects=True, vmem_limit_bytes=62 << 20),
        cost_estimate=pl.CostEstimate(flops=12 * tall * width * share, bytes_accessed=2 * (3 * width * share + 4 * tall * width), transcendentals=tall * share),
        name="weight_gradients",
    )(own_n, all_n, own_g, part_g, rest_g, gate_t, up_t, down, back)
TILE = 128
CHUNK = 256

def turn(values, cosine, sine):
    lane = lax.broadcasted_iota(jnp.int32, values.shape, 1)
    swapped = jnp.where(lane % HEAD_SIZE < HEAD_SIZE // 2,
                        pltpu.roll(values, 128 - HEAD_SIZE // 2, 1), pltpu.roll(values, HEAD_SIZE // 2, 1))
    return values * cosine + swapped * sine

def place(values, head, side):
    v = values if head == side else pltpu.roll(values, HEAD_SIZE, 1)
    lane = lax.broadcasted_iota(jnp.int32, values.shape, 1)
    return jnp.where(lane // HEAD_SIZE == side, v, jnp.zeros_like(v))

def column_of(row):
    a = lax.broadcasted_iota(jnp.int32, (128, 128), 0)
    b = lax.broadcasted_iota(jnp.int32, (128, 128), 1)
    return jnp.sum(jnp.where(a == b, row.astype(jnp.float32), 0.0), axis=1, keepdims=True)

def bias_of(ids_col, ids_row, row0, col0, shape, window):
    q = lax.broadcasted_iota(jnp.int32, shape, 0) + row0
    k = lax.broadcasted_iota(jnp.int32, shape, 1) + col0
    return jnp.where((ids_col == ids_row) & (k <= q), 0.0, -1e30)

def attention_kernel(n_dp, n_tensor, x_hbm, gain1, wq_hbm, wk_hbm, wv_hbm, wo_hbm, gain2, cos_ref, sin_ref, ids_row, g_hbm, gate_hbm, up_hbm,
                     normed_ref, q_ref, kv_ref, idrow_ref, mixed_ref, res_ref, normed2_ref, gate_t, up_t, part_g,
                     x, wq, wk, wv, wo, raw_gate, raw_up, kvar, vvar, tile32, partial, out1, in1, mid, in2, total, load, far, halo, ar):
    rows, width = x.shape
    groups = n_dp // PAIR
    me_dp, me_t = lax.axis_index("dp"), lax.axis_index("tensor")
    right = lax.rem(me_dp + PAIR, n_dp)
    left = lax.rem(me_dp + n_dp - PAIR, n_dp)
    after = lax.rem(me_dp + 1, n_dp)
    before = lax.rem(me_dp + n_dp - 1, n_dp)
    core, across = flip(me_t, 1), flip(me_t, 2)
    piece = rows // n_tensor
    def part(t):
        return pl.ds(pl.multiple_of(t * piece, piece), piece)
    count = [0]
    def cp(s, d):
        c = pltpu.make_async_copy(s, d, load.at[count[0]]); count[0] += 1
        c.start(); return c
    share = raw_gate.shape[1]
    w_x = cp(x_hbm, x); w_k = cp(wk_hbm, wk); w_v = cp(wv_hbm, wv); w_q = cp(wq_hbm, wq); w_o = cp(wo_hbm, wo)
    mine = pl.ds(pl.multiple_of(me_dp // PAIR * share, share), share)
    w_gate = cp(gate_hbm.at[:, mine], raw_gate); w_up = cp(up_hbm.at[:, mine], raw_up)
    meet(("dp", after), ("dp", before), ("dp", right), ("dp", left), ("tensor", core), ("tensor", across))
    def first_part(j):
        first = pl.ds(pl.multiple_of(me_t * piece + j * (piece // 2), piece // 2), piece // 2)
        return send(g_hbm.at[first, :], part_g.at[0].at[pl.ds(j * (piece // 2), piece // 2), :], far, j, "dp", right)
    ring0 = first_part(0)
    ids_go = send(ids_row, idrow_ref.at[0], halo, 0, "dp", after)
    idrow_ref[1] = ids_row[...]

    w_x.wait()
    def norm_one(i, _):
        r = pl.ds(pl.multiple_of(i * TILE, TILE), TILE)
        v = x[r, :].astype(jnp.float32)
        root = lax.rsqrt(jnp.mean(v * v, axis=1, keepdims=True) + EPS)
        normed_ref[r, :] = (v * root * gain1[...]).astype(jnp.bfloat16)
        return 0
    lax.fori_loop(0, rows // TILE, norm_one, 0)
    w_k.wait(); w_v.wait()
    own = pl.ds(rows, rows)
    kv_ref[1, :, 0:128] = turn(nn(normed_ref[...], wk[...]), cos_ref[...], sin_ref[...]).astype(jnp.bfloat16)
    kv_ref[1, :, 128:256] = nn(normed_ref[...], wv[...]).astype(jnp.bfloat16)
    w_q.wait()
    pairs = wq.shape[1] // 128
    def q_pair(p, _):
        c = pl.ds(pl.multiple_of(p * 256, 256), 256)
        raw = nn(normed_ref[...], wq[:, c])
        for s in range(2):
            d = pl.ds(pl.multiple_of(p * 256 + s * 128, 128), 128)
            q_ref[:, d] = (turn(raw[:, s * 128:(s + 1) * 128], cos_ref[...], sin_ref[...]).astype(jnp.bfloat16) * HEAD_SIZE ** -0.5).astype(jnp.bfloat16)
        return 0
    kv_go = send(kv_ref.at[1], kv_ref.at[0], halo, 1, "dp", after)
    lax.fori_loop(0, pairs // 2, q_pair, 0)
    def variants(side_rows, b):
        for g in range(2):
            for s in range(2):
                kvar[g, s, side_rows, :] = place(kv_ref[b, :, 0:128], g, s)
                vvar[g, s, side_rows, :] = place(kv_ref[b, :, 128:256], g, s)
    variants(own, 1)
    ids_go.wait(); kv_go.wait()
    ring1 = first_part(1)
    variants(pl.ds(0, rows), 0)
    w_o.wait()

    window = rows + TILE
    def attend(i):
        r = pl.ds(i * TILE, TILE)
        k = pl.ds(i * TILE, window)
        ids_k = jnp.concatenate([idrow_ref[0], idrow_ref[1]], axis=1)[:, i * TILE:i * TILE + window]
        bias = bias_of(column_of(idrow_ref[1][:, i * TILE:(i + 1) * TILE]), ids_k.astype(jnp.float32), rows, 0, (TILE, window), window)
        bias = jnp.concatenate([bias, bias], axis=0)
        for g in range(2):
            q2 = jnp.concatenate([q_ref[r, (2 * g) * 128:(2 * g + 1) * 128], q_ref[r, (2 * g + 1) * 128:(2 * g + 2) * 128]], axis=0)
            mixed = None
            for s in range(2):
                score = nt(q2, kvar[g, s, k, :]) + bias
                peak = jnp.max(score, axis=1, keepdims=True)
                e = jnp.exp(score - peak)
                l = jnp.sum(e, axis=1, keepdims=True)
                prob = (e * (1.0 / l)).astype(jnp.bfloat16)
                m = nn(prob, vvar[g, s, k, :])
                mixed = m if mixed is None else mixed + m
            for b in range(2):
                mixed_ref[r, (2 * g + b) * 128:(2 * g + b + 1) * 128] = mixed[b * TILE:(b + 1) * TILE, :].astype(jnp.bfloat16)

    hrow = CHUNK // 2
    low = lax.rem(me_t, 2)
    def own_rows(c):
        return pl.ds(pl.multiple_of(c * CHUNK + low * hrow, hrow), hrow)
    def oth_rows(c):
        return pl.ds(pl.multiple_of(c * CHUNK + (1 - low) * hrow, hrow), hrow)
    def project(c):
        r = pl.ds(c * CHUNK, CHUNK)
        def body(j, _):
            d = pl.ds(pl.multiple_of(j * 512, 512), 512)
            tile32[...] = nn(mixed_ref[r, :], wo[:, d])
            out1[c, :, d] = tile32[pl.ds(pl.multiple_of((1 - low) * hrow, hrow), hrow), :].astype(jnp.bfloat16)
            partial[c, :, d] = tile32[pl.ds(pl.multiple_of(low * hrow, hrow), hrow), :]
            return 0
        lax.fori_loop(0, width // 512, body, 0)
    def step1(c):
        return send(out1.at[c], in1.at[c], ar, 3 * c, "tensor", core)
    def step2(c):
        mid[c] = (partial[c] + in1[c].astype(jnp.float32)).astype(jnp.bfloat16)
        return send(mid.at[c], in2.at[c], ar, 3 * c + 1, "tensor", across)
    def step3(c):
        total[own_rows(c), :] = (mid[c].astype(jnp.float32) + in2[c].astype(jnp.float32)).astype(jnp.bfloat16)
        return send(total.at[own_rows(c), :], total.at[own_rows(c), :], ar, 3 * c + 2, "tensor", core)
    def finish(r):
        v = x[r, :].astype(jnp.float32) + total[r, :].astype(jnp.float32)
        res_ref[r, :] = v
        root = lax.rsqrt(jnp.mean(v * v, axis=1, keepdims=True) + EPS)
        normed2_ref[r, :] = (v * root * gain2[...]).astype(jnp.bfloat16)

    chunks = rows // CHUNK
    per = CHUNK // TILE
    flights = {}
    steps = groups - 1
    def ring(s):
        return send(part_g.at[s - 2], part_g.at[s - 1], far, s, "dp", right)
    for i in range(rows // TILE):
        attend(i)
        c = i // per
        if i % per == per - 1:
            project(c)
            flights[1, c] = step1(c)
        elif c > 0:
            flights[1, c - 1].wait()
            flights[2, c - 1] = step2(c - 1)
        if i == 1:
            ring0.wait()
            ring1.wait()
            turn_on = ring(2) if steps > 1 else None
    c = chunks - 1
    def transpose_into(dst, raw):
        def body(j, _):
            r = pl.ds(pl.multiple_of(j * 256, 256), 256)
            dst[:, r] = raw[r, :].T
            return 0
        lax.fori_loop(0, width // 256, body, 0)
    flights[1, c].wait()
    flights[2, c] = step2(c)
    w_gate.wait()
    transpose_into(gate_t, raw_gate)
    for s in range(3, steps + 1):
        turn_on.wait()
        turn_on = ring(s)
    for c in range(chunks - 1):
        flights[2, c].wait()
        flights[3, c] = step3(c)
        finish(own_rows(c))
    w_up.wait()
    transpose_into(up_t, raw_up)
    for c in range(chunks - 1):
        flights[3, c].wait()
        finish(oth_rows(c))
    c = chunks - 1
    flights[2, c].wait()
    flights[3, c] = step3(c)
    finish(own_rows(c))
    flights[3, c].wait()
    finish(oth_rows(c))
    if turn_on is not None:
        turn_on.wait()

def attend_forward(x, gain1, wq, wk, wv, wo, gain2, cosine, sine, ids, grad_output, w_gate, w_up, n_dp, n_tensor):
    rows, width = x.shape
    groups = n_dp // PAIR
    anyspec = pl.BlockSpec(memory_space=pl.ANY)
    vm = pl.BlockSpec(memory_space=pltpu.VMEM)
    bf, f32 = jnp.bfloat16, jnp.float32
    sd = jax.ShapeDtypeStruct
    V = pltpu.VMEM
    piece = rows // n_tensor
    chunks = rows // CHUNK
    qc = wq.shape[1]
    share = w_gate.shape[1] // groups
    D = pltpu.SemaphoreType.DMA
    return pl.pallas_call(
        functools.partial(attention_kernel, n_dp, n_tensor),
        out_shape=(sd((rows, width), bf), sd((rows, qc), bf), sd((2, rows, 256), bf), sd((2, 1, rows), jnp.int32),
                   sd((rows, qc), bf), sd((rows, width), f32), sd((rows, width), bf), sd((share, width), bf), sd((share, width), bf),
                   sd((groups - 1, piece, width), bf)),
        in_specs=[anyspec, vm, anyspec, anyspec, anyspec, anyspec, vm, vm, vm, vm, anyspec, anyspec, anyspec],
        out_specs=(vm,) * 9 + (anyspec,),
        scratch_shapes=[V((rows, width), bf), V((width, qc), bf), V((width, 128), bf), V((width, 128), bf), V((qc, width), bf), V((width, share), bf), V((width, share), bf),
                        V((2, 2, 2 * rows, 128), bf), V((2, 2, 2 * rows, 128), bf), V((CHUNK, 512), f32),
                        V((chunks, CHUNK // 2, width), f32), V((chunks, CHUNK // 2, width), bf), V((chunks, CHUNK // 2, width), bf),
                        V((chunks, CHUNK // 2, width), bf), V((chunks, CHUNK // 2, width), bf), V((rows, width), bf),
                        D((7,)), D((2, groups + 2)), D((2, 2)), D((2, 3 * chunks))],
        compiler_params=pltpu.CompilerParams(collective_id=1, has_side_effects=True, vmem_limit_bytes=60 << 20),
        cost_estimate=pl.CostEstimate(flops=2 * rows * width * (2 * qc + 256) + 16 * rows * rows * 5 * 128, bytes_accessed=2 * (width * (2 * qc + 256) + 6 * rows * width), transcendentals=8 * rows * rows),
        name="attention_forward",
    )(x, gain1.reshape(1, width), wq, wk, wv, wo, gain2.reshape(1, width), cosine, sine, ids.reshape(1, rows), grad_output, w_gate, w_up)

def backward_kernel(n_dp, n_tensor, gn_hbm, res_hbm, x_hbm, go_hbm, mlp_hbm, normed_hbm, wo_hbm, wq_hbm, wk_hbm, wv_hbm,
                    g_sum, u_own_hbm, u_send, d_send, mixed_hbm, q_hbm, kv_hbm, gain1, gain2, gain2_part, id_rows, ids_row, cos_ref, sin_ref,
                    out_hbm, gin_hbm, gz, uz, d_in, wz, qz, gains_ref,
                    gn, res, go, normed, wo, wq, wk, wv, mixed, q_ref, kv_ref, resid, low_res, gm, kvar, vvar, kvart, dk, dv, ids_col,
                    low, lowt, tile32, wsend, wown, win, own_block, u_own, uyin, usum, qsend, qown, qin,
                    amine, amid, min1, min2, ain1, ain2, hprev, hin, gacc, gs, gown, gyi, gzi, gt, gti,
                    load, sy, sz, sx, sh, sg):
    rows, width = go.shape
    groups = n_dp // PAIR
    me_dp, me_t = lax.axis_index("dp"), lax.axis_index("tensor")
    group, member = me_dp // PAIR, lax.rem(me_dp, PAIR)
    pair = flip(me_dp, 1)
    after = lax.rem(me_dp + 1, n_dp)
    before = lax.rem(me_dp + n_dp - 1, n_dp)
    core, across = flip(me_t, 1), flip(me_t, 2)
    low_t = lax.rem(me_t, 2)
    def at_group(s):
        return lax.rem(group + s, groups)
    def from_group(s):
        return lax.rem(group + groups - s, groups)
    f32, bf = jnp.float32, jnp.bfloat16
    qc = wq.shape[1]
    dcols = width // n_dp
    half = rows // 2
    def rows_of(start, size):
        return pl.ds(pl.multiple_of(start, size), size)
    def half_rows(c):
        return rows_of(c * half, half)
    def cp(s, d, i):
        c = pltpu.make_async_copy(s, d, load.at[i])
        c.start()
        return c
    w_gn = cp(gn_hbm, gn, 0); w_res = cp(res_hbm, res, 1); w_go = cp(go_hbm, go, 2)
    w_wo = cp(wo_hbm, wo, 3); w_mlp = cp(mlp_hbm.at[half_rows(low_t), :], amine, 4)
    w_kv = cp(kv_hbm, kv_ref, 5); w_mx = cp(mixed_hbm, mixed, 6); w_qr = cp(q_hbm, q_ref, 7)
    w_own = cp(u_own_hbm, u_own, 8); w_nm = cp(normed_hbm, normed, 9)
    w_q = cp(wq_hbm, wq, 10); w_k = cp(wk_hbm, wk, 11); w_v = cp(wv_hbm, wv, 12)
    meet(("dp", pair), ("dp", after), ("dp", before), ("tensor", core), ("tensor", across),
         *[("dp", at_group(s) * PAIR + member) for s in range(1, groups)])
    def exchange(src, dst, base):
        return [send(src.at[at_group(s)], dst.at[group], sz, base + s - 1, "dp", at_group(s) * PAIR + member) for s in range(1, groups)]
    y_u = send(u_send, uyin, sy, 0, "dp", pair)
    z_g = exchange(g_sum, gz, 0)
    cp(g_sum.at[group], own_block, 13).wait()
    w_g = cp(own_block, gz.at[group], 13)
    m1 = send(mlp_hbm.at[half_rows(1 - low_t), :], min1, sx, 0, "tensor", core)

    w_gn.wait(); w_res.wait(); w_go.wait()
    NR = 64
    def norm_two(i, _):
        r = rows_of(i * NR, NR)
        v = res[r, :]
        root = lax.rsqrt(jnp.mean(v * v, axis=1, keepdims=True) + EPS)
        up = gn[r, :].astype(f32) * gain2[...]
        mean = jnp.mean(up * v, axis=1, keepdims=True)
        d = go[r, :].astype(f32) + root * up - v * (root * root * root * mean)
        resid[r, :] = d
        low_res[r, :] = d.astype(bf)
        return 0
    lax.fori_loop(0, rows // NR, norm_two, 0)
    w_wo.wait()
    def mix_tile(i, _):
        r = rows_of(i * half, half)
        gm[r, :] = nt(low_res[r, :], wo[...]).astype(bf)
        return 0
    lax.fori_loop(0, 2, mix_tile, 0)
    w_mlp.wait(); m1.wait()
    amid[...] = (amine[...].astype(f32) + min1[...].astype(f32)).astype(bf)
    w_kv.wait()
    for g in range(2):
        for s in range(2):
            for b in range(2):
                kvar[g, s, pl.ds(b * rows, rows), :] = place(kv_ref[b, :, 0:128], g, s)
                vvar[g, s, pl.ds(b * rows, rows), :] = place(kv_ref[b, :, 128:256], g, s)
            kvart[g, s] = kvar[g, s].T
    dk[...] = jnp.zeros_like(dk)
    dv[...] = jnp.zeros_like(dv)
    m2 = send(amid, min2, sx, 1, "tensor", across)
    w_mx.wait()
    lowt[0:qc, :] = mixed[...].T
    hrow = qc // n_dp
    def wout_tile(j, _):
        c = rows_of(j * 256, 256)
        tile32[...] = nn(lowt[0:qc, :], low_res[:, c])
        for z in range(groups):
            wown[z, :, c] = tile32[rows_of((z * PAIR + member) * hrow, hrow), :].astype(bf)
            wsend[z, :, c] = tile32[rows_of((z * PAIR + 1 - member) * hrow, hrow), :].astype(bf)
        return 0
    lax.fori_loop(0, width // 256, wout_tile, 0)
    w_qr.wait()
    for b in range(2):
        for j in range(rows // 128):
            ids_col[b * rows + j * 128:b * rows + (j + 1) * 128, :] = column_of(id_rows[b][:, j * 128:(j + 1) * 128])
    window = rows + TILE
    def attend(i, _):
        r = rows_of(i * TILE, TILE)
        k = pl.ds(pl.multiple_of(i * TILE, TILE), window)
        kpos = lax.broadcasted_iota(jnp.int32, (window, TILE), 0)
        qpos = lax.broadcasted_iota(jnp.int32, (window, TILE), 1) + rows
        bias = jnp.where((ids_col[k, :] == ids_row[:, r].astype(f32)) & (kpos <= qpos), 0.0, -1e30)
        bias = jnp.concatenate([bias, bias], axis=1)
        for g in range(2):
            q2 = jnp.concatenate([q_ref[r, (2 * g) * 128:(2 * g + 1) * 128], q_ref[r, (2 * g + 1) * 128:(2 * g + 2) * 128]], axis=0)
            do2 = jnp.concatenate([gm[r, (2 * g) * 128:(2 * g + 1) * 128], gm[r, (2 * g + 1) * 128:(2 * g + 2) * 128]], axis=0)
            dqt = None
            for s in range(2):
                st = nt(kvar[g, s, k, :], q2) + bias
                peak = jnp.max(st, axis=0, keepdims=True)
                e = jnp.exp(st - peak)
                pt = e * (1.0 / jnp.sum(e, axis=0, keepdims=True))
                dpt = nt(vvar[g, s, k, :], do2)
                delta = jnp.sum(pt * dpt, axis=0, keepdims=True)
                dst = (pt * (dpt - delta)).astype(bf)
                dv[g, s, k, :] += nn(pt.astype(bf), do2)
                dk[g, s, k, :] += nn(dst, q2)
                part = nn(kvart[g, s, :, k], dst)
                dqt = part if dqt is None else dqt + part
            d = dqt.T * HEAD_SIZE ** -0.5
            for b in range(2):
                low[r, (2 * g + b) * 128:(2 * g + b + 1) * 128] = turn(d[b * TILE:(b + 1) * TILE, :], cos_ref[r, :], -sin_ref[r, :]).astype(bf)
        return 0
    lax.fori_loop(0, rows // TILE // 2, attend, 0)
    y_u.wait()
    w_own.wait()
    for z in range(groups):
        usum[z] = (u_own[z].astype(f32) + uyin[z].astype(f32)).astype(bf)
    y_w = send(wsend, win, sy, 1, "dp", pair)
    w_u = cp(usum.at[group], uz.at[group], 8)
    z_u = exchange(usum, uz, groups)
    lax.fori_loop(rows // TILE // 2, rows // TILE, attend, 0)

    def gathered(acc, b):
        r = pl.ds(b * rows, rows)
        lane = lax.broadcasted_iota(jnp.int32, (rows, 128), 1)
        first = acc[0, 0, r, :] + pltpu.roll(acc[0, 1, r, :], HEAD_SIZE, 1)
        second = pltpu.roll(acc[1, 0, r, :], HEAD_SIZE, 1) + acc[1, 1, r, :]
        return jnp.where(lane < HEAD_SIZE, first, second)
    hprev[:, 0:128] = gathered(dk, 0).astype(bf)
    hprev[:, 128:256] = gathered(dv, 0).astype(bf)
    halo = send(hprev, hin, sh, 0, "dp", before)
    m2.wait()
    def out_rows(i, _):
        r = rows_of(low_t * half + i * NR, NR)
        m = rows_of(i * NR, NR)
        summed = (amid[m, :].astype(f32) + min2[m, :].astype(f32)).astype(bf)
        go[r, :] = (res[r, :] + summed.astype(f32)).astype(bf)
        return 0
    lax.fori_loop(0, half // NR, out_rows, 0)
    w_out = cp(go.at[half_rows(low_t), :], out_hbm.at[half_rows(low_t), :], 2)
    m3 = send(go.at[half_rows(low_t), :], out_hbm.at[half_rows(low_t), :], sx, 2, "tensor", core)
    lowt[0:qc, :] = low[:, 0:qc].T
    w_nm.wait()
    def grad_cols(row0, count):
        def body(z, _):
            a = rows_of((z * PAIR + member) * dcols, dcols)
            b = rows_of((z * PAIR + 1 - member) * dcols, dcols)
            t = lowt[row0:row0 + count, :]
            qsend[z, row0:row0 + count, :] = nn(t, normed[:, b]).astype(bf)
            qown[z, row0:row0 + count, :] = nn(t, normed[:, a]).astype(bf)
            return 0
        lax.fori_loop(0, groups, body, 0)
    grad_cols(0, qc)
    y_w.wait()
    y_q = [send(qsend.at[:, 0:qc, :], qin.at[:, 0:qc, :], sy, 2, "dp", pair)]
    for z in range(groups):
        wown[z] = (wown[z].astype(f32) + win[z].astype(f32)).astype(bf)
    w_w = cp(wown.at[group], wz.at[group], 3)
    halo.wait()
    kraw = gathered(dk, 1) + hin[:, 0:128].astype(f32)
    low[:, qc:qc + 128] = turn(kraw, cos_ref[...], -sin_ref[...]).astype(bf)
    low[:, qc + 128:qc + 256] = (gathered(dv, 1) + hin[:, 128:256].astype(f32)).astype(bf)
    z_w = exchange(wown, wz, 2 * groups)
    w_q.wait(); w_k.wait(); w_v.wait()
    def normed_part(j, _):
        c = rows_of(j * 256, 256)
        p = (nt(low[:, 0:qc], wq[c, :]) + nt(low[:, qc:qc + 128], wk[c, :]) + nt(low[:, qc + 128:qc + 256], wv[c, :]))
        res[:, c] = p
        gacc[0:1, c] = jnp.sum(p * normed[:, c].astype(f32), axis=0, keepdims=True) / gain1[0:1, c]
        gacc[1:2, c] = gain2_part[0:1, c] / gain2[0:1, c]
        return 0
    lax.fori_loop(0, width // 256, normed_part, 0)
    hchunk = CHUNK // 2
    chunks = rows // CHUNK
    def own_rows(c):
        return rows_of(c * CHUNK + low_t * hchunk, hchunk)
    def oth_rows(c):
        return rows_of(c * CHUNK + (1 - low_t) * hchunk, hchunk)
    def buf(c):
        return pl.ds(c * hchunk, hchunk)
    flights = {}
    for c in range(chunks):
        amine[buf(c), :] = res[oth_rows(c), :].astype(bf)
        flights[1, c] = send(amine.at[buf(c), :], ain1.at[buf(c), :], sx, 3 + 3 * c, "tensor", core)
    for z in range(groups):
        for m in range(PAIR):
            d0 = (z * PAIR + m) * dcols
            gs[m, z, 0:2, :] = gacc[0:2, d0:d0 + dcols]
    gown[...] = gs[member]
    y_gain = send(gs.at[1 - member], gyi, sg, 0, "dp", pair)
    lowt[qc:qc + 256, :] = low[:, qc:qc + 256].T
    grad_cols(qc, 256)
    y_q.append(send(qsend.at[:, qc:qc + 256, :], qin.at[:, qc:qc + 256, :], sy, 3, "dp", pair))
    y_d = send(d_send, d_in, sy, 4, "dp", pair)
    for c in range(chunks):
        flights[1, c].wait()
        amid[buf(c), :] = (res[own_rows(c), :] + ain1[buf(c), :].astype(f32)).astype(bf)
        flights[2, c] = send(amid.at[buf(c), :], ain2.at[buf(c), :], sx, 4 + 3 * c, "tensor", across)
    y_gain.wait()
    gown[...] = gown[...] + gyi[...]
    w_x = cp(x_hbm, normed, 9)
    z_gain = [send(gown.at[at_group(s)], gzi.at[s - 1], sg, s, "dp", at_group(s) * PAIR + member) for s in range(1, groups)]
    w_x.wait()
    def norm_one(r):
        v = normed[r, :].astype(f32)
        root = lax.rsqrt(jnp.mean(v * v, axis=1, keepdims=True) + EPS)
        up = gn[r, :].astype(f32) * gain1[...]
        mean = jnp.mean(up * v, axis=1, keepdims=True)
        low_res[r, :] = (resid[r, :] + root * up - v * (root * root * root * mean)).astype(bf)
    for c in range(chunks):
        flights[2, c].wait()
        gn[own_rows(c), :] = (amid[buf(c), :].astype(f32) + ain2[buf(c), :].astype(f32)).astype(bf)
        flights[3, c] = send(gn.at[own_rows(c), :], gn.at[own_rows(c), :], sx, 5 + 3 * c, "tensor", core)
        norm_one(own_rows(c))
        flights[3, c].wait()
        norm_one(oth_rows(c))
    w_gin = cp(low_res, gin_hbm, 1)
    for q in z_gain:
        q.wait()
    total = gown[group]
    for s in range(1, groups):
        total = total + gzi[s - 1]
    gt[0] = total
    t1 = send(gt.at[0], gti.at[0], sg, groups, "tensor", core)
    t1.wait()
    gt[1] = gt[0] + gti[0]
    t2 = send(gt.at[1], gti.at[1], sg, groups + 1, "tensor", across)
    t2.wait()
    gains_ref[...] = gt[1] + gti[1]
    w_q2 = []
    z_q = []
    for j, r in enumerate((slice(0, qc), slice(qc, qc + 256))):
        y_q[j].wait()
        for z in range(groups):
            qown[z, r, :] = (qown[z, r, :].astype(f32) + qin[z, r, :].astype(f32)).astype(bf)
        z_q = z_q + [send(qown.at[at_group(s), r, :], qz.at[group, r, :], sz, (3 + j) * groups + s - 1, "dp", at_group(s) * PAIR + member) for s in range(1, groups)]
        w_q2.append(cp(qown.at[group, r, :], qz.at[group, r, :], 14 + j))
    for q in z_g + z_u + z_w + z_q + [y_d, m3]:
        q.wait()
    for q in [w_g, w_u, w_w, w_gin, w_out] + w_q2:
        q.wait()

def backward(gn, residual, x, grad_output, mlp_part, normed, wo, wq, wk, wv, g_sum, u_own, u_send, d_send, mixed, q, kv, gain1, gain2, gain2_part,
             id_rows, ids_row, cosine, sine, n_dp, n_tensor):
    rows, width = x.shape
    groups = n_dp // PAIR
    share = g_sum.shape[1]
    dcols = width // n_dp
    qc = wq.shape[1]
    cols = qc + 256
    A = pl.BlockSpec(memory_space=pl.ANY)
    vm = pl.BlockSpec(memory_space=pltpu.VMEM)
    bf, f32 = jnp.bfloat16, jnp.float32
    sd = jax.ShapeDtypeStruct
    V = pltpu.VMEM
    D = pltpu.SemaphoreType.DMA
    half = rows // 2
    hrow = qc // n_dp
    act = V((rows, width), bf)
    return pl.pallas_call(
        functools.partial(backward_kernel, n_dp, n_tensor),
        out_shape=(sd((rows, width), bf), sd((rows, width), bf), sd((groups, share, dcols), bf), sd((groups, share, dcols), bf),
                   sd(d_send.shape, bf), sd((groups, hrow, width), bf), sd((groups, cols, dcols), bf), sd((8, dcols), f32)),
        in_specs=[A] * 17 + [vm] * 7,
        out_specs=(A,) * 7 + (vm,),
        scratch_shapes=[act, V((rows, width), f32), act, act, V((qc, width), bf), V((width, qc), bf), V((width, 128), bf), V((width, 128), bf),
                        V((rows, qc), bf), V((rows, qc), bf), V((2, rows, 256), bf), V((rows, width), f32), act, V((rows, qc), bf),
                        V((2, 2, 2 * rows, 128), bf), V((2, 2, 2 * rows, 128), bf), V((2, 2, 128, 2 * rows), bf),
                        V((2, 2, 2 * rows, 128), f32), V((2, 2, 2 * rows, 128), f32), V((2 * rows, 1), f32),
                        V((rows, cols), bf), V((cols, rows), bf), V((qc, 256), f32),
                        V((groups, hrow, width), bf), V((groups, hrow, width), bf), V((groups, hrow, width), bf),
                        V((share, dcols), bf), *[V((groups, share, dcols), bf)] * 3,
                        V((groups, cols, dcols), bf), V((groups, cols, dcols), bf), V((groups, cols, dcols), bf),
                        *[V((half, width), bf)] * 6,
                        V((rows, 256), bf), V((rows, 256), bf), V((8, width), f32), V((PAIR, groups, 8, dcols), f32), V((groups, 8, dcols), f32),
                        V((groups, 8, dcols), f32), V((groups - 1, 8, dcols), f32), V((2, 8, dcols), f32), V((2, 8, dcols), f32),
                        D((16,)), D((2, 5)), D((2, 5 * groups)), D((2, 3 + 3 * (rows // CHUNK))), D((2, 1)), D((2, groups + 2))],
        compiler_params=pltpu.CompilerParams(collective_id=4, has_side_effects=True, vmem_limit_bytes=67043328),
        cost_estimate=pl.CostEstimate(flops=4 * rows * width * (2 * qc + 256) + 40 * rows * rows * 5 * 128, bytes_accessed=40 * rows * width, transcendentals=8 * rows * rows),
        name="attention_backward",
    )(gn, residual, x, grad_output, mlp_part, normed, wo, wq, wk, wv, g_sum, u_own, u_send, d_send, mixed, q, kv,
      gain1.reshape(1, width), gain2.reshape(1, width), gain2_part, id_rows, ids_row, cosine, sine)

def finish_kernel(qc, kc, out_hbm, gin_hbm, gz_hbm, uz_hbm, d_own_hbm, d_in_hbm, wz_hbm, qz_hbm,
                  out_o, gin_o, gate_o, up_o, down_o, wout_o, query_o, key_o, value_o,
                  act1, act2, gz, uz, d_own, d_in, wz, qz, gate, up, down, wout, query, key, value, ins, outs):
    f32 = jnp.float32
    groups, share, dcols = gz.shape
    loads = [pltpu.make_async_copy(s, d, ins.at[i]) for i, (s, d) in enumerate([
        (gz_hbm, gz), (uz_hbm, uz), (out_hbm, act1), (gin_hbm, act2), (d_own_hbm, d_own), (d_in_hbm, d_in), (wz_hbm, wz), (qz_hbm, qz)])]
    for c in loads:
        c.start()
    stores = []
    def store(src, dst):
        c = pltpu.make_async_copy(src, dst, outs.at[len(stores)])
        c.start()
        stores.append(c)
    for got, held, dst, i in ((gz, gate, gate_o, 0), (uz, up, up_o, 1)):
        loads[i].wait()
        for z in range(groups):
            for h in range(share // 256):
                held[:, z * share + h * 256:z * share + (h + 1) * 256] = got[z, h * 256:(h + 1) * 256, :].astype(f32).T
        store(held, dst)
    loads[2].wait()
    store(act1, out_o)
    loads[3].wait()
    store(act2, gin_o)
    loads[4].wait()
    loads[5].wait()
    down[...] = d_own[...].astype(f32) + d_in[...].astype(f32)
    store(down, down_o)
    loads[6].wait()
    acc = wz[0].astype(f32)
    for z in range(1, groups):
        acc = acc + wz[z].astype(f32)
    wout[...] = acc
    store(wout, wout_o)
    loads[7].wait()
    def total(r0, r1):
        acc = qz[0, r0:r1, :].astype(f32)
        for z in range(1, groups):
            acc = acc + qz[z, r0:r1, :].astype(f32)
        return acc.T
    for h in range(qc // 256):
        query[:, h * 256:(h + 1) * 256] = total(h * 256, (h + 1) * 256)
    key[...] = total(qc, qc + kc)
    value[...] = total(qc + kc, qc + 2 * kc)
    store(query, query_o)
    store(key, key_o)
    store(value, value_o)
    for c in stores:
        c.wait()

def finish_all(out, gin, gz, uz, d_own, d_in, wz, qz, qc, kc):
    A = pl.BlockSpec(memory_space=pl.ANY)
    bf, f32 = jnp.bfloat16, jnp.float32
    sd = jax.ShapeDtypeStruct
    V = pltpu.VMEM
    groups, share, dcols = gz.shape
    shapes = [(dcols, groups * share), (dcols, groups * share), d_own.shape, wz.shape[1:], (dcols, qc), (dcols, kc), (dcols, kc)]
    return pl.pallas_call(
        functools.partial(finish_kernel, qc, kc),
        out_shape=(sd(out.shape, bf), sd(gin.shape, bf)) + tuple(sd(s, f32) for s in shapes),
        in_specs=[A] * 8, out_specs=(A,) * 9,
        scratch_shapes=[V(a.shape, bf) for a in (out, gin, gz, uz, d_own, d_in, wz, qz)] + [V(s, f32) for s in shapes] + [pltpu.SemaphoreType.DMA((8,)), pltpu.SemaphoreType.DMA((9,))],
        compiler_params=pltpu.CompilerParams(vmem_limit_bytes=48 << 20),
        cost_estimate=pl.CostEstimate(flops=8 * out.size, bytes_accessed=24 << 20, transcendentals=0),
        name="finish",
    )(out, gin, gz, uz, d_own, d_in, wz, qz)


def rope_table(half_count):
    adjusted = []
    for index in range(half_count):
        base_value = 500000.0 ** (-index / half_count)
        wave_length = 2.0 * math.pi / base_value
        smooth = (8192.0 / wave_length - 1.0) / 3.0
        if wave_length > 8192.0:
            adjusted.append(base_value / 32.0)
        elif wave_length >= 2048.0:
            adjusted.append((1.0 - smooth) * base_value / 32.0 + smooth * base_value)
        else:
            adjusted.append(base_value)
    return jnp.asarray(adjusted, dtype=jnp.float32)


def rope_angles(start_row, count_rows, half_count):
    positions = (start_row + jnp.arange(count_rows, dtype=jnp.int32)).astype(jnp.float32)
    phase_angle = positions[:, None] * rope_table(half_count)[None, :]
    return (jnp.cos(phase_angle)[:, None, :], jnp.sin(phase_angle)[:, None, :])


def rotate_halves(values, cosine_table, sine_values):
    half_size = values.shape[-1] // 2
    first_half = values[..., :half_size]
    second_half = values[..., half_size:]
    return jnp.concatenate(
        [
            first_half * cosine_table - second_half * sine_values,
            second_half * cosine_table + first_half * sine_values,
        ],
        axis=-1,
    )


def norm_rows(values, gain_row):
    inverse_root = lax.rsqrt(jnp.mean(values * values, axis=-1, keepdims=True) + NORM_EPSILON)
    return (inverse_root, values * inverse_root * gain_row)


def norm_back(values, inverse_root, gain_row, upstream):
    scaled = gain_row * upstream
    return inverse_root * scaled - values * inverse_root**3 * jnp.mean(
        scaled * values, axis=-1, keepdims=True
    )


def passed_along(block, axis, distance):
    devices = range(lax.axis_size(axis))
    route = [(i - distance, i) for i in devices if i - distance in devices]
    return lax.ppermute(block, axis, route)


def tensor_swap(block, bit):
    return lax.ppermute(block, "tensor", [(i, i ^ bit) for i in range(lax.axis_size("tensor"))])


def pair_swap(block):
    return lax.ppermute(block, "dp", [(i, i ^ 1) for i in range(lax.axis_size("dp"))])


def group_shift(block, distance):
    count = lax.axis_size("dp")
    groups = count // PAIR
    return lax.ppermute(
        block,
        "dp",
        [(i, ((i // PAIR + distance) % groups) * PAIR + i % PAIR) for i in range(count)],
    )


def tensor_sum(part):
    half = part.shape[1] // 2
    low = lax.axis_index("tensor") % 2
    first, second = part[:, :half], part[:, half:]
    mine = jnp.where(low == 0, first, second)
    other = jnp.where(low == 0, second, first).astype(jnp.bfloat16)
    mine = mine + tensor_swap(other, 1).astype(jnp.float32)
    bit = 2
    while bit < lax.axis_size("tensor"):
        rounded = mine.astype(jnp.bfloat16)
        mine = rounded.astype(jnp.float32) + tensor_swap(rounded, bit).astype(jnp.float32)
        bit *= 2
    mine = mine.astype(jnp.bfloat16)
    other = tensor_swap(mine, 1)
    return jnp.concatenate(
        [jnp.where(low == 0, mine, other), jnp.where(low == 0, other, mine)], axis=1
    ).astype(jnp.float32)


def gather_groups(block):
    half = block.shape[1] // 2
    low = lax.axis_index("tensor") % 2
    piece = lax.dynamic_slice_in_dim(block, low * half, half, axis=1)
    rows = [block]
    for _ in range(lax.axis_size("dp") // PAIR - 1):
        piece = group_shift(piece, 1)
        other = tensor_swap(piece, 1)
        rows.append(
            jnp.concatenate(
                [jnp.where(low == 0, piece, other), jnp.where(low == 0, other, piece)], axis=1
            )
        )
    return jnp.concatenate(rows, axis=0)


def pair_sum(part):
    member = lax.axis_index("dp") % PAIR
    mine = lax.dynamic_index_in_dim(part, member, 1, keepdims=False)
    other = lax.dynamic_index_in_dim(part, 1 - member, 1, keepdims=False)
    return mine + pair_swap(other.astype(jnp.bfloat16)).astype(jnp.float32)


def group_exchange(blocks):
    groups = blocks.shape[0]
    group = lax.axis_index("dp") // PAIR
    received = []
    for distance in range(groups):
        block = lax.dynamic_index_in_dim(blocks, (group + distance) % groups, 0, keepdims=False)
        received.append(block if distance == 0 else group_shift(block, distance))
    return received


def scatter_sum(part):
    summed = pair_sum(part)
    groups = summed.shape[0]
    group = lax.axis_index("dp") // PAIR
    total = lax.dynamic_index_in_dim(summed, group, 0, keepdims=False)
    rounded = summed.astype(jnp.bfloat16)
    for block in group_exchange(rounded)[1:]:
        total = total + block.astype(jnp.float32)
    return total


def block_scores(query_rows, key_rows, query_ids, key_ids, query_pos, key_pos):
    scores = jnp.einsum(
        "qgrd,kgd->grqk", query_rows, key_rows, preferred_element_type=jnp.float32
    ) * HEAD_SIZE ** (-0.5)
    allowed = (query_ids[:, None] == key_ids[None, :]) & (key_pos[None, :] <= query_pos[:, None])
    return jnp.where(allowed, scores, -1e30)


def block_forward(query_rows, key_rows, value_rows, query_ids, key_ids, query_pos, key_pos):
    scores = block_scores(query_rows, key_rows, query_ids, key_ids, query_pos, key_pos)
    row_peak = jnp.max(scores, axis=-1, keepdims=True)
    logsum = row_peak + jnp.log(jnp.sum(jnp.exp(scores - row_peak), axis=-1, keepdims=True))
    prob_low = jnp.exp(scores - logsum).astype(jnp.bfloat16)
    mixed_rows = jnp.einsum(
        "grqk,kgd->qgrd", prob_low, value_rows, preferred_element_type=jnp.float32
    )
    return (mixed_rows.astype(jnp.bfloat16), logsum)


def block_backward(
    query_rows,
    key_rows,
    value_rows,
    out_rows,
    grad_rows,
    logsum,
    query_ids,
    key_ids,
    query_pos,
    key_pos,
):
    scores = block_scores(query_rows, key_rows, query_ids, key_ids, query_pos, key_pos)
    prob_rows = jnp.exp(scores - logsum)
    grad_vals = jnp.einsum(
        "grqk,qgrd->kgd",
        prob_rows.astype(jnp.bfloat16),
        grad_rows,
        preferred_element_type=jnp.float32,
    )
    delta_rows = jnp.sum(out_rows.astype(jnp.float32) * grad_rows.astype(jnp.float32), axis=-1)
    grad_probs = jnp.einsum(
        "qgrd,kgd->grqk", grad_rows, value_rows, preferred_element_type=jnp.float32
    )
    grad_scores = (
        prob_rows * (grad_probs - jnp.transpose(delta_rows, (1, 2, 0))[..., None])
    ).astype(jnp.bfloat16)
    grad_query_rows = jnp.einsum(
        "grqk,kgd->qgrd", grad_scores, key_rows, preferred_element_type=jnp.float32
    ) * HEAD_SIZE ** (-0.5)
    grad_key_rows = jnp.einsum(
        "grqk,qgrd->kgd", grad_scores, query_rows, preferred_element_type=jnp.float32
    ) * HEAD_SIZE ** (-0.5)
    return (grad_query_rows, grad_key_rows, grad_vals)


def dot(form, left, right):
    return jnp.einsum(form, left, right, preferred_element_type=jnp.float32)


def gated(gate_value, up_value):
    return (jax.nn.silu(gate_value) * up_value).astype(jnp.bfloat16)


def gated_back(grad_hidden, gate_value, up_value):
    sigmoid_gate = jax.nn.sigmoid(gate_value)
    grad_gate_low = (
        grad_hidden * up_value * sigmoid_gate * (1.0 + gate_value * (1.0 - sigmoid_gate))
    ).astype(jnp.bfloat16)
    return grad_gate_low, (grad_hidden * jax.nn.silu(gate_value)).astype(jnp.bfloat16)


def shards_plain(
    inputs,
    norm1_gain,
    query_weight,
    key_weight,
    value_weight,
    w_out,
    norm2_gain,
    w_gate,
    w_up,
    w_down,
    doc_ids,
    grad_output,
):
    tok_rows, width = inputs.shape
    heads_here = query_weight.shape[1] // HEAD_SIZE
    kv_here = key_weight.shape[1] // HEAD_SIZE
    group_size = heads_here // kv_here
    n_dp = lax.axis_size("dp")
    groups = n_dp // PAIR
    group = lax.axis_index("dp") // PAIR
    offset = lax.axis_index("dp") * tok_rows
    grad_all = gather_groups(grad_output)

    cosine_table, sine_values = rope_angles(offset, tok_rows, HEAD_SIZE // 2)
    inputs_wide = inputs.astype(jnp.float32)
    root_one, normed = norm_rows(inputs_wide, norm1_gain)
    normed_low = normed.astype(jnp.bfloat16)
    query_raw = dot("td,dh->th", normed_low, query_weight).reshape(tok_rows, heads_here, HEAD_SIZE)
    key_raw = dot("td,dh->th", normed_low, key_weight).reshape(tok_rows, kv_here, HEAD_SIZE)
    value_low = dot("td,dh->th", normed_low, value_weight).astype(jnp.bfloat16)
    query_low = (
        rotate_halves(query_raw, cosine_table, sine_values)
        .astype(jnp.bfloat16)
        .reshape(tok_rows, kv_here, group_size, HEAD_SIZE)
    )
    key_low = (
        rotate_halves(key_raw, cosine_table, sine_values)
        .astype(jnp.bfloat16)
        .reshape(tok_rows, kv_here * HEAD_SIZE)
    )
    query_ids = doc_ids + 1
    tail = jnp.concatenate([key_low, value_low], axis=1)
    prev_tail = passed_along(tail, "dp", 1)
    prev_ids = passed_along(query_ids, "dp", 1)
    both = jnp.concatenate([prev_tail, tail], axis=0)
    keys_all = both[:, : kv_here * HEAD_SIZE].reshape(2 * DOC_MAX, kv_here, HEAD_SIZE)
    values_all = both[:, kv_here * HEAD_SIZE :].reshape(2 * DOC_MAX, kv_here, HEAD_SIZE)
    ids_all = jnp.concatenate([prev_ids, query_ids])
    pos_all = offset - DOC_MAX + jnp.arange(tok_rows + DOC_MAX, dtype=jnp.int32)
    query_pos = pos_all[DOC_MAX:]
    mixed_block, logsum_block = block_forward(
        query_low, keys_all, values_all, query_ids, ids_all, query_pos, pos_all
    )
    mixed_low = mixed_block.reshape(tok_rows, heads_here * HEAD_SIZE)
    residual = inputs_wide + tensor_sum(dot("te,ed->td", mixed_low, w_out))

    root_two, normed_two = norm_rows(residual, norm2_gain)
    normed_two_low = normed_two.astype(jnp.bfloat16)
    normed_all = gather_groups(normed_two_low)
    gate_value = dot("td,df->tf", normed_two_low, w_gate)
    up_value = dot("td,df->tf", normed_two_low, w_up)
    grad_hidden = dot("td,fd->tf", grad_output, w_down)
    hidden_low = gated(gate_value, up_value)
    grad_gate_low, grad_up_low = gated_back(grad_hidden, gate_value, up_value)
    normed_two_part = dot("tf,df->td", grad_gate_low, w_gate) + dot("tf,df->td", grad_up_low, w_up)
    grad_normed_two = tensor_sum(normed_two_part)
    gain_two_part = jnp.sum(normed_two_part * residual * root_two, axis=0)
    output = (residual + tensor_sum(dot("tf,fd->td", hidden_low, w_down))).astype(jnp.bfloat16)

    share = w_gate.shape[1] // groups
    gate_share = lax.dynamic_slice_in_dim(w_gate, group * share, share, axis=1)
    up_share = lax.dynamic_slice_in_dim(w_up, group * share, share, axis=1)
    down_share = lax.dynamic_slice_in_dim(w_down, group * share, share, axis=0)
    gate_all = dot("td,df->tf", normed_all, gate_share)
    up_all = dot("td,df->tf", normed_all, up_share)
    grad_hidden_all = dot("td,fd->tf", grad_all, down_share)
    hidden_all = gated(gate_all, up_all)
    gate_low_all, up_low_all = gated_back(grad_hidden_all, gate_all, up_all)
    down_part = dot("tf,td->fd", hidden_all, grad_all)
    grad_wdown = pair_sum(down_part.reshape(1, PAIR, share // PAIR, width))[0]
    rows_here = width // n_dp

    def column_grad(low_all):
        part = dot("td,tf->df", normed_all, low_all)
        summed = pair_sum(part.reshape(groups, PAIR, rows_here, share)).astype(jnp.bfloat16)
        full = jnp.zeros((rows_here, groups * share), jnp.float32)
        for distance, block in enumerate(group_exchange(summed)):
            full = lax.dynamic_update_slice_in_dim(
                full, block.astype(jnp.float32), ((group - distance) % groups) * share, axis=1
            )
        return full

    grad_wgate = column_grad(gate_low_all)
    grad_wup = column_grad(up_low_all)

    grad_residual = grad_output.astype(jnp.float32) + norm_back(
        residual, root_two, norm2_gain, grad_normed_two
    )
    grad_res_low = grad_residual.astype(jnp.bfloat16)
    wout_part = dot("te,td->ed", mixed_low, grad_res_low)
    grad_wout = scatter_sum(wout_part.reshape(groups, PAIR, -1, width))
    grad_mixed = (
        dot("td,ed->te", grad_res_low, w_out)
        .astype(jnp.bfloat16)
        .reshape(tok_rows, kv_here, group_size, HEAD_SIZE)
    )
    mixed_view = mixed_low.reshape(tok_rows, kv_here, group_size, HEAD_SIZE)
    grad_query_rows, grad_key_rows, grad_value_rows = block_backward(
        query_low,
        keys_all,
        values_all,
        mixed_view,
        grad_mixed,
        logsum_block,
        query_ids,
        ids_all,
        query_pos,
        pos_all,
    )
    sent = jnp.concatenate(
        [
            grad_key_rows.reshape(2 * DOC_MAX, kv_here * HEAD_SIZE),
            grad_value_rows.reshape(2 * DOC_MAX, kv_here * HEAD_SIZE),
        ],
        axis=1,
    )
    back = passed_along(sent[:DOC_MAX].astype(jnp.bfloat16), "dp", -1).astype(jnp.float32)
    own = sent[DOC_MAX:] + back
    grad_qraw = grad_query_rows.reshape(tok_rows, heads_here, HEAD_SIZE)
    query_low_gradient = (
        rotate_halves(grad_qraw, cosine_table, -sine_values)
        .astype(jnp.bfloat16)
        .reshape(tok_rows, heads_here * HEAD_SIZE)
    )
    key_low_gradient = (
        rotate_halves(
            own[:, : kv_here * HEAD_SIZE].reshape(tok_rows, kv_here, HEAD_SIZE),
            cosine_table,
            -sine_values,
        )
        .astype(jnp.bfloat16)
        .reshape(tok_rows, kv_here * HEAD_SIZE)
    )
    value_low_gradient = own[:, kv_here * HEAD_SIZE :].astype(jnp.bfloat16)
    low_gradient = jnp.concatenate(
        [query_low_gradient, key_low_gradient, value_low_gradient], axis=1
    )
    normed_one_part = (
        dot("kl,ql->kq", query_low_gradient, query_weight)
        + dot("kl,ql->kq", key_low_gradient, key_weight)
        + dot("kl,ql->kq", value_low_gradient, value_weight)
    )
    grad_normed_one = tensor_sum(normed_one_part)
    gain_one_part = jnp.sum(normed_one_part * inputs_wide * root_one, axis=0)
    qkv_part = dot("wj,wq->jq", normed_low, low_gradient)
    columns = qkv_part.shape[1]
    gains = jnp.stack(
        [gain_one_part.reshape(n_dp, rows_here), gain_two_part.reshape(n_dp, rows_here)], axis=1
    )
    gains = jnp.pad(gains, ((0, 0), (0, 14), (0, columns - rows_here)))
    qkv_part = jnp.concatenate([qkv_part.reshape(n_dp, rows_here, columns), gains], axis=1)
    qkv_sum = scatter_sum(qkv_part.reshape(groups, PAIR, rows_here + 16, columns))
    grad_qkv = qkv_sum[:rows_here]
    gain_sums = qkv_sum[rows_here : rows_here + 16, :rows_here]
    bit = 1
    while bit < lax.axis_size("tensor"):
        gain_sums = gain_sums + tensor_swap(gain_sums, bit)
        bit *= 2
    grad_input_norm = norm_back(inputs_wide, root_one, norm1_gain, grad_normed_one)
    grad_inputs = (grad_residual + grad_input_norm).astype(jnp.bfloat16)
    q_columns = query_weight.shape[1]
    k_columns = key_weight.shape[1]
    return (
        output,
        grad_inputs,
        gain_sums[0],
        grad_qkv[:, :q_columns],
        grad_qkv[:, q_columns : q_columns + k_columns],
        grad_qkv[:, q_columns + k_columns :],
        grad_wout,
        gain_sums[1],
        grad_wgate,
        grad_wup,
        grad_wdown,
    )


def shards(
    inputs,
    norm1_gain,
    query_weight,
    key_weight,
    value_weight,
    w_out,
    norm2_gain,
    w_gate,
    w_up,
    w_down,
    doc_ids,
    grad_output,
):
    tok_rows, width = inputs.shape
    heads_here = query_weight.shape[1] // HEAD_SIZE
    kv_here = key_weight.shape[1] // HEAD_SIZE
    group_size = heads_here // kv_here
    n_dp = lax.axis_size("dp")
    groups = n_dp // PAIR
    group = lax.axis_index("dp") // PAIR
    offset = lax.axis_index("dp") * tok_rows
    n_tensor = lax.axis_size("tensor")
    half = HEAD_SIZE // 2
    lanes = jnp.arange(4 * half, dtype=jnp.int32)
    positions = (offset + jnp.arange(tok_rows, dtype=jnp.int32)).astype(jnp.float32)
    angles = positions[:, None] * jnp.tile(rope_table(half), 4)[None, :]
    cosine = jnp.cos(angles)
    sine = jnp.sin(angles) * jnp.where(lanes % HEAD_SIZE < half, -1.0, 1.0)[None, :]
    normed_low, query_scaled, kv, id_rows, mixed_low, residual, normed_two_low, gate_t, up_t, part_g = attend_forward(
        inputs, norm1_gain, query_weight, key_weight, value_weight, w_out, norm2_gain, cosine, sine, doc_ids, grad_output,
        w_gate, w_up, n_dp, n_tensor)
    mlp_part, back_part, normed_rest, rest_g, gain_two_part = mlp(normed_two_low, grad_output, part_g, w_gate, w_up, w_down, n_dp, n_tensor)
    d_own, d_send, g_sum, u_own, u_send, grad_normed_two = wgrad(
        normed_two_low, normed_rest, grad_output, part_g, rest_g, gate_t, up_t, w_down, back_part, n_dp, n_tensor)
    output, grad_inputs, gate_blocks, up_blocks, d_in, wout_blocks, qkv_blocks, gain_sums = backward(
        grad_normed_two, residual, inputs, grad_output, mlp_part, normed_low, w_out, query_weight, key_weight, value_weight,
        g_sum, u_own, u_send, d_send, mixed_low, query_scaled, kv, norm1_gain, norm2_gain, gain_two_part,
        id_rows, doc_ids.reshape(1, tok_rows), cosine, sine, n_dp, n_tensor)
    output, grad_inputs, grad_wgate, grad_wup, grad_wdown, grad_wout, grad_wquery, grad_wkey, grad_wvalue = finish_all(
        output, grad_inputs, gate_blocks, up_blocks, d_own, d_in, wout_blocks, qkv_blocks, query_weight.shape[1], key_weight.shape[1])
    return (
        output,
        grad_inputs,
        gain_sums[0],
        grad_wquery,
        grad_wkey,
        grad_wvalue,
        grad_wout,
        gain_sums[1],
        grad_wgate,
        grad_wup,
        grad_wdown,
    )


def kernels_fit(mesh, *args):
    n_dp, n_tensor = mesh.shape["dp"], mesh.shape["tensor"]
    width = args[0].shape[1]
    return (
        n_dp % PAIR == 0
        and n_dp // PAIR <= 4
        and n_tensor == 4
        and width // n_dp in (128, 256)
        and args[7].shape[1] // n_tensor // (n_dp // PAIR) % 256 == 0
        and args[0].shape[0] // n_dp == DOC_MAX
        and args[3].shape[1] // n_tensor == 2 * HEAD_SIZE
        and args[2].shape[1] == 4 * args[3].shape[1]
    )


def solution(mesh):
    def step(*args):
        return mapped(mesh, shards if kernels_fit(mesh, *args) else shards_plain)(*args)

    return step


def mapped(mesh, function):
    return jax.shard_map(
        function,
        mesh=mesh,
        in_specs=(
            P("dp", None),
            P(),
            P(None, "tensor"),
            P(None, "tensor"),
            P(None, "tensor"),
            P("tensor", None),
            P(),
            P(None, "tensor"),
            P(None, "tensor"),
            P("tensor", None),
            P("dp"),
            P("dp", None),
        ),
        out_specs=(
            P("dp", None),
            P("dp", None),
            P("dp"),
            P("dp", "tensor"),
            P("dp", "tensor"),
            P("dp", "tensor"),
            P(("tensor", "dp"), None),
            P("dp"),
            P("dp", "tensor"),
            P("dp", "tensor"),
            P(("tensor", "dp"), None),
        ),
        check_vma=False,
    )
```

```python
import functools
import math

import jax
import jax.numpy as jnp
from jax import lax
from jax.experimental import pallas as pl
from jax.experimental.pallas import tpu as pltpu
from jax.sharding import PartitionSpec as P

HEAD_SIZE = 64
DOC_MAX = 512
NORM_EPSILON = 1e-05

PAIR = 2
MESH = pl.DeviceIdType.MESH
EPS = NORM_EPSILON


def nn(a, b):
    return lax.dot_general(a, b, (((1,), (0,)), ((), ())), preferred_element_type=jnp.float32)
def nt(a, b):
    return lax.dot_general(a, b, (((1,), (1,)), ((), ())), preferred_element_type=jnp.float32)

def flip(index, bit):
    return index + bit - 2 * bit * ((index // bit) % 2)

def meet(*partners):
    barrier = pltpu.get_barrier_semaphore()
    for axis, index in partners:
        pl.semaphore_signal(barrier, inc=1, device_id={axis: index}, device_id_type=MESH)
    pl.semaphore_wait(barrier, len(partners))

def remote(src, dst, sems, slot, axis, index):
    return pltpu.make_async_remote_copy(
        src_ref=src, dst_ref=dst, send_sem=sems.at[0, slot], recv_sem=sems.at[1, slot],
        device_id={axis: index}, device_id_type=MESH)

def send(src, dst, sems, slot, axis, index):
    copy = remote(src, dst, sems, slot, axis, index)
    copy.start()
    return copy

def swiglu(gate, up, grad):
    sig = 0.5 * (1.0 + jnp.tanh(0.5 * gate))
    silu = gate * sig
    hidden = (silu * up).astype(jnp.bfloat16)
    grad_gate = (grad * up * sig * (1.0 + gate * (1.0 - sig))).astype(jnp.bfloat16)
    grad_up = (grad * silu).astype(jnp.bfloat16)
    return hidden, grad_gate, grad_up

def mlp_kernel(n_dp, n_tensor, normed_hbm, grad_hbm, part_g, cross_g, gate_hbm, up_hbm, down_hbm,
               out_ref, back_ref, all_hbm, rest_g, gain_ref,
               normed, grad, gate_w, up_w, down_w, hid, low_gate, low_up, load, far):
    rows, width = normed.shape
    cols = gate_w.shape[1]
    groups = n_dp // PAIR
    me_dp, me_t = lax.axis_index("dp"), lax.axis_index("tensor")
    right = lax.rem(me_dp + PAIR, n_dp)
    left = lax.rem(me_dp + n_dp - PAIR, n_dp)
    core, across = flip(me_t, 1), flip(me_t, 2)
    tile = 256
    tiles = cols // tile
    def cp(s, d, i):
        return pltpu.make_async_copy(s, d, load.at[i])
    def gate_tile(c, f):
        return cp(gate_hbm.at[:, c], gate_w.at[:, c], 2 + 3 * f)
    def up_tile(c, f):
        return cp(up_hbm.at[:, c], up_w.at[:, c], 3 + 3 * f)
    def down_tile(c, f):
        return cp(down_hbm.at[c, :], down_w.at[c, :], 4 + 3 * f)
    cp(normed_hbm, normed, 0).start()
    def load_tile(f):
        c = pl.ds(pl.multiple_of(f * tile, tile), tile)
        gate_tile(c, f).start()
        up_tile(c, f).start()
        down_tile(c, f).start()
    load_tile(0)
    cp(grad_hbm, grad, 1).start()
    for f in range(1, tiles):
        load_tile(f)
    meet(("dp", right), ("dp", left), ("tensor", core), ("tensor", across))
    piece = rows // n_tensor
    def part(t):
        return pl.ds(pl.multiple_of(t * piece, piece), piece)
    steps = groups - 1
    per = 4
    def ring(s):
        src = (normed_hbm if s == 1 else all_hbm.at[s - 2]).at[part(me_t), :]
        return send(src, all_hbm.at[s - 1].at[part(me_t), :], far, s * per, "dp", right)
    def spread_n(s, level):
        block = all_hbm.at[s - 1]
        held, other = [me_t, across][:level + 1], [across, core][level]
        return [send(block.at[part(h), :], block.at[part(h), :], far, s * per + 1 + level + i, "tensor", other) for i, h in enumerate(held)]
    def spread_g(b, level):
        base = (steps + 1 + b) * per
        if level == 0:
            return [send(part_g.at[b], rest_g.at[b].at[part(me_t), :], far, base, "tensor", across)]
        cross = cross_g if b == 0 else rest_g.at[b].at[part(across), :]
        return [send(part_g.at[b], rest_g.at[b].at[part(me_t), :], far, base + 1, "tensor", core),
                send(cross, rest_g.at[b].at[part(across), :], far, base + 2, "tensor", core)]
    def wait(copies):
        for c in copies:
            c.wait()

    ring_n = ring(1)
    g_core = spread_g(0, 1)
    g_x = {}
    last_g = steps - 1 if steps > 1 else steps
    if last_g > 1:
        g_x[1] = spread_g(1, 0)

    cp(normed_hbm, normed, 0).wait()
    cp(grad_hbm, grad, 1).wait()
    def first(f, _):
        c = pl.ds(pl.multiple_of(f * tile, tile), tile)
        gate_tile(c, f).wait()
        up_tile(c, f).wait()
        down_tile(c, f).wait()
        g = nn(normed[...], gate_w[:, c])
        u = nn(normed[...], up_w[:, c])
        h = nt(grad[...], down_w[c, :])
        a, b, d = swiglu(g, u, h)
        hid[:, c] = a
        low_gate[:, c] = b
        low_up[:, c] = d
        return 0
    early = min(5, tiles)
    n_x = {}
    def pass_g(b):
        nonlocal g_core
        if b in g_x:
            wait(g_x.pop(b))
            g_core = g_core + spread_g(b, 1)
            if b + 1 < last_g:
                g_x[b + 1] = spread_g(b + 1, 0)
    lax.fori_loop(0, early, first, 0)
    ring_n.wait()
    if steps > 1:
        ring_n = ring(2)
    pass_g(1)
    n_x[1] = spread_n(1, 0)
    lax.fori_loop(early, tiles, first, 0)
    wtile = 256
    wtiles = width // wtile
    def second(j, _):
        c = pl.ds(pl.multiple_of(j * wtile, wtile), wtile)
        b = nt(low_gate[...], gate_w[c, :]) + nt(low_up[...], up_w[c, :])
        back_ref[:, c] = b.astype(back_ref.dtype)
        gain_ref[0:1, c] = jnp.sum(b * normed[:, c].astype(jnp.float32), axis=0, keepdims=True)
        return 0
    def third(j, _):
        c = pl.ds(pl.multiple_of(j * wtile, wtile), wtile)
        out_ref[:, c] = nn(hid[...], down_w[:, c]).astype(out_ref.dtype)
        return 0
    lax.fori_loop(0, wtiles, third, 0)
    n_core = []
    def pass_n(s):
        nonlocal n_core
        if s in n_x:
            wait(n_x.pop(s))
            n_core = n_core + spread_n(s, 1)
    if steps > 1:
        ring_n.wait()
        if steps > 2:
            ring_n = ring(3)
            n_x[2] = spread_n(2, 0)
    pass_g(2)
    lax.fori_loop(0, wtiles // 2, second, 0)
    pass_n(1)
    lax.fori_loop(wtiles // 2, wtiles, second, 0)
    for s in range(3, steps + 1):
        ring_n.wait()
        if s < steps:
            ring_n = ring(s + 1)
            n_x[s] = spread_n(s, 0)
    for b in range(3, steps):
        pass_g(b)
    for s in range(2, steps):
        pass_n(s)
    wait(n_core)
    wait(g_core)

def mlp(normed, grad_output, part_g, cross_g, w_gate, w_up, w_down, n_dp, n_tensor):
    rows, width = normed.shape
    cols = w_gate.shape[1]
    groups = n_dp // PAIR
    tiles = cols // 256
    anyspec = pl.BlockSpec(memory_space=pl.ANY)
    vm = pl.BlockSpec(memory_space=pltpu.VMEM)
    bf = jnp.bfloat16
    return pl.pallas_call(
        functools.partial(mlp_kernel, n_dp, n_tensor),
        out_shape=(jax.ShapeDtypeStruct((rows, width), bf), jax.ShapeDtypeStruct((rows, width), bf),
                   jax.ShapeDtypeStruct((groups - 1, rows, width), bf), jax.ShapeDtypeStruct((groups - 1, rows, width), bf), jax.ShapeDtypeStruct((1, width), jnp.float32)),
        in_specs=[anyspec] * 7, out_specs=(vm, vm, anyspec, anyspec, vm),
        scratch_shapes=[pltpu.VMEM((rows, width), bf), pltpu.VMEM((rows, width), bf),
                        pltpu.VMEM((width, cols), bf), pltpu.VMEM((width, cols), bf), pltpu.VMEM((cols, width), bf),
                        pltpu.VMEM((rows, cols), bf), pltpu.VMEM((rows, cols), bf), pltpu.VMEM((rows, cols), bf),
                        pltpu.SemaphoreType.DMA((2 + 3 * tiles,)),
                        pltpu.SemaphoreType.DMA((2, 8 * groups)),
                        ],
        compiler_params=pltpu.CompilerParams(collective_id=2, has_side_effects=True, vmem_limit_bytes=60 << 20),
        cost_estimate=pl.CostEstimate(flops=12 * rows * width * cols, bytes_accessed=2 * (3 * width * cols + 8 * rows * width), transcendentals=rows * cols),
        name="feed_forward",
    )(normed, grad_output, part_g, cross_g, w_gate, w_up, w_down)

def wgrad_kernel(n_dp, n_tensor, own_n, all_n, own_g, part_g, cross_g, rest_g, gate_t, up_t, down_hbm, back_hbm,
                 d_own_o, d_send_o, g_sum_o, u_own_o, u_send_o, sum_o,
                 d_own, d_send, g_sum, u_own, u_send, sum_ref, g_own, g_send, g_in, n_all, g_all, wg, wu, wd, hid, lowg, lowu, mine, in1, mid, in2, load, far, ar, sy, outs):
    rows, width = own_n.shape
    share = gate_t.shape[0]
    groups = n_dp // PAIR
    me_dp, me_t = lax.axis_index("dp"), lax.axis_index("tensor")
    member = lax.rem(me_dp, PAIR)
    bits = []
    bit = n_tensor // 2
    while bit:
        bits.append(bit); bit //= 2
    piece = rows // n_tensor
    def part(t):
        return pl.ds(pl.multiple_of(t * piece, piece), piece)
    def at(r, t):
        return pl.ds(pl.multiple_of(r * rows + t * piece, piece), piece)
    count = [0]
    def cp(s, d):
        c = pltpu.make_async_copy(s, d, load.at[count[0]]); count[0] += 1
        c.start(); return c
    half = rows // 2
    low = lax.rem(me_t, 2)
    def half_rows(c):
        return pl.ds(pl.multiple_of(c * half, half), half)
    last = groups - 1
    if last > 0:
        w_last = cp(all_n.at[last - 1].at[part(me_t), :], n_all.at[at(last, me_t), :])
    w1 = [cp(gate_t, wg), cp(own_n, n_all.at[pl.ds(0, rows), :])]
    w2 = [cp(up_t, wu)]
    w3 = [cp(down_hbm.at[pl.ds(pl.multiple_of(me_dp // PAIR * share, share), share), :], wd), cp(own_g, g_all.at[pl.ds(0, rows), :])]
    w4 = [cp(back_hbm.at[half_rows(low), :], mine)]
    first_block = count[0]
    def load_block(r):
        i = first_block + (r - 1) * (1 + n_tensor)
        def one(s, d, j):
            return pltpu.make_async_copy(s, d, load.at[i + j])
        out = []
        if r < last:
            out.append(one(all_n.at[r - 1], n_all.at[pl.ds(r * rows, rows), :], 0))
        out.append(one(part_g.at[r - 1], g_all.at[at(r, me_t), :], 1))
        if r == last and last > 1:
            return out
        for j, h in enumerate((flip(me_t, 1), flip(me_t, 2), flip(flip(me_t, 1), 2))):
            src = cross_g if r == 1 and j == 1 else rest_g.at[r - 1].at[part(h), :]
            out.append(one(src, g_all.at[at(r, h), :], 2 + j))
        return out
    def start(cs):
        for c in cs:
            c.start()
    pair = flip(me_dp, 1)
    core, across = flip(me_t, 1), flip(me_t, 2)
    right, left = lax.rem(me_dp + PAIR, n_dp), lax.rem(me_dp + n_dp - PAIR, n_dp)
    meet(("dp", pair), ("dp", right), ("dp", left), ("tensor", core), ("tensor", across))
    last_g = []
    if last > 1:
        src = cross_g if last == 2 else rest_g.at[last - 2].at[part(across), :]
        last_g = [lambda: remote(src, g_all.at[at(last, across), :], far, 3, "dp", right),
                  lambda: remote(part_g.at[last - 1], g_all.at[at(last, me_t), :], far, 4, "tensor", core),
                  lambda: remote(g_all.at[at(last, across), :], g_all.at[at(last, across), :], far, 5, "tensor", core)]
        last_g[0]().start()
    ar1 = send(back_hbm.at[half_rows(1 - low), :], in1, ar, 0, "tensor", core)
    def wait(cs):
        for c in cs:
            c.wait()
    def spread(level):
        held, other = [me_t, across][:level + 1], [across, core][level]
        return [remote(n_all.at[at(last, h), :], n_all.at[at(last, h), :], far, level + i, "tensor", other) for i, h in enumerate(held)]
    if last > 0:
        w_last.wait()
        start(spread(0))
    if last > 1:
        last_g[1]().start()

    sum2 = lambda: remote(mid, in2, ar, 1, "tensor", across)
    def pass_a(r, _):
        for k in range(groups):
            @pl.when(r == k)
            def _():
                if k == 0:
                    wait(w1)
                    wait(w2)
                    wait(w3)
                else:
                    wait(load_block(k))
                if k < last:
                    start(load_block(k + 1))
                if k == max(last - 1, 1):
                    wait(spread(0))
                    start(spread(1))
                    if last > 1:
                        last_g[0]().wait()
                        last_g[2]().start()
                    sum2().start()
                if k == last:
                    wait(spread(1))
                    if last > 1:
                        last_g[1]().wait()
                        last_g[2]().wait()
        rs = pl.ds(pl.multiple_of(r * rows, rows), rows)
        g = nt(wg[...], n_all[rs, :])
        u = nt(wu[...], n_all[rs, :])
        h = nt(wd[...], g_all[rs, :])
        a, b, d = swiglu(g, u, h)
        hid[:, rs] = a
        lowg[:, rs] = b
        lowu[:, rs] = d
        @pl.when(r == 0)
        def _():
            wait(w4)
            ar1.wait()
            mid[...] = (mine[...].astype(jnp.float32) + in1[...].astype(jnp.float32)).astype(jnp.bfloat16)
        return 0
    lax.fori_loop(0, groups, pass_a, 0)
    ar2 = sum2()
    dcols = width // n_dp
    def col_tile(low_ref, own_ref, send_ref):
        def body(q, _):
            a = pl.ds(pl.multiple_of((q * PAIR + member) * dcols, dcols), dcols)
            b = pl.ds(pl.multiple_of((q * PAIR + 1 - member) * dcols, dcols), dcols)
            send_ref[q] = nn(low_ref[...], n_all[:, b]).astype(jnp.bfloat16)
            own_ref[q] = nn(low_ref[...], n_all[:, a]).astype(jnp.bfloat16)
            return 0
        return body
    def to_pair(q):
        return remote(g_send.at[q], g_in.at[q], sy, q, "dp", pair)
    def gate_tile(q, _):
        col_tile(lowg, g_own, g_send)(q, 0)
        to_pair(q).start()
        return 0
    lax.fori_loop(0, groups, gate_tile, 0)
    hrows = share // PAIR
    def down_tile(j, _):
        c = pl.ds(pl.multiple_of(j * 512, 512), 512)
        d_send[:, c] = nn(hid[pl.ds(pl.multiple_of((1 - member) * hrows, hrows), hrows), :], g_all[:, c]).astype(jnp.bfloat16)
        d_own[:, c] = nn(hid[pl.ds(pl.multiple_of(member * hrows, hrows), hrows), :], g_all[:, c]).astype(jnp.bfloat16)
        return 0
    lax.fori_loop(0, width // 512, down_tile, 0)
    stores = []
    def store(src, dst):
        c = pltpu.make_async_copy(src, dst, outs.at[len(stores)])
        c.start()
        stores.append(c)
    store(d_own, d_own_o)
    store(d_send, d_send_o)
    lax.fori_loop(0, groups, col_tile(lowu, u_own, u_send), 0)
    store(u_own, u_own_o)
    store(u_send, u_send_o)
    ar2.wait()
    sum_ref[half_rows(low), :] = (mid[...].astype(jnp.float32) + in2[...].astype(jnp.float32)).astype(jnp.bfloat16)
    ar3 = send(sum_ref.at[half_rows(low), :], sum_ref.at[half_rows(low), :], ar, 2, "tensor", core)
    for q in range(groups):
        to_pair(q).wait()
        g_sum[q] = (g_own[q].astype(jnp.float32) + g_in[q].astype(jnp.float32)).astype(jnp.bfloat16)
    store(g_sum, g_sum_o)
    ar3.wait()
    store(sum_ref, sum_o)
    wait(stores)

def wgrad(own_n, all_n, own_g, part_g, cross_g, rest_g, gate_t, up_t, down, back, n_dp, n_tensor):
    rows, width = own_n.shape
    share = gate_t.shape[0]
    groups = n_dp // PAIR
    anyspec = pl.BlockSpec(memory_space=pl.ANY)
    vm = pl.BlockSpec(memory_space=pltpu.VMEM)
    bf, f32 = jnp.bfloat16, jnp.float32
    sd = jax.ShapeDtypeStruct
    dcols = width // n_dp
    V = pltpu.VMEM
    tall = groups * rows
    return pl.pallas_call(
        functools.partial(wgrad_kernel, n_dp, n_tensor),
        out_shape=(sd((share // PAIR, width), bf), sd((share // PAIR, width), bf), sd((groups, share, dcols), bf),
                   sd((groups, share, dcols), bf), sd((groups, share, dcols), bf), sd((rows, width), bf)),
        in_specs=[anyspec] * 10, out_specs=(anyspec,) * 6,
        scratch_shapes=[*[V((share // PAIR, width), bf)] * 2, *[V((groups, share, dcols), bf)] * 3, V((rows, width), bf), *[V((groups, share, dcols), bf)] * 3, V((tall, width), bf), V((tall, width), bf),
                        V((share, width), bf), V((share, width), bf), V((share, width), bf),
                        V((share, tall), bf), V((share, tall), bf), V((share, tall), bf),
                        *[V((rows // 2, width), bf)] * 4,
                        pltpu.SemaphoreType.DMA((7 + (groups - 1) * (1 + n_tensor),)),
                        pltpu.SemaphoreType.DMA((2, 6)), pltpu.SemaphoreType.DMA((2, 3)), pltpu.SemaphoreType.DMA((2, groups)), pltpu.SemaphoreType.DMA((6,))],
        compiler_params=pltpu.CompilerParams(collective_id=3, has_side_effects=True, vmem_limit_bytes=62 << 20),
        cost_estimate=pl.CostEstimate(flops=12 * tall * width * share, bytes_accessed=2 * (3 * width * share + 4 * tall * width), transcendentals=tall * share),
        name="weight_gradients",
    )(own_n, all_n, own_g, part_g, cross_g, rest_g, gate_t, up_t, down, back)
TILE = 128
CHUNK = 128

def turn(values, cosine, sine):
    lane = lax.broadcasted_iota(jnp.int32, values.shape, 1)
    swapped = jnp.where(lane % HEAD_SIZE < HEAD_SIZE // 2,
                        pltpu.roll(values, 128 - HEAD_SIZE // 2, 1), pltpu.roll(values, HEAD_SIZE // 2, 1))
    return values * cosine + swapped * sine

def place(values, head, side):
    v = values if head == side else pltpu.roll(values, HEAD_SIZE, 1)
    lane = lax.broadcasted_iota(jnp.int32, values.shape, 1)
    return jnp.where(lane // HEAD_SIZE == side, v, jnp.zeros_like(v))

def column_of(row):
    a = lax.broadcasted_iota(jnp.int32, (128, 128), 0)
    b = lax.broadcasted_iota(jnp.int32, (128, 128), 1)
    return jnp.sum(jnp.where(a == b, row.astype(jnp.float32), 0.0), axis=1, keepdims=True)

def bias_of(ids_col, ids_row, row0, col0, shape, window):
    q = lax.broadcasted_iota(jnp.int32, shape, 0) + row0
    k = lax.broadcasted_iota(jnp.int32, shape, 1) + col0
    return jnp.where((ids_col == ids_row) & (k <= q), 0.0, -1e30)

def attention_kernel(n_dp, n_tensor, x_hbm, gain1, wq_hbm, wk_hbm, wv_hbm, wo_hbm, gain2, cos_ref, sin_ref, ids_row, g_hbm, gate_hbm, up_hbm,
                     normed_o, q_o, kv_o, idrow_o, mixed_o, res_o, normed2_o, gate_o, up_o, part_g, cross_g,
                     normed_ref, q_ref, kv_ref, idrow_ref, mixed_ref, res_ref, normed2_ref, gate_t, up_t,
                     x, wq, wk, wv, wo, raw_gate, raw_up, kvar, vvar, ids_flat, tile32, partial, out1, in1, mid, in2, total, load, outs, far, halo, ar):
    rows, width = x.shape
    groups = n_dp // PAIR
    me_dp, me_t = lax.axis_index("dp"), lax.axis_index("tensor")
    right = lax.rem(me_dp + PAIR, n_dp)
    left = lax.rem(me_dp + n_dp - PAIR, n_dp)
    after = lax.rem(me_dp + 1, n_dp)
    before = lax.rem(me_dp + n_dp - 1, n_dp)
    core, across = flip(me_t, 1), flip(me_t, 2)
    piece = rows // n_tensor
    def part(t):
        return pl.ds(pl.multiple_of(t * piece, piece), piece)
    count = [0]
    def cp(s, d):
        c = pltpu.make_async_copy(s, d, load.at[count[0]]); count[0] += 1
        c.start(); return c
    share = raw_gate.shape[1]
    stores = []
    def store(src, dst):
        c = pltpu.make_async_copy(src, dst, outs.at[len(stores)])
        c.start()
        stores.append(c)
    share = raw_gate.shape[1]
    w_x = cp(x_hbm, x); w_k = cp(wk_hbm, wk); w_v = cp(wv_hbm, wv)
    meet(("dp", after), ("dp", before), ("dp", right), ("dp", left), ("tensor", core), ("tensor", across))
    ids_go = send(ids_row, idrow_ref.at[0], halo, 0, "dp", after)
    fine = piece // 2
    def first_part(j):
        first = pl.ds(pl.multiple_of(me_t * piece + j * fine, fine), fine)
        return remote(g_hbm.at[first, :], part_g.at[0].at[pl.ds(j * fine, fine), :], far, j, "dp", right)
    def cross_first():
        return send(part_g.at[0].at[pl.ds(0, fine), :], cross_g.at[pl.ds(0, fine), :], far, groups, "tensor", across)
    def cross_second():
        second = pl.ds(pl.multiple_of(across * piece + fine, fine), fine)
        return remote(g_hbm.at[second, :], cross_g.at[pl.ds(fine, fine), :], far, groups + 1, "dp", right)
    ring0 = first_part(0)
    ring0.start()
    w_q = cp(wq_hbm, wq)
    idrow_ref[1] = ids_row[...]

    w_x.wait()
    def norm_one(i, _):
        r = pl.ds(pl.multiple_of(i * TILE, TILE), TILE)
        v = x[r, :].astype(jnp.float32)
        root = lax.rsqrt(jnp.mean(v * v, axis=1, keepdims=True) + EPS)
        normed_ref[r, :] = (v * root * gain1[...]).astype(jnp.bfloat16)
        return 0
    lax.fori_loop(0, rows // TILE, norm_one, 0)
    w_k.wait(); w_v.wait()
    own = pl.ds(rows, rows)
    kv_ref[1, :, 0:128] = turn(nn(normed_ref[...], wk[...]), cos_ref[...], sin_ref[...]).astype(jnp.bfloat16)
    kv_ref[1, :, 128:256] = nn(normed_ref[...], wv[...]).astype(jnp.bfloat16)
    w_q.wait()
    pairs = wq.shape[1] // 128
    def q_pair(p, _):
        c = pl.ds(pl.multiple_of(p * 256, 256), 256)
        raw = nn(normed_ref[...], wq[:, c])
        for s in range(2):
            d = pl.ds(pl.multiple_of(p * 256 + s * 128, 128), 128)
            q_ref[:, d] = (turn(raw[:, s * 128:(s + 1) * 128], cos_ref[...], sin_ref[...]).astype(jnp.bfloat16) * HEAD_SIZE ** -0.5).astype(jnp.bfloat16)
        return 0
    kv_go = send(kv_ref.at[1], kv_ref.at[0], halo, 1, "dp", after)
    w_o = cp(wo_hbm, wo)
    store(normed_ref, normed_o)
    lax.fori_loop(0, pairs // 2, q_pair, 0)
    def variants(side_rows, b):
        for g in range(2):
            for s in range(2):
                kvar[g, s, side_rows, :] = place(kv_ref[b, :, 0:128], g, s)
                vvar[g, s, side_rows, :] = place(kv_ref[b, :, 128:256], g, s)
    variants(own, 1)
    ids_go.wait(); kv_go.wait()
    ring0.wait()
    cross0 = cross_first()
    first_part(1).start()
    store(q_ref, q_o)
    store(kv_ref, kv_o)
    store(idrow_ref, idrow_o)
    mine = pl.ds(pl.multiple_of(me_dp // PAIR * share, share), share)
    w_gate = cp(gate_hbm.at[:, mine], raw_gate); w_up = cp(up_hbm.at[:, mine], raw_up)
    variants(pl.ds(0, rows), 0)
    w_o.wait()
    ids_flat[:, 0:rows] = idrow_ref[0]
    ids_flat[:, rows:2 * rows] = idrow_ref[1]

    window = rows + TILE
    def attend(i):
        start = pl.multiple_of(i * TILE, TILE)
        r = pl.ds(start, TILE)
        k = pl.ds(start, window)
        ids_k = ids_flat[:, k]
        bias = bias_of(column_of(ids_flat[:, pl.ds(start + rows, TILE)]), ids_k.astype(jnp.float32), rows, 0, (TILE, window), window)
        bias = jnp.concatenate([bias, bias], axis=0)
        for g in range(2):
            q2 = jnp.concatenate([q_ref[r, (2 * g) * 128:(2 * g + 1) * 128], q_ref[r, (2 * g + 1) * 128:(2 * g + 2) * 128]], axis=0)
            mixed = None
            for s in range(2):
                score = nt(q2, kvar[g, s, k, :]) + bias
                peak = jnp.max(score, axis=1, keepdims=True)
                e = jnp.exp(score - peak)
                l = jnp.sum(e, axis=1, keepdims=True)
                prob = (e * (1.0 / l)).astype(jnp.bfloat16)
                m = nn(prob, vvar[g, s, k, :])
                mixed = m if mixed is None else mixed + m
            for b in range(2):
                mixed_ref[r, (2 * g + b) * 128:(2 * g + b + 1) * 128] = mixed[b * TILE:(b + 1) * TILE, :].astype(jnp.bfloat16)

    hrow = CHUNK // 2
    low = lax.rem(me_t, 2)
    def own_rows(c):
        return pl.ds(pl.multiple_of(c * CHUNK + low * hrow, hrow), hrow)
    def oth_rows(c):
        return pl.ds(pl.multiple_of(c * CHUNK + (1 - low) * hrow, hrow), hrow)
    def project(c):
        r = pl.ds(pl.multiple_of(c * CHUNK, CHUNK), CHUNK)
        def body(j, _):
            d = pl.ds(pl.multiple_of(j * 512, 512), 512)
            tile32[...] = nn(mixed_ref[r, :], wo[:, d])
            out1[c, :, d] = tile32[pl.ds(pl.multiple_of((1 - low) * hrow, hrow), hrow), :].astype(jnp.bfloat16)
            partial[c, :, d] = tile32[pl.ds(pl.multiple_of(low * hrow, hrow), hrow), :]
            return 0
        lax.fori_loop(0, width // 512, body, 0)
    def step1(c):
        return remote(out1.at[c], in1.at[c], ar, 3 * c, "tensor", core)
    def step2(c):
        return remote(mid.at[c], in2.at[c], ar, 3 * c + 1, "tensor", across)
    def add_core(c):
        step1(c).wait()
        mid[c] = (partial[c] + in1[c].astype(jnp.float32)).astype(jnp.bfloat16)
        step2(c).start()
    def step3(c):
        total[own_rows(c), :] = (mid[c].astype(jnp.float32) + in2[c].astype(jnp.float32)).astype(jnp.bfloat16)
        return send(total.at[own_rows(c), :], total.at[own_rows(c), :], ar, 3 * c + 2, "tensor", core)
    def finish(r):
        v = x[r, :].astype(jnp.float32) + total[r, :].astype(jnp.float32)
        res_ref[r, :] = v
        root = lax.rsqrt(jnp.mean(v * v, axis=1, keepdims=True) + EPS)
        normed2_ref[r, :] = (v * root * gain2[...]).astype(jnp.bfloat16)

    chunks = rows // CHUNK
    flights = {}
    steps = groups - 1
    def ring(s):
        return remote(part_g.at[s - 2], part_g.at[s - 1], far, s, "dp", right)
    def tile_step(i, _):
        attend(i)
        @pl.when(i > 0)
        def _():
            add_core(i - 1)
        project(i)
        step1(i).start()
        @pl.when(i == 0)
        def _():
            first_part(1).wait()
            cross_second().start()
            if steps > 1:
                ring(2).start()
        return 0
    lax.fori_loop(0, rows // TILE, tile_step, 0)
    c = chunks - 1
    store(mixed_ref, mixed_o)
    def transpose_into(dst, raw):
        def body(j, _):
            r = pl.ds(pl.multiple_of(j * 256, 256), 256)
            dst[:, r] = raw[r, :].T
            return 0
        lax.fori_loop(0, width // 256, body, 0)
    add_core(c)
    w_gate.wait()
    transpose_into(gate_t, raw_gate)
    store(gate_t, gate_o)
    w_up.wait()
    transpose_into(up_t, raw_up)
    store(up_t, up_o)
    def out_rows(c):
        flights[3, c].wait()
        finish(oth_rows(c))
        r = pl.ds(c * CHUNK, CHUNK)
        store(res_ref.at[r, :], res_o.at[r, :])
        store(normed2_ref.at[r, :], normed2_o.at[r, :])
    for c in range(chunks):
        if 3 <= c + 2 <= steps:
            ring(c + 1).wait()
            ring(c + 2).start()
        step2(c).wait()
        flights[3, c] = step3(c)
        finish(own_rows(c))
        if c > 0:
            out_rows(c - 1)
    out_rows(chunks - 1)
    if steps > 1:
        ring(steps).wait()
    cross0.wait()
    cross_second().wait()
    for q in stores:
        q.wait()

def attend_forward(x, gain1, wq, wk, wv, wo, gain2, cosine, sine, ids, grad_output, w_gate, w_up, n_dp, n_tensor):
    rows, width = x.shape
    groups = n_dp // PAIR
    anyspec = pl.BlockSpec(memory_space=pl.ANY)
    vm = pl.BlockSpec(memory_space=pltpu.VMEM)
    bf, f32 = jnp.bfloat16, jnp.float32
    sd = jax.ShapeDtypeStruct
    V = pltpu.VMEM
    piece = rows // n_tensor
    chunks = rows // CHUNK
    qc = wq.shape[1]
    share = w_gate.shape[1] // groups
    D = pltpu.SemaphoreType.DMA
    return pl.pallas_call(
        functools.partial(attention_kernel, n_dp, n_tensor),
        out_shape=(sd((rows, width), bf), sd((rows, qc), bf), sd((2, rows, 256), bf), sd((2, 1, rows), jnp.int32),
                   sd((rows, qc), bf), sd((rows, width), f32), sd((rows, width), bf), sd((share, width), bf), sd((share, width), bf),
                   sd((groups - 1, piece, width), bf), sd((piece, width), bf)),
        in_specs=[anyspec, vm, anyspec, anyspec, anyspec, anyspec, vm, vm, vm, vm, anyspec, anyspec, anyspec],
        out_specs=(anyspec,) * 11,
        scratch_shapes=[V((rows, width), bf), V((rows, qc), bf), V((2, rows, 256), bf), V((2, 1, rows), jnp.int32), V((rows, qc), bf),
                        V((rows, width), f32), V((rows, width), bf), V((share, width), bf), V((share, width), bf),
                        V((rows, width), bf), V((width, qc), bf), V((width, 128), bf), V((width, 128), bf), V((qc, width), bf), V((width, share), bf), V((width, share), bf),
                        V((2, 2, 2 * rows, 128), bf), V((2, 2, 2 * rows, 128), bf), V((1, 2 * rows), jnp.int32), V((CHUNK, 512), f32),
                        V((chunks, CHUNK // 2, width), f32), V((chunks, CHUNK // 2, width), bf), V((chunks, CHUNK // 2, width), bf),
                        V((chunks, CHUNK // 2, width), bf), V((chunks, CHUNK // 2, width), bf), V((rows, width), bf),
                        D((7,)), D((7 + 2 * chunks,)), D((2, groups + 2)), D((2, 2)), D((2, 3 * chunks))],
        compiler_params=pltpu.CompilerParams(collective_id=1, has_side_effects=True, vmem_limit_bytes=62 << 20),
        cost_estimate=pl.CostEstimate(flops=2 * rows * width * (2 * qc + 256) + 16 * rows * rows * 5 * 128, bytes_accessed=2 * (width * (2 * qc + 256) + 6 * rows * width), transcendentals=8 * rows * rows),
        name="attention_forward",
    )(x, gain1.reshape(1, width), wq, wk, wv, wo, gain2.reshape(1, width), cosine, sine, ids.reshape(1, rows), grad_output, w_gate, w_up)

def backward_kernel(n_dp, n_tensor, gn_hbm, res_hbm, x_hbm, go_hbm, mlp_hbm, normed_hbm, wo_hbm, wq_hbm, wk_hbm, wv_hbm,
                    g_sum, u_own_hbm, u_send, d_send, mixed_hbm, q_hbm, kv_hbm, gain1, gain2, gain2_part, id_rows, ids_row, cos_ref, sin_ref,
                    out_hbm, gin_hbm, gz, uz, d_in, wz, qz, gains_ref,
                    gn, res, go, normed, wo, wq, wk, wv, mixed, q_ref, kv_ref, resid, low_res, gm, kvar, vvar, kvart, dk, dv, ids_col,
                    low, lowt, tile32, wsend, wown, win, own_block, u_own, uyin, usum, qsend, qown, qin,
                    amine, amid, min1, min2, ain1, ain2, hprev, hin, gacc, gs, gown, gyi, gzi, gt, gti,
                    load, sy, sz, sx, sh, sg):
    rows, width = go.shape
    groups = n_dp // PAIR
    me_dp, me_t = lax.axis_index("dp"), lax.axis_index("tensor")
    group, member = me_dp // PAIR, lax.rem(me_dp, PAIR)
    pair = flip(me_dp, 1)
    after = lax.rem(me_dp + 1, n_dp)
    before = lax.rem(me_dp + n_dp - 1, n_dp)
    core, across = flip(me_t, 1), flip(me_t, 2)
    low_t = lax.rem(me_t, 2)
    def at_group(s):
        return lax.rem(group + s, groups)
    def from_group(s):
        return lax.rem(group + groups - s, groups)
    f32, bf = jnp.float32, jnp.bfloat16
    qc = wq.shape[1]
    dcols = width // n_dp
    half = rows // 2
    def rows_of(start, size):
        return pl.ds(pl.multiple_of(start, size), size)
    def half_rows(c):
        return rows_of(c * half, half)
    def cp(s, d, i):
        c = pltpu.make_async_copy(s, d, load.at[i])
        c.start()
        return c
    w_gn = cp(gn_hbm, gn, 0); w_res = cp(res_hbm, res, 1); w_go = cp(go_hbm, go, 2)
    w_wo = cp(wo_hbm, wo, 3); w_mlp = cp(mlp_hbm.at[half_rows(low_t), :], amine, 4)
    w_kv = cp(kv_hbm, kv_ref, 5); w_mx = cp(mixed_hbm, mixed, 6); w_qr = cp(q_hbm, q_ref, 7)
    w_own = cp(u_own_hbm, u_own, 8); w_nm = cp(normed_hbm, normed, 9)
    w_q = cp(wq_hbm, wq, 10); w_k = cp(wk_hbm, wk, 11); w_v = cp(wv_hbm, wv, 12)
    meet(("dp", pair), ("dp", after), ("dp", before), ("tensor", core), ("tensor", across),
         *[("dp", at_group(s) * PAIR + member) for s in range(1, groups)])
    def exchange(src, dst, base):
        return [send(src.at[at_group(s)], dst.at[group], sz, base + s - 1, "dp", at_group(s) * PAIR + member) for s in range(1, groups)]
    y_u = send(u_send, uyin, sy, 0, "dp", pair)
    z_g = exchange(g_sum, gz, 0)
    cp(g_sum.at[group], own_block, 13).wait()
    w_g = cp(own_block, gz.at[group], 13)
    m1 = send(mlp_hbm.at[half_rows(1 - low_t), :], min1, sx, 0, "tensor", core)

    w_gn.wait(); w_res.wait(); w_go.wait()
    NR = 64
    def norm_two(i, _):
        r = rows_of(i * NR, NR)
        v = res[r, :]
        root = lax.rsqrt(jnp.mean(v * v, axis=1, keepdims=True) + EPS)
        up = gn[r, :].astype(f32) * gain2[...]
        mean = jnp.mean(up * v, axis=1, keepdims=True)
        d = go[r, :].astype(f32) + root * up - v * (root * root * root * mean)
        resid[r, :] = d
        low_res[r, :] = d.astype(bf)
        return 0
    lax.fori_loop(0, rows // NR, norm_two, 0)
    w_wo.wait()
    def mix_tile(i, _):
        r = rows_of(i * half, half)
        gm[r, :] = nt(low_res[r, :], wo[...]).astype(bf)
        return 0
    lax.fori_loop(0, 2, mix_tile, 0)
    w_mlp.wait(); m1.wait()
    amid[...] = (amine[...].astype(f32) + min1[...].astype(f32)).astype(bf)
    w_kv.wait()
    for g in range(2):
        for s in range(2):
            for b in range(2):
                kvar[g, s, pl.ds(b * rows, rows), :] = place(kv_ref[b, :, 0:128], g, s)
                vvar[g, s, pl.ds(b * rows, rows), :] = place(kv_ref[b, :, 128:256], g, s)
            kvart[g, s] = kvar[g, s].T
    dk[...] = jnp.zeros_like(dk)
    dv[...] = jnp.zeros_like(dv)
    m2 = send(amid, min2, sx, 1, "tensor", across)
    w_mx.wait()
    lowt[0:qc, :] = mixed[...].T
    hrow = qc // n_dp
    def wout_tile(j, _):
        c = rows_of(j * 256, 256)
        tile32[...] = nn(lowt[0:qc, :], low_res[:, c])
        for z in range(groups):
            wown[z, :, c] = tile32[rows_of((z * PAIR + member) * hrow, hrow), :].astype(bf)
            wsend[z, :, c] = tile32[rows_of((z * PAIR + 1 - member) * hrow, hrow), :].astype(bf)
        return 0
    lax.fori_loop(0, width // 256, wout_tile, 0)
    w_qr.wait()
    for b in range(2):
        for j in range(rows // 128):
            ids_col[b * rows + j * 128:b * rows + (j + 1) * 128, :] = column_of(id_rows[b][:, j * 128:(j + 1) * 128])
    window = rows + TILE
    def attend(i, _):
        r = rows_of(i * TILE, TILE)
        k = pl.ds(pl.multiple_of(i * TILE, TILE), window)
        kpos = lax.broadcasted_iota(jnp.int32, (window, TILE), 0)
        qpos = lax.broadcasted_iota(jnp.int32, (window, TILE), 1) + rows
        bias = jnp.where((ids_col[k, :] == ids_row[:, r].astype(f32)) & (kpos <= qpos), 0.0, -1e30)
        bias = jnp.concatenate([bias, bias], axis=1)
        for g in range(2):
            q2 = jnp.concatenate([q_ref[r, (2 * g) * 128:(2 * g + 1) * 128], q_ref[r, (2 * g + 1) * 128:(2 * g + 2) * 128]], axis=0)
            do2 = jnp.concatenate([gm[r, (2 * g) * 128:(2 * g + 1) * 128], gm[r, (2 * g + 1) * 128:(2 * g + 2) * 128]], axis=0)
            dqt = None
            for s in range(2):
                st = nt(kvar[g, s, k, :], q2) + bias
                peak = jnp.max(st, axis=0, keepdims=True)
                e = jnp.exp(st - peak)
                pt = e * (1.0 / jnp.sum(e, axis=0, keepdims=True))
                dpt = nt(vvar[g, s, k, :], do2)
                delta = jnp.sum(pt * dpt, axis=0, keepdims=True)
                dst = (pt * (dpt - delta)).astype(bf)
                dv[g, s, k, :] += nn(pt.astype(bf), do2)
                dk[g, s, k, :] += nn(dst, q2)
                part = nn(kvart[g, s, :, k], dst)
                dqt = part if dqt is None else dqt + part
            d = dqt.T * HEAD_SIZE ** -0.5
            for b in range(2):
                low[r, (2 * g + b) * 128:(2 * g + b + 1) * 128] = turn(d[b * TILE:(b + 1) * TILE, :], cos_ref[r, :], -sin_ref[r, :]).astype(bf)
        return 0
    lax.fori_loop(0, rows // TILE // 2, attend, 0)
    y_u.wait()
    w_own.wait()
    for z in range(groups):
        usum[z] = (u_own[z].astype(f32) + uyin[z].astype(f32)).astype(bf)
    y_w = send(wsend, win, sy, 1, "dp", pair)
    w_u = cp(usum.at[group], uz.at[group], 8)
    z_u = exchange(usum, uz, groups)
    lax.fori_loop(rows // TILE // 2, rows // TILE, attend, 0)

    def gathered(acc, b):
        r = pl.ds(b * rows, rows)
        lane = lax.broadcasted_iota(jnp.int32, (rows, 128), 1)
        first = acc[0, 0, r, :] + pltpu.roll(acc[0, 1, r, :], HEAD_SIZE, 1)
        second = pltpu.roll(acc[1, 0, r, :], HEAD_SIZE, 1) + acc[1, 1, r, :]
        return jnp.where(lane < HEAD_SIZE, first, second)
    hprev[:, 0:128] = gathered(dk, 0).astype(bf)
    hprev[:, 128:256] = gathered(dv, 0).astype(bf)
    halo = send(hprev, hin, sh, 0, "dp", before)
    m2.wait()
    def out_rows(i, _):
        r = rows_of(low_t * half + i * NR, NR)
        m = rows_of(i * NR, NR)
        summed = (amid[m, :].astype(f32) + min2[m, :].astype(f32)).astype(bf)
        go[r, :] = (res[r, :] + summed.astype(f32)).astype(bf)
        return 0
    lax.fori_loop(0, half // NR, out_rows, 0)
    w_out = cp(go.at[half_rows(low_t), :], out_hbm.at[half_rows(low_t), :], 2)
    m3 = send(go.at[half_rows(low_t), :], out_hbm.at[half_rows(low_t), :], sx, 2, "tensor", core)
    lowt[0:qc, :] = low[:, 0:qc].T
    w_nm.wait()
    def grad_cols(row0, count):
        def body(z, _):
            a = rows_of((z * PAIR + member) * dcols, dcols)
            b = rows_of((z * PAIR + 1 - member) * dcols, dcols)
            t = lowt[row0:row0 + count, :]
            qsend[z, row0:row0 + count, :] = nn(t, normed[:, b]).astype(bf)
            qown[z, row0:row0 + count, :] = nn(t, normed[:, a]).astype(bf)
            return 0
        lax.fori_loop(0, groups, body, 0)
    grad_cols(0, qc)
    y_w.wait()
    y_q = [send(qsend.at[:, 0:qc, :], qin.at[:, 0:qc, :], sy, 2, "dp", pair)]
    for z in range(groups):
        wown[z] = (wown[z].astype(f32) + win[z].astype(f32)).astype(bf)
    w_w = cp(wown.at[group], wz.at[group], 3)
    halo.wait()
    kraw = gathered(dk, 1) + hin[:, 0:128].astype(f32)
    low[:, qc:qc + 128] = turn(kraw, cos_ref[...], -sin_ref[...]).astype(bf)
    low[:, qc + 128:qc + 256] = (gathered(dv, 1) + hin[:, 128:256].astype(f32)).astype(bf)
    z_w = exchange(wown, wz, 2 * groups)
    w_q.wait(); w_k.wait(); w_v.wait()
    def normed_part(j, _):
        c = rows_of(j * 256, 256)
        p = (nt(low[:, 0:qc], wq[c, :]) + nt(low[:, qc:qc + 128], wk[c, :]) + nt(low[:, qc + 128:qc + 256], wv[c, :]))
        res[:, c] = p
        gacc[0:1, c] = jnp.sum(p * normed[:, c].astype(f32), axis=0, keepdims=True) / gain1[0:1, c]
        gacc[1:2, c] = gain2_part[0:1, c] / gain2[0:1, c]
        return 0
    lax.fori_loop(0, width // 256, normed_part, 0)
    hchunk = CHUNK // 2
    chunks = rows // CHUNK
    def own_rows(c):
        return rows_of(c * CHUNK + low_t * hchunk, hchunk)
    def oth_rows(c):
        return rows_of(c * CHUNK + (1 - low_t) * hchunk, hchunk)
    def buf(c):
        return pl.ds(c * hchunk, hchunk)
    flights = {}
    for c in range(chunks):
        amine[buf(c), :] = res[oth_rows(c), :].astype(bf)
        flights[1, c] = send(amine.at[buf(c), :], ain1.at[buf(c), :], sx, 3 + 3 * c, "tensor", core)
    for z in range(groups):
        for m in range(PAIR):
            d0 = (z * PAIR + m) * dcols
            gs[m, z, 0:2, :] = gacc[0:2, d0:d0 + dcols]
    gown[...] = gs[member]
    lowt[qc:qc + 256, :] = low[:, qc:qc + 256].T
    grad_cols(qc, 256)
    y_q.append(send(qsend.at[:, qc:qc + 256, :], qin.at[:, qc:qc + 256, :], sy, 3, "dp", pair))
    y_gain = send(gs.at[1 - member], gyi, sg, 0, "dp", pair)
    y_d = send(d_send, d_in, sy, 4, "dp", pair)
    for c in range(chunks):
        flights[1, c].wait()
        amid[buf(c), :] = (res[own_rows(c), :] + ain1[buf(c), :].astype(f32)).astype(bf)
        flights[2, c] = send(amid.at[buf(c), :], ain2.at[buf(c), :], sx, 4 + 3 * c, "tensor", across)
    w_x = cp(x_hbm, normed, 9)
    def send_q(j, r):
        y_q[j].wait()
        for z in range(groups):
            qown[z, r, :] = (qown[z, r, :].astype(f32) + qin[z, r, :].astype(f32)).astype(bf)
        w = cp(qown.at[group, r, :], qz.at[group, r, :], 14 + j)
        return w, [send(qown.at[at_group(s), r, :], qz.at[group, r, :], sz, (3 + j) * groups + s - 1, "dp", at_group(s) * PAIR + member) for s in range(1, groups)]
    w_q2, z_q = send_q(0, slice(0, qc))
    w_x.wait()
    def norm_one(r):
        v = normed[r, :].astype(f32)
        root = lax.rsqrt(jnp.mean(v * v, axis=1, keepdims=True) + EPS)
        up = gn[r, :].astype(f32) * gain1[...]
        mean = jnp.mean(up * v, axis=1, keepdims=True)
        low_res[r, :] = (resid[r, :] + root * up - v * (root * root * root * mean)).astype(bf)
    for c in range(chunks):
        flights[2, c].wait()
        gn[own_rows(c), :] = (amid[buf(c), :].astype(f32) + ain2[buf(c), :].astype(f32)).astype(bf)
        flights[3, c] = send(gn.at[own_rows(c), :], gn.at[own_rows(c), :], sx, 5 + 3 * c, "tensor", core)
        norm_one(own_rows(c))
        flights[3, c].wait()
        norm_one(oth_rows(c))
    w_gin = cp(low_res, gin_hbm, 1)
    w_kv2, z_kv = send_q(1, slice(qc, qc + 256))
    y_gain.wait()
    gown[...] = gown[...] + gyi[...]
    z_gain = [send(gown.at[at_group(s)], gzi.at[s - 1], sg, s, "dp", at_group(s) * PAIR + member) for s in range(1, groups)]
    for q in z_gain:
        q.wait()
    total = gown[group]
    for s in range(1, groups):
        total = total + gzi[s - 1]
    gt[0] = total
    t1 = send(gt.at[0], gti.at[0], sg, groups, "tensor", core)
    t1.wait()
    gt[1] = gt[0] + gti[0]
    t2 = send(gt.at[1], gti.at[1], sg, groups + 1, "tensor", across)
    t2.wait()
    gains_ref[...] = gt[1] + gti[1]
    for q in z_g + z_u + z_w + z_q + z_kv + [y_d, m3]:
        q.wait()
    for q in [w_g, w_u, w_w, w_gin, w_out, w_q2, w_kv2]:
        q.wait()

def backward(gn, residual, x, grad_output, mlp_part, normed, wo, wq, wk, wv, g_sum, u_own, u_send, d_send, mixed, q, kv, gain1, gain2, gain2_part,
             id_rows, ids_row, cosine, sine, n_dp, n_tensor):
    rows, width = x.shape
    groups = n_dp // PAIR
    share = g_sum.shape[1]
    dcols = width // n_dp
    qc = wq.shape[1]
    cols = qc + 256
    A = pl.BlockSpec(memory_space=pl.ANY)
    vm = pl.BlockSpec(memory_space=pltpu.VMEM)
    bf, f32 = jnp.bfloat16, jnp.float32
    sd = jax.ShapeDtypeStruct
    V = pltpu.VMEM
    D = pltpu.SemaphoreType.DMA
    half = rows // 2
    hrow = qc // n_dp
    act = V((rows, width), bf)
    return pl.pallas_call(
        functools.partial(backward_kernel, n_dp, n_tensor),
        out_shape=(sd((rows, width), bf), sd((rows, width), bf), sd((groups, share, dcols), bf), sd((groups, share, dcols), bf),
                   sd(d_send.shape, bf), sd((groups, hrow, width), bf), sd((groups, cols, dcols), bf), sd((8, dcols), f32)),
        in_specs=[A] * 17 + [vm] * 7,
        out_specs=(A,) * 7 + (vm,),
        scratch_shapes=[act, V((rows, width), f32), act, act, V((qc, width), bf), V((width, qc), bf), V((width, 128), bf), V((width, 128), bf),
                        V((rows, qc), bf), V((rows, qc), bf), V((2, rows, 256), bf), V((rows, width), f32), act, V((rows, qc), bf),
                        V((2, 2, 2 * rows, 128), bf), V((2, 2, 2 * rows, 128), bf), V((2, 2, 128, 2 * rows), bf),
                        V((2, 2, 2 * rows, 128), f32), V((2, 2, 2 * rows, 128), f32), V((2 * rows, 1), f32),
                        V((rows, cols), bf), V((cols, rows), bf), V((qc, 256), f32),
                        V((groups, hrow, width), bf), V((groups, hrow, width), bf), V((groups, hrow, width), bf),
                        V((share, dcols), bf), *[V((groups, share, dcols), bf)] * 3,
                        V((groups, cols, dcols), bf), V((groups, cols, dcols), bf), V((groups, cols, dcols), bf),
                        *[V((half, width), bf)] * 6,
                        V((rows, 256), bf), V((rows, 256), bf), V((8, width), f32), V((PAIR, groups, 8, dcols), f32), V((groups, 8, dcols), f32),
                        V((groups, 8, dcols), f32), V((groups - 1, 8, dcols), f32), V((2, 8, dcols), f32), V((2, 8, dcols), f32),
                        D((16,)), D((2, 5)), D((2, 5 * groups)), D((2, 3 + 3 * (rows // CHUNK))), D((2, 1)), D((2, groups + 2))],
        compiler_params=pltpu.CompilerParams(collective_id=4, has_side_effects=True, vmem_limit_bytes=67043328),
        cost_estimate=pl.CostEstimate(flops=4 * rows * width * (2 * qc + 256) + 40 * rows * rows * 5 * 128, bytes_accessed=40 * rows * width, transcendentals=8 * rows * rows),
        name="attention_backward",
    )(gn, residual, x, grad_output, mlp_part, normed, wo, wq, wk, wv, g_sum, u_own, u_send, d_send, mixed, q, kv,
      gain1.reshape(1, width), gain2.reshape(1, width), gain2_part, id_rows, ids_row, cosine, sine)

def finish_kernel(qc, kc, out_hbm, gin_hbm, gz_hbm, uz_hbm, d_own_hbm, d_in_hbm, wz_hbm, qz_hbm, gains,
                  gain1_o, gain2_o, out_o, gin_o, gate_o, up_o, down_o, wout_o, query_o, key_o, value_o,
                  act1, act2, gz, uz, d_own, d_in, wz, qz, gate, up, down, wout, query, key, value, ins, outs):
    f32 = jnp.float32
    groups, share, dcols = gz.shape
    gain1_o[...] = gains[0:1, :]
    gain2_o[...] = gains[1:2, :]
    loads = [pltpu.make_async_copy(s, d, ins.at[i]) for i, (s, d) in enumerate([
        (gz_hbm, gz), (uz_hbm, uz), (out_hbm, act1), (gin_hbm, act2), (d_own_hbm, d_own), (d_in_hbm, d_in), (wz_hbm, wz), (qz_hbm, qz)])]
    for c in loads:
        c.start()
    stores = []
    def store(src, dst):
        c = pltpu.make_async_copy(src, dst, outs.at[len(stores)])
        c.start()
        stores.append(c)
    for got, held, dst, i in ((gz, gate, gate_o, 0), (uz, up, up_o, 1)):
        loads[i].wait()
        for z in range(groups):
            for h in range(share // 256):
                held[:, z * share + h * 256:z * share + (h + 1) * 256] = got[z, h * 256:(h + 1) * 256, :].astype(f32).T
        store(held, dst)
    loads[2].wait()
    store(act1, out_o)
    loads[3].wait()
    store(act2, gin_o)
    loads[4].wait()
    loads[5].wait()
    down[...] = d_own[...].astype(f32) + d_in[...].astype(f32)
    store(down, down_o)
    loads[6].wait()
    acc = wz[0].astype(f32)
    for z in range(1, groups):
        acc = acc + wz[z].astype(f32)
    wout[...] = acc
    store(wout, wout_o)
    loads[7].wait()
    def total(r0, r1):
        acc = qz[0, r0:r1, :].astype(f32)
        for z in range(1, groups):
            acc = acc + qz[z, r0:r1, :].astype(f32)
        return acc.T
    for h in range(qc // 256):
        query[:, h * 256:(h + 1) * 256] = total(h * 256, (h + 1) * 256)
    key[...] = total(qc, qc + kc)
    value[...] = total(qc + kc, qc + 2 * kc)
    store(query, query_o)
    store(key, key_o)
    store(value, value_o)
    for c in stores:
        c.wait()

def finish_all(out, gin, gz, uz, d_own, d_in, wz, qz, gains, qc, kc):
    vm = pl.BlockSpec(memory_space=pltpu.VMEM)
    A = pl.BlockSpec(memory_space=pl.ANY)
    bf, f32 = jnp.bfloat16, jnp.float32
    sd = jax.ShapeDtypeStruct
    V = pltpu.VMEM
    groups, share, dcols = gz.shape
    shapes = [(dcols, groups * share), (dcols, groups * share), d_own.shape, wz.shape[1:], (dcols, qc), (dcols, kc), (dcols, kc)]
    return pl.pallas_call(
        functools.partial(finish_kernel, qc, kc),
        out_shape=(sd((1, dcols), f32), sd((1, dcols), f32), sd(out.shape, bf), sd(gin.shape, bf)) + tuple(sd(s, f32) for s in shapes),
        in_specs=[A] * 8 + [vm], out_specs=(vm,) * 2 + (A,) * 9,
        scratch_shapes=[V(a.shape, bf) for a in (out, gin, gz, uz, d_own, d_in, wz, qz)] + [V(s, f32) for s in shapes] + [pltpu.SemaphoreType.DMA((8,)), pltpu.SemaphoreType.DMA((9,))],
        compiler_params=pltpu.CompilerParams(vmem_limit_bytes=67043328),
        cost_estimate=pl.CostEstimate(flops=8 * out.size, bytes_accessed=24 << 20, transcendentals=0),
        name="finish",
    )(out, gin, gz, uz, d_own, d_in, wz, qz, gains)


def rope_table(half_count, copies=1):
    adjusted = []
    for index in range(half_count):
        base_value = 500000.0 ** (-index / half_count)
        wave_length = 2.0 * math.pi / base_value
        smooth = (8192.0 / wave_length - 1.0) / 3.0
        if wave_length > 8192.0:
            adjusted.append(base_value / 32.0)
        elif wave_length >= 2048.0:
            adjusted.append((1.0 - smooth) * base_value / 32.0 + smooth * base_value)
        else:
            adjusted.append(base_value)
    return jnp.asarray(adjusted * copies, dtype=jnp.float32)


def rope_angles(start_row, count_rows, half_count):
    positions = (start_row + jnp.arange(count_rows, dtype=jnp.int32)).astype(jnp.float32)
    phase_angle = positions[:, None] * rope_table(half_count)[None, :]
    return (jnp.cos(phase_angle)[:, None, :], jnp.sin(phase_angle)[:, None, :])


def rotate_halves(values, cosine_table, sine_values):
    half_size = values.shape[-1] // 2
    first_half = values[..., :half_size]
    second_half = values[..., half_size:]
    return jnp.concatenate(
        [
            first_half * cosine_table - second_half * sine_values,
            second_half * cosine_table + first_half * sine_values,
        ],
        axis=-1,
    )


def norm_rows(values, gain_row):
    inverse_root = lax.rsqrt(jnp.mean(values * values, axis=-1, keepdims=True) + NORM_EPSILON)
    return (inverse_root, values * inverse_root * gain_row)


def norm_back(values, inverse_root, gain_row, upstream):
    scaled = gain_row * upstream
    return inverse_root * scaled - values * inverse_root**3 * jnp.mean(
        scaled * values, axis=-1, keepdims=True
    )


def passed_along(block, axis, distance):
    devices = range(lax.axis_size(axis))
    route = [(i - distance, i) for i in devices if i - distance in devices]
    return lax.ppermute(block, axis, route)


def tensor_swap(block, bit):
    return lax.ppermute(block, "tensor", [(i, i ^ bit) for i in range(lax.axis_size("tensor"))])


def pair_swap(block):
    return lax.ppermute(block, "dp", [(i, i ^ 1) for i in range(lax.axis_size("dp"))])


def group_shift(block, distance):
    count = lax.axis_size("dp")
    groups = count // PAIR
    return lax.ppermute(
        block,
        "dp",
        [(i, ((i // PAIR + distance) % groups) * PAIR + i % PAIR) for i in range(count)],
    )


def tensor_sum(part):
    half = part.shape[1] // 2
    low = lax.axis_index("tensor") % 2
    first, second = part[:, :half], part[:, half:]
    mine = jnp.where(low == 0, first, second)
    other = jnp.where(low == 0, second, first).astype(jnp.bfloat16)
    mine = mine + tensor_swap(other, 1).astype(jnp.float32)
    bit = 2
    while bit < lax.axis_size("tensor"):
        rounded = mine.astype(jnp.bfloat16)
        mine = rounded.astype(jnp.float32) + tensor_swap(rounded, bit).astype(jnp.float32)
        bit *= 2
    mine = mine.astype(jnp.bfloat16)
    other = tensor_swap(mine, 1)
    return jnp.concatenate(
        [jnp.where(low == 0, mine, other), jnp.where(low == 0, other, mine)], axis=1
    ).astype(jnp.float32)


def gather_groups(block):
    half = block.shape[1] // 2
    low = lax.axis_index("tensor") % 2
    piece = lax.dynamic_slice_in_dim(block, low * half, half, axis=1)
    rows = [block]
    for _ in range(lax.axis_size("dp") // PAIR - 1):
        piece = group_shift(piece, 1)
        other = tensor_swap(piece, 1)
        rows.append(
            jnp.concatenate(
                [jnp.where(low == 0, piece, other), jnp.where(low == 0, other, piece)], axis=1
            )
        )
    return jnp.concatenate(rows, axis=0)


def pair_sum(part):
    member = lax.axis_index("dp") % PAIR
    mine = lax.dynamic_index_in_dim(part, member, 1, keepdims=False)
    other = lax.dynamic_index_in_dim(part, 1 - member, 1, keepdims=False)
    return mine + pair_swap(other.astype(jnp.bfloat16)).astype(jnp.float32)


def group_exchange(blocks):
    groups = blocks.shape[0]
    group = lax.axis_index("dp") // PAIR
    received = []
    for distance in range(groups):
        block = lax.dynamic_index_in_dim(blocks, (group + distance) % groups, 0, keepdims=False)
        received.append(block if distance == 0 else group_shift(block, distance))
    return received


def scatter_sum(part):
    summed = pair_sum(part)
    groups = summed.shape[0]
    group = lax.axis_index("dp") // PAIR
    total = lax.dynamic_index_in_dim(summed, group, 0, keepdims=False)
    rounded = summed.astype(jnp.bfloat16)
    for block in group_exchange(rounded)[1:]:
        total = total + block.astype(jnp.float32)
    return total


def block_scores(query_rows, key_rows, query_ids, key_ids, query_pos, key_pos):
    scores = jnp.einsum(
        "qgrd,kgd->grqk", query_rows, key_rows, preferred_element_type=jnp.float32
    ) * HEAD_SIZE ** (-0.5)
    allowed = (query_ids[:, None] == key_ids[None, :]) & (key_pos[None, :] <= query_pos[:, None])
    return jnp.where(allowed, scores, -1e30)


def block_forward(query_rows, key_rows, value_rows, query_ids, key_ids, query_pos, key_pos):
    scores = block_scores(query_rows, key_rows, query_ids, key_ids, query_pos, key_pos)
    row_peak = jnp.max(scores, axis=-1, keepdims=True)
    logsum = row_peak + jnp.log(jnp.sum(jnp.exp(scores - row_peak), axis=-1, keepdims=True))
    prob_low = jnp.exp(scores - logsum).astype(jnp.bfloat16)
    mixed_rows = jnp.einsum(
        "grqk,kgd->qgrd", prob_low, value_rows, preferred_element_type=jnp.float32
    )
    return (mixed_rows.astype(jnp.bfloat16), logsum)


def block_backward(
    query_rows,
    key_rows,
    value_rows,
    out_rows,
    grad_rows,
    logsum,
    query_ids,
    key_ids,
    query_pos,
    key_pos,
):
    scores = block_scores(query_rows, key_rows, query_ids, key_ids, query_pos, key_pos)
    prob_rows = jnp.exp(scores - logsum)
    grad_vals = jnp.einsum(
        "grqk,qgrd->kgd",
        prob_rows.astype(jnp.bfloat16),
        grad_rows,
        preferred_element_type=jnp.float32,
    )
    delta_rows = jnp.sum(out_rows.astype(jnp.float32) * grad_rows.astype(jnp.float32), axis=-1)
    grad_probs = jnp.einsum(
        "qgrd,kgd->grqk", grad_rows, value_rows, preferred_element_type=jnp.float32
    )
    grad_scores = (
        prob_rows * (grad_probs - jnp.transpose(delta_rows, (1, 2, 0))[..., None])
    ).astype(jnp.bfloat16)
    grad_query_rows = jnp.einsum(
        "grqk,kgd->qgrd", grad_scores, key_rows, preferred_element_type=jnp.float32
    ) * HEAD_SIZE ** (-0.5)
    grad_key_rows = jnp.einsum(
        "grqk,qgrd->kgd", grad_scores, query_rows, preferred_element_type=jnp.float32
    ) * HEAD_SIZE ** (-0.5)
    return (grad_query_rows, grad_key_rows, grad_vals)


def dot(form, left, right):
    return jnp.einsum(form, left, right, preferred_element_type=jnp.float32)


def gated(gate_value, up_value):
    return (jax.nn.silu(gate_value) * up_value).astype(jnp.bfloat16)


def gated_back(grad_hidden, gate_value, up_value):
    sigmoid_gate = jax.nn.sigmoid(gate_value)
    grad_gate_low = (
        grad_hidden * up_value * sigmoid_gate * (1.0 + gate_value * (1.0 - sigmoid_gate))
    ).astype(jnp.bfloat16)
    return grad_gate_low, (grad_hidden * jax.nn.silu(gate_value)).astype(jnp.bfloat16)


def shards_plain(
    inputs,
    norm1_gain,
    query_weight,
    key_weight,
    value_weight,
    w_out,
    norm2_gain,
    w_gate,
    w_up,
    w_down,
    doc_ids,
    grad_output,
):
    tok_rows, width = inputs.shape
    heads_here = query_weight.shape[1] // HEAD_SIZE
    kv_here = key_weight.shape[1] // HEAD_SIZE
    group_size = heads_here // kv_here
    n_dp = lax.axis_size("dp")
    groups = n_dp // PAIR
    group = lax.axis_index("dp") // PAIR
    offset = lax.axis_index("dp") * tok_rows
    grad_all = gather_groups(grad_output)

    cosine_table, sine_values = rope_angles(offset, tok_rows, HEAD_SIZE // 2)
    inputs_wide = inputs.astype(jnp.float32)
    root_one, normed = norm_rows(inputs_wide, norm1_gain)
    normed_low = normed.astype(jnp.bfloat16)
    query_raw = dot("td,dh->th", normed_low, query_weight).reshape(tok_rows, heads_here, HEAD_SIZE)
    key_raw = dot("td,dh->th", normed_low, key_weight).reshape(tok_rows, kv_here, HEAD_SIZE)
    value_low = dot("td,dh->th", normed_low, value_weight).astype(jnp.bfloat16)
    query_low = (
        rotate_halves(query_raw, cosine_table, sine_values)
        .astype(jnp.bfloat16)
        .reshape(tok_rows, kv_here, group_size, HEAD_SIZE)
    )
    key_low = (
        rotate_halves(key_raw, cosine_table, sine_values)
        .astype(jnp.bfloat16)
        .reshape(tok_rows, kv_here * HEAD_SIZE)
    )
    query_ids = doc_ids + 1
    tail = jnp.concatenate([key_low, value_low], axis=1)
    prev_tail = passed_along(tail, "dp", 1)
    prev_ids = passed_along(query_ids, "dp", 1)
    both = jnp.concatenate([prev_tail, tail], axis=0)
    keys_all = both[:, : kv_here * HEAD_SIZE].reshape(2 * DOC_MAX, kv_here, HEAD_SIZE)
    values_all = both[:, kv_here * HEAD_SIZE :].reshape(2 * DOC_MAX, kv_here, HEAD_SIZE)
    ids_all = jnp.concatenate([prev_ids, query_ids])
    pos_all = offset - DOC_MAX + jnp.arange(tok_rows + DOC_MAX, dtype=jnp.int32)
    query_pos = pos_all[DOC_MAX:]
    mixed_block, logsum_block = block_forward(
        query_low, keys_all, values_all, query_ids, ids_all, query_pos, pos_all
    )
    mixed_low = mixed_block.reshape(tok_rows, heads_here * HEAD_SIZE)
    residual = inputs_wide + tensor_sum(dot("te,ed->td", mixed_low, w_out))

    root_two, normed_two = norm_rows(residual, norm2_gain)
    normed_two_low = normed_two.astype(jnp.bfloat16)
    normed_all = gather_groups(normed_two_low)
    gate_value = dot("td,df->tf", normed_two_low, w_gate)
    up_value = dot("td,df->tf", normed_two_low, w_up)
    grad_hidden = dot("td,fd->tf", grad_output, w_down)
    hidden_low = gated(gate_value, up_value)
    grad_gate_low, grad_up_low = gated_back(grad_hidden, gate_value, up_value)
    normed_two_part = dot("tf,df->td", grad_gate_low, w_gate) + dot("tf,df->td", grad_up_low, w_up)
    grad_normed_two = tensor_sum(normed_two_part)
    gain_two_part = jnp.sum(normed_two_part * residual * root_two, axis=0)
    output = (residual + tensor_sum(dot("tf,fd->td", hidden_low, w_down))).astype(jnp.bfloat16)

    share = w_gate.shape[1] // groups
    gate_share = lax.dynamic_slice_in_dim(w_gate, group * share, share, axis=1)
    up_share = lax.dynamic_slice_in_dim(w_up, group * share, share, axis=1)
    down_share = lax.dynamic_slice_in_dim(w_down, group * share, share, axis=0)
    gate_all = dot("td,df->tf", normed_all, gate_share)
    up_all = dot("td,df->tf", normed_all, up_share)
    grad_hidden_all = dot("td,fd->tf", grad_all, down_share)
    hidden_all = gated(gate_all, up_all)
    gate_low_all, up_low_all = gated_back(grad_hidden_all, gate_all, up_all)
    down_part = dot("tf,td->fd", hidden_all, grad_all)
    grad_wdown = pair_sum(down_part.reshape(1, PAIR, share // PAIR, width))[0]
    rows_here = width // n_dp

    def column_grad(low_all):
        part = dot("td,tf->df", normed_all, low_all)
        summed = pair_sum(part.reshape(groups, PAIR, rows_here, share)).astype(jnp.bfloat16)
        full = jnp.zeros((rows_here, groups * share), jnp.float32)
        for distance, block in enumerate(group_exchange(summed)):
            full = lax.dynamic_update_slice_in_dim(
                full, block.astype(jnp.float32), ((group - distance) % groups) * share, axis=1
            )
        return full

    grad_wgate = column_grad(gate_low_all)
    grad_wup = column_grad(up_low_all)

    grad_residual = grad_output.astype(jnp.float32) + norm_back(
        residual, root_two, norm2_gain, grad_normed_two
    )
    grad_res_low = grad_residual.astype(jnp.bfloat16)
    wout_part = dot("te,td->ed", mixed_low, grad_res_low)
    grad_wout = scatter_sum(wout_part.reshape(groups, PAIR, -1, width))
    grad_mixed = (
        dot("td,ed->te", grad_res_low, w_out)
        .astype(jnp.bfloat16)
        .reshape(tok_rows, kv_here, group_size, HEAD_SIZE)
    )
    mixed_view = mixed_low.reshape(tok_rows, kv_here, group_size, HEAD_SIZE)
    grad_query_rows, grad_key_rows, grad_value_rows = block_backward(
        query_low,
        keys_all,
        values_all,
        mixed_view,
        grad_mixed,
        logsum_block,
        query_ids,
        ids_all,
        query_pos,
        pos_all,
    )
    sent = jnp.concatenate(
        [
            grad_key_rows.reshape(2 * DOC_MAX, kv_here * HEAD_SIZE),
            grad_value_rows.reshape(2 * DOC_MAX, kv_here * HEAD_SIZE),
        ],
        axis=1,
    )
    back = passed_along(sent[:DOC_MAX].astype(jnp.bfloat16), "dp", -1).astype(jnp.float32)
    own = sent[DOC_MAX:] + back
    grad_qraw = grad_query_rows.reshape(tok_rows, heads_here, HEAD_SIZE)
    query_low_gradient = (
        rotate_halves(grad_qraw, cosine_table, -sine_values)
        .astype(jnp.bfloat16)
        .reshape(tok_rows, heads_here * HEAD_SIZE)
    )
    key_low_gradient = (
        rotate_halves(
            own[:, : kv_here * HEAD_SIZE].reshape(tok_rows, kv_here, HEAD_SIZE),
            cosine_table,
            -sine_values,
        )
        .astype(jnp.bfloat16)
        .reshape(tok_rows, kv_here * HEAD_SIZE)
    )
    value_low_gradient = own[:, kv_here * HEAD_SIZE :].astype(jnp.bfloat16)
    low_gradient = jnp.concatenate(
        [query_low_gradient, key_low_gradient, value_low_gradient], axis=1
    )
    normed_one_part = (
        dot("kl,ql->kq", query_low_gradient, query_weight)
        + dot("kl,ql->kq", key_low_gradient, key_weight)
        + dot("kl,ql->kq", value_low_gradient, value_weight)
    )
    grad_normed_one = tensor_sum(normed_one_part)
    gain_one_part = jnp.sum(normed_one_part * inputs_wide * root_one, axis=0)
    qkv_part = dot("wj,wq->jq", normed_low, low_gradient)
    columns = qkv_part.shape[1]
    gains = jnp.stack(
        [gain_one_part.reshape(n_dp, rows_here), gain_two_part.reshape(n_dp, rows_here)], axis=1
    )
    gains = jnp.pad(gains, ((0, 0), (0, 14), (0, columns - rows_here)))
    qkv_part = jnp.concatenate([qkv_part.reshape(n_dp, rows_here, columns), gains], axis=1)
    qkv_sum = scatter_sum(qkv_part.reshape(groups, PAIR, rows_here + 16, columns))
    grad_qkv = qkv_sum[:rows_here]
    gain_sums = qkv_sum[rows_here : rows_here + 16, :rows_here]
    bit = 1
    while bit < lax.axis_size("tensor"):
        gain_sums = gain_sums + tensor_swap(gain_sums, bit)
        bit *= 2
    grad_input_norm = norm_back(inputs_wide, root_one, norm1_gain, grad_normed_one)
    grad_inputs = (grad_residual + grad_input_norm).astype(jnp.bfloat16)
    q_columns = query_weight.shape[1]
    k_columns = key_weight.shape[1]
    return (
        output,
        grad_inputs,
        gain_sums[0],
        grad_qkv[:, :q_columns],
        grad_qkv[:, q_columns : q_columns + k_columns],
        grad_qkv[:, q_columns + k_columns :],
        grad_wout,
        gain_sums[1],
        grad_wgate,
        grad_wup,
        grad_wdown,
    )


def shards(
    inputs,
    norm1_gain,
    query_weight,
    key_weight,
    value_weight,
    w_out,
    norm2_gain,
    w_gate,
    w_up,
    w_down,
    doc_ids,
    grad_output,
):
    tok_rows, width = inputs.shape
    heads_here = query_weight.shape[1] // HEAD_SIZE
    kv_here = key_weight.shape[1] // HEAD_SIZE
    group_size = heads_here // kv_here
    n_dp = lax.axis_size("dp")
    groups = n_dp // PAIR
    group = lax.axis_index("dp") // PAIR
    offset = lax.axis_index("dp") * tok_rows
    n_tensor = lax.axis_size("tensor")
    half = HEAD_SIZE // 2
    lanes = jnp.arange(4 * half, dtype=jnp.int32)
    positions = (offset + jnp.arange(tok_rows, dtype=jnp.int32)).astype(jnp.float32)
    angles = positions[:, None] * rope_table(half, 4)[None, :]
    cosine = jnp.cos(angles)
    sine = jnp.sin(angles) * jnp.where(lanes % HEAD_SIZE < half, -1.0, 1.0)[None, :]
    normed_low, query_scaled, kv, id_rows, mixed_low, residual, normed_two_low, gate_t, up_t, part_g, cross_g = attend_forward(
        inputs, norm1_gain, query_weight, key_weight, value_weight, w_out, norm2_gain, cosine, sine, doc_ids, grad_output,
        w_gate, w_up, n_dp, n_tensor)
    mlp_part, back_part, normed_rest, rest_g, gain_two_part = mlp(normed_two_low, grad_output, part_g, cross_g, w_gate, w_up, w_down, n_dp, n_tensor)
    d_own, d_send, g_sum, u_own, u_send, grad_normed_two = wgrad(
        normed_two_low, normed_rest, grad_output, part_g, cross_g, rest_g, gate_t, up_t, w_down, back_part, n_dp, n_tensor)
    output, grad_inputs, gate_blocks, up_blocks, d_in, wout_blocks, qkv_blocks, gain_sums = backward(
        grad_normed_two, residual, inputs, grad_output, mlp_part, normed_low, w_out, query_weight, key_weight, value_weight,
        g_sum, u_own, u_send, d_send, mixed_low, query_scaled, kv, norm1_gain, norm2_gain, gain_two_part,
        id_rows, doc_ids.reshape(1, tok_rows), cosine, sine, n_dp, n_tensor)
    gain_one, gain_two, output, grad_inputs, grad_wgate, grad_wup, grad_wdown, grad_wout, grad_wquery, grad_wkey, grad_wvalue = finish_all(
        output, grad_inputs, gate_blocks, up_blocks, d_own, d_in, wout_blocks, qkv_blocks, gain_sums, query_weight.shape[1], key_weight.shape[1])
    rows_here = width // n_dp
    return (
        output,
        grad_inputs,
        gain_one.reshape(rows_here),
        grad_wquery,
        grad_wkey,
        grad_wvalue,
        grad_wout,
        gain_two.reshape(rows_here),
        grad_wgate,
        grad_wup,
        grad_wdown,
    )


def kernels_fit(mesh, *args):
    n_dp, n_tensor = mesh.shape["dp"], mesh.shape["tensor"]
    width = args[0].shape[1]
    return (
        n_dp % PAIR == 0
        and n_dp // PAIR <= 4
        and n_tensor == 4
        and width // n_dp in (128, 256)
        and args[7].shape[1] // n_tensor // (n_dp // PAIR) % 256 == 0
        and args[0].shape[0] // n_dp == DOC_MAX
        and args[3].shape[1] // n_tensor == 2 * HEAD_SIZE
        and args[2].shape[1] == 4 * args[3].shape[1]
    )


def solution(mesh):
    def step(*args):
        return mapped(mesh, shards if kernels_fit(mesh, *args) else shards_plain)(*args)

    return step


def mapped(mesh, function):
    return jax.shard_map(
        function,
        mesh=mesh,
        in_specs=(
            P("dp", None),
            P(),
            P(None, "tensor"),
            P(None, "tensor"),
            P(None, "tensor"),
            P("tensor", None),
            P(),
            P(None, "tensor"),
            P(None, "tensor"),
            P("tensor", None),
            P("dp"),
            P("dp", None),
        ),
        out_specs=(
            P("dp", None),
            P("dp", None),
            P("dp"),
            P("dp", "tensor"),
            P("dp", "tensor"),
            P("dp", "tensor"),
            P(("tensor", "dp"), None),
            P("dp"),
            P("dp", "tensor"),
            P("dp", "tensor"),
            P(("tensor", "dp"), None),
        ),
        check_vma=False,
    )
```

```python
import functools
import math

import jax
import jax.numpy as jnp
from jax import lax
from jax.experimental import pallas as pl
from jax.experimental.pallas import tpu as pltpu
from jax.sharding import PartitionSpec as P

HEAD_SIZE = 64
DOC_MAX = 512
NORM_EPSILON = 1e-05

PAIR = 2
MESH = pl.DeviceIdType.MESH
EPS = NORM_EPSILON


def nn(a, b):
    return lax.dot_general(a, b, (((1,), (0,)), ((), ())), preferred_element_type=jnp.float32)
def nt(a, b):
    return lax.dot_general(a, b, (((1,), (1,)), ((), ())), preferred_element_type=jnp.float32)

def flip(index, bit):
    return index + bit - 2 * bit * ((index // bit) % 2)

def meet(*partners):
    barrier = pltpu.get_barrier_semaphore()
    for axis, index in partners:
        pl.semaphore_signal(barrier, inc=1, device_id={axis: index}, device_id_type=MESH)
    pl.semaphore_wait(barrier, len(partners))

def remote(src, dst, sems, slot, axis, index):
    return pltpu.make_async_remote_copy(
        src_ref=src, dst_ref=dst, send_sem=sems.at[0, slot], recv_sem=sems.at[1, slot],
        device_id={axis: index}, device_id_type=MESH)

def send(src, dst, sems, slot, axis, index):
    copy = remote(src, dst, sems, slot, axis, index)
    copy.start()
    return copy

def swiglu(gate, up, grad):
    sig = 0.5 * (1.0 + jnp.tanh(0.5 * gate))
    silu = gate * sig
    hidden = (silu * up).astype(jnp.bfloat16)
    grad_gate = (grad * up * sig * (1.0 + gate * (1.0 - sig))).astype(jnp.bfloat16)
    grad_up = (grad * silu).astype(jnp.bfloat16)
    return hidden, grad_gate, grad_up

def mlp_kernel(n_dp, n_tensor, normed_hbm, grad_hbm, part_g, cross_g, gate_hbm, up_hbm, down_hbm,
               out_ref, back_ref, all_hbm, rest_g, gain_ref,
               normed, grad, gate_w, up_w, down_w, hid, low_gate, low_up, load, far):
    rows, width = normed.shape
    cols = gate_w.shape[1]
    groups = n_dp // PAIR
    me_dp, me_t = lax.axis_index("dp"), lax.axis_index("tensor")
    right = lax.rem(me_dp + PAIR, n_dp)
    left = lax.rem(me_dp + n_dp - PAIR, n_dp)
    core, across = flip(me_t, 1), flip(me_t, 2)
    tile = 256
    tiles = cols // tile
    def cp(s, d, i):
        return pltpu.make_async_copy(s, d, load.at[i])
    def gate_tile(c, f):
        return cp(gate_hbm.at[:, c], gate_w.at[:, c], 2 + 3 * f)
    def up_tile(c, f):
        return cp(up_hbm.at[:, c], up_w.at[:, c], 3 + 3 * f)
    def down_tile(c, f):
        return cp(down_hbm.at[c, :], down_w.at[c, :], 4 + 3 * f)
    cp(normed_hbm, normed, 0).start()
    def load_tile(f):
        c = pl.ds(pl.multiple_of(f * tile, tile), tile)
        gate_tile(c, f).start()
        up_tile(c, f).start()
        down_tile(c, f).start()
    load_tile(0)
    cp(grad_hbm, grad, 1).start()
    for f in range(1, tiles):
        load_tile(f)
    meet(("dp", right), ("dp", left), ("tensor", core), ("tensor", across))
    piece = rows // n_tensor
    def part(t):
        return pl.ds(pl.multiple_of(t * piece, piece), piece)
    steps = groups - 1
    per = 4
    def ring(s):
        src = (normed_hbm if s == 1 else all_hbm.at[s - 2]).at[part(me_t), :]
        return send(src, all_hbm.at[s - 1].at[part(me_t), :], far, s * per, "dp", right)
    def spread_n(s, level):
        block = all_hbm.at[s - 1]
        held, other = [me_t, across][:level + 1], [across, core][level]
        return [send(block.at[part(h), :], block.at[part(h), :], far, s * per + 1 + level + i, "tensor", other) for i, h in enumerate(held)]
    def spread_g(b, level):
        base = (steps + 1 + b) * per
        if level == 0:
            return [send(part_g.at[b], rest_g.at[b].at[part(me_t), :], far, base, "tensor", across)]
        cross = cross_g if b == 0 else rest_g.at[b].at[part(across), :]
        return [send(part_g.at[b], rest_g.at[b].at[part(me_t), :], far, base + 1, "tensor", core),
                send(cross, rest_g.at[b].at[part(across), :], far, base + 2, "tensor", core)]
    def wait(copies):
        for c in copies:
            c.wait()

    ring_n = ring(1)
    g_core = spread_g(0, 1)
    g_x = {}
    last_g = steps - 1 if steps > 1 else steps
    if last_g > 1:
        g_x[1] = spread_g(1, 0)

    cp(normed_hbm, normed, 0).wait()
    cp(grad_hbm, grad, 1).wait()
    def first(f, _):
        c = pl.ds(pl.multiple_of(f * tile, tile), tile)
        gate_tile(c, f).wait()
        up_tile(c, f).wait()
        down_tile(c, f).wait()
        g = nn(normed[...], gate_w[:, c])
        u = nn(normed[...], up_w[:, c])
        h = nt(grad[...], down_w[c, :])
        a, b, d = swiglu(g, u, h)
        hid[:, c] = a
        low_gate[:, c] = b
        low_up[:, c] = d
        return 0
    early = min(5, tiles)
    n_x = {}
    def pass_g(b):
        nonlocal g_core
        if b in g_x:
            wait(g_x.pop(b))
            g_core = g_core + spread_g(b, 1)
            if b + 1 < last_g:
                g_x[b + 1] = spread_g(b + 1, 0)
    lax.fori_loop(0, early, first, 0)
    ring_n.wait()
    if steps > 1:
        ring_n = ring(2)
    pass_g(1)
    n_x[1] = spread_n(1, 0)
    lax.fori_loop(early, tiles, first, 0)
    wtile = 256
    wtiles = width // wtile
    def second(j, _):
        c = pl.ds(pl.multiple_of(j * wtile, wtile), wtile)
        b = nt(low_gate[...], gate_w[c, :]) + nt(low_up[...], up_w[c, :])
        back_ref[:, c] = b.astype(back_ref.dtype)
        gain_ref[0:1, c] = jnp.sum(b * normed[:, c].astype(jnp.float32), axis=0, keepdims=True)
        return 0
    def third(j, _):
        c = pl.ds(pl.multiple_of(j * wtile, wtile), wtile)
        out_ref[:, c] = nn(hid[...], down_w[:, c]).astype(out_ref.dtype)
        return 0
    lax.fori_loop(0, wtiles, third, 0)
    n_core = []
    def pass_n(s):
        nonlocal n_core
        if s in n_x:
            wait(n_x.pop(s))
            n_core = n_core + spread_n(s, 1)
    if steps > 1:
        ring_n.wait()
        if steps > 2:
            ring_n = ring(3)
            n_x[2] = spread_n(2, 0)
    pass_g(2)
    lax.fori_loop(0, wtiles // 2, second, 0)
    pass_n(1)
    lax.fori_loop(wtiles // 2, wtiles, second, 0)
    for s in range(3, steps + 1):
        ring_n.wait()
        if s < steps:
            ring_n = ring(s + 1)
            n_x[s] = spread_n(s, 0)
    for b in range(3, steps):
        pass_g(b)
    for s in range(2, steps):
        pass_n(s)
    wait(n_core)
    wait(g_core)

def mlp(normed, grad_output, part_g, cross_g, w_gate, w_up, w_down, n_dp, n_tensor):
    rows, width = normed.shape
    cols = w_gate.shape[1]
    groups = n_dp // PAIR
    tiles = cols // 256
    anyspec = pl.BlockSpec(memory_space=pl.ANY)
    vm = pl.BlockSpec(memory_space=pltpu.VMEM)
    bf = jnp.bfloat16
    return pl.pallas_call(
        functools.partial(mlp_kernel, n_dp, n_tensor),
        out_shape=(jax.ShapeDtypeStruct((rows, width), bf), jax.ShapeDtypeStruct((rows, width), bf),
                   jax.ShapeDtypeStruct((groups - 1, rows, width), bf), jax.ShapeDtypeStruct((groups - 1, rows, width), bf), jax.ShapeDtypeStruct((1, width), jnp.float32)),
        in_specs=[anyspec] * 7, out_specs=(vm, vm, anyspec, anyspec, vm),
        scratch_shapes=[pltpu.VMEM((rows, width), bf), pltpu.VMEM((rows, width), bf),
                        pltpu.VMEM((width, cols), bf), pltpu.VMEM((width, cols), bf), pltpu.VMEM((cols, width), bf),
                        pltpu.VMEM((rows, cols), bf), pltpu.VMEM((rows, cols), bf), pltpu.VMEM((rows, cols), bf),
                        pltpu.SemaphoreType.DMA((2 + 3 * tiles,)),
                        pltpu.SemaphoreType.DMA((2, 8 * groups)),
                        ],
        compiler_params=pltpu.CompilerParams(collective_id=2, has_side_effects=True, vmem_limit_bytes=60 << 20),
        cost_estimate=pl.CostEstimate(flops=12 * rows * width * cols, bytes_accessed=2 * (3 * width * cols + 8 * rows * width), transcendentals=rows * cols),
        name="feed_forward",
    )(normed, grad_output, part_g, cross_g, w_gate, w_up, w_down)

def wgrad_kernel(n_dp, n_tensor, own_n, all_n, own_g, part_g, cross_g, rest_g, gate_t, up_t, down_hbm, back_hbm, first_hbm,
                 d_own_o, d_send_o, g_sum_o, u_own_o, u_send_o, sum_o, first_o,
                 d_own, d_send, g_sum, u_own, u_send, sum_ref, g_own, g_send, g_in, n_all, g_all, wg, wu, wd, hid, lowg, lowu, mine, in1, mid, in2, load, far, ar, sy, outs):
    rows, width = own_n.shape
    share = gate_t.shape[0]
    groups = n_dp // PAIR
    me_dp, me_t = lax.axis_index("dp"), lax.axis_index("tensor")
    member = lax.rem(me_dp, PAIR)
    bits = []
    bit = n_tensor // 2
    while bit:
        bits.append(bit); bit //= 2
    piece = rows // n_tensor
    def part(t):
        return pl.ds(pl.multiple_of(t * piece, piece), piece)
    def at(r, t):
        return pl.ds(pl.multiple_of(r * rows + t * piece, piece), piece)
    count = [0]
    def cp(s, d):
        c = pltpu.make_async_copy(s, d, load.at[count[0]]); count[0] += 1
        c.start(); return c
    half = rows // 2
    low = lax.rem(me_t, 2)
    def half_rows(c):
        return pl.ds(pl.multiple_of(c * half, half), half)
    last = groups - 1
    if last > 0:
        w_last = cp(all_n.at[last - 1].at[part(me_t), :], n_all.at[at(last, me_t), :])
    w1 = [cp(gate_t, wg), cp(own_n, n_all.at[pl.ds(0, rows), :])]
    w2 = [cp(up_t, wu)]
    w3 = [cp(down_hbm.at[pl.ds(pl.multiple_of(me_dp // PAIR * share, share), share), :], wd), cp(own_g, g_all.at[pl.ds(0, rows), :])]
    w4 = [cp(back_hbm.at[half_rows(low), :], mine)]
    first_block = count[0]
    def load_block(r):
        i = first_block + (r - 1) * (1 + n_tensor)
        def one(s, d, j):
            return pltpu.make_async_copy(s, d, load.at[i + j])
        out = []
        if r < last:
            out.append(one(all_n.at[r - 1], n_all.at[pl.ds(r * rows, rows), :], 0))
        out.append(one(part_g.at[r - 1], g_all.at[at(r, me_t), :], 1))
        if r == last and last > 1:
            return out
        for j, h in enumerate((flip(me_t, 1), flip(me_t, 2), flip(flip(me_t, 1), 2))):
            src = cross_g if r == 1 and j == 1 else rest_g.at[r - 1].at[part(h), :]
            out.append(one(src, g_all.at[at(r, h), :], 2 + j))
        return out
    def start(cs):
        for c in cs:
            c.start()
    pair = flip(me_dp, 1)
    core, across = flip(me_t, 1), flip(me_t, 2)
    right, left = lax.rem(me_dp + PAIR, n_dp), lax.rem(me_dp + n_dp - PAIR, n_dp)
    meet(("dp", pair), ("dp", right), ("dp", left), ("tensor", core), ("tensor", across))
    last_g = []
    if last > 1:
        src = cross_g if last == 2 else rest_g.at[last - 2].at[part(across), :]
        last_g = [lambda: remote(src, g_all.at[at(last, across), :], far, 3, "dp", right),
                  lambda: remote(part_g.at[last - 1], g_all.at[at(last, me_t), :], far, 4, "tensor", core),
                  lambda: remote(g_all.at[at(last, across), :], g_all.at[at(last, across), :], far, 5, "tensor", core)]
        last_g[0]().start()
    def ring(k):
        src = first_hbm.at[part(me_t), :] if k == 1 else first_o.at[k - 2]
        return remote(src, first_o.at[k - 1], far, 5 + k, "dp", right)
    if last > 0:
        ring(1).start()
    ar1 = send(back_hbm.at[half_rows(1 - low), :], in1, ar, 0, "tensor", core)
    def wait(cs):
        for c in cs:
            c.wait()
    def spread(level):
        held, other = [me_t, across][:level + 1], [across, core][level]
        return [remote(n_all.at[at(last, h), :], n_all.at[at(last, h), :], far, level + i, "tensor", other) for i, h in enumerate(held)]
    if last > 0:
        w_last.wait()
        start(spread(0))
    if last > 1:
        last_g[1]().start()

    sum2 = lambda: remote(mid, in2, ar, 1, "tensor", across)
    def pass_a(r, _):
        for k in range(groups):
            @pl.when(r == k)
            def _():
                if k == 0:
                    wait(w1)
                    wait(w2)
                    wait(w3)
                else:
                    wait(load_block(k))
                if k < last:
                    start(load_block(k + 1))
                if k == max(last - 1, 1):
                    wait(spread(0))
                    start(spread(1))
                    if last > 1:
                        last_g[0]().wait()
                        last_g[2]().start()
                    sum2().start()
                if k == last:
                    wait(spread(1))
                    if last > 1:
                        last_g[1]().wait()
                        last_g[2]().wait()
        rs = pl.ds(pl.multiple_of(r * rows, rows), rows)
        g = nt(wg[...], n_all[rs, :])
        u = nt(wu[...], n_all[rs, :])
        h = nt(wd[...], g_all[rs, :])
        a, b, d = swiglu(g, u, h)
        hid[:, rs] = a
        lowg[:, rs] = b
        lowu[:, rs] = d
        @pl.when(r == 0)
        def _():
            wait(w4)
            ar1.wait()
            mid[...] = (mine[...].astype(jnp.float32) + in1[...].astype(jnp.float32)).astype(jnp.bfloat16)
        return 0
    lax.fori_loop(0, groups, pass_a, 0)
    ar2 = sum2()
    dcols = width // n_dp
    def col_tile(low_ref, own_ref, send_ref):
        def body(q, _):
            a = pl.ds(pl.multiple_of((q * PAIR + member) * dcols, dcols), dcols)
            b = pl.ds(pl.multiple_of((q * PAIR + 1 - member) * dcols, dcols), dcols)
            send_ref[q] = nn(low_ref[...], n_all[:, b]).astype(jnp.bfloat16)
            own_ref[q] = nn(low_ref[...], n_all[:, a]).astype(jnp.bfloat16)
            return 0
        return body
    def to_pair(q):
        return remote(g_send.at[q], g_in.at[q], sy, q, "dp", pair)
    def gate_tile(q, _):
        col_tile(lowg, g_own, g_send)(q, 0)
        to_pair(q).start()
        @pl.when(q == 1)
        def _():
            if last > 1:
                ring(1).wait()
                ring(2).start()
        return 0
    lax.fori_loop(0, groups, gate_tile, 0)
    hrows = share // PAIR
    def down_tile(j, _):
        c = pl.ds(pl.multiple_of(j * 512, 512), 512)
        d_send[:, c] = nn(hid[pl.ds(pl.multiple_of((1 - member) * hrows, hrows), hrows), :], g_all[:, c]).astype(jnp.bfloat16)
        d_own[:, c] = nn(hid[pl.ds(pl.multiple_of(member * hrows, hrows), hrows), :], g_all[:, c]).astype(jnp.bfloat16)
        return 0
    lax.fori_loop(0, width // 512, down_tile, 0)
    stores = []
    def store(src, dst):
        c = pltpu.make_async_copy(src, dst, outs.at[len(stores)])
        c.start()
        stores.append(c)
    store(d_own, d_own_o)
    store(d_send, d_send_o)
    def up_tile(q, _):
        @pl.when(q == groups // 2)
        def _():
            if last > 2:
                ring(2).wait()
                ring(3).start()
        return col_tile(lowu, u_own, u_send)(q, 0)
    lax.fori_loop(0, groups, up_tile, 0)
    store(u_own, u_own_o)
    store(u_send, u_send_o)
    ar2.wait()
    sum_ref[half_rows(low), :] = (mid[...].astype(jnp.float32) + in2[...].astype(jnp.float32)).astype(jnp.bfloat16)
    ar3 = send(sum_ref.at[half_rows(low), :], sum_ref.at[half_rows(low), :], ar, 2, "tensor", core)
    for q in range(groups):
        to_pair(q).wait()
        g_sum[q] = (g_own[q].astype(jnp.float32) + g_in[q].astype(jnp.float32)).astype(jnp.bfloat16)
    store(g_sum, g_sum_o)
    ar3.wait()
    store(sum_ref, sum_o)
    if last > 0:
        ring(last).wait()
    wait(stores)

def wgrad(own_n, all_n, own_g, part_g, cross_g, rest_g, gate_t, up_t, down, back, first, n_dp, n_tensor):
    rows, width = own_n.shape
    share = gate_t.shape[0]
    groups = n_dp // PAIR
    anyspec = pl.BlockSpec(memory_space=pl.ANY)
    vm = pl.BlockSpec(memory_space=pltpu.VMEM)
    bf, f32 = jnp.bfloat16, jnp.float32
    sd = jax.ShapeDtypeStruct
    dcols = width // n_dp
    V = pltpu.VMEM
    tall = groups * rows
    return pl.pallas_call(
        functools.partial(wgrad_kernel, n_dp, n_tensor),
        out_shape=(sd((share // PAIR, width), bf), sd((share // PAIR, width), bf), sd((groups, share, dcols), bf),
                   sd((groups, share, dcols), bf), sd((groups, share, dcols), bf), sd((rows, width), bf),
                   sd((groups - 1, rows // n_tensor, width), bf)),
        in_specs=[anyspec] * 11, out_specs=(anyspec,) * 7,
        scratch_shapes=[*[V((share // PAIR, width), bf)] * 2, *[V((groups, share, dcols), bf)] * 3, V((rows, width), bf), *[V((groups, share, dcols), bf)] * 3, V((tall, width), bf), V((tall, width), bf),
                        V((share, width), bf), V((share, width), bf), V((share, width), bf),
                        V((share, tall), bf), V((share, tall), bf), V((share, tall), bf),
                        *[V((rows // 2, width), bf)] * 4,
                        pltpu.SemaphoreType.DMA((7 + (groups - 1) * (1 + n_tensor),)),
                        pltpu.SemaphoreType.DMA((2, 6 + groups)), pltpu.SemaphoreType.DMA((2, 3)), pltpu.SemaphoreType.DMA((2, groups)), pltpu.SemaphoreType.DMA((6,))],
        compiler_params=pltpu.CompilerParams(collective_id=3, has_side_effects=True, vmem_limit_bytes=62 << 20),
        cost_estimate=pl.CostEstimate(flops=12 * tall * width * share, bytes_accessed=2 * (3 * width * share + 4 * tall * width), transcendentals=tall * share),
        name="weight_gradients",
    )(own_n, all_n, own_g, part_g, cross_g, rest_g, gate_t, up_t, down, back, first)
TILE = 128
CHUNK = 128

def turn(values, cosine, sine):
    lane = lax.broadcasted_iota(jnp.int32, values.shape, 1)
    swapped = jnp.where(lane % HEAD_SIZE < HEAD_SIZE // 2,
                        pltpu.roll(values, 128 - HEAD_SIZE // 2, 1), pltpu.roll(values, HEAD_SIZE // 2, 1))
    return values * cosine + swapped * sine

def place(values, head, side):
    v = values if head == side else pltpu.roll(values, HEAD_SIZE, 1)
    lane = lax.broadcasted_iota(jnp.int32, values.shape, 1)
    return jnp.where(lane // HEAD_SIZE == side, v, jnp.zeros_like(v))

def column_of(row):
    a = lax.broadcasted_iota(jnp.int32, (128, 128), 0)
    b = lax.broadcasted_iota(jnp.int32, (128, 128), 1)
    return jnp.sum(jnp.where(a == b, row.astype(jnp.float32), 0.0), axis=1, keepdims=True)

def bias_of(ids_col, ids_row, row0, col0, shape, window):
    q = lax.broadcasted_iota(jnp.int32, shape, 0) + row0
    k = lax.broadcasted_iota(jnp.int32, shape, 1) + col0
    return jnp.where((ids_col == ids_row) & (k <= q), 0.0, -1e30)

def attention_kernel(n_dp, n_tensor, x_hbm, gain1, wq_hbm, wk_hbm, wv_hbm, wo_hbm, gain2, cos_ref, sin_ref, ids_row, g_hbm, gate_hbm, up_hbm,
                     normed_o, q_o, kv_o, idrow_o, mixed_o, res_o, normed2_o, gate_o, up_o, part_g, cross_g,
                     normed_ref, q_ref, kv_ref, idrow_ref, mixed_ref, res_ref, normed2_ref, gate_t, up_t,
                     x, wq, wk, wv, wo, raw_gate, raw_up, kvar, vvar, ids_flat, tile32, partial, out1, in1, mid, in2, total, load, outs, far, halo, ar):
    rows, width = x.shape
    groups = n_dp // PAIR
    me_dp, me_t = lax.axis_index("dp"), lax.axis_index("tensor")
    right = lax.rem(me_dp + PAIR, n_dp)
    left = lax.rem(me_dp + n_dp - PAIR, n_dp)
    after = lax.rem(me_dp + 1, n_dp)
    before = lax.rem(me_dp + n_dp - 1, n_dp)
    core, across = flip(me_t, 1), flip(me_t, 2)
    piece = rows // n_tensor
    def part(t):
        return pl.ds(pl.multiple_of(t * piece, piece), piece)
    count = [0]
    def cp(s, d):
        c = pltpu.make_async_copy(s, d, load.at[count[0]]); count[0] += 1
        c.start(); return c
    share = raw_gate.shape[1]
    stores = []
    def store(src, dst):
        c = pltpu.make_async_copy(src, dst, outs.at[len(stores)])
        c.start()
        stores.append(c)
    share = raw_gate.shape[1]
    w_x = cp(x_hbm, x); w_k = cp(wk_hbm, wk); w_v = cp(wv_hbm, wv)
    meet(("dp", after), ("dp", before), ("dp", right), ("dp", left), ("tensor", core), ("tensor", across))
    ids_go = send(ids_row, idrow_ref.at[0], halo, 0, "dp", after)
    fine = piece // 2
    def first_part(j):
        first = pl.ds(pl.multiple_of(me_t * piece + j * fine, fine), fine)
        return remote(g_hbm.at[first, :], part_g.at[0].at[pl.ds(j * fine, fine), :], far, j, "dp", right)
    def cross_first():
        return send(part_g.at[0].at[pl.ds(0, fine), :], cross_g.at[pl.ds(0, fine), :], far, groups, "tensor", across)
    def cross_second():
        second = pl.ds(pl.multiple_of(across * piece + fine, fine), fine)
        return remote(g_hbm.at[second, :], cross_g.at[pl.ds(fine, fine), :], far, groups + 1, "dp", right)
    ring0 = first_part(0)
    ring0.start()
    w_q = cp(wq_hbm, wq)
    idrow_ref[1] = ids_row[...]

    w_x.wait()
    def norm_one(i, _):
        r = pl.ds(pl.multiple_of(i * TILE, TILE), TILE)
        v = x[r, :].astype(jnp.float32)
        root = lax.rsqrt(jnp.mean(v * v, axis=1, keepdims=True) + EPS)
        normed_ref[r, :] = (v * root * gain1[...]).astype(jnp.bfloat16)
        return 0
    lax.fori_loop(0, rows // TILE, norm_one, 0)
    w_k.wait(); w_v.wait()
    own = pl.ds(rows, rows)
    kv_ref[1, :, 0:128] = turn(nn(normed_ref[...], wk[...]), cos_ref[...], sin_ref[...]).astype(jnp.bfloat16)
    kv_ref[1, :, 128:256] = nn(normed_ref[...], wv[...]).astype(jnp.bfloat16)
    w_q.wait()
    pairs = wq.shape[1] // 128
    def q_pair(p, _):
        c = pl.ds(pl.multiple_of(p * 256, 256), 256)
        raw = nn(normed_ref[...], wq[:, c])
        for s in range(2):
            d = pl.ds(pl.multiple_of(p * 256 + s * 128, 128), 128)
            q_ref[:, d] = (turn(raw[:, s * 128:(s + 1) * 128], cos_ref[...], sin_ref[...]).astype(jnp.bfloat16) * HEAD_SIZE ** -0.5).astype(jnp.bfloat16)
        return 0
    kv_go = send(kv_ref.at[1], kv_ref.at[0], halo, 1, "dp", after)
    w_o = cp(wo_hbm, wo)
    store(normed_ref, normed_o)
    lax.fori_loop(0, pairs // 2, q_pair, 0)
    def variants(side_rows, b):
        for g in range(2):
            for s in range(2):
                kvar[g, s, side_rows, :] = place(kv_ref[b, :, 0:128], g, s)
                vvar[g, s, side_rows, :] = place(kv_ref[b, :, 128:256], g, s)
    variants(own, 1)
    ids_go.wait(); kv_go.wait()
    ring0.wait()
    cross0 = cross_first()
    first_part(1).start()
    store(q_ref, q_o)
    store(kv_ref, kv_o)
    store(idrow_ref, idrow_o)
    mine = pl.ds(pl.multiple_of(me_dp // PAIR * share, share), share)
    w_gate = cp(gate_hbm.at[:, mine], raw_gate); w_up = cp(up_hbm.at[:, mine], raw_up)
    variants(pl.ds(0, rows), 0)
    w_o.wait()
    ids_flat[:, 0:rows] = idrow_ref[0]
    ids_flat[:, rows:2 * rows] = idrow_ref[1]

    window = rows + TILE
    def attend(i):
        start = pl.multiple_of(i * TILE, TILE)
        r = pl.ds(start, TILE)
        k = pl.ds(start, window)
        ids_k = ids_flat[:, k]
        bias = bias_of(column_of(ids_flat[:, pl.ds(start + rows, TILE)]), ids_k.astype(jnp.float32), rows, 0, (TILE, window), window)
        bias = jnp.concatenate([bias, bias], axis=0)
        for g in range(2):
            q2 = jnp.concatenate([q_ref[r, (2 * g) * 128:(2 * g + 1) * 128], q_ref[r, (2 * g + 1) * 128:(2 * g + 2) * 128]], axis=0)
            mixed = None
            for s in range(2):
                score = nt(q2, kvar[g, s, k, :]) + bias
                peak = jnp.max(score, axis=1, keepdims=True)
                e = jnp.exp(score - peak)
                l = jnp.sum(e, axis=1, keepdims=True)
                prob = (e * (1.0 / l)).astype(jnp.bfloat16)
                m = nn(prob, vvar[g, s, k, :])
                mixed = m if mixed is None else mixed + m
            for b in range(2):
                mixed_ref[r, (2 * g + b) * 128:(2 * g + b + 1) * 128] = mixed[b * TILE:(b + 1) * TILE, :].astype(jnp.bfloat16)

    hrow = CHUNK // 2
    low = lax.rem(me_t, 2)
    def own_rows(c):
        return pl.ds(pl.multiple_of(c * CHUNK + low * hrow, hrow), hrow)
    def oth_rows(c):
        return pl.ds(pl.multiple_of(c * CHUNK + (1 - low) * hrow, hrow), hrow)
    def project(c):
        r = pl.ds(pl.multiple_of(c * CHUNK, CHUNK), CHUNK)
        def body(j, _):
            d = pl.ds(pl.multiple_of(j * 512, 512), 512)
            tile32[...] = nn(mixed_ref[r, :], wo[:, d])
            out1[c, :, d] = tile32[pl.ds(pl.multiple_of((1 - low) * hrow, hrow), hrow), :].astype(jnp.bfloat16)
            partial[c, :, d] = tile32[pl.ds(pl.multiple_of(low * hrow, hrow), hrow), :]
            return 0
        lax.fori_loop(0, width // 512, body, 0)
    def step1(c):
        return remote(out1.at[c], in1.at[c], ar, 3 * c, "tensor", core)
    def step2(c):
        return remote(mid.at[c], in2.at[c], ar, 3 * c + 1, "tensor", across)
    def add_core(c):
        step1(c).wait()
        mid[c] = (partial[c] + in1[c].astype(jnp.float32)).astype(jnp.bfloat16)
        step2(c).start()
    def step3(c):
        total[own_rows(c), :] = (mid[c].astype(jnp.float32) + in2[c].astype(jnp.float32)).astype(jnp.bfloat16)
        return send(total.at[own_rows(c), :], total.at[own_rows(c), :], ar, 3 * c + 2, "tensor", core)
    def finish(r):
        v = x[r, :].astype(jnp.float32) + total[r, :].astype(jnp.float32)
        res_ref[r, :] = v
        root = lax.rsqrt(jnp.mean(v * v, axis=1, keepdims=True) + EPS)
        normed2_ref[r, :] = (v * root * gain2[...]).astype(jnp.bfloat16)

    chunks = rows // CHUNK
    flights = {}
    steps = groups - 1
    def ring(s):
        return remote(part_g.at[s - 2], part_g.at[s - 1], far, s, "dp", right)
    def tile_step(i, _):
        attend(i)
        @pl.when(i > 0)
        def _():
            add_core(i - 1)
        project(i)
        step1(i).start()
        @pl.when(i == 0)
        def _():
            first_part(1).wait()
            cross_second().start()
            if steps > 1:
                ring(2).start()
        return 0
    lax.fori_loop(0, rows // TILE, tile_step, 0)
    c = chunks - 1
    store(mixed_ref, mixed_o)
    def transpose_into(dst, raw):
        def body(j, _):
            r = pl.ds(pl.multiple_of(j * 256, 256), 256)
            dst[:, r] = raw[r, :].T
            return 0
        lax.fori_loop(0, width // 256, body, 0)
    add_core(c)
    w_gate.wait()
    transpose_into(gate_t, raw_gate)
    store(gate_t, gate_o)
    w_up.wait()
    transpose_into(up_t, raw_up)
    store(up_t, up_o)
    def out_rows(c):
        flights[3, c].wait()
        finish(oth_rows(c))
        r = pl.ds(c * CHUNK, CHUNK)
        store(res_ref.at[r, :], res_o.at[r, :])
        store(normed2_ref.at[r, :], normed2_o.at[r, :])
    for c in range(chunks):
        if 3 <= c + 2 <= steps:
            ring(c + 1).wait()
            ring(c + 2).start()
        step2(c).wait()
        flights[3, c] = step3(c)
        finish(own_rows(c))
        if c > 0:
            out_rows(c - 1)
    out_rows(chunks - 1)
    if steps > 1:
        ring(steps).wait()
    cross0.wait()
    cross_second().wait()
    for q in stores:
        q.wait()

def attend_forward(x, gain1, wq, wk, wv, wo, gain2, cosine, sine, ids, grad_output, w_gate, w_up, n_dp, n_tensor):
    rows, width = x.shape
    groups = n_dp // PAIR
    anyspec = pl.BlockSpec(memory_space=pl.ANY)
    vm = pl.BlockSpec(memory_space=pltpu.VMEM)
    bf, f32 = jnp.bfloat16, jnp.float32
    sd = jax.ShapeDtypeStruct
    V = pltpu.VMEM
    piece = rows // n_tensor
    chunks = rows // CHUNK
    qc = wq.shape[1]
    share = w_gate.shape[1] // groups
    D = pltpu.SemaphoreType.DMA
    return pl.pallas_call(
        functools.partial(attention_kernel, n_dp, n_tensor),
        out_shape=(sd((rows, width), bf), sd((rows, qc), bf), sd((2, rows, 256), bf), sd((2, 1, rows), jnp.int32),
                   sd((rows, qc), bf), sd((rows, width), f32), sd((rows, width), bf), sd((share, width), bf), sd((share, width), bf),
                   sd((groups - 1, piece, width), bf), sd((piece, width), bf)),
        in_specs=[anyspec, vm, anyspec, anyspec, anyspec, anyspec, vm, vm, vm, vm, anyspec, anyspec, anyspec],
        out_specs=(anyspec,) * 11,
        scratch_shapes=[V((rows, width), bf), V((rows, qc), bf), V((2, rows, 256), bf), V((2, 1, rows), jnp.int32), V((rows, qc), bf),
                        V((rows, width), f32), V((rows, width), bf), V((share, width), bf), V((share, width), bf),
                        V((rows, width), bf), V((width, qc), bf), V((width, 128), bf), V((width, 128), bf), V((qc, width), bf), V((width, share), bf), V((width, share), bf),
                        V((2, 2, 2 * rows, 128), bf), V((2, 2, 2 * rows, 128), bf), V((1, 2 * rows), jnp.int32), V((CHUNK, 512), f32),
                        V((chunks, CHUNK // 2, width), f32), V((chunks, CHUNK // 2, width), bf), V((chunks, CHUNK // 2, width), bf),
                        V((chunks, CHUNK // 2, width), bf), V((chunks, CHUNK // 2, width), bf), V((rows, width), bf),
                        D((7,)), D((7 + 2 * chunks,)), D((2, groups + 2)), D((2, 2)), D((2, 3 * chunks))],
        compiler_params=pltpu.CompilerParams(collective_id=1, has_side_effects=True, vmem_limit_bytes=62 << 20),
        cost_estimate=pl.CostEstimate(flops=2 * rows * width * (2 * qc + 256) + 16 * rows * rows * 5 * 128, bytes_accessed=2 * (width * (2 * qc + 256) + 6 * rows * width), transcendentals=8 * rows * rows),
        name="attention_forward",
    )(x, gain1.reshape(1, width), wq, wk, wv, wo, gain2.reshape(1, width), cosine, sine, ids.reshape(1, rows), grad_output, w_gate, w_up)

def backward_kernel(n_dp, n_tensor, gn_hbm, res_hbm, x_hbm, go_hbm, mlp_hbm, normed_hbm, wo_hbm, wq_hbm, wk_hbm, wv_hbm,
                    g_sum, u_own_hbm, u_send, d_send, mixed_hbm, q_hbm, kv_hbm, first_part, gain1, gain2, gain2_part, id_rows, ids_row, cos_ref, sin_ref,
                    out_hbm, gin_hbm, gz, uz, d_in, wz, qz, first_all, gains_ref,
                    gn, res, go, normed, wo, wq, wk, wv, mixed, q_ref, kv_ref, resid, low_res, gm, kvar, vvar, kvart, dk, dv, ids_col,
                    low, lowt, tile32, wsend, wown, win, win2, own_block, u_own, uyin, usum, lg, qsend, qown, qin,
                    amine, amid, min1, min2, ain1, ain2, hprev, hin, gacc, gs, gown, gyi, gzi, gt, gti,
                    load, sy, sz, sx, sh, sg):
    rows, width = go.shape
    groups = n_dp // PAIR
    me_dp, me_t = lax.axis_index("dp"), lax.axis_index("tensor")
    group, member = me_dp // PAIR, lax.rem(me_dp, PAIR)
    pair = flip(me_dp, 1)
    after = lax.rem(me_dp + 1, n_dp)
    before = lax.rem(me_dp + n_dp - 1, n_dp)
    core, across = flip(me_t, 1), flip(me_t, 2)
    low_t = lax.rem(me_t, 2)
    def at_group(s):
        return lax.rem(group + s, groups)
    def from_group(s):
        return lax.rem(group + groups - s, groups)
    f32, bf = jnp.float32, jnp.bfloat16
    qc = wq.shape[1]
    dcols = width // n_dp
    half = rows // 2
    def rows_of(start, size):
        return pl.ds(pl.multiple_of(start, size), size)
    def half_rows(c):
        return rows_of(c * half, half)
    def cp(s, d, i):
        c = pltpu.make_async_copy(s, d, load.at[i])
        c.start()
        return c
    w_gn = cp(gn_hbm, gn, 0); w_res = cp(res_hbm, res, 1); w_go = cp(go_hbm, go, 2)
    w_wo = cp(wo_hbm, wo, 3); w_mlp = cp(mlp_hbm.at[half_rows(low_t), :], amine, 4)
    w_g = cp(g_sum.at[group], own_block, 13)
    w_kv = cp(kv_hbm, kv_ref, 5); w_mx = cp(mixed_hbm, mixed, 6); w_qr = cp(q_hbm, q_ref, 7)
    w_own = cp(u_own_hbm, u_own, 8); w_nm = cp(normed_hbm, normed, 9)
    w_q = cp(wq_hbm, wq, 10); w_k = cp(wk_hbm, wk, 11); w_v = cp(wv_hbm, wv, 12)
    meet(("dp", pair), ("dp", after), ("dp", before), ("tensor", core), ("tensor", across),
         *[("dp", at_group(s) * PAIR + member) for s in range(1, groups)])
    def exchange(src, dst, base, distances=range(1, groups)):
        return [send(src.at[at_group(s)], dst.at[group], sz, base + s - 1, "dp", at_group(s) * PAIR + member) for s in distances]
    y_u = send(u_send, uyin, sy, 0, "dp", pair)
    z_g = exchange(g_sum, gz, 0)
    m1 = send(mlp_hbm.at[half_rows(1 - low_t), :], min1, sx, 0, "tensor", core)
    steps = groups - 1
    piece = rows // n_tensor
    def part(t):
        return rows_of(t * piece, piece)
    at_x = 3 + 3 * (rows // CHUNK)
    def first_piece(k):
        return first_part.at[k]
    def spread_x(k):
        return send(first_piece(k), first_all.at[k].at[part(me_t), :], sx, at_x + k, "tensor", across)
    def spread_core(k, t):
        src = first_piece(k) if t is me_t else first_all.at[k].at[part(t), :]
        return send(src, first_all.at[k].at[part(t), :], sx, at_x + (1 + (t is not me_t)) * steps + k, "tensor", core)
    first_x = [spread_x(0)]
    first_c = [spread_core(0, me_t)]

    w_gn.wait(); w_res.wait(); w_go.wait()
    NR = 64
    def norm_two(i, _):
        r = rows_of(i * NR, NR)
        v = res[r, :]
        root = lax.rsqrt(jnp.mean(v * v, axis=1, keepdims=True) + EPS)
        up = gn[r, :].astype(f32) * gain2[...]
        mean = jnp.mean(up * v, axis=1, keepdims=True)
        d = go[r, :].astype(f32) + root * up - v * (root * root * root * mean)
        resid[r, :] = d
        low_res[r, :] = d.astype(bf)
        return 0
    lax.fori_loop(0, rows // NR, norm_two, 0)
    w_wo.wait()
    def mix_tile(i, _):
        r = rows_of(i * half, half)
        gm[r, :] = nt(low_res[r, :], wo[...]).astype(bf)
        return 0
    lax.fori_loop(0, 2, mix_tile, 0)
    w_mlp.wait(); m1.wait()
    amid[...] = (amine[...].astype(f32) + min1[...].astype(f32)).astype(bf)
    w_kv.wait()
    for g in range(2):
        for s in range(2):
            for b in range(2):
                kvar[g, s, pl.ds(b * rows, rows), :] = place(kv_ref[b, :, 0:128], g, s)
                vvar[g, s, pl.ds(b * rows, rows), :] = place(kv_ref[b, :, 128:256], g, s)
            kvart[g, s] = kvar[g, s].T
    dk[...] = jnp.zeros_like(dk)
    dv[...] = jnp.zeros_like(dv)
    m2 = send(amid, min2, sx, 1, "tensor", across)
    for k in range(1, steps):
        first_x.append(spread_x(k))
        first_c.append(spread_core(k, me_t))
    w_g.wait()
    w_g = cp(own_block, gz.at[group], 13)
    w_mx.wait()
    lowt[0:qc, :] = mixed[...].T
    hrow = qc // n_dp
    def wout_tile(j, _):
        c = rows_of(j * 256, 256)
        tile32[...] = nn(lowt[0:qc, :], low_res[:, c])
        for z in range(groups):
            wown[z, :, c] = tile32[rows_of((z * PAIR + member) * hrow, hrow), :].astype(bf)
            wsend[z, :, c] = tile32[rows_of((z * PAIR + 1 - member) * hrow, hrow), :].astype(bf)
        return 0
    lax.fori_loop(0, width // 256, wout_tile, 0)
    w_qr.wait()
    for b in range(2):
        for j in range(rows // 128):
            ids_col[b * rows + j * 128:b * rows + (j + 1) * 128, :] = column_of(id_rows[b][:, j * 128:(j + 1) * 128])
    window = rows + TILE
    def attend(i, _):
        r = rows_of(i * TILE, TILE)
        k = pl.ds(pl.multiple_of(i * TILE, TILE), window)
        kpos = lax.broadcasted_iota(jnp.int32, (window, TILE), 0)
        qpos = lax.broadcasted_iota(jnp.int32, (window, TILE), 1) + rows
        bias = jnp.where((ids_col[k, :] == ids_row[:, r].astype(f32)) & (kpos <= qpos), 0.0, -1e30)
        bias = jnp.concatenate([bias, bias], axis=1)
        for g in range(2):
            q2 = jnp.concatenate([q_ref[r, (2 * g) * 128:(2 * g + 1) * 128], q_ref[r, (2 * g + 1) * 128:(2 * g + 2) * 128]], axis=0)
            do2 = jnp.concatenate([gm[r, (2 * g) * 128:(2 * g + 1) * 128], gm[r, (2 * g + 1) * 128:(2 * g + 2) * 128]], axis=0)
            dqt = None
            for s in range(2):
                st = nt(kvar[g, s, k, :], q2) + bias
                peak = jnp.max(st, axis=0, keepdims=True)
                e = jnp.exp(st - peak)
                pt = e * (1.0 / jnp.sum(e, axis=0, keepdims=True))
                dpt = nt(vvar[g, s, k, :], do2)
                delta = jnp.sum(pt * dpt, axis=0, keepdims=True)
                dst = (pt * (dpt - delta)).astype(bf)
                dv[g, s, k, :] += nn(pt.astype(bf), do2)
                dk[g, s, k, :] += nn(dst, q2)
                part = nn(kvart[g, s, :, k], dst)
                dqt = part if dqt is None else dqt + part
            d = dqt.T * HEAD_SIZE ** -0.5
            for b in range(2):
                low[r, (2 * g + b) * 128:(2 * g + b + 1) * 128] = turn(d[b * TILE:(b + 1) * TILE, :], cos_ref[r, :], -sin_ref[r, :]).astype(bf)
        return 0
    lax.fori_loop(0, rows // TILE // 2, attend, 0)
    y_u.wait()
    w_own.wait()
    for z in range(groups):
        usum[z] = (u_own[z].astype(f32) + uyin[z].astype(f32)).astype(bf)
    wpart = [pl.ds(0, groups // 2), pl.ds(groups // 2, groups // 2)]
    y_w = [send(wsend.at[wpart[0]], win.at[wpart[0]], sy, 1, "dp", pair)]
    w_u = cp(usum.at[group], uz.at[group], 8)
    z_u = exchange(usum, uz, groups, [1])
    lax.fori_loop(rows // TILE // 2, rows // TILE, attend, 0)

    def gathered(acc, b):
        r = pl.ds(b * rows, rows)
        lane = lax.broadcasted_iota(jnp.int32, (rows, 128), 1)
        first = acc[0, 0, r, :] + pltpu.roll(acc[0, 1, r, :], HEAD_SIZE, 1)
        second = pltpu.roll(acc[1, 0, r, :], HEAD_SIZE, 1) + acc[1, 1, r, :]
        return jnp.where(lane < HEAD_SIZE, first, second)
    hprev[:, 0:128] = gathered(dk, 0).astype(bf)
    hprev[:, 128:256] = gathered(dv, 0).astype(bf)
    halo = send(hprev, hin, sh, 0, "dp", before)
    y_w.append(send(wsend.at[wpart[1]], win.at[wpart[1]], sy, 5, "dp", pair))
    z_u = z_u + exchange(usum, uz, groups, range(2, groups))
    qs, ks = qc // groups, 128 // groups
    def to_groups(row0, count, offset, base):
        lg[0, offset:offset + count, :] = lowt[rows_of(row0 + group * count, count), :]
        return [send(lowt.at[rows_of(row0 + at_group(s) * count, count), :], lg.at[s, offset:offset + count, :], sz, base + s - 1,
                     "dp", at_group(s) * PAIR + member) for s in range(1, groups)]
    lowt[0:qc, :] = low[:, 0:qc].T
    z_low = to_groups(0, qs, 0, 3 * groups)
    m2.wait()
    def out_rows(i, _):
        r = rows_of(low_t * half + i * NR, NR)
        m = rows_of(i * NR, NR)
        summed = (amid[m, :].astype(f32) + min2[m, :].astype(f32)).astype(bf)
        go[r, :] = (res[r, :] + summed.astype(f32)).astype(bf)
        return 0
    lax.fori_loop(0, half // NR, out_rows, 0)
    w_out = cp(go.at[half_rows(low_t), :], out_hbm.at[half_rows(low_t), :], 2)
    m3 = send(go.at[half_rows(low_t), :], out_hbm.at[half_rows(low_t), :], sx, 2, "tensor", core)
    w_nm.wait()
    halo.wait()
    kraw = gathered(dk, 1) + hin[:, 0:128].astype(f32)
    low[:, qc:qc + 128] = turn(kraw, cos_ref[...], -sin_ref[...]).astype(bf)
    low[:, qc + 128:qc + 256] = (gathered(dv, 1) + hin[:, 128:256].astype(f32)).astype(bf)
    lowt[qc:qc + 256, :] = low[:, qc:qc + 256].T
    z_low = z_low + to_groups(qc, ks, qs, 4 * groups) + to_groups(qc + 128, ks, qs + ks, 5 * groups)
    for q in y_w:
        q.wait()
    for z in range(groups):
        wown[z] = (wown[z].astype(f32) + win[z].astype(f32)).astype(bf)
    near = flip(group, 1)
    far_group = flip(group, 2) if groups == 4 else near
    z_w = []
    if groups == 4:
        z_w = [send(wown.at[t], win2.at[i], sz, 2 * groups + i, "dp", near * PAIR + member) for i, t in enumerate((near, flip(near, 2)))]
    w_q.wait(); w_k.wait(); w_v.wait()
    def normed_part(j, _):
        c = rows_of(j * 256, 256)
        p = (nt(low[:, 0:qc], wq[c, :]) + nt(low[:, qc:qc + 128], wk[c, :]) + nt(low[:, qc + 128:qc + 256], wv[c, :]))
        res[:, c] = p
        gacc[0:1, c] = jnp.sum(p * normed[:, c].astype(f32), axis=0, keepdims=True) / gain1[0:1, c]
        gacc[1:2, c] = gain2_part[0:1, c] / gain2[0:1, c]
        return 0
    lax.fori_loop(0, width // 256, normed_part, 0)
    hchunk = CHUNK // 2
    chunks = rows // CHUNK
    def own_rows(c):
        return rows_of(c * CHUNK + low_t * hchunk, hchunk)
    def oth_rows(c):
        return rows_of(c * CHUNK + (1 - low_t) * hchunk, hchunk)
    def buf(c):
        return pl.ds(c * hchunk, hchunk)
    flights = {}
    for c in range(chunks):
        amine[buf(c), :] = res[oth_rows(c), :].astype(bf)
        flights[1, c] = send(amine.at[buf(c), :], ain1.at[buf(c), :], sx, 3 + 3 * c, "tensor", core)
    for z in range(groups):
        for m in range(PAIR):
            d0 = (z * PAIR + m) * dcols
            gs[m, z, 0:2, :] = gacc[0:2, d0:d0 + dcols]
    gown[...] = gs[member]
    y_gain = send(gs.at[1 - member], gyi, sg, 0, "dp", pair)
    dhalf = d_send.shape[0] // 2
    y_d = [send(d_send.at[pl.ds(0, dhalf), :], d_in.at[pl.ds(0, dhalf), :], sy, 3, "dp", pair)]
    for c in range(chunks):
        flights[1, c].wait()
        amid[buf(c), :] = (res[own_rows(c), :] + ain1[buf(c), :].astype(f32)).astype(bf)
        flights[2, c] = send(amid.at[buf(c), :], ain2.at[buf(c), :], sx, 4 + 3 * c, "tensor", across)
    for q in first_x:
        q.wait()
    first_c = first_c + [spread_core(k, across) for k in range(steps)]
    for q in first_c + [m3]:
        q.wait()
    w_out.wait()
    tokens = [normed, wo, low_res, go][:groups]
    w_first = []
    for k in range(steps):
        for i, t in enumerate((me_t, core, across, flip(core, 2))):
            src = first_piece(k) if i == 0 else first_all.at[k].at[part(t), :]
            w_first.append(cp(src, tokens[k + 1].at[part(t), :], 16 + k * n_tensor + i))
    for q in z_low + w_first:
        q.wait()
    for q in z_w:
        q.wait()
    keep, give = wown[group].astype(f32), wown[far_group].astype(f32)
    if groups == 4:
        keep, give = keep + win2[0].astype(f32), give + win2[1].astype(f32)
    wsend[0] = keep.astype(bf)
    wsend[1] = give.astype(bf)
    y_gain.wait()
    gown[...] = gown[...] + gyi[...]
    z_gain = [send(gown.at[at_group(s)], gzi.at[s - 1], sg, s, "dp", at_group(s) * PAIR + member) for s in range(1, groups)]
    w_w = cp(wsend.at[0], wz.at[0], 3)
    z_w = [send(wsend.at[1], wz.at[1], sz, 2 * groups + 2, "dp", far_group * PAIR + member)]
    def share_cols(z, _):
        for dst, m in ((qsend, 1 - member), (qown, member)):
            c = rows_of((z * PAIR + m) * dcols, dcols)
            t = nn(lg[0], tokens[0][:, c])
            for k in range(1, groups):
                t = t + nn(lg[k], tokens[k][:, c])
            dst[z] = t.astype(bf)
        return 0
    lax.fori_loop(0, groups, share_cols, 0)
    y_q = send(qsend, qin, sy, 2, "dp", pair)
    y_d.append(send(d_send.at[pl.ds(dhalf, dhalf), :], d_in.at[pl.ds(dhalf, dhalf), :], sy, 4, "dp", pair))
    w_x = cp(x_hbm, normed, 9)
    w_x.wait()
    def norm_one(r):
        v = normed[r, :].astype(f32)
        root = lax.rsqrt(jnp.mean(v * v, axis=1, keepdims=True) + EPS)
        up = gn[r, :].astype(f32) * gain1[...]
        mean = jnp.mean(up * v, axis=1, keepdims=True)
        low_res[r, :] = (resid[r, :] + root * up - v * (root * root * root * mean)).astype(bf)
    for c in range(chunks):
        flights[2, c].wait()
        gn[own_rows(c), :] = (amid[buf(c), :].astype(f32) + ain2[buf(c), :].astype(f32)).astype(bf)
        flights[3, c] = send(gn.at[own_rows(c), :], gn.at[own_rows(c), :], sx, 5 + 3 * c, "tensor", core)
        norm_one(own_rows(c))
        flights[3, c].wait()
        norm_one(oth_rows(c))
    w_gin = cp(low_res, gin_hbm, 1)
    y_q.wait()
    for z in range(groups):
        qown[z] = (qown[z].astype(f32) + qin[z].astype(f32)).astype(bf)
    w_q2 = cp(qown.at[group], qz.at[group], 14)
    z_q = exchange(qown, qz, 6 * groups)
    for q in z_gain:
        q.wait()
    total = gown[group]
    for s in range(1, groups):
        total = total + gzi[s - 1]
    gt[0] = total
    t1 = send(gt.at[0], gti.at[0], sg, groups, "tensor", core)
    t1.wait()
    gt[1] = gt[0] + gti[0]
    t2 = send(gt.at[1], gti.at[1], sg, groups + 1, "tensor", across)
    t2.wait()
    gains_ref[...] = gt[1] + gti[1]
    for q in z_g + z_u + z_w + z_q + y_d:
        q.wait()
    for q in [w_g, w_u, w_w, w_gin, w_q2]:
        q.wait()

def backward(gn, residual, x, grad_output, mlp_part, normed, wo, wq, wk, wv, g_sum, u_own, u_send, d_send, mixed, q, kv, first, gain1, gain2, gain2_part,
             id_rows, ids_row, cosine, sine, n_dp, n_tensor):
    rows, width = x.shape
    groups = n_dp // PAIR
    share = g_sum.shape[1]
    dcols = width // n_dp
    qc = wq.shape[1]
    cols = qc + 256
    share_q = cols // groups
    A = pl.BlockSpec(memory_space=pl.ANY)
    vm = pl.BlockSpec(memory_space=pltpu.VMEM)
    bf, f32 = jnp.bfloat16, jnp.float32
    sd = jax.ShapeDtypeStruct
    V = pltpu.VMEM
    D = pltpu.SemaphoreType.DMA
    half = rows // 2
    hrow = qc // n_dp
    act = V((rows, width), bf)
    return pl.pallas_call(
        functools.partial(backward_kernel, n_dp, n_tensor),
        out_shape=(sd((rows, width), bf), sd((rows, width), bf), sd((groups, share, dcols), bf), sd((groups, share, dcols), bf),
                   sd(d_send.shape, bf), sd((2, hrow, width), bf), sd((groups, share_q, dcols), bf),
                   sd((groups - 1, rows, width), bf), sd((8, dcols), f32)),
        in_specs=[A] * 18 + [vm] * 7,
        out_specs=(A,) * 8 + (vm,),
        scratch_shapes=[act, V((rows, width), f32), act, act, V((qc, width), bf), V((width, qc), bf), V((width, 128), bf), V((width, 128), bf),
                        V((rows, qc), bf), V((rows, qc), bf), V((2, rows, 256), bf), V((rows, width), f32), act, V((rows, qc), bf),
                        V((2, 2, 2 * rows, 128), bf), V((2, 2, 2 * rows, 128), bf), V((2, 2, 128, 2 * rows), bf),
                        V((2, 2, 2 * rows, 128), f32), V((2, 2, 2 * rows, 128), f32), V((2 * rows, 1), f32),
                        V((rows, cols), bf), V((cols, rows), bf), V((qc, 256), f32),
                        V((groups, hrow, width), bf), V((groups, hrow, width), bf), V((groups, hrow, width), bf), V((2, hrow, width), bf),
                        V((share, dcols), bf), *[V((groups, share, dcols), bf)] * 3,
                        V((groups, share_q, rows), bf), *[V((groups, share_q, dcols), bf)] * 3,
                        *[V((half, width), bf)] * 6,
                        V((rows, 256), bf), V((rows, 256), bf), V((8, width), f32), V((PAIR, groups, 8, dcols), f32), V((groups, 8, dcols), f32),
                        V((groups, 8, dcols), f32), V((groups - 1, 8, dcols), f32), V((2, 8, dcols), f32), V((2, 8, dcols), f32),
                        D((16 + groups * n_tensor,)), D((2, 6)), D((2, 8 * groups)), D((2, 3 + 3 * (rows // CHUNK) + 3 * groups)), D((2, 1)), D((2, groups + 2))],
        compiler_params=pltpu.CompilerParams(collective_id=4, has_side_effects=True, vmem_limit_bytes=67043328),
        cost_estimate=pl.CostEstimate(flops=4 * rows * width * (2 * qc + 256) + 40 * rows * rows * 5 * 128, bytes_accessed=40 * rows * width, transcendentals=8 * rows * rows),
        name="attention_backward",
    )(gn, residual, x, grad_output, mlp_part, normed, wo, wq, wk, wv, g_sum, u_own, u_send, d_send, mixed, q, kv, first,
      gain1.reshape(1, width), gain2.reshape(1, width), gain2_part, id_rows, ids_row, cosine, sine)

def finish_kernel(qc, kc, out_hbm, gin_hbm, gz_hbm, uz_hbm, d_own_hbm, d_in_hbm, wz_hbm, qz_hbm, gains,
                  gain1_o, gain2_o, out_o, gin_o, gate_o, up_o, down_o, wout_o, query_o, key_o, value_o,
                  act1, act2, gz, uz, d_own, d_in, wz, qz, gate, up, down, wout, query, key, value, ins, outs):
    f32 = jnp.float32
    groups, share, dcols = gz.shape
    gain1_o[...] = gains[0:1, :]
    gain2_o[...] = gains[1:2, :]
    loads = [pltpu.make_async_copy(s, d, ins.at[i]) for i, (s, d) in enumerate([
        (gz_hbm, gz), (uz_hbm, uz), (out_hbm, act1), (gin_hbm, act2), (d_own_hbm, d_own), (d_in_hbm, d_in), (wz_hbm, wz), (qz_hbm, qz)])]
    for c in loads:
        c.start()
    stores = []
    def store(src, dst):
        c = pltpu.make_async_copy(src, dst, outs.at[len(stores)])
        c.start()
        stores.append(c)
    for got, held, dst, i in ((gz, gate, gate_o, 0), (uz, up, up_o, 1)):
        loads[i].wait()
        for z in range(groups):
            for h in range(share // 256):
                held[:, z * share + h * 256:z * share + (h + 1) * 256] = got[z, h * 256:(h + 1) * 256, :].astype(f32).T
        store(held, dst)
    loads[2].wait()
    store(act1, out_o)
    loads[3].wait()
    store(act2, gin_o)
    loads[4].wait()
    loads[5].wait()
    down[...] = d_own[...].astype(f32) + d_in[...].astype(f32)
    store(down, down_o)
    loads[6].wait()
    wout[...] = wz[0].astype(f32) + wz[1].astype(f32)
    store(wout, wout_o)
    loads[7].wait()
    qs, ks = qc // groups, kc // groups
    for z in range(groups):
        query[:, z * qs:(z + 1) * qs] = qz[z, 0:qs, :].astype(f32).T
    key[...] = jnp.concatenate([qz[z, qs:qs + ks, :] for z in range(groups)], axis=0).astype(f32).T
    value[...] = jnp.concatenate([qz[z, qs + ks:qs + 2 * ks, :] for z in range(groups)], axis=0).astype(f32).T
    store(query, query_o)
    store(key, key_o)
    store(value, value_o)
    for c in stores:
        c.wait()

def finish_all(out, gin, gz, uz, d_own, d_in, wz, qz, gains, qc, kc):
    vm = pl.BlockSpec(memory_space=pltpu.VMEM)
    A = pl.BlockSpec(memory_space=pl.ANY)
    bf, f32 = jnp.bfloat16, jnp.float32
    sd = jax.ShapeDtypeStruct
    V = pltpu.VMEM
    groups, share, dcols = gz.shape
    shapes = [(dcols, groups * share), (dcols, groups * share), d_own.shape, wz.shape[1:], (dcols, qc), (dcols, kc), (dcols, kc)]
    return pl.pallas_call(
        functools.partial(finish_kernel, qc, kc),
        out_shape=(sd((1, dcols), f32), sd((1, dcols), f32), sd(out.shape, bf), sd(gin.shape, bf)) + tuple(sd(s, f32) for s in shapes),
        in_specs=[A] * 8 + [vm], out_specs=(vm,) * 2 + (A,) * 9,
        scratch_shapes=[V(a.shape, bf) for a in (out, gin, gz, uz, d_own, d_in, wz, qz)] + [V(s, f32) for s in shapes] + [pltpu.SemaphoreType.DMA((8,)), pltpu.SemaphoreType.DMA((9,))],
        compiler_params=pltpu.CompilerParams(vmem_limit_bytes=67043328),
        cost_estimate=pl.CostEstimate(flops=8 * out.size, bytes_accessed=24 << 20, transcendentals=0),
        name="finish",
    )(out, gin, gz, uz, d_own, d_in, wz, qz, gains)


def rope_table(half_count, copies=1):
    adjusted = []
    for index in range(half_count):
        base_value = 500000.0 ** (-index / half_count)
        wave_length = 2.0 * math.pi / base_value
        smooth = (8192.0 / wave_length - 1.0) / 3.0
        if wave_length > 8192.0:
            adjusted.append(base_value / 32.0)
        elif wave_length >= 2048.0:
            adjusted.append((1.0 - smooth) * base_value / 32.0 + smooth * base_value)
        else:
            adjusted.append(base_value)
    return jnp.asarray(adjusted * copies, dtype=jnp.float32)


def rope_angles(start_row, count_rows, half_count):
    positions = (start_row + jnp.arange(count_rows, dtype=jnp.int32)).astype(jnp.float32)
    phase_angle = positions[:, None] * rope_table(half_count)[None, :]
    return (jnp.cos(phase_angle)[:, None, :], jnp.sin(phase_angle)[:, None, :])


def rotate_halves(values, cosine_table, sine_values):
    half_size = values.shape[-1] // 2
    first_half = values[..., :half_size]
    second_half = values[..., half_size:]
    return jnp.concatenate(
        [
            first_half * cosine_table - second_half * sine_values,
            second_half * cosine_table + first_half * sine_values,
        ],
        axis=-1,
    )


def norm_rows(values, gain_row):
    inverse_root = lax.rsqrt(jnp.mean(values * values, axis=-1, keepdims=True) + NORM_EPSILON)
    return (inverse_root, values * inverse_root * gain_row)


def norm_back(values, inverse_root, gain_row, upstream):
    scaled = gain_row * upstream
    return inverse_root * scaled - values * inverse_root**3 * jnp.mean(
        scaled * values, axis=-1, keepdims=True
    )


def passed_along(block, axis, distance):
    devices = range(lax.axis_size(axis))
    route = [(i - distance, i) for i in devices if i - distance in devices]
    return lax.ppermute(block, axis, route)


def tensor_swap(block, bit):
    return lax.ppermute(block, "tensor", [(i, i ^ bit) for i in range(lax.axis_size("tensor"))])


def pair_swap(block):
    return lax.ppermute(block, "dp", [(i, i ^ 1) for i in range(lax.axis_size("dp"))])


def group_shift(block, distance):
    count = lax.axis_size("dp")
    groups = count // PAIR
    return lax.ppermute(
        block,
        "dp",
        [(i, ((i // PAIR + distance) % groups) * PAIR + i % PAIR) for i in range(count)],
    )


def tensor_sum(part):
    half = part.shape[1] // 2
    low = lax.axis_index("tensor") % 2
    first, second = part[:, :half], part[:, half:]
    mine = jnp.where(low == 0, first, second)
    other = jnp.where(low == 0, second, first).astype(jnp.bfloat16)
    mine = mine + tensor_swap(other, 1).astype(jnp.float32)
    bit = 2
    while bit < lax.axis_size("tensor"):
        rounded = mine.astype(jnp.bfloat16)
        mine = rounded.astype(jnp.float32) + tensor_swap(rounded, bit).astype(jnp.float32)
        bit *= 2
    mine = mine.astype(jnp.bfloat16)
    other = tensor_swap(mine, 1)
    return jnp.concatenate(
        [jnp.where(low == 0, mine, other), jnp.where(low == 0, other, mine)], axis=1
    ).astype(jnp.float32)


def gather_groups(block):
    half = block.shape[1] // 2
    low = lax.axis_index("tensor") % 2
    piece = lax.dynamic_slice_in_dim(block, low * half, half, axis=1)
    rows = [block]
    for _ in range(lax.axis_size("dp") // PAIR - 1):
        piece = group_shift(piece, 1)
        other = tensor_swap(piece, 1)
        rows.append(
            jnp.concatenate(
                [jnp.where(low == 0, piece, other), jnp.where(low == 0, other, piece)], axis=1
            )
        )
    return jnp.concatenate(rows, axis=0)


def pair_sum(part):
    member = lax.axis_index("dp") % PAIR
    mine = lax.dynamic_index_in_dim(part, member, 1, keepdims=False)
    other = lax.dynamic_index_in_dim(part, 1 - member, 1, keepdims=False)
    return mine + pair_swap(other.astype(jnp.bfloat16)).astype(jnp.float32)


def group_exchange(blocks):
    groups = blocks.shape[0]
    group = lax.axis_index("dp") // PAIR
    received = []
    for distance in range(groups):
        block = lax.dynamic_index_in_dim(blocks, (group + distance) % groups, 0, keepdims=False)
        received.append(block if distance == 0 else group_shift(block, distance))
    return received


def scatter_sum(part):
    summed = pair_sum(part)
    groups = summed.shape[0]
    group = lax.axis_index("dp") // PAIR
    total = lax.dynamic_index_in_dim(summed, group, 0, keepdims=False)
    rounded = summed.astype(jnp.bfloat16)
    for block in group_exchange(rounded)[1:]:
        total = total + block.astype(jnp.float32)
    return total


def block_scores(query_rows, key_rows, query_ids, key_ids, query_pos, key_pos):
    scores = jnp.einsum(
        "qgrd,kgd->grqk", query_rows, key_rows, preferred_element_type=jnp.float32
    ) * HEAD_SIZE ** (-0.5)
    allowed = (query_ids[:, None] == key_ids[None, :]) & (key_pos[None, :] <= query_pos[:, None])
    return jnp.where(allowed, scores, -1e30)


def block_forward(query_rows, key_rows, value_rows, query_ids, key_ids, query_pos, key_pos):
    scores = block_scores(query_rows, key_rows, query_ids, key_ids, query_pos, key_pos)
    row_peak = jnp.max(scores, axis=-1, keepdims=True)
    logsum = row_peak + jnp.log(jnp.sum(jnp.exp(scores - row_peak), axis=-1, keepdims=True))
    prob_low = jnp.exp(scores - logsum).astype(jnp.bfloat16)
    mixed_rows = jnp.einsum(
        "grqk,kgd->qgrd", prob_low, value_rows, preferred_element_type=jnp.float32
    )
    return (mixed_rows.astype(jnp.bfloat16), logsum)


def block_backward(
    query_rows,
    key_rows,
    value_rows,
    out_rows,
    grad_rows,
    logsum,
    query_ids,
    key_ids,
    query_pos,
    key_pos,
):
    scores = block_scores(query_rows, key_rows, query_ids, key_ids, query_pos, key_pos)
    prob_rows = jnp.exp(scores - logsum)
    grad_vals = jnp.einsum(
        "grqk,qgrd->kgd",
        prob_rows.astype(jnp.bfloat16),
        grad_rows,
        preferred_element_type=jnp.float32,
    )
    delta_rows = jnp.sum(out_rows.astype(jnp.float32) * grad_rows.astype(jnp.float32), axis=-1)
    grad_probs = jnp.einsum(
        "qgrd,kgd->grqk", grad_rows, value_rows, preferred_element_type=jnp.float32
    )
    grad_scores = (
        prob_rows * (grad_probs - jnp.transpose(delta_rows, (1, 2, 0))[..., None])
    ).astype(jnp.bfloat16)
    grad_query_rows = jnp.einsum(
        "grqk,kgd->qgrd", grad_scores, key_rows, preferred_element_type=jnp.float32
    ) * HEAD_SIZE ** (-0.5)
    grad_key_rows = jnp.einsum(
        "grqk,qgrd->kgd", grad_scores, query_rows, preferred_element_type=jnp.float32
    ) * HEAD_SIZE ** (-0.5)
    return (grad_query_rows, grad_key_rows, grad_vals)


def dot(form, left, right):
    return jnp.einsum(form, left, right, preferred_element_type=jnp.float32)


def gated(gate_value, up_value):
    return (jax.nn.silu(gate_value) * up_value).astype(jnp.bfloat16)


def gated_back(grad_hidden, gate_value, up_value):
    sigmoid_gate = jax.nn.sigmoid(gate_value)
    grad_gate_low = (
        grad_hidden * up_value * sigmoid_gate * (1.0 + gate_value * (1.0 - sigmoid_gate))
    ).astype(jnp.bfloat16)
    return grad_gate_low, (grad_hidden * jax.nn.silu(gate_value)).astype(jnp.bfloat16)


def shards_plain(
    inputs,
    norm1_gain,
    query_weight,
    key_weight,
    value_weight,
    w_out,
    norm2_gain,
    w_gate,
    w_up,
    w_down,
    doc_ids,
    grad_output,
):
    tok_rows, width = inputs.shape
    heads_here = query_weight.shape[1] // HEAD_SIZE
    kv_here = key_weight.shape[1] // HEAD_SIZE
    group_size = heads_here // kv_here
    n_dp = lax.axis_size("dp")
    groups = n_dp // PAIR
    group = lax.axis_index("dp") // PAIR
    offset = lax.axis_index("dp") * tok_rows
    grad_all = gather_groups(grad_output)

    cosine_table, sine_values = rope_angles(offset, tok_rows, HEAD_SIZE // 2)
    inputs_wide = inputs.astype(jnp.float32)
    root_one, normed = norm_rows(inputs_wide, norm1_gain)
    normed_low = normed.astype(jnp.bfloat16)
    query_raw = dot("td,dh->th", normed_low, query_weight).reshape(tok_rows, heads_here, HEAD_SIZE)
    key_raw = dot("td,dh->th", normed_low, key_weight).reshape(tok_rows, kv_here, HEAD_SIZE)
    value_low = dot("td,dh->th", normed_low, value_weight).astype(jnp.bfloat16)
    query_low = (
        rotate_halves(query_raw, cosine_table, sine_values)
        .astype(jnp.bfloat16)
        .reshape(tok_rows, kv_here, group_size, HEAD_SIZE)
    )
    key_low = (
        rotate_halves(key_raw, cosine_table, sine_values)
        .astype(jnp.bfloat16)
        .reshape(tok_rows, kv_here * HEAD_SIZE)
    )
    query_ids = doc_ids + 1
    tail = jnp.concatenate([key_low, value_low], axis=1)
    prev_tail = passed_along(tail, "dp", 1)
    prev_ids = passed_along(query_ids, "dp", 1)
    both = jnp.concatenate([prev_tail, tail], axis=0)
    keys_all = both[:, : kv_here * HEAD_SIZE].reshape(2 * DOC_MAX, kv_here, HEAD_SIZE)
    values_all = both[:, kv_here * HEAD_SIZE :].reshape(2 * DOC_MAX, kv_here, HEAD_SIZE)
    ids_all = jnp.concatenate([prev_ids, query_ids])
    pos_all = offset - DOC_MAX + jnp.arange(tok_rows + DOC_MAX, dtype=jnp.int32)
    query_pos = pos_all[DOC_MAX:]
    mixed_block, logsum_block = block_forward(
        query_low, keys_all, values_all, query_ids, ids_all, query_pos, pos_all
    )
    mixed_low = mixed_block.reshape(tok_rows, heads_here * HEAD_SIZE)
    residual = inputs_wide + tensor_sum(dot("te,ed->td", mixed_low, w_out))

    root_two, normed_two = norm_rows(residual, norm2_gain)
    normed_two_low = normed_two.astype(jnp.bfloat16)
    normed_all = gather_groups(normed_two_low)
    gate_value = dot("td,df->tf", normed_two_low, w_gate)
    up_value = dot("td,df->tf", normed_two_low, w_up)
    grad_hidden = dot("td,fd->tf", grad_output, w_down)
    hidden_low = gated(gate_value, up_value)
    grad_gate_low, grad_up_low = gated_back(grad_hidden, gate_value, up_value)
    normed_two_part = dot("tf,df->td", grad_gate_low, w_gate) + dot("tf,df->td", grad_up_low, w_up)
    grad_normed_two = tensor_sum(normed_two_part)
    gain_two_part = jnp.sum(normed_two_part * residual * root_two, axis=0)
    output = (residual + tensor_sum(dot("tf,fd->td", hidden_low, w_down))).astype(jnp.bfloat16)

    share = w_gate.shape[1] // groups
    gate_share = lax.dynamic_slice_in_dim(w_gate, group * share, share, axis=1)
    up_share = lax.dynamic_slice_in_dim(w_up, group * share, share, axis=1)
    down_share = lax.dynamic_slice_in_dim(w_down, group * share, share, axis=0)
    gate_all = dot("td,df->tf", normed_all, gate_share)
    up_all = dot("td,df->tf", normed_all, up_share)
    grad_hidden_all = dot("td,fd->tf", grad_all, down_share)
    hidden_all = gated(gate_all, up_all)
    gate_low_all, up_low_all = gated_back(grad_hidden_all, gate_all, up_all)
    down_part = dot("tf,td->fd", hidden_all, grad_all)
    grad_wdown = pair_sum(down_part.reshape(1, PAIR, share // PAIR, width))[0]
    rows_here = width // n_dp

    def column_grad(low_all):
        part = dot("td,tf->df", normed_all, low_all)
        summed = pair_sum(part.reshape(groups, PAIR, rows_here, share)).astype(jnp.bfloat16)
        full = jnp.zeros((rows_here, groups * share), jnp.float32)
        for distance, block in enumerate(group_exchange(summed)):
            full = lax.dynamic_update_slice_in_dim(
                full, block.astype(jnp.float32), ((group - distance) % groups) * share, axis=1
            )
        return full

    grad_wgate = column_grad(gate_low_all)
    grad_wup = column_grad(up_low_all)

    grad_residual = grad_output.astype(jnp.float32) + norm_back(
        residual, root_two, norm2_gain, grad_normed_two
    )
    grad_res_low = grad_residual.astype(jnp.bfloat16)
    wout_part = dot("te,td->ed", mixed_low, grad_res_low)
    grad_wout = scatter_sum(wout_part.reshape(groups, PAIR, -1, width))
    grad_mixed = (
        dot("td,ed->te", grad_res_low, w_out)
        .astype(jnp.bfloat16)
        .reshape(tok_rows, kv_here, group_size, HEAD_SIZE)
    )
    mixed_view = mixed_low.reshape(tok_rows, kv_here, group_size, HEAD_SIZE)
    grad_query_rows, grad_key_rows, grad_value_rows = block_backward(
        query_low,
        keys_all,
        values_all,
        mixed_view,
        grad_mixed,
        logsum_block,
        query_ids,
        ids_all,
        query_pos,
        pos_all,
    )
    sent = jnp.concatenate(
        [
            grad_key_rows.reshape(2 * DOC_MAX, kv_here * HEAD_SIZE),
            grad_value_rows.reshape(2 * DOC_MAX, kv_here * HEAD_SIZE),
        ],
        axis=1,
    )
    back = passed_along(sent[:DOC_MAX].astype(jnp.bfloat16), "dp", -1).astype(jnp.float32)
    own = sent[DOC_MAX:] + back
    grad_qraw = grad_query_rows.reshape(tok_rows, heads_here, HEAD_SIZE)
    query_low_gradient = (
        rotate_halves(grad_qraw, cosine_table, -sine_values)
        .astype(jnp.bfloat16)
        .reshape(tok_rows, heads_here * HEAD_SIZE)
    )
    key_low_gradient = (
        rotate_halves(
            own[:, : kv_here * HEAD_SIZE].reshape(tok_rows, kv_here, HEAD_SIZE),
            cosine_table,
            -sine_values,
        )
        .astype(jnp.bfloat16)
        .reshape(tok_rows, kv_here * HEAD_SIZE)
    )
    value_low_gradient = own[:, kv_here * HEAD_SIZE :].astype(jnp.bfloat16)
    low_gradient = jnp.concatenate(
        [query_low_gradient, key_low_gradient, value_low_gradient], axis=1
    )
    normed_one_part = (
        dot("kl,ql->kq", query_low_gradient, query_weight)
        + dot("kl,ql->kq", key_low_gradient, key_weight)
        + dot("kl,ql->kq", value_low_gradient, value_weight)
    )
    grad_normed_one = tensor_sum(normed_one_part)
    gain_one_part = jnp.sum(normed_one_part * inputs_wide * root_one, axis=0)
    qkv_part = dot("wj,wq->jq", normed_low, low_gradient)
    columns = qkv_part.shape[1]
    gains = jnp.stack(
        [gain_one_part.reshape(n_dp, rows_here), gain_two_part.reshape(n_dp, rows_here)], axis=1
    )
    gains = jnp.pad(gains, ((0, 0), (0, 14), (0, columns - rows_here)))
    qkv_part = jnp.concatenate([qkv_part.reshape(n_dp, rows_here, columns), gains], axis=1)
    qkv_sum = scatter_sum(qkv_part.reshape(groups, PAIR, rows_here + 16, columns))
    grad_qkv = qkv_sum[:rows_here]
    gain_sums = qkv_sum[rows_here : rows_here + 16, :rows_here]
    bit = 1
    while bit < lax.axis_size("tensor"):
        gain_sums = gain_sums + tensor_swap(gain_sums, bit)
        bit *= 2
    grad_input_norm = norm_back(inputs_wide, root_one, norm1_gain, grad_normed_one)
    grad_inputs = (grad_residual + grad_input_norm).astype(jnp.bfloat16)
    q_columns = query_weight.shape[1]
    k_columns = key_weight.shape[1]
    return (
        output,
        grad_inputs,
        gain_sums[0],
        grad_qkv[:, :q_columns],
        grad_qkv[:, q_columns : q_columns + k_columns],
        grad_qkv[:, q_columns + k_columns :],
        grad_wout,
        gain_sums[1],
        grad_wgate,
        grad_wup,
        grad_wdown,
    )


def shards(
    inputs,
    norm1_gain,
    query_weight,
    key_weight,
    value_weight,
    w_out,
    norm2_gain,
    w_gate,
    w_up,
    w_down,
    doc_ids,
    grad_output,
):
    tok_rows, width = inputs.shape
    heads_here = query_weight.shape[1] // HEAD_SIZE
    kv_here = key_weight.shape[1] // HEAD_SIZE
    group_size = heads_here // kv_here
    n_dp = lax.axis_size("dp")
    groups = n_dp // PAIR
    group = lax.axis_index("dp") // PAIR
    offset = lax.axis_index("dp") * tok_rows
    n_tensor = lax.axis_size("tensor")
    half = HEAD_SIZE // 2
    lanes = jnp.arange(4 * half, dtype=jnp.int32)
    positions = (offset + jnp.arange(tok_rows, dtype=jnp.int32)).astype(jnp.float32)
    angles = positions[:, None] * rope_table(half, 4)[None, :]
    cosine = jnp.cos(angles)
    sine = jnp.sin(angles) * jnp.where(lanes % HEAD_SIZE < half, -1.0, 1.0)[None, :]
    normed_low, query_scaled, kv, id_rows, mixed_low, residual, normed_two_low, gate_t, up_t, part_g, cross_g = attend_forward(
        inputs, norm1_gain, query_weight, key_weight, value_weight, w_out, norm2_gain, cosine, sine, doc_ids, grad_output,
        w_gate, w_up, n_dp, n_tensor)
    mlp_part, back_part, normed_rest, rest_g, gain_two_part = mlp(normed_two_low, grad_output, part_g, cross_g, w_gate, w_up, w_down, n_dp, n_tensor)
    d_own, d_send, g_sum, u_own, u_send, grad_normed_two, first_part = wgrad(
        normed_two_low, normed_rest, grad_output, part_g, cross_g, rest_g, gate_t, up_t, w_down, back_part, normed_low, n_dp, n_tensor)
    output, grad_inputs, gate_blocks, up_blocks, d_in, wout_blocks, qkv_blocks, _, gain_sums = backward(
        grad_normed_two, residual, inputs, grad_output, mlp_part, normed_low, w_out, query_weight, key_weight, value_weight,
        g_sum, u_own, u_send, d_send, mixed_low, query_scaled, kv, first_part, norm1_gain, norm2_gain, gain_two_part,
        id_rows, doc_ids.reshape(1, tok_rows), cosine, sine, n_dp, n_tensor)
    gain_one, gain_two, output, grad_inputs, grad_wgate, grad_wup, grad_wdown, grad_wout, grad_wquery, grad_wkey, grad_wvalue = finish_all(
        output, grad_inputs, gate_blocks, up_blocks, d_own, d_in, wout_blocks, qkv_blocks, gain_sums, query_weight.shape[1], key_weight.shape[1])
    rows_here = width // n_dp
    return (
        output,
        grad_inputs,
        gain_one.reshape(rows_here),
        grad_wquery,
        grad_wkey,
        grad_wvalue,
        grad_wout,
        gain_two.reshape(rows_here),
        grad_wgate,
        grad_wup,
        grad_wdown,
    )


def kernels_fit(mesh, *args):
    n_dp, n_tensor = mesh.shape["dp"], mesh.shape["tensor"]
    width = args[0].shape[1]
    return (
        n_dp % PAIR == 0
        and n_dp // PAIR in (2, 4)
        and n_tensor == 4
        and width // n_dp in (128, 256)
        and args[7].shape[1] // n_tensor // (n_dp // PAIR) % 256 == 0
        and args[0].shape[0] // n_dp == DOC_MAX
        and args[3].shape[1] // n_tensor == 2 * HEAD_SIZE
        and args[2].shape[1] == 4 * args[3].shape[1]
    )


def solution(mesh):
    def step(*args):
        return mapped(mesh, shards if kernels_fit(mesh, *args) else shards_plain)(*args)

    return step


def mapped(mesh, function):
    return jax.shard_map(
        function,
        mesh=mesh,
        in_specs=(
            P("dp", None),
            P(),
            P(None, "tensor"),
            P(None, "tensor"),
            P(None, "tensor"),
            P("tensor", None),
            P(),
            P(None, "tensor"),
            P(None, "tensor"),
            P("tensor", None),
            P("dp"),
            P("dp", None),
        ),
        out_specs=(
            P("dp", None),
            P("dp", None),
            P("dp"),
            P("dp", "tensor"),
            P("dp", "tensor"),
            P("dp", "tensor"),
            P(("tensor", "dp"), None),
            P("dp"),
            P("dp", "tensor"),
            P("dp", "tensor"),
            P(("tensor", "dp"), None),
        ),
        check_vma=False,
    )
```

```python
import functools
import math

import jax
import jax.numpy as jnp
from jax import lax
from jax.experimental import pallas as pl
from jax.experimental.pallas import tpu as pltpu
from jax.sharding import PartitionSpec as P

HEAD_SIZE = 64
DOC_MAX = 512
NORM_EPSILON = 1e-05

PAIR = 2
MESH = pl.DeviceIdType.MESH
EPS = NORM_EPSILON


def nn(a, b):
    return lax.dot_general(a, b, (((1,), (0,)), ((), ())), preferred_element_type=jnp.float32)
def nt(a, b):
    return lax.dot_general(a, b, (((1,), (1,)), ((), ())), preferred_element_type=jnp.float32)

def flip(index, bit):
    return index + bit - 2 * bit * ((index // bit) % 2)

def meet(*partners):
    barrier = pltpu.get_barrier_semaphore()
    for axis, index in partners:
        pl.semaphore_signal(barrier, inc=1, device_id={axis: index}, device_id_type=MESH)
    pl.semaphore_wait(barrier, len(partners))

def remote(src, dst, sems, slot, axis, index):
    return pltpu.make_async_remote_copy(
        src_ref=src, dst_ref=dst, send_sem=sems.at[0, slot], recv_sem=sems.at[1, slot],
        device_id={axis: index}, device_id_type=MESH)

def send(src, dst, sems, slot, axis, index):
    copy = remote(src, dst, sems, slot, axis, index)
    copy.start()
    return copy

def swiglu(gate, up, grad):
    sig = 0.5 * (1.0 + jnp.tanh(0.5 * gate))
    silu = gate * sig
    hidden = (silu * up).astype(jnp.bfloat16)
    grad_gate = (grad * up * sig * (1.0 + gate * (1.0 - sig))).astype(jnp.bfloat16)
    grad_up = (grad * silu).astype(jnp.bfloat16)
    return hidden, grad_gate, grad_up

def mlp_kernel(n_dp, n_tensor, normed_hbm, grad_hbm, part_g, cross_g, gate_hbm, up_hbm, down_hbm,
               out_o, back_o, all_hbm, rest_g, gain_ref, out_ref, back_ref,
               normed, grad, gate_w, up_w, down_w, hid, low_gate, low_up, load, far):
    rows, width = normed.shape
    cols = gate_w.shape[1]
    groups = n_dp // PAIR
    me_dp, me_t = lax.axis_index("dp"), lax.axis_index("tensor")
    right = lax.rem(me_dp + PAIR, n_dp)
    left = lax.rem(me_dp + n_dp - PAIR, n_dp)
    core, across = flip(me_t, 1), flip(me_t, 2)
    tile = 256
    tiles = cols // tile
    def cp(s, d, i):
        return pltpu.make_async_copy(s, d, load.at[i])
    def gate_tile(c, f):
        return cp(gate_hbm.at[:, c], gate_w.at[:, c], 2 + 3 * f)
    def up_tile(c, f):
        return cp(up_hbm.at[:, c], up_w.at[:, c], 3 + 3 * f)
    def down_tile(c, f):
        return cp(down_hbm.at[c, :], down_w.at[c, :], 4 + 3 * f)
    cp(normed_hbm, normed, 0).start()
    def load_tile(f):
        c = pl.ds(pl.multiple_of(f * tile, tile), tile)
        gate_tile(c, f).start()
        up_tile(c, f).start()
        down_tile(c, f).start()
    load_tile(0)
    cp(grad_hbm, grad, 1).start()
    for f in range(1, tiles):
        load_tile(f)
    meet(("dp", right), ("dp", left), ("tensor", core), ("tensor", across))
    piece = rows // n_tensor
    def part(t):
        return pl.ds(pl.multiple_of(t * piece, piece), piece)
    steps = groups - 1
    per = 4
    def ring(s):
        src = (normed_hbm if s == 1 else all_hbm.at[s - 2]).at[part(me_t), :]
        return send(src, all_hbm.at[s - 1].at[part(me_t), :], far, s * per, "dp", right)
    def spread_n(s, level):
        block = all_hbm.at[s - 1]
        held, other = [me_t, across][:level + 1], [across, core][level]
        return [send(block.at[part(h), :], block.at[part(h), :], far, s * per + 1 + level + i, "tensor", other) for i, h in enumerate(held)]
    def spread_g(b, level):
        base = (steps + 1 + b) * per
        if level == 0:
            return [send(part_g.at[b], rest_g.at[b].at[part(me_t), :], far, base, "tensor", across)]
        cross = cross_g if b == 0 else rest_g.at[b].at[part(across), :]
        return [send(part_g.at[b], rest_g.at[b].at[part(me_t), :], far, base + 1, "tensor", core),
                send(cross, rest_g.at[b].at[part(across), :], far, base + 2, "tensor", core)]
    def wait(copies):
        for c in copies:
            c.wait()

    ring_n = ring(1)
    g_core = spread_g(0, 1)
    g_x = {}
    last_g = steps - 1 if steps > 1 else steps
    if last_g > 1:
        g_x[1] = spread_g(1, 0)

    cp(normed_hbm, normed, 0).wait()
    cp(grad_hbm, grad, 1).wait()
    def first(f, _):
        c = pl.ds(pl.multiple_of(f * tile, tile), tile)
        gate_tile(c, f).wait()
        up_tile(c, f).wait()
        down_tile(c, f).wait()
        g = nn(normed[...], gate_w[:, c])
        u = nn(normed[...], up_w[:, c])
        h = nt(grad[...], down_w[c, :])
        a, b, d = swiglu(g, u, h)
        hid[:, c] = a
        low_gate[:, c] = b
        low_up[:, c] = d
        return 0
    early = min(5, tiles)
    n_x = {}
    def pass_g(b):
        nonlocal g_core
        if b in g_x:
            wait(g_x.pop(b))
            g_core = g_core + spread_g(b, 1)
            if b + 1 < last_g:
                g_x[b + 1] = spread_g(b + 1, 0)
    lax.fori_loop(0, early, first, 0)
    ring_n.wait()
    if steps > 1:
        ring_n = ring(2)
    pass_g(1)
    n_x[1] = spread_n(1, 0)
    lax.fori_loop(early, tiles, first, 0)
    wtile = 256
    wtiles = width // wtile
    def second(j, _):
        c = pl.ds(pl.multiple_of(j * wtile, wtile), wtile)
        b = nt(low_gate[...], gate_w[c, :]) + nt(low_up[...], up_w[c, :])
        back_ref[:, c] = b.astype(back_ref.dtype)
        gain_ref[0:1, c] = jnp.sum(b * normed[:, c].astype(jnp.float32), axis=0, keepdims=True)
        return 0
    def third(j, _):
        c = pl.ds(pl.multiple_of(j * wtile, wtile), wtile)
        out_ref[:, c] = nn(hid[...], down_w[:, c]).astype(out_ref.dtype)
        return 0
    most = wtiles * 3 // 4
    lax.fori_loop(0, most, third, 0)
    n_core = []
    def pass_n(s):
        nonlocal n_core
        if s in n_x:
            wait(n_x.pop(s))
            n_core = n_core + spread_n(s, 1)
    if steps > 1:
        ring_n.wait()
        if steps > 2:
            ring_n = ring(3)
            n_x[2] = spread_n(2, 0)
    lax.fori_loop(most, wtiles, third, 0)
    w_out = pltpu.make_async_copy(out_ref, out_o, load.at[0])
    w_out.start()
    lax.fori_loop(0, wtiles // 2, second, 0)
    pass_n(1)
    lax.fori_loop(wtiles // 2, wtiles, second, 0)
    w_back = pltpu.make_async_copy(back_ref, back_o, load.at[1])
    w_back.start()
    for s in range(3, steps + 1):
        ring_n.wait()
        if s < steps:
            ring_n = ring(s + 1)
            n_x[s] = spread_n(s, 0)
    for b in range(3, steps):
        pass_g(b)
    for s in range(2, steps):
        pass_n(s)
    wait(n_core)
    wait(g_core)
    w_out.wait()
    w_back.wait()

def mlp(normed, grad_output, part_g, cross_g, w_gate, w_up, w_down, n_dp, n_tensor):
    rows, width = normed.shape
    cols = w_gate.shape[1]
    groups = n_dp // PAIR
    tiles = cols // 256
    anyspec = pl.BlockSpec(memory_space=pl.ANY)
    vm = pl.BlockSpec(memory_space=pltpu.VMEM)
    bf = jnp.bfloat16
    return pl.pallas_call(
        functools.partial(mlp_kernel, n_dp, n_tensor),
        out_shape=(jax.ShapeDtypeStruct((rows, width), bf), jax.ShapeDtypeStruct((rows, width), bf),
                   jax.ShapeDtypeStruct((groups - 1, rows, width), bf), jax.ShapeDtypeStruct((groups - 1, rows, width), bf), jax.ShapeDtypeStruct((1, width), jnp.float32)),
        in_specs=[anyspec] * 7, out_specs=(anyspec, anyspec, anyspec, anyspec, vm),
        scratch_shapes=[pltpu.VMEM((rows, width), bf), pltpu.VMEM((rows, width), bf), pltpu.VMEM((rows, width), bf), pltpu.VMEM((rows, width), bf),
                        pltpu.VMEM((width, cols), bf), pltpu.VMEM((width, cols), bf), pltpu.VMEM((cols, width), bf),
                        pltpu.VMEM((rows, cols), bf), pltpu.VMEM((rows, cols), bf), pltpu.VMEM((rows, cols), bf),
                        pltpu.SemaphoreType.DMA((2 + 3 * tiles,)),
                        pltpu.SemaphoreType.DMA((2, 8 * groups)),
                        ],
        compiler_params=pltpu.CompilerParams(collective_id=2, has_side_effects=True, vmem_limit_bytes=60 << 20),
        cost_estimate=pl.CostEstimate(flops=12 * rows * width * cols, bytes_accessed=2 * (3 * width * cols + 8 * rows * width), transcendentals=rows * cols),
        name="feed_forward",
    )(normed, grad_output, part_g, cross_g, w_gate, w_up, w_down)

def wgrad_kernel(n_dp, n_tensor, own_n, all_n, own_g, part_g, cross_g, rest_g, gate_t, up_t, down_hbm, back_hbm, first_hbm,
                 d_own_o, d_send_o, g_sum_o, u_own_o, u_send_o, sum_o, first_o,
                 d_own, d_send, g_sum, u_own, u_send, sum_ref, g_own, g_send, g_in, n_all, g_all, wg, wu, wd, hid, lowg, lowu, mine, in1, mid, in2, load, far, ar, sy, outs):
    rows, width = own_n.shape
    share = gate_t.shape[0]
    groups = n_dp // PAIR
    me_dp, me_t = lax.axis_index("dp"), lax.axis_index("tensor")
    member = lax.rem(me_dp, PAIR)
    bits = []
    bit = n_tensor // 2
    while bit:
        bits.append(bit); bit //= 2
    piece = rows // n_tensor
    def part(t):
        return pl.ds(pl.multiple_of(t * piece, piece), piece)
    def at(r, t):
        return pl.ds(pl.multiple_of(r * rows + t * piece, piece), piece)
    count = [0]
    def cp(s, d):
        c = pltpu.make_async_copy(s, d, load.at[count[0]]); count[0] += 1
        c.start(); return c
    half = rows // 2
    low = lax.rem(me_t, 2)
    def half_rows(c):
        return pl.ds(pl.multiple_of(c * half, half), half)
    last = groups - 1
    if last > 0:
        w_last = cp(all_n.at[last - 1].at[part(me_t), :], n_all.at[at(last, me_t), :])
    w1 = [cp(gate_t, wg), cp(own_n, n_all.at[pl.ds(0, rows), :])]
    w2 = [cp(up_t, wu)]
    w3 = [cp(down_hbm.at[pl.ds(pl.multiple_of(me_dp // PAIR * share, share), share), :], wd), cp(own_g, g_all.at[pl.ds(0, rows), :])]
    w4 = [cp(back_hbm.at[half_rows(low), :], mine)]
    first_block = count[0]
    def load_block(r):
        i = first_block + (r - 1) * (1 + n_tensor)
        def one(s, d, j):
            return pltpu.make_async_copy(s, d, load.at[i + j])
        out = []
        if r < last:
            out.append(one(all_n.at[r - 1], n_all.at[pl.ds(r * rows, rows), :], 0))
        out.append(one(part_g.at[r - 1], g_all.at[at(r, me_t), :], 1))
        if r == last and last > 1:
            return out
        for j, h in enumerate((flip(me_t, 1), flip(me_t, 2), flip(flip(me_t, 1), 2))):
            src = cross_g if r == 1 and j == 1 else rest_g.at[r - 1].at[part(h), :]
            out.append(one(src, g_all.at[at(r, h), :], 2 + j))
        return out
    def start(cs):
        for c in cs:
            c.start()
    pair = flip(me_dp, 1)
    core, across = flip(me_t, 1), flip(me_t, 2)
    right, left = lax.rem(me_dp + PAIR, n_dp), lax.rem(me_dp + n_dp - PAIR, n_dp)
    meet(("dp", pair), ("dp", right), ("dp", left), ("tensor", core), ("tensor", across))
    last_g = []
    if last > 1:
        src = cross_g if last == 2 else rest_g.at[last - 2].at[part(across), :]
        last_g = [lambda: remote(src, g_all.at[at(last, across), :], far, 3, "dp", right),
                  lambda: remote(part_g.at[last - 1], g_all.at[at(last, me_t), :], far, 4, "tensor", core),
                  lambda: remote(g_all.at[at(last, across), :], g_all.at[at(last, across), :], far, 5, "tensor", core)]
        last_g[0]().start()
    def ring(k):
        src = first_hbm.at[part(me_t), :] if k == 1 else first_o.at[k - 2]
        return remote(src, first_o.at[k - 1], far, 5 + k, "dp", right)
    if last > 0:
        ring(1).start()
    ar1 = send(back_hbm.at[half_rows(1 - low), :], in1, ar, 0, "tensor", core)
    def wait(cs):
        for c in cs:
            c.wait()
    def spread(level):
        held, other = [me_t, across][:level + 1], [across, core][level]
        return [remote(n_all.at[at(last, h), :], n_all.at[at(last, h), :], far, level + i, "tensor", other) for i, h in enumerate(held)]
    if last > 0:
        w_last.wait()
        start(spread(0))
    if last > 1:
        last_g[1]().start()

    sum2 = lambda: remote(mid, in2, ar, 1, "tensor", across)
    def pass_a(r, _):
        for k in range(groups):
            @pl.when(r == k)
            def _():
                if k == 0:
                    wait(w1)
                    wait(w2)
                    wait(w3)
                else:
                    wait(load_block(k))
                if k < last:
                    start(load_block(k + 1))
                if k == max(last - 1, 1):
                    sum2().start()
                if k == last:
                    wait(spread(0))
                    start(spread(1))
                    if last > 1:
                        last_g[0]().wait()
                        last_g[2]().start()
                    wait(spread(1))
                    if last > 1:
                        last_g[1]().wait()
                        last_g[2]().wait()
        rs = pl.ds(pl.multiple_of(r * rows, rows), rows)
        g = nt(wg[...], n_all[rs, :])
        u = nt(wu[...], n_all[rs, :])
        h = nt(wd[...], g_all[rs, :])
        a, b, d = swiglu(g, u, h)
        hid[:, rs] = a
        lowg[:, rs] = b
        lowu[:, rs] = d
        @pl.when(r == 0)
        def _():
            wait(w4)
            ar1.wait()
            mid[...] = (mine[...].astype(jnp.float32) + in1[...].astype(jnp.float32)).astype(jnp.bfloat16)
        return 0
    lax.fori_loop(0, groups, pass_a, 0)
    ar2 = sum2()
    dcols = width // n_dp
    def col_tile(low_ref, own_ref, send_ref):
        def body(q, _):
            a = pl.ds(pl.multiple_of((q * PAIR + member) * dcols, dcols), dcols)
            b = pl.ds(pl.multiple_of((q * PAIR + 1 - member) * dcols, dcols), dcols)
            send_ref[q] = nn(low_ref[...], n_all[:, b]).astype(jnp.bfloat16)
            own_ref[q] = nn(low_ref[...], n_all[:, a]).astype(jnp.bfloat16)
            return 0
        return body
    def to_pair(q):
        return remote(g_send.at[q], g_in.at[q], sy, q, "dp", pair)
    def gate_tile(q, _):
        col_tile(lowg, g_own, g_send)(q, 0)
        to_pair(q).start()
        @pl.when(q == 1)
        def _():
            if last > 1:
                ring(1).wait()
                ring(2).start()
        return 0
    lax.fori_loop(0, groups, gate_tile, 0)
    hrows = share // PAIR
    def down_tile(j, _):
        c = pl.ds(pl.multiple_of(j * 512, 512), 512)
        d_send[:, c] = nn(hid[pl.ds(pl.multiple_of((1 - member) * hrows, hrows), hrows), :], g_all[:, c]).astype(jnp.bfloat16)
        d_own[:, c] = nn(hid[pl.ds(pl.multiple_of(member * hrows, hrows), hrows), :], g_all[:, c]).astype(jnp.bfloat16)
        return 0
    lax.fori_loop(0, width // 512, down_tile, 0)
    stores = []
    def store(src, dst):
        c = pltpu.make_async_copy(src, dst, outs.at[len(stores)])
        c.start()
        stores.append(c)
    store(d_own, d_own_o)
    store(d_send, d_send_o)
    def up_tile(q, _):
        @pl.when(q == groups // 2)
        def _():
            if last > 2:
                ring(2).wait()
                ring(3).start()
        return col_tile(lowu, u_own, u_send)(q, 0)
    lax.fori_loop(0, groups, up_tile, 0)
    store(u_own, u_own_o)
    store(u_send, u_send_o)
    ar2.wait()
    sum_ref[half_rows(low), :] = (mid[...].astype(jnp.float32) + in2[...].astype(jnp.float32)).astype(jnp.bfloat16)
    ar3 = send(sum_ref.at[half_rows(low), :], sum_ref.at[half_rows(low), :], ar, 2, "tensor", core)
    for q in range(groups):
        to_pair(q).wait()
        g_sum[q] = (g_own[q].astype(jnp.float32) + g_in[q].astype(jnp.float32)).astype(jnp.bfloat16)
    store(g_sum, g_sum_o)
    ar3.wait()
    store(sum_ref, sum_o)
    if last > 0:
        ring(last).wait()
    wait(stores)

def wgrad(own_n, all_n, own_g, part_g, cross_g, rest_g, gate_t, up_t, down, back, first, n_dp, n_tensor):
    rows, width = own_n.shape
    share = gate_t.shape[0]
    groups = n_dp // PAIR
    anyspec = pl.BlockSpec(memory_space=pl.ANY)
    vm = pl.BlockSpec(memory_space=pltpu.VMEM)
    bf, f32 = jnp.bfloat16, jnp.float32
    sd = jax.ShapeDtypeStruct
    dcols = width // n_dp
    V = pltpu.VMEM
    tall = groups * rows
    return pl.pallas_call(
        functools.partial(wgrad_kernel, n_dp, n_tensor),
        out_shape=(sd((share // PAIR, width), bf), sd((share // PAIR, width), bf), sd((groups, share, dcols), bf),
                   sd((groups, share, dcols), bf), sd((groups, share, dcols), bf), sd((rows, width), bf),
                   sd((groups - 1, rows // n_tensor, width), bf)),
        in_specs=[anyspec] * 11, out_specs=(anyspec,) * 7,
        scratch_shapes=[*[V((share // PAIR, width), bf)] * 2, *[V((groups, share, dcols), bf)] * 3, V((rows, width), bf), *[V((groups, share, dcols), bf)] * 3, V((tall, width), bf), V((tall, width), bf),
                        V((share, width), bf), V((share, width), bf), V((share, width), bf),
                        V((share, tall), bf), V((share, tall), bf), V((share, tall), bf),
                        *[V((rows // 2, width), bf)] * 4,
                        pltpu.SemaphoreType.DMA((7 + (groups - 1) * (1 + n_tensor),)),
                        pltpu.SemaphoreType.DMA((2, 6 + groups)), pltpu.SemaphoreType.DMA((2, 3)), pltpu.SemaphoreType.DMA((2, groups)), pltpu.SemaphoreType.DMA((6,))],
        compiler_params=pltpu.CompilerParams(collective_id=3, has_side_effects=True, vmem_limit_bytes=62 << 20),
        cost_estimate=pl.CostEstimate(flops=12 * tall * width * share, bytes_accessed=2 * (3 * width * share + 4 * tall * width), transcendentals=tall * share),
        name="weight_gradients",
    )(own_n, all_n, own_g, part_g, cross_g, rest_g, gate_t, up_t, down, back, first)
TILE = 128
CHUNK = 128

def turn(values, cosine, sine):
    lane = lax.broadcasted_iota(jnp.int32, values.shape, 1)
    swapped = jnp.where(lane % HEAD_SIZE < HEAD_SIZE // 2,
                        pltpu.roll(values, 128 - HEAD_SIZE // 2, 1), pltpu.roll(values, HEAD_SIZE // 2, 1))
    return values * cosine + swapped * sine

def place(values, head, side):
    v = values if head == side else pltpu.roll(values, HEAD_SIZE, 1)
    lane = lax.broadcasted_iota(jnp.int32, values.shape, 1)
    return jnp.where(lane // HEAD_SIZE == side, v, jnp.zeros_like(v))

def column_of(row):
    a = lax.broadcasted_iota(jnp.int32, (128, 128), 0)
    b = lax.broadcasted_iota(jnp.int32, (128, 128), 1)
    return jnp.sum(jnp.where(a == b, row.astype(jnp.float32), 0.0), axis=1, keepdims=True)

def bias_of(ids_col, ids_row, row0, col0, shape, window):
    q = lax.broadcasted_iota(jnp.int32, shape, 0) + row0
    k = lax.broadcasted_iota(jnp.int32, shape, 1) + col0
    return jnp.where((ids_col == ids_row) & (k <= q), 0.0, -1e30)

def attention_kernel(n_dp, n_tensor, x_hbm, gain1, wq_hbm, wk_hbm, wv_hbm, wo_hbm, gain2, cos_ref, sin_ref, ids_row, g_hbm, gate_hbm, up_hbm,
                     normed_o, q_o, kv_o, idrow_o, mixed_o, res_o, normed2_o, gate_o, up_o, part_g, cross_g,
                     normed_ref, q_ref, kv_ref, idrow_ref, mixed_ref, res_ref, normed2_ref, gate_t, up_t,
                     x, wq, wk, wv, wo, raw_gate, raw_up, kvar, vvar, ids_flat, tile32, partial, out1, in1, mid, in2, total, load, outs, far, halo, ar):
    rows, width = x.shape
    groups = n_dp // PAIR
    me_dp, me_t = lax.axis_index("dp"), lax.axis_index("tensor")
    right = lax.rem(me_dp + PAIR, n_dp)
    left = lax.rem(me_dp + n_dp - PAIR, n_dp)
    after = lax.rem(me_dp + 1, n_dp)
    before = lax.rem(me_dp + n_dp - 1, n_dp)
    core, across = flip(me_t, 1), flip(me_t, 2)
    piece = rows // n_tensor
    def part(t):
        return pl.ds(pl.multiple_of(t * piece, piece), piece)
    count = [0]
    def cp(s, d):
        c = pltpu.make_async_copy(s, d, load.at[count[0]]); count[0] += 1
        c.start(); return c
    share = raw_gate.shape[1]
    stores = []
    def store(src, dst):
        c = pltpu.make_async_copy(src, dst, outs.at[len(stores)])
        c.start()
        stores.append(c)
    share = raw_gate.shape[1]
    w_x = cp(x_hbm, x); w_k = cp(wk_hbm, wk); w_v = cp(wv_hbm, wv)
    meet(("dp", after), ("dp", before), ("dp", right), ("dp", left), ("tensor", core), ("tensor", across))
    ids_go = send(ids_row, idrow_ref.at[0], halo, 0, "dp", after)
    fine = piece // 2
    def first_part(j):
        first = pl.ds(pl.multiple_of(me_t * piece + j * fine, fine), fine)
        return remote(g_hbm.at[first, :], part_g.at[0].at[pl.ds(j * fine, fine), :], far, j, "dp", right)
    def cross_first():
        return send(part_g.at[0].at[pl.ds(0, fine), :], cross_g.at[pl.ds(0, fine), :], far, groups, "tensor", across)
    def cross_second():
        second = pl.ds(pl.multiple_of(across * piece + fine, fine), fine)
        return remote(g_hbm.at[second, :], cross_g.at[pl.ds(fine, fine), :], far, groups + 1, "dp", right)
    ring0 = first_part(0)
    ring0.start()
    w_q = cp(wq_hbm, wq)
    idrow_ref[1] = ids_row[...]

    w_x.wait()
    def norm_one(i, _):
        r = pl.ds(pl.multiple_of(i * TILE, TILE), TILE)
        v = x[r, :].astype(jnp.float32)
        root = lax.rsqrt(jnp.mean(v * v, axis=1, keepdims=True) + EPS)
        normed_ref[r, :] = (v * root * gain1[...]).astype(jnp.bfloat16)
        return 0
    lax.fori_loop(0, rows // TILE, norm_one, 0)
    w_k.wait(); w_v.wait()
    own = pl.ds(rows, rows)
    kv_ref[1, :, 0:128] = turn(nn(normed_ref[...], wk[...]), cos_ref[...], sin_ref[...]).astype(jnp.bfloat16)
    kv_ref[1, :, 128:256] = nn(normed_ref[...], wv[...]).astype(jnp.bfloat16)
    w_q.wait()
    pairs = wq.shape[1] // 128
    def q_pair(p, _):
        c = pl.ds(pl.multiple_of(p * 256, 256), 256)
        raw = nn(normed_ref[...], wq[:, c])
        for s in range(2):
            d = pl.ds(pl.multiple_of(p * 256 + s * 128, 128), 128)
            q_ref[:, d] = (turn(raw[:, s * 128:(s + 1) * 128], cos_ref[...], sin_ref[...]).astype(jnp.bfloat16) * HEAD_SIZE ** -0.5).astype(jnp.bfloat16)
        return 0
    early = [pl.ds(rows // 2, rows // 2), pl.ds(0, rows // 2)]
    def kv_half(h):
        return remote(kv_ref.at[1].at[early[h], :], kv_ref.at[0].at[early[h], :], halo, 1 + h, "dp", after)
    kv_half(0).start()
    kv_half(1).start()
    w_o = cp(wo_hbm, wo)
    store(normed_ref, normed_o)
    lax.fori_loop(0, pairs // 2, q_pair, 0)
    def variants(b, r0, count):
        src = pl.ds(r0, count)
        dst = pl.ds(b * rows + r0, count)
        for g in range(2):
            for s in range(2):
                kvar[g, s, dst, :] = place(kv_ref[b, src, 0:128], g, s)
                vvar[g, s, dst, :] = place(kv_ref[b, src, 128:256], g, s)
    variants(1, 0, rows)
    ids_go.wait()
    kv_half(0).wait()
    ring0.wait()
    cross0 = cross_first()
    first_part(1).start()
    store(q_ref, q_o)
    store(idrow_ref, idrow_o)
    mine = pl.ds(pl.multiple_of(me_dp // PAIR * share, share), share)
    w_gate = cp(gate_hbm.at[:, mine], raw_gate); w_up = cp(up_hbm.at[:, mine], raw_up)
    variants(0, rows // 2, rows // 2)
    w_o.wait()
    ids_flat[:, 0:rows] = idrow_ref[0]
    ids_flat[:, rows:2 * rows] = idrow_ref[1]

    window = rows + TILE
    def attend(i):
        start = pl.multiple_of(i * TILE, TILE)
        r = pl.ds(start, TILE)
        k = pl.ds(start, window)
        ids_k = ids_flat[:, k]
        bias = bias_of(column_of(ids_flat[:, pl.ds(start + rows, TILE)]), ids_k.astype(jnp.float32), rows, 0, (TILE, window), window)
        bias = jnp.concatenate([bias, bias], axis=0)
        for g in range(2):
            q2 = jnp.concatenate([q_ref[r, (2 * g) * 128:(2 * g + 1) * 128], q_ref[r, (2 * g + 1) * 128:(2 * g + 2) * 128]], axis=0)
            mixed = None
            for s in range(2):
                score = nt(q2, kvar[g, s, k, :]) + bias
                peak = jnp.max(score, axis=1, keepdims=True)
                e = jnp.exp(score - peak)
                l = jnp.sum(e, axis=1, keepdims=True)
                prob = (e * (1.0 / l)).astype(jnp.bfloat16)
                m = nn(prob, vvar[g, s, k, :])
                mixed = m if mixed is None else mixed + m
            for b in range(2):
                mixed_ref[r, (2 * g + b) * 128:(2 * g + b + 1) * 128] = mixed[b * TILE:(b + 1) * TILE, :].astype(jnp.bfloat16)

    hrow = CHUNK // 2
    low = lax.rem(me_t, 2)
    def own_rows(c):
        return pl.ds(pl.multiple_of(c * CHUNK + low * hrow, hrow), hrow)
    def oth_rows(c):
        return pl.ds(pl.multiple_of(c * CHUNK + (1 - low) * hrow, hrow), hrow)
    def project(c):
        r = pl.ds(pl.multiple_of(c * CHUNK, CHUNK), CHUNK)
        def body(j, _):
            d = pl.ds(pl.multiple_of(j * 512, 512), 512)
            tile32[...] = nn(mixed_ref[r, :], wo[:, d])
            out1[c, :, d] = tile32[pl.ds(pl.multiple_of((1 - low) * hrow, hrow), hrow), :].astype(jnp.bfloat16)
            partial[c, :, d] = tile32[pl.ds(pl.multiple_of(low * hrow, hrow), hrow), :]
            return 0
        lax.fori_loop(0, width // 512, body, 0)
    def step1(c):
        return remote(out1.at[c], in1.at[c], ar, 3 * c, "tensor", core)
    def step2(c):
        return remote(mid.at[c], in2.at[c], ar, 3 * c + 1, "tensor", across)
    def add_core(c):
        step1(c).wait()
        mid[c] = (partial[c] + in1[c].astype(jnp.float32)).astype(jnp.bfloat16)
        step2(c).start()
    def step3(c):
        total[own_rows(c), :] = (mid[c].astype(jnp.float32) + in2[c].astype(jnp.float32)).astype(jnp.bfloat16)
        return send(total.at[own_rows(c), :], total.at[own_rows(c), :], ar, 3 * c + 2, "tensor", core)
    def finish(r):
        v = x[r, :].astype(jnp.float32) + total[r, :].astype(jnp.float32)
        res_ref[r, :] = v
        root = lax.rsqrt(jnp.mean(v * v, axis=1, keepdims=True) + EPS)
        normed2_ref[r, :] = (v * root * gain2[...]).astype(jnp.bfloat16)

    chunks = rows // CHUNK
    flights = {}
    steps = groups - 1
    def ring(s):
        return remote(part_g.at[s - 2], part_g.at[s - 1], far, s, "dp", right)
    tiles = rows // TILE
    def tile_step(j, _):
        @pl.when(j == tiles // 2)
        def _():
            kv_half(1).wait()
            variants(0, 0, rows // 2)
        i = tiles - 1 - j
        attend(i)
        @pl.when(j > 0)
        def _():
            add_core(i + 1)
        project(i)
        step1(i).start()
        @pl.when(j == 0)
        def _():
            first_part(1).wait()
            cross_second().start()
            if steps > 1:
                ring(2).start()
        return 0
    lax.fori_loop(0, tiles, tile_step, 0)
    store(mixed_ref, mixed_o)
    store(kv_ref, kv_o)
    def transpose_into(dst, raw):
        def body(j, _):
            r = pl.ds(pl.multiple_of(j * 256, 256), 256)
            dst[:, r] = raw[r, :].T
            return 0
        lax.fori_loop(0, width // 256, body, 0)
    add_core(0)
    w_gate.wait()
    transpose_into(gate_t, raw_gate)
    store(gate_t, gate_o)
    w_up.wait()
    transpose_into(up_t, raw_up)
    store(up_t, up_o)
    def out_rows(c):
        flights[3, c].wait()
        finish(oth_rows(c))
        r = pl.ds(c * CHUNK, CHUNK)
        store(res_ref.at[r, :], res_o.at[r, :])
        store(normed2_ref.at[r, :], normed2_o.at[r, :])
    for n in range(chunks):
        c = chunks - 1 - n
        if 3 <= n + 2 <= steps:
            ring(n + 1).wait()
            ring(n + 2).start()
        step2(c).wait()
        flights[3, c] = step3(c)
        finish(own_rows(c))
        if n > 0:
            out_rows(c + 1)
    out_rows(0)
    if steps > 1:
        ring(steps).wait()
    cross0.wait()
    cross_second().wait()
    for q in stores:
        q.wait()

def attend_forward(x, gain1, wq, wk, wv, wo, gain2, cosine, sine, ids, grad_output, w_gate, w_up, n_dp, n_tensor):
    rows, width = x.shape
    groups = n_dp // PAIR
    anyspec = pl.BlockSpec(memory_space=pl.ANY)
    vm = pl.BlockSpec(memory_space=pltpu.VMEM)
    bf, f32 = jnp.bfloat16, jnp.float32
    sd = jax.ShapeDtypeStruct
    V = pltpu.VMEM
    piece = rows // n_tensor
    chunks = rows // CHUNK
    qc = wq.shape[1]
    share = w_gate.shape[1] // groups
    D = pltpu.SemaphoreType.DMA
    return pl.pallas_call(
        functools.partial(attention_kernel, n_dp, n_tensor),
        out_shape=(sd((rows, width), bf), sd((rows, qc), bf), sd((2, rows, 256), bf), sd((2, 1, rows), jnp.int32),
                   sd((rows, qc), bf), sd((rows, width), f32), sd((rows, width), bf), sd((share, width), bf), sd((share, width), bf),
                   sd((groups - 1, piece, width), bf), sd((piece, width), bf)),
        in_specs=[anyspec, vm, anyspec, anyspec, anyspec, anyspec, vm, vm, vm, vm, anyspec, anyspec, anyspec],
        out_specs=(anyspec,) * 11,
        scratch_shapes=[V((rows, width), bf), V((rows, qc), bf), V((2, rows, 256), bf), V((2, 1, rows), jnp.int32), V((rows, qc), bf),
                        V((rows, width), f32), V((rows, width), bf), V((share, width), bf), V((share, width), bf),
                        V((rows, width), bf), V((width, qc), bf), V((width, 128), bf), V((width, 128), bf), V((qc, width), bf), V((width, share), bf), V((width, share), bf),
                        V((2, 2, 2 * rows, 128), bf), V((2, 2, 2 * rows, 128), bf), V((1, 2 * rows), jnp.int32), V((CHUNK, 512), f32),
                        V((chunks, CHUNK // 2, width), f32), V((chunks, CHUNK // 2, width), bf), V((chunks, CHUNK // 2, width), bf),
                        V((chunks, CHUNK // 2, width), bf), V((chunks, CHUNK // 2, width), bf), V((rows, width), bf),
                        D((7,)), D((7 + 2 * chunks,)), D((2, groups + 2)), D((2, 3)), D((2, 3 * chunks))],
        compiler_params=pltpu.CompilerParams(collective_id=1, has_side_effects=True, vmem_limit_bytes=62 << 20),
        cost_estimate=pl.CostEstimate(flops=2 * rows * width * (2 * qc + 256) + 16 * rows * rows * 5 * 128, bytes_accessed=2 * (width * (2 * qc + 256) + 6 * rows * width), transcendentals=8 * rows * rows),
        name="attention_forward",
    )(x, gain1.reshape(1, width), wq, wk, wv, wo, gain2.reshape(1, width), cosine, sine, ids.reshape(1, rows), grad_output, w_gate, w_up)

def backward_kernel(n_dp, n_tensor, gn_hbm, res_hbm, x_hbm, go_hbm, mlp_hbm, normed_hbm, wo_hbm, wq_hbm, wk_hbm, wv_hbm,
                    g_sum, u_own_hbm, u_send, d_send, mixed_hbm, q_hbm, kv_hbm, first_part, gain1, gain2, gain2_part, id_rows, ids_row, cos_ref, sin_ref,
                    out_hbm, gin_hbm, gz, uz, d_in, wz, qz, first_all, gains_ref,
                    gn, res, go, normed, wo, wq, wk, wv, mixed, q_ref, kv_ref, resid, low_res, gm, kvar, vvar, kvart, dk, dv, ids_col,
                    low, lowt, tile32, wsend, wown, win, win2, own_block, u_own, uyin, usum, lg, qsend, qown, qin,
                    amine, amid, min1, min2, ain1, ain2, hprev, hin, gacc, gs, gown, gyi, gzi, gt, gti,
                    load, sy, sz, sx, sh, sg):
    rows, width = go.shape
    groups = n_dp // PAIR
    me_dp, me_t = lax.axis_index("dp"), lax.axis_index("tensor")
    group, member = me_dp // PAIR, lax.rem(me_dp, PAIR)
    pair = flip(me_dp, 1)
    after = lax.rem(me_dp + 1, n_dp)
    before = lax.rem(me_dp + n_dp - 1, n_dp)
    core, across = flip(me_t, 1), flip(me_t, 2)
    low_t = lax.rem(me_t, 2)
    def at_group(s):
        return lax.rem(group + s, groups)
    def from_group(s):
        return lax.rem(group + groups - s, groups)
    f32, bf = jnp.float32, jnp.bfloat16
    qc = wq.shape[1]
    dcols = width // n_dp
    half = rows // 2
    def rows_of(start, size):
        return pl.ds(pl.multiple_of(start, size), size)
    def half_rows(c):
        return rows_of(c * half, half)
    def cp(s, d, i):
        c = pltpu.make_async_copy(s, d, load.at[i])
        c.start()
        return c
    w_gn = cp(gn_hbm, gn, 0); w_res = cp(res_hbm, res, 1); w_go = cp(go_hbm, go, 2)
    w_wo = cp(wo_hbm, wo, 3); w_mlp = cp(mlp_hbm.at[half_rows(low_t), :], amine, 4)
    w_g = cp(g_sum.at[group], own_block, 13)
    w_kv = cp(kv_hbm, kv_ref, 5); w_mx = cp(mixed_hbm, mixed, 6); w_qr = cp(q_hbm, q_ref, 7)
    w_own = cp(u_own_hbm, u_own, 8); w_nm = cp(normed_hbm, normed, 9)
    w_q = cp(wq_hbm, wq, 10); w_k = cp(wk_hbm, wk, 11); w_v = cp(wv_hbm, wv, 12)
    meet(("dp", pair), ("dp", after), ("dp", before), ("tensor", core), ("tensor", across),
         *[("dp", at_group(s) * PAIR + member) for s in range(1, groups)])
    def exchange(src, dst, base, distances=range(1, groups)):
        return [send(src.at[at_group(s)], dst.at[group], sz, base + s - 1, "dp", at_group(s) * PAIR + member) for s in distances]
    y_u = send(u_send, uyin, sy, 0, "dp", pair)
    z_g = exchange(g_sum, gz, 0)
    m1 = send(mlp_hbm.at[half_rows(1 - low_t), :], min1, sx, 0, "tensor", core)
    steps = groups - 1
    piece = rows // n_tensor
    def part(t):
        return rows_of(t * piece, piece)
    at_x = 3 + 3 * (rows // CHUNK)
    def first_piece(k):
        return first_part.at[k]
    def spread_x(k):
        return send(first_piece(k), first_all.at[k].at[part(me_t), :], sx, at_x + k, "tensor", across)
    def spread_core(k, t):
        src = first_piece(k) if t is me_t else first_all.at[k].at[part(t), :]
        return send(src, first_all.at[k].at[part(t), :], sx, at_x + (1 + (t is not me_t)) * steps + k, "tensor", core)
    first_x = [spread_x(0)]
    first_c = [spread_core(0, me_t)]

    w_gn.wait(); w_res.wait(); w_go.wait()
    NR = 64
    def norm_two(i, _):
        r = rows_of(i * NR, NR)
        v = res[r, :]
        root = lax.rsqrt(jnp.mean(v * v, axis=1, keepdims=True) + EPS)
        up = gn[r, :].astype(f32) * gain2[...]
        mean = jnp.mean(up * v, axis=1, keepdims=True)
        d = go[r, :].astype(f32) + root * up - v * (root * root * root * mean)
        resid[r, :] = d
        low_res[r, :] = d.astype(bf)
        return 0
    lax.fori_loop(0, rows // NR, norm_two, 0)
    w_wo.wait()
    def mix_tile(i, _):
        r = rows_of(i * half, half)
        gm[r, :] = nt(low_res[r, :], wo[...]).astype(bf)
        return 0
    lax.fori_loop(0, 2, mix_tile, 0)
    w_mlp.wait(); m1.wait()
    amid[...] = (amine[...].astype(f32) + min1[...].astype(f32)).astype(bf)
    w_kv.wait()
    for g in range(2):
        for s in range(2):
            for b in range(2):
                kvar[g, s, pl.ds(b * rows, rows), :] = place(kv_ref[b, :, 0:128], g, s)
                vvar[g, s, pl.ds(b * rows, rows), :] = place(kv_ref[b, :, 128:256], g, s)
            kvart[g, s] = kvar[g, s].T
    dk[...] = jnp.zeros_like(dk)
    dv[...] = jnp.zeros_like(dv)
    m2 = send(amid, min2, sx, 1, "tensor", across)
    for k in range(1, steps):
        first_x.append(spread_x(k))
        first_c.append(spread_core(k, me_t))
    w_g.wait()
    w_g = cp(own_block, gz.at[group], 13)
    w_mx.wait()
    lowt[0:qc, :] = mixed[...].T
    hrow = qc // n_dp
    def wout_tile(j, _):
        c = rows_of(j * 256, 256)
        tile32[...] = nn(lowt[0:qc, :], low_res[:, c])
        for z in range(groups):
            wown[z, :, c] = tile32[rows_of((z * PAIR + member) * hrow, hrow), :].astype(bf)
            wsend[z, :, c] = tile32[rows_of((z * PAIR + 1 - member) * hrow, hrow), :].astype(bf)
        return 0
    lax.fori_loop(0, width // 256, wout_tile, 0)
    w_qr.wait()
    for b in range(2):
        for j in range(rows // 128):
            ids_col[b * rows + j * 128:b * rows + (j + 1) * 128, :] = column_of(id_rows[b][:, j * 128:(j + 1) * 128])
    window = rows + TILE
    def attend(i, _):
        r = rows_of(i * TILE, TILE)
        k = pl.ds(pl.multiple_of(i * TILE, TILE), window)
        kpos = lax.broadcasted_iota(jnp.int32, (window, TILE), 0)
        qpos = lax.broadcasted_iota(jnp.int32, (window, TILE), 1) + rows
        bias = jnp.where((ids_col[k, :] == ids_row[:, r].astype(f32)) & (kpos <= qpos), 0.0, -1e30)
        bias = jnp.concatenate([bias, bias], axis=1)
        for g in range(2):
            q2 = jnp.concatenate([q_ref[r, (2 * g) * 128:(2 * g + 1) * 128], q_ref[r, (2 * g + 1) * 128:(2 * g + 2) * 128]], axis=0)
            do2 = jnp.concatenate([gm[r, (2 * g) * 128:(2 * g + 1) * 128], gm[r, (2 * g + 1) * 128:(2 * g + 2) * 128]], axis=0)
            dqt = None
            for s in range(2):
                st = nt(kvar[g, s, k, :], q2) + bias
                peak = jnp.max(st, axis=0, keepdims=True)
                e = jnp.exp(st - peak)
                pt = e * (1.0 / jnp.sum(e, axis=0, keepdims=True))
                dpt = nt(vvar[g, s, k, :], do2)
                delta = jnp.sum(pt * dpt, axis=0, keepdims=True)
                dst = (pt * (dpt - delta)).astype(bf)
                dv[g, s, k, :] += nn(pt.astype(bf), do2)
                dk[g, s, k, :] += nn(dst, q2)
                part = nn(kvart[g, s, :, k], dst)
                dqt = part if dqt is None else dqt + part
            d = dqt.T * HEAD_SIZE ** -0.5
            for b in range(2):
                low[r, (2 * g + b) * 128:(2 * g + b + 1) * 128] = turn(d[b * TILE:(b + 1) * TILE, :], cos_ref[r, :], -sin_ref[r, :]).astype(bf)
        return 0
    wpart = [pl.ds(0, groups // 2), pl.ds(groups // 2, groups // 2)]
    def pair_wout(j):
        return remote(wsend.at[wpart[j]], win.at[wpart[j]], sy, 1 + 4 * j, "dp", pair)
    def own_up():
        return pltpu.make_async_copy(usum.at[group], uz.at[group], load.at[8])
    def up_near():
        return remote(usum.at[at_group(1)], uz.at[group], sz, groups, "dp", at_group(1) * PAIR + member)
    def attend_step(i, _):
        attend(i, 0)
        @pl.when(i == rows // TILE // 2 - 1)
        def _():
            y_u.wait()
            w_own.wait()
            for z in range(groups):
                usum[z] = (u_own[z].astype(f32) + uyin[z].astype(f32)).astype(bf)
            pair_wout(0).start()
            own_up().start()
            up_near().start()
        return 0
    lax.fori_loop(0, rows // TILE, attend_step, 0)
    w_u = own_up()
    z_u = [up_near()]

    def gathered(acc, b):
        r = pl.ds(b * rows, rows)
        lane = lax.broadcasted_iota(jnp.int32, (rows, 128), 1)
        first = acc[0, 0, r, :] + pltpu.roll(acc[0, 1, r, :], HEAD_SIZE, 1)
        second = pltpu.roll(acc[1, 0, r, :], HEAD_SIZE, 1) + acc[1, 1, r, :]
        return jnp.where(lane < HEAD_SIZE, first, second)
    hprev[:, 0:128] = gathered(dk, 0).astype(bf)
    hprev[:, 128:256] = gathered(dv, 0).astype(bf)
    halo = send(hprev, hin, sh, 0, "dp", before)
    pair_wout(1).start()
    y_w = [pair_wout(0), pair_wout(1)]
    z_u = z_u + exchange(usum, uz, groups, range(2, groups))
    qs, ks = qc // groups, 128 // groups
    def to_groups(row0, count, offset, base):
        lg[0, offset:offset + count, :] = lowt[rows_of(row0 + group * count, count), :]
        return [send(lowt.at[rows_of(row0 + at_group(s) * count, count), :], lg.at[s, offset:offset + count, :], sz, base + s - 1,
                     "dp", at_group(s) * PAIR + member) for s in range(1, groups)]
    lowt[0:qc, :] = low[:, 0:qc].T
    z_low = to_groups(0, qs, 0, 3 * groups)
    m2.wait()
    def out_rows(i, _):
        r = rows_of(low_t * half + i * NR, NR)
        m = rows_of(i * NR, NR)
        summed = (amid[m, :].astype(f32) + min2[m, :].astype(f32)).astype(bf)
        go[r, :] = (res[r, :] + summed.astype(f32)).astype(bf)
        return 0
    lax.fori_loop(0, half // NR, out_rows, 0)
    w_out = cp(go.at[half_rows(low_t), :], out_hbm.at[half_rows(low_t), :], 2)
    m3 = send(go.at[half_rows(low_t), :], out_hbm.at[half_rows(low_t), :], sx, 2, "tensor", core)
    w_nm.wait()
    halo.wait()
    kraw = gathered(dk, 1) + hin[:, 0:128].astype(f32)
    low[:, qc:qc + 128] = turn(kraw, cos_ref[...], -sin_ref[...]).astype(bf)
    low[:, qc + 128:qc + 256] = (gathered(dv, 1) + hin[:, 128:256].astype(f32)).astype(bf)
    lowt[qc:qc + 256, :] = low[:, qc:qc + 256].T
    z_low = z_low + to_groups(qc, ks, qs, 4 * groups) + to_groups(qc + 128, ks, qs + ks, 5 * groups)
    for q in y_w:
        q.wait()
    quarter = d_send.shape[0] // 4
    def pair_down(first, count, slot):
        r = pl.ds(first * quarter, count * quarter)
        return send(d_send.at[r, :], d_in.at[r, :], sy, slot, "dp", pair)
    y_d = [pair_down(0, 2, 3)]
    for z in range(groups):
        wown[z] = (wown[z].astype(f32) + win[z].astype(f32)).astype(bf)
    near = flip(group, 1)
    far_group = flip(group, 2) if groups == 4 else near
    z_w = []
    if groups == 4:
        z_w = [send(wown.at[t], win2.at[i], sz, 2 * groups + i, "dp", near * PAIR + member) for i, t in enumerate((near, flip(near, 2)))]
    w_q.wait(); w_k.wait(); w_v.wait()
    def normed_part(j, _):
        c = rows_of(j * 256, 256)
        p = (nt(low[:, 0:qc], wq[c, :]) + nt(low[:, qc:qc + 128], wk[c, :]) + nt(low[:, qc + 128:qc + 256], wv[c, :]))
        res[:, c] = p
        gacc[0:1, c] = jnp.sum(p * normed[:, c].astype(f32), axis=0, keepdims=True) / gain1[0:1, c]
        gacc[1:2, c] = gain2_part[0:1, c] / gain2[0:1, c]
        return 0
    lax.fori_loop(0, width // 256, normed_part, 0)
    hchunk = CHUNK // 2
    chunks = rows // CHUNK
    def own_rows(c):
        return rows_of(c * CHUNK + low_t * hchunk, hchunk)
    def oth_rows(c):
        return rows_of(c * CHUNK + (1 - low_t) * hchunk, hchunk)
    def buf(c):
        return pl.ds(c * hchunk, hchunk)
    flights = {}
    for c in range(chunks):
        amine[buf(c), :] = res[oth_rows(c), :].astype(bf)
        flights[1, c] = send(amine.at[buf(c), :], ain1.at[buf(c), :], sx, 3 + 3 * c, "tensor", core)
    for z in range(groups):
        for m in range(PAIR):
            d0 = (z * PAIR + m) * dcols
            gs[m, z, 0:2, :] = gacc[0:2, d0:d0 + dcols]
    gown[...] = gs[member]
    y_gain = send(gs.at[1 - member], gyi, sg, 0, "dp", pair)
    for c in range(chunks):
        flights[1, c].wait()
        amid[buf(c), :] = (res[own_rows(c), :] + ain1[buf(c), :].astype(f32)).astype(bf)
        flights[2, c] = send(amid.at[buf(c), :], ain2.at[buf(c), :], sx, 4 + 3 * c, "tensor", across)
    for q in first_x:
        q.wait()
    first_c = first_c + [spread_core(k, across) for k in range(steps)]
    for q in first_c + [m3]:
        q.wait()
    w_out.wait()
    tokens = [normed, wo, low_res, go][:groups]
    w_first = []
    for k in range(steps):
        for i, t in enumerate((me_t, core, across, flip(core, 2))):
            src = first_piece(k) if i == 0 else first_all.at[k].at[part(t), :]
            w_first.append(cp(src, tokens[k + 1].at[part(t), :], 16 + k * n_tensor + i))
    y_d.append(pair_down(2, 1, 4))
    for q in z_low + w_first:
        q.wait()
    for q in z_w:
        q.wait()
    keep, give = wown[group].astype(f32), wown[far_group].astype(f32)
    if groups == 4:
        keep, give = keep + win2[0].astype(f32), give + win2[1].astype(f32)
    wsend[0] = keep.astype(bf)
    wsend[1] = give.astype(bf)
    y_gain.wait()
    gown[...] = gown[...] + gyi[...]
    z_gain = [send(gown.at[at_group(s)], gzi.at[s - 1], sg, s, "dp", at_group(s) * PAIR + member) for s in range(1, groups)]
    w_w = cp(wsend.at[0], wz.at[0], 3)
    z_w = [send(wsend.at[1], wz.at[1], sz, 2 * groups + 2, "dp", far_group * PAIR + member)]
    hg = groups // 2
    def share_cols(j, _):
        z = at_group(j + 1)
        for dst, m in ((qsend, 1 - member), (qown, member)):
            c = rows_of((z * PAIR + m) * dcols, dcols)
            t = nn(lg[0], tokens[0][:, c])
            for k in range(1, groups):
                t = t + nn(lg[k], tokens[k][:, c])
            dst[j] = t.astype(bf)
        @pl.when(j == hg - 1)
        def _():
            pair_q(0).start()
        return 0
    def pair_q(h):
        r = pl.ds(h * hg, hg)
        return remote(qsend.at[r], qin.at[r], sy, 2 + 4 * h, "dp", pair)
    lax.fori_loop(0, groups, share_cols, 0)
    pair_q(1).start()
    y_d.append(pair_down(3, 1, 7))
    w_x = cp(x_hbm, normed, 9)
    w_x.wait()
    def norm_one(r):
        v = normed[r, :].astype(f32)
        root = lax.rsqrt(jnp.mean(v * v, axis=1, keepdims=True) + EPS)
        up = gn[r, :].astype(f32) * gain1[...]
        mean = jnp.mean(up * v, axis=1, keepdims=True)
        low_res[r, :] = (resid[r, :] + root * up - v * (root * root * root * mean)).astype(bf)
    def sum_q(h):
        pair_q(h).wait()
        for j in range(h * hg, h * hg + hg):
            qown[j] = (qown[j].astype(f32) + qin[j].astype(f32)).astype(bf)
        return [send(qown.at[j], qz.at[group], sz, 6 * groups + j, "dp", at_group(j + 1) * PAIR + member) for j in range(h * hg, min(h * hg + hg, groups - 1))]
    for c in range(chunks):
        flights[2, c].wait()
        gn[own_rows(c), :] = (amid[buf(c), :].astype(f32) + ain2[buf(c), :].astype(f32)).astype(bf)
        flights[3, c] = send(gn.at[own_rows(c), :], gn.at[own_rows(c), :], sx, 5 + 3 * c, "tensor", core)
        norm_one(own_rows(c))
        flights[3, c].wait()
        norm_one(oth_rows(c))
        if c == chunks // 2 - 1:
            z_q = sum_q(0)
    w_gin = cp(low_res, gin_hbm, 1)
    z_q = z_q + sum_q(1)
    w_q2 = cp(qown.at[groups - 1], qz.at[group], 14)
    for q in z_gain:
        q.wait()
    total = gown[group]
    for s in range(1, groups):
        total = total + gzi[s - 1]
    gt[0] = total
    t1 = send(gt.at[0], gti.at[0], sg, groups, "tensor", core)
    t1.wait()
    gt[1] = gt[0] + gti[0]
    t2 = send(gt.at[1], gti.at[1], sg, groups + 1, "tensor", across)
    t2.wait()
    gains_ref[...] = gt[1] + gti[1]
    for q in z_g + z_u + z_w + z_q + y_d:
        q.wait()
    for q in [w_g, w_u, w_w, w_gin, w_q2]:
        q.wait()

def backward(gn, residual, x, grad_output, mlp_part, normed, wo, wq, wk, wv, g_sum, u_own, u_send, d_send, mixed, q, kv, first, gain1, gain2, gain2_part,
             id_rows, ids_row, cosine, sine, n_dp, n_tensor):
    rows, width = x.shape
    groups = n_dp // PAIR
    share = g_sum.shape[1]
    dcols = width // n_dp
    qc = wq.shape[1]
    cols = qc + 256
    share_q = cols // groups
    A = pl.BlockSpec(memory_space=pl.ANY)
    vm = pl.BlockSpec(memory_space=pltpu.VMEM)
    bf, f32 = jnp.bfloat16, jnp.float32
    sd = jax.ShapeDtypeStruct
    V = pltpu.VMEM
    D = pltpu.SemaphoreType.DMA
    half = rows // 2
    hrow = qc // n_dp
    act = V((rows, width), bf)
    return pl.pallas_call(
        functools.partial(backward_kernel, n_dp, n_tensor),
        out_shape=(sd((rows, width), bf), sd((rows, width), bf), sd((groups, share, dcols), bf), sd((groups, share, dcols), bf),
                   sd(d_send.shape, bf), sd((2, hrow, width), bf), sd((groups, share_q, dcols), bf),
                   sd((groups - 1, rows, width), bf), sd((8, dcols), f32)),
        in_specs=[A] * 18 + [vm] * 7,
        out_specs=(A,) * 8 + (vm,),
        scratch_shapes=[act, V((rows, width), f32), act, act, V((qc, width), bf), V((width, qc), bf), V((width, 128), bf), V((width, 128), bf),
                        V((rows, qc), bf), V((rows, qc), bf), V((2, rows, 256), bf), V((rows, width), f32), act, V((rows, qc), bf),
                        V((2, 2, 2 * rows, 128), bf), V((2, 2, 2 * rows, 128), bf), V((2, 2, 128, 2 * rows), bf),
                        V((2, 2, 2 * rows, 128), f32), V((2, 2, 2 * rows, 128), f32), V((2 * rows, 1), f32),
                        V((rows, cols), bf), V((cols, rows), bf), V((qc, 256), f32),
                        V((groups, hrow, width), bf), V((groups, hrow, width), bf), V((groups, hrow, width), bf), V((2, hrow, width), bf),
                        V((share, dcols), bf), *[V((groups, share, dcols), bf)] * 3,
                        V((groups, share_q, rows), bf), *[V((groups, share_q, dcols), bf)] * 3,
                        *[V((half, width), bf)] * 6,
                        V((rows, 256), bf), V((rows, 256), bf), V((8, width), f32), V((PAIR, groups, 8, dcols), f32), V((groups, 8, dcols), f32),
                        V((groups, 8, dcols), f32), V((groups - 1, 8, dcols), f32), V((2, 8, dcols), f32), V((2, 8, dcols), f32),
                        D((16 + groups * n_tensor,)), D((2, 8)), D((2, 8 * groups)), D((2, 3 + 3 * (rows // CHUNK) + 3 * groups)), D((2, 1)), D((2, groups + 2))],
        compiler_params=pltpu.CompilerParams(collective_id=4, has_side_effects=True, vmem_limit_bytes=67043328),
        cost_estimate=pl.CostEstimate(flops=4 * rows * width * (2 * qc + 256) + 40 * rows * rows * 5 * 128, bytes_accessed=40 * rows * width, transcendentals=8 * rows * rows),
        name="attention_backward",
    )(gn, residual, x, grad_output, mlp_part, normed, wo, wq, wk, wv, g_sum, u_own, u_send, d_send, mixed, q, kv, first,
      gain1.reshape(1, width), gain2.reshape(1, width), gain2_part, id_rows, ids_row, cosine, sine)

def finish_kernel(qc, kc, out_hbm, gin_hbm, gz_hbm, uz_hbm, d_own_hbm, d_in_hbm, wz_hbm, qz_hbm, gains,
                  gain1_o, gain2_o, out_o, gin_o, gate_o, up_o, down_o, wout_o, query_o, key_o, value_o,
                  act1, act2, gz, uz, d_own, d_in, wz, qz, gate, up, down, wout, query, key, value, ins, outs):
    f32 = jnp.float32
    groups, share, dcols = gz.shape
    gain1_o[...] = gains[0:1, :]
    gain2_o[...] = gains[1:2, :]
    loads = [pltpu.make_async_copy(s, d, ins.at[i]) for i, (s, d) in enumerate([
        (gz_hbm, gz), (uz_hbm, uz), (out_hbm, act1), (gin_hbm, act2), (d_own_hbm, d_own), (d_in_hbm, d_in), (wz_hbm, wz), (qz_hbm, qz)])]
    for c in loads:
        c.start()
    stores = []
    def store(src, dst):
        c = pltpu.make_async_copy(src, dst, outs.at[len(stores)])
        c.start()
        stores.append(c)
    for got, held, dst, i in ((gz, gate, gate_o, 0), (uz, up, up_o, 1)):
        loads[i].wait()
        for z in range(groups):
            for h in range(share // 256):
                held[:, z * share + h * 256:z * share + (h + 1) * 256] = got[z, h * 256:(h + 1) * 256, :].astype(f32).T
        store(held, dst)
    loads[2].wait()
    store(act1, out_o)
    loads[3].wait()
    store(act2, gin_o)
    loads[4].wait()
    loads[5].wait()
    down[...] = d_own[...].astype(f32) + d_in[...].astype(f32)
    store(down, down_o)
    loads[6].wait()
    wout[...] = wz[0].astype(f32) + wz[1].astype(f32)
    store(wout, wout_o)
    loads[7].wait()
    qs, ks = qc // groups, kc // groups
    for z in range(groups):
        query[:, z * qs:(z + 1) * qs] = qz[z, 0:qs, :].astype(f32).T
    key[...] = jnp.concatenate([qz[z, qs:qs + ks, :] for z in range(groups)], axis=0).astype(f32).T
    value[...] = jnp.concatenate([qz[z, qs + ks:qs + 2 * ks, :] for z in range(groups)], axis=0).astype(f32).T
    store(query, query_o)
    store(key, key_o)
    store(value, value_o)
    for c in stores:
        c.wait()

def finish_all(out, gin, gz, uz, d_own, d_in, wz, qz, gains, qc, kc):
    vm = pl.BlockSpec(memory_space=pltpu.VMEM)
    A = pl.BlockSpec(memory_space=pl.ANY)
    bf, f32 = jnp.bfloat16, jnp.float32
    sd = jax.ShapeDtypeStruct
    V = pltpu.VMEM
    groups, share, dcols = gz.shape
    shapes = [(dcols, groups * share), (dcols, groups * share), d_own.shape, wz.shape[1:], (dcols, qc), (dcols, kc), (dcols, kc)]
    return pl.pallas_call(
        functools.partial(finish_kernel, qc, kc),
        out_shape=(sd((1, dcols), f32), sd((1, dcols), f32), sd(out.shape, bf), sd(gin.shape, bf)) + tuple(sd(s, f32) for s in shapes),
        in_specs=[A] * 8 + [vm], out_specs=(vm,) * 2 + (A,) * 9,
        scratch_shapes=[V(a.shape, bf) for a in (out, gin, gz, uz, d_own, d_in, wz, qz)] + [V(s, f32) for s in shapes] + [pltpu.SemaphoreType.DMA((8,)), pltpu.SemaphoreType.DMA((9,))],
        compiler_params=pltpu.CompilerParams(vmem_limit_bytes=67043328),
        cost_estimate=pl.CostEstimate(flops=8 * out.size, bytes_accessed=24 << 20, transcendentals=0),
        name="finish",
    )(out, gin, gz, uz, d_own, d_in, wz, qz, gains)


def rope_table(half_count, copies=1):
    adjusted = []
    for index in range(half_count):
        base_value = 500000.0 ** (-index / half_count)
        wave_length = 2.0 * math.pi / base_value
        smooth = (8192.0 / wave_length - 1.0) / 3.0
        if wave_length > 8192.0:
            adjusted.append(base_value / 32.0)
        elif wave_length >= 2048.0:
            adjusted.append((1.0 - smooth) * base_value / 32.0 + smooth * base_value)
        else:
            adjusted.append(base_value)
    return jnp.asarray(adjusted * copies, dtype=jnp.float32)


def rope_angles(start_row, count_rows, half_count):
    positions = (start_row + jnp.arange(count_rows, dtype=jnp.int32)).astype(jnp.float32)
    phase_angle = positions[:, None] * rope_table(half_count)[None, :]
    return (jnp.cos(phase_angle)[:, None, :], jnp.sin(phase_angle)[:, None, :])


def rotate_halves(values, cosine_table, sine_values):
    half_size = values.shape[-1] // 2
    first_half = values[..., :half_size]
    second_half = values[..., half_size:]
    return jnp.concatenate(
        [
            first_half * cosine_table - second_half * sine_values,
            second_half * cosine_table + first_half * sine_values,
        ],
        axis=-1,
    )


def norm_rows(values, gain_row):
    inverse_root = lax.rsqrt(jnp.mean(values * values, axis=-1, keepdims=True) + NORM_EPSILON)
    return (inverse_root, values * inverse_root * gain_row)


def norm_back(values, inverse_root, gain_row, upstream):
    scaled = gain_row * upstream
    return inverse_root * scaled - values * inverse_root**3 * jnp.mean(
        scaled * values, axis=-1, keepdims=True
    )


def passed_along(block, axis, distance):
    devices = range(lax.axis_size(axis))
    route = [(i - distance, i) for i in devices if i - distance in devices]
    return lax.ppermute(block, axis, route)


def tensor_swap(block, bit):
    return lax.ppermute(block, "tensor", [(i, i ^ bit) for i in range(lax.axis_size("tensor"))])


def pair_swap(block):
    return lax.ppermute(block, "dp", [(i, i ^ 1) for i in range(lax.axis_size("dp"))])


def group_shift(block, distance):
    count = lax.axis_size("dp")
    groups = count // PAIR
    return lax.ppermute(
        block,
        "dp",
        [(i, ((i // PAIR + distance) % groups) * PAIR + i % PAIR) for i in range(count)],
    )


def tensor_sum(part):
    half = part.shape[1] // 2
    low = lax.axis_index("tensor") % 2
    first, second = part[:, :half], part[:, half:]
    mine = jnp.where(low == 0, first, second)
    other = jnp.where(low == 0, second, first).astype(jnp.bfloat16)
    mine = mine + tensor_swap(other, 1).astype(jnp.float32)
    bit = 2
    while bit < lax.axis_size("tensor"):
        rounded = mine.astype(jnp.bfloat16)
        mine = rounded.astype(jnp.float32) + tensor_swap(rounded, bit).astype(jnp.float32)
        bit *= 2
    mine = mine.astype(jnp.bfloat16)
    other = tensor_swap(mine, 1)
    return jnp.concatenate(
        [jnp.where(low == 0, mine, other), jnp.where(low == 0, other, mine)], axis=1
    ).astype(jnp.float32)


def gather_groups(block):
    half = block.shape[1] // 2
    low = lax.axis_index("tensor") % 2
    piece = lax.dynamic_slice_in_dim(block, low * half, half, axis=1)
    rows = [block]
    for _ in range(lax.axis_size("dp") // PAIR - 1):
        piece = group_shift(piece, 1)
        other = tensor_swap(piece, 1)
        rows.append(
            jnp.concatenate(
                [jnp.where(low == 0, piece, other), jnp.where(low == 0, other, piece)], axis=1
            )
        )
    return jnp.concatenate(rows, axis=0)


def pair_sum(part):
    member = lax.axis_index("dp") % PAIR
    mine = lax.dynamic_index_in_dim(part, member, 1, keepdims=False)
    other = lax.dynamic_index_in_dim(part, 1 - member, 1, keepdims=False)
    return mine + pair_swap(other.astype(jnp.bfloat16)).astype(jnp.float32)


def group_exchange(blocks):
    groups = blocks.shape[0]
    group = lax.axis_index("dp") // PAIR
    received = []
    for distance in range(groups):
        block = lax.dynamic_index_in_dim(blocks, (group + distance) % groups, 0, keepdims=False)
        received.append(block if distance == 0 else group_shift(block, distance))
    return received


def scatter_sum(part):
    summed = pair_sum(part)
    groups = summed.shape[0]
    group = lax.axis_index("dp") // PAIR
    total = lax.dynamic_index_in_dim(summed, group, 0, keepdims=False)
    rounded = summed.astype(jnp.bfloat16)
    for block in group_exchange(rounded)[1:]:
        total = total + block.astype(jnp.float32)
    return total


def block_scores(query_rows, key_rows, query_ids, key_ids, query_pos, key_pos):
    scores = jnp.einsum(
        "qgrd,kgd->grqk", query_rows, key_rows, preferred_element_type=jnp.float32
    ) * HEAD_SIZE ** (-0.5)
    allowed = (query_ids[:, None] == key_ids[None, :]) & (key_pos[None, :] <= query_pos[:, None])
    return jnp.where(allowed, scores, -1e30)


def block_forward(query_rows, key_rows, value_rows, query_ids, key_ids, query_pos, key_pos):
    scores = block_scores(query_rows, key_rows, query_ids, key_ids, query_pos, key_pos)
    row_peak = jnp.max(scores, axis=-1, keepdims=True)
    logsum = row_peak + jnp.log(jnp.sum(jnp.exp(scores - row_peak), axis=-1, keepdims=True))
    prob_low = jnp.exp(scores - logsum).astype(jnp.bfloat16)
    mixed_rows = jnp.einsum(
        "grqk,kgd->qgrd", prob_low, value_rows, preferred_element_type=jnp.float32
    )
    return (mixed_rows.astype(jnp.bfloat16), logsum)


def block_backward(
    query_rows,
    key_rows,
    value_rows,
    out_rows,
    grad_rows,
    logsum,
    query_ids,
    key_ids,
    query_pos,
    key_pos,
):
    scores = block_scores(query_rows, key_rows, query_ids, key_ids, query_pos, key_pos)
    prob_rows = jnp.exp(scores - logsum)
    grad_vals = jnp.einsum(
        "grqk,qgrd->kgd",
        prob_rows.astype(jnp.bfloat16),
        grad_rows,
        preferred_element_type=jnp.float32,
    )
    delta_rows = jnp.sum(out_rows.astype(jnp.float32) * grad_rows.astype(jnp.float32), axis=-1)
    grad_probs = jnp.einsum(
        "qgrd,kgd->grqk", grad_rows, value_rows, preferred_element_type=jnp.float32
    )
    grad_scores = (
        prob_rows * (grad_probs - jnp.transpose(delta_rows, (1, 2, 0))[..., None])
    ).astype(jnp.bfloat16)
    grad_query_rows = jnp.einsum(
        "grqk,kgd->qgrd", grad_scores, key_rows, preferred_element_type=jnp.float32
    ) * HEAD_SIZE ** (-0.5)
    grad_key_rows = jnp.einsum(
        "grqk,qgrd->kgd", grad_scores, query_rows, preferred_element_type=jnp.float32
    ) * HEAD_SIZE ** (-0.5)
    return (grad_query_rows, grad_key_rows, grad_vals)


def dot(form, left, right):
    return jnp.einsum(form, left, right, preferred_element_type=jnp.float32)


def gated(gate_value, up_value):
    return (jax.nn.silu(gate_value) * up_value).astype(jnp.bfloat16)


def gated_back(grad_hidden, gate_value, up_value):
    sigmoid_gate = jax.nn.sigmoid(gate_value)
    grad_gate_low = (
        grad_hidden * up_value * sigmoid_gate * (1.0 + gate_value * (1.0 - sigmoid_gate))
    ).astype(jnp.bfloat16)
    return grad_gate_low, (grad_hidden * jax.nn.silu(gate_value)).astype(jnp.bfloat16)


def shards_plain(
    inputs,
    norm1_gain,
    query_weight,
    key_weight,
    value_weight,
    w_out,
    norm2_gain,
    w_gate,
    w_up,
    w_down,
    doc_ids,
    grad_output,
):
    tok_rows, width = inputs.shape
    heads_here = query_weight.shape[1] // HEAD_SIZE
    kv_here = key_weight.shape[1] // HEAD_SIZE
    group_size = heads_here // kv_here
    n_dp = lax.axis_size("dp")
    groups = n_dp // PAIR
    group = lax.axis_index("dp") // PAIR
    offset = lax.axis_index("dp") * tok_rows
    grad_all = gather_groups(grad_output)

    cosine_table, sine_values = rope_angles(offset, tok_rows, HEAD_SIZE // 2)
    inputs_wide = inputs.astype(jnp.float32)
    root_one, normed = norm_rows(inputs_wide, norm1_gain)
    normed_low = normed.astype(jnp.bfloat16)
    query_raw = dot("td,dh->th", normed_low, query_weight).reshape(tok_rows, heads_here, HEAD_SIZE)
    key_raw = dot("td,dh->th", normed_low, key_weight).reshape(tok_rows, kv_here, HEAD_SIZE)
    value_low = dot("td,dh->th", normed_low, value_weight).astype(jnp.bfloat16)
    query_low = (
        rotate_halves(query_raw, cosine_table, sine_values)
        .astype(jnp.bfloat16)
        .reshape(tok_rows, kv_here, group_size, HEAD_SIZE)
    )
    key_low = (
        rotate_halves(key_raw, cosine_table, sine_values)
        .astype(jnp.bfloat16)
        .reshape(tok_rows, kv_here * HEAD_SIZE)
    )
    query_ids = doc_ids + 1
    tail = jnp.concatenate([key_low, value_low], axis=1)
    prev_tail = passed_along(tail, "dp", 1)
    prev_ids = passed_along(query_ids, "dp", 1)
    both = jnp.concatenate([prev_tail, tail], axis=0)
    keys_all = both[:, : kv_here * HEAD_SIZE].reshape(2 * DOC_MAX, kv_here, HEAD_SIZE)
    values_all = both[:, kv_here * HEAD_SIZE :].reshape(2 * DOC_MAX, kv_here, HEAD_SIZE)
    ids_all = jnp.concatenate([prev_ids, query_ids])
    pos_all = offset - DOC_MAX + jnp.arange(tok_rows + DOC_MAX, dtype=jnp.int32)
    query_pos = pos_all[DOC_MAX:]
    mixed_block, logsum_block = block_forward(
        query_low, keys_all, values_all, query_ids, ids_all, query_pos, pos_all
    )
    mixed_low = mixed_block.reshape(tok_rows, heads_here * HEAD_SIZE)
    residual = inputs_wide + tensor_sum(dot("te,ed->td", mixed_low, w_out))

    root_two, normed_two = norm_rows(residual, norm2_gain)
    normed_two_low = normed_two.astype(jnp.bfloat16)
    normed_all = gather_groups(normed_two_low)
    gate_value = dot("td,df->tf", normed_two_low, w_gate)
    up_value = dot("td,df->tf", normed_two_low, w_up)
    grad_hidden = dot("td,fd->tf", grad_output, w_down)
    hidden_low = gated(gate_value, up_value)
    grad_gate_low, grad_up_low = gated_back(grad_hidden, gate_value, up_value)
    normed_two_part = dot("tf,df->td", grad_gate_low, w_gate) + dot("tf,df->td", grad_up_low, w_up)
    grad_normed_two = tensor_sum(normed_two_part)
    gain_two_part = jnp.sum(normed_two_part * residual * root_two, axis=0)
    output = (residual + tensor_sum(dot("tf,fd->td", hidden_low, w_down))).astype(jnp.bfloat16)

    share = w_gate.shape[1] // groups
    gate_share = lax.dynamic_slice_in_dim(w_gate, group * share, share, axis=1)
    up_share = lax.dynamic_slice_in_dim(w_up, group * share, share, axis=1)
    down_share = lax.dynamic_slice_in_dim(w_down, group * share, share, axis=0)
    gate_all = dot("td,df->tf", normed_all, gate_share)
    up_all = dot("td,df->tf", normed_all, up_share)
    grad_hidden_all = dot("td,fd->tf", grad_all, down_share)
    hidden_all = gated(gate_all, up_all)
    gate_low_all, up_low_all = gated_back(grad_hidden_all, gate_all, up_all)
    down_part = dot("tf,td->fd", hidden_all, grad_all)
    grad_wdown = pair_sum(down_part.reshape(1, PAIR, share // PAIR, width))[0]
    rows_here = width // n_dp

    def column_grad(low_all):
        part = dot("td,tf->df", normed_all, low_all)
        summed = pair_sum(part.reshape(groups, PAIR, rows_here, share)).astype(jnp.bfloat16)
        full = jnp.zeros((rows_here, groups * share), jnp.float32)
        for distance, block in enumerate(group_exchange(summed)):
            full = lax.dynamic_update_slice_in_dim(
                full, block.astype(jnp.float32), ((group - distance) % groups) * share, axis=1
            )
        return full

    grad_wgate = column_grad(gate_low_all)
    grad_wup = column_grad(up_low_all)

    grad_residual = grad_output.astype(jnp.float32) + norm_back(
        residual, root_two, norm2_gain, grad_normed_two
    )
    grad_res_low = grad_residual.astype(jnp.bfloat16)
    wout_part = dot("te,td->ed", mixed_low, grad_res_low)
    grad_wout = scatter_sum(wout_part.reshape(groups, PAIR, -1, width))
    grad_mixed = (
        dot("td,ed->te", grad_res_low, w_out)
        .astype(jnp.bfloat16)
        .reshape(tok_rows, kv_here, group_size, HEAD_SIZE)
    )
    mixed_view = mixed_low.reshape(tok_rows, kv_here, group_size, HEAD_SIZE)
    grad_query_rows, grad_key_rows, grad_value_rows = block_backward(
        query_low,
        keys_all,
        values_all,
        mixed_view,
        grad_mixed,
        logsum_block,
        query_ids,
        ids_all,
        query_pos,
        pos_all,
    )
    sent = jnp.concatenate(
        [
            grad_key_rows.reshape(2 * DOC_MAX, kv_here * HEAD_SIZE),
            grad_value_rows.reshape(2 * DOC_MAX, kv_here * HEAD_SIZE),
        ],
        axis=1,
    )
    back = passed_along(sent[:DOC_MAX].astype(jnp.bfloat16), "dp", -1).astype(jnp.float32)
    own = sent[DOC_MAX:] + back
    grad_qraw = grad_query_rows.reshape(tok_rows, heads_here, HEAD_SIZE)
    query_low_gradient = (
        rotate_halves(grad_qraw, cosine_table, -sine_values)
        .astype(jnp.bfloat16)
        .reshape(tok_rows, heads_here * HEAD_SIZE)
    )
    key_low_gradient = (
        rotate_halves(
            own[:, : kv_here * HEAD_SIZE].reshape(tok_rows, kv_here, HEAD_SIZE),
            cosine_table,
            -sine_values,
        )
        .astype(jnp.bfloat16)
        .reshape(tok_rows, kv_here * HEAD_SIZE)
    )
    value_low_gradient = own[:, kv_here * HEAD_SIZE :].astype(jnp.bfloat16)
    low_gradient = jnp.concatenate(
        [query_low_gradient, key_low_gradient, value_low_gradient], axis=1
    )
    normed_one_part = (
        dot("kl,ql->kq", query_low_gradient, query_weight)
        + dot("kl,ql->kq", key_low_gradient, key_weight)
        + dot("kl,ql->kq", value_low_gradient, value_weight)
    )
    grad_normed_one = tensor_sum(normed_one_part)
    gain_one_part = jnp.sum(normed_one_part * inputs_wide * root_one, axis=0)
    qkv_part = dot("wj,wq->jq", normed_low, low_gradient)
    columns = qkv_part.shape[1]
    gains = jnp.stack(
        [gain_one_part.reshape(n_dp, rows_here), gain_two_part.reshape(n_dp, rows_here)], axis=1
    )
    gains = jnp.pad(gains, ((0, 0), (0, 14), (0, columns - rows_here)))
    qkv_part = jnp.concatenate([qkv_part.reshape(n_dp, rows_here, columns), gains], axis=1)
    qkv_sum = scatter_sum(qkv_part.reshape(groups, PAIR, rows_here + 16, columns))
    grad_qkv = qkv_sum[:rows_here]
    gain_sums = qkv_sum[rows_here : rows_here + 16, :rows_here]
    bit = 1
    while bit < lax.axis_size("tensor"):
        gain_sums = gain_sums + tensor_swap(gain_sums, bit)
        bit *= 2
    grad_input_norm = norm_back(inputs_wide, root_one, norm1_gain, grad_normed_one)
    grad_inputs = (grad_residual + grad_input_norm).astype(jnp.bfloat16)
    q_columns = query_weight.shape[1]
    k_columns = key_weight.shape[1]
    return (
        output,
        grad_inputs,
        gain_sums[0],
        grad_qkv[:, :q_columns],
        grad_qkv[:, q_columns : q_columns + k_columns],
        grad_qkv[:, q_columns + k_columns :],
        grad_wout,
        gain_sums[1],
        grad_wgate,
        grad_wup,
        grad_wdown,
    )


def shards(
    inputs,
    norm1_gain,
    query_weight,
    key_weight,
    value_weight,
    w_out,
    norm2_gain,
    w_gate,
    w_up,
    w_down,
    doc_ids,
    grad_output,
):
    tok_rows, width = inputs.shape
    heads_here = query_weight.shape[1] // HEAD_SIZE
    kv_here = key_weight.shape[1] // HEAD_SIZE
    group_size = heads_here // kv_here
    n_dp = lax.axis_size("dp")
    groups = n_dp // PAIR
    group = lax.axis_index("dp") // PAIR
    offset = lax.axis_index("dp") * tok_rows
    n_tensor = lax.axis_size("tensor")
    half = HEAD_SIZE // 2
    lanes = jnp.arange(4 * half, dtype=jnp.int32)
    positions = (offset + jnp.arange(tok_rows, dtype=jnp.int32)).astype(jnp.float32)
    angles = positions[:, None] * rope_table(half, 4)[None, :]
    cosine = jnp.cos(angles)
    sine = jnp.sin(angles) * jnp.where(lanes % HEAD_SIZE < half, -1.0, 1.0)[None, :]
    normed_low, query_scaled, kv, id_rows, mixed_low, residual, normed_two_low, gate_t, up_t, part_g, cross_g = attend_forward(
        inputs, norm1_gain, query_weight, key_weight, value_weight, w_out, norm2_gain, cosine, sine, doc_ids, grad_output,
        w_gate, w_up, n_dp, n_tensor)
    mlp_part, back_part, normed_rest, rest_g, gain_two_part = mlp(normed_two_low, grad_output, part_g, cross_g, w_gate, w_up, w_down, n_dp, n_tensor)
    d_own, d_send, g_sum, u_own, u_send, grad_normed_two, first_part = wgrad(
        normed_two_low, normed_rest, grad_output, part_g, cross_g, rest_g, gate_t, up_t, w_down, back_part, normed_low, n_dp, n_tensor)
    output, grad_inputs, gate_blocks, up_blocks, d_in, wout_blocks, qkv_blocks, _, gain_sums = backward(
        grad_normed_two, residual, inputs, grad_output, mlp_part, normed_low, w_out, query_weight, key_weight, value_weight,
        g_sum, u_own, u_send, d_send, mixed_low, query_scaled, kv, first_part, norm1_gain, norm2_gain, gain_two_part,
        id_rows, doc_ids.reshape(1, tok_rows), cosine, sine, n_dp, n_tensor)
    gain_one, gain_two, output, grad_inputs, grad_wgate, grad_wup, grad_wdown, grad_wout, grad_wquery, grad_wkey, grad_wvalue = finish_all(
        output, grad_inputs, gate_blocks, up_blocks, d_own, d_in, wout_blocks, qkv_blocks, gain_sums, query_weight.shape[1], key_weight.shape[1])
    rows_here = width // n_dp
    return (
        output,
        grad_inputs,
        gain_one.reshape(rows_here),
        grad_wquery,
        grad_wkey,
        grad_wvalue,
        grad_wout,
        gain_two.reshape(rows_here),
        grad_wgate,
        grad_wup,
        grad_wdown,
    )


def kernels_fit(mesh, *args):
    n_dp, n_tensor = mesh.shape["dp"], mesh.shape["tensor"]
    width = args[0].shape[1]
    return (
        n_dp % PAIR == 0
        and n_dp // PAIR in (2, 4)
        and n_tensor == 4
        and width // n_dp in (128, 256)
        and args[7].shape[1] // n_tensor // (n_dp // PAIR) % 256 == 0
        and args[0].shape[0] // n_dp == DOC_MAX
        and args[3].shape[1] // n_tensor == 2 * HEAD_SIZE
        and args[2].shape[1] == 4 * args[3].shape[1]
    )


def solution(mesh):
    def step(*args):
        return mapped(mesh, shards if kernels_fit(mesh, *args) else shards_plain)(*args)

    return step


def mapped(mesh, function):
    return jax.shard_map(
        function,
        mesh=mesh,
        in_specs=(
            P("dp", None),
            P(),
            P(None, "tensor"),
            P(None, "tensor"),
            P(None, "tensor"),
            P("tensor", None),
            P(),
            P(None, "tensor"),
            P(None, "tensor"),
            P("tensor", None),
            P("dp"),
            P("dp", None),
        ),
        out_specs=(
            P("dp", None),
            P("dp", None),
            P("dp"),
            P("dp", "tensor"),
            P("dp", "tensor"),
            P("dp", "tensor"),
            P(("tensor", "dp"), None),
            P("dp"),
            P("dp", "tensor"),
            P("dp", "tensor"),
            P(("tensor", "dp"), None),
        ),
        check_vma=False,
    )
```

```python
import functools
import math

import jax
import jax.numpy as jnp
from jax import lax
from jax.experimental import pallas as pl
from jax.experimental.pallas import tpu as pltpu
from jax.sharding import PartitionSpec as P

HEAD_SIZE = 64
DOC_MAX = 512
NORM_EPSILON = 1e-05

PAIR = 2
MESH = pl.DeviceIdType.MESH
EPS = NORM_EPSILON


def nn(a, b):
    return lax.dot_general(a, b, (((1,), (0,)), ((), ())), preferred_element_type=jnp.float32)
def nt(a, b):
    return lax.dot_general(a, b, (((1,), (1,)), ((), ())), preferred_element_type=jnp.float32)

def flip(index, bit):
    return index + bit - 2 * bit * ((index // bit) % 2)

def meet(*partners):
    barrier = pltpu.get_barrier_semaphore()
    for axis, index in partners:
        pl.semaphore_signal(barrier, inc=1, device_id={axis: index}, device_id_type=MESH)
    pl.semaphore_wait(barrier, len(partners))

def remote(src, dst, sems, slot, axis, index):
    return pltpu.make_async_remote_copy(
        src_ref=src, dst_ref=dst, send_sem=sems.at[0, slot], recv_sem=sems.at[1, slot],
        device_id={axis: index}, device_id_type=MESH)

def send(src, dst, sems, slot, axis, index):
    copy = remote(src, dst, sems, slot, axis, index)
    copy.start()
    return copy

def swiglu(gate, up, grad):
    sig = 0.5 * (1.0 + jnp.tanh(0.5 * gate))
    silu = gate * sig
    hidden = (silu * up).astype(jnp.bfloat16)
    grad_gate = (grad * up * sig * (1.0 + gate * (1.0 - sig))).astype(jnp.bfloat16)
    grad_up = (grad * silu).astype(jnp.bfloat16)
    return hidden, grad_gate, grad_up

def mlp_kernel(n_dp, n_tensor, normed_hbm, grad_hbm, part_g, cross_g, gate_hbm, up_hbm, down_hbm,
               out_o, back_o, all_hbm, rest_g, gain_ref, out_ref, back_ref,
               normed, grad, gate_w, up_w, down_w, hid, low_gate, low_up, load, far):
    rows, width = normed.shape
    cols = gate_w.shape[1]
    groups = n_dp // PAIR
    me_dp, me_t = lax.axis_index("dp"), lax.axis_index("tensor")
    right = lax.rem(me_dp + PAIR, n_dp)
    left = lax.rem(me_dp + n_dp - PAIR, n_dp)
    core, across = flip(me_t, 1), flip(me_t, 2)
    tile = 256
    tiles = cols // tile
    def cp(s, d, i):
        return pltpu.make_async_copy(s, d, load.at[i])
    def gate_tile(c, f):
        return cp(gate_hbm.at[:, c], gate_w.at[:, c], 2 + 3 * f)
    def up_tile(c, f):
        return cp(up_hbm.at[:, c], up_w.at[:, c], 3 + 3 * f)
    def down_tile(c, f):
        return cp(down_hbm.at[c, :], down_w.at[c, :], 4 + 3 * f)
    cp(normed_hbm, normed, 0).start()
    def load_tile(f):
        c = pl.ds(pl.multiple_of(f * tile, tile), tile)
        gate_tile(c, f).start()
        up_tile(c, f).start()
        down_tile(c, f).start()
    load_tile(0)
    cp(grad_hbm, grad, 1).start()
    for f in range(1, tiles):
        load_tile(f)
    meet(("dp", right), ("dp", left), ("tensor", core), ("tensor", across))
    piece = rows // n_tensor
    def part(t):
        return pl.ds(pl.multiple_of(t * piece, piece), piece)
    steps = groups - 1
    per = 4
    def ring(s):
        src = (normed_hbm if s == 1 else all_hbm.at[s - 2]).at[part(me_t), :]
        return send(src, all_hbm.at[s - 1].at[part(me_t), :], far, s * per, "dp", right)
    def spread_n(s, level):
        block = all_hbm.at[s - 1]
        if level == 0:
            r = part(me_t)
            return [send(block.at[r, :], block.at[r, :], far, s * per + 1 + i, "tensor", t) for i, t in enumerate((across, core))]
        r = part(across)
        return [send(block.at[r, :], block.at[r, :], far, s * per + 3, "tensor", core)]
    def spread_g(b, level):
        base = (steps + 1 + b) * per
        if level == 0:
            return [send(part_g.at[b], rest_g.at[b].at[part(me_t), :], far, base, "tensor", across)]
        cross = cross_g if b == 0 else rest_g.at[b].at[part(across), :]
        return [send(part_g.at[b], rest_g.at[b].at[part(me_t), :], far, base + 1, "tensor", core),
                send(cross, rest_g.at[b].at[part(across), :], far, base + 2, "tensor", core)]
    def wait(copies):
        for c in copies:
            c.wait()

    ring_n = ring(1)
    g_core = spread_g(0, 1)
    g_x = {}
    last_g = steps - 1 if steps > 1 else steps
    if last_g > 1:
        g_x[1] = spread_g(1, 0)

    cp(normed_hbm, normed, 0).wait()
    cp(grad_hbm, grad, 1).wait()
    def first(f, _):
        c = pl.ds(pl.multiple_of(f * tile, tile), tile)
        gate_tile(c, f).wait()
        up_tile(c, f).wait()
        down_tile(c, f).wait()
        g = nn(normed[...], gate_w[:, c])
        u = nn(normed[...], up_w[:, c])
        h = nt(grad[...], down_w[c, :])
        a, b, d = swiglu(g, u, h)
        hid[:, c] = a
        low_gate[:, c] = b
        low_up[:, c] = d
        return 0
    early = min(5, tiles)
    n_x = {}
    def pass_g(b):
        nonlocal g_core
        if b in g_x:
            wait(g_x.pop(b))
            g_core = g_core + spread_g(b, 1)
            if b + 1 < last_g:
                g_x[b + 1] = spread_g(b + 1, 0)
    lax.fori_loop(0, early, first, 0)
    ring_n.wait()
    if steps > 1:
        ring_n = ring(2)
    pass_g(1)
    n_x[1] = spread_n(1, 0)
    lax.fori_loop(early, tiles, first, 0)
    wtile = 256
    wtiles = width // wtile
    def second(j, _):
        c = pl.ds(pl.multiple_of(j * wtile, wtile), wtile)
        b = nt(low_gate[...], gate_w[c, :]) + nt(low_up[...], up_w[c, :])
        back_ref[:, c] = b.astype(back_ref.dtype)
        gain_ref[0:1, c] = jnp.sum(b * normed[:, c].astype(jnp.float32), axis=0, keepdims=True)
        return 0
    def third(j, _):
        c = pl.ds(pl.multiple_of(j * wtile, wtile), wtile)
        out_ref[:, c] = nn(hid[...], down_w[:, c]).astype(out_ref.dtype)
        return 0
    most = wtiles * 3 // 4
    lax.fori_loop(0, most, third, 0)
    n_core = []
    def pass_n(s):
        nonlocal n_core
        if s in n_x:
            wait(n_x.pop(s))
            if s < steps - 1:
                n_core = n_core + spread_n(s, 1)
    if steps > 1:
        ring_n.wait()
        if steps > 2:
            ring_n = ring(3)
            n_x[2] = spread_n(2, 0)
    lax.fori_loop(most, wtiles, third, 0)
    w_out = pltpu.make_async_copy(out_ref, out_o, load.at[0])
    w_out.start()
    lax.fori_loop(0, wtiles // 2, second, 0)
    pass_n(1)
    lax.fori_loop(wtiles // 2, wtiles, second, 0)
    w_back = pltpu.make_async_copy(back_ref, back_o, load.at[1])
    w_back.start()
    for s in range(3, steps + 1):
        ring_n.wait()
        if s < steps:
            ring_n = ring(s + 1)
            n_x[s] = spread_n(s, 0)
    for b in range(3, steps):
        pass_g(b)
    for s in range(2, steps):
        pass_n(s)
    wait(n_core)
    wait(g_core)
    w_out.wait()
    w_back.wait()

def mlp(normed, grad_output, part_g, cross_g, w_gate, w_up, w_down, n_dp, n_tensor):
    rows, width = normed.shape
    cols = w_gate.shape[1]
    groups = n_dp // PAIR
    tiles = cols // 256
    anyspec = pl.BlockSpec(memory_space=pl.ANY)
    vm = pl.BlockSpec(memory_space=pltpu.VMEM)
    bf = jnp.bfloat16
    return pl.pallas_call(
        functools.partial(mlp_kernel, n_dp, n_tensor),
        out_shape=(jax.ShapeDtypeStruct((rows, width), bf), jax.ShapeDtypeStruct((rows, width), bf),
                   jax.ShapeDtypeStruct((groups - 1, rows, width), bf), jax.ShapeDtypeStruct((groups - 1, rows, width), bf), jax.ShapeDtypeStruct((1, width), jnp.float32)),
        in_specs=[anyspec] * 7, out_specs=(anyspec, anyspec, anyspec, anyspec, vm),
        scratch_shapes=[pltpu.VMEM((rows, width), bf), pltpu.VMEM((rows, width), bf), pltpu.VMEM((rows, width), bf), pltpu.VMEM((rows, width), bf),
                        pltpu.VMEM((width, cols), bf), pltpu.VMEM((width, cols), bf), pltpu.VMEM((cols, width), bf),
                        pltpu.VMEM((rows, cols), bf), pltpu.VMEM((rows, cols), bf), pltpu.VMEM((rows, cols), bf),
                        pltpu.SemaphoreType.DMA((2 + 3 * tiles,)),
                        pltpu.SemaphoreType.DMA((2, 8 * groups)),
                        ],
        compiler_params=pltpu.CompilerParams(collective_id=2, has_side_effects=True, vmem_limit_bytes=60 << 20),
        cost_estimate=pl.CostEstimate(flops=12 * rows * width * cols, bytes_accessed=2 * (3 * width * cols + 8 * rows * width), transcendentals=rows * cols),
        name="feed_forward",
    )(normed, grad_output, part_g, cross_g, w_gate, w_up, w_down)

def wgrad_kernel(n_dp, n_tensor, own_n, all_n, own_g, part_g, cross_g, rest_g, gate_t, up_t, down_hbm, back_hbm, first_hbm,
                 d_own_o, d_send_o, g_sum_o, u_own_o, u_send_o, sum_o, first_o,
                 d_own, d_send, g_sum, u_own, u_send, sum_ref, g_own, g_send, g_in, n_all, g_all, wg, wu, wd, hid, lowg, lowu, mine, in1, mid, in2, load, far, ar, sy, outs):
    rows, width = own_n.shape
    share = gate_t.shape[0]
    groups = n_dp // PAIR
    me_dp, me_t = lax.axis_index("dp"), lax.axis_index("tensor")
    member = lax.rem(me_dp, PAIR)
    bits = []
    bit = n_tensor // 2
    while bit:
        bits.append(bit); bit //= 2
    piece = rows // n_tensor
    def part(t):
        return pl.ds(pl.multiple_of(t * piece, piece), piece)
    def at(r, t):
        return pl.ds(pl.multiple_of(r * rows + t * piece, piece), piece)
    count = [0]
    def cp(s, d):
        c = pltpu.make_async_copy(s, d, load.at[count[0]]); count[0] += 1
        c.start(); return c
    half = rows // 2
    low = lax.rem(me_t, 2)
    def half_rows(c):
        return pl.ds(pl.multiple_of(c * half, half), half)
    last = groups - 1
    core, across = flip(me_t, 1), flip(me_t, 2)
    late = last - 1 if last > 1 else 0
    def late_piece():
        return remote(all_n.at[late - 1].at[part(across), :], n_all.at[at(late, across), :], far, 5 + groups, "tensor", core)
    if last > 0:
        w_last = cp(all_n.at[last - 1].at[part(me_t), :], n_all.at[at(last, me_t), :])
    w1 = [cp(gate_t, wg), cp(own_n, n_all.at[pl.ds(0, rows), :])]
    w2 = [cp(up_t, wu)]
    w3 = [cp(down_hbm.at[pl.ds(pl.multiple_of(me_dp // PAIR * share, share), share), :], wd), cp(own_g, g_all.at[pl.ds(0, rows), :])]
    w4 = [cp(back_hbm.at[half_rows(low), :], mine)]
    first_block = count[0]
    def load_block(r):
        i = first_block + (r - 1) * (1 + n_tensor)
        def one(s, d, j):
            return pltpu.make_async_copy(s, d, load.at[i + j])
        out = []
        if r == late:
            for j, t in enumerate((me_t, across, core)):
                out.append(one(all_n.at[r - 1].at[part(t), :], n_all.at[at(r, t), :], (groups - r) * (1 + n_tensor) + j))
        elif r < last:
            out.append(one(all_n.at[r - 1], n_all.at[pl.ds(r * rows, rows), :], 0))
        out.append(one(part_g.at[r - 1], g_all.at[at(r, me_t), :], 1))
        if r == last and last > 1:
            return out
        for j, h in enumerate((flip(me_t, 1), flip(me_t, 2), flip(flip(me_t, 1), 2))):
            src = cross_g if r == 1 and j == 1 else rest_g.at[r - 1].at[part(h), :]
            out.append(one(src, g_all.at[at(r, h), :], 2 + j))
        return out
    def start(cs):
        for c in cs:
            c.start()
    pair = flip(me_dp, 1)
    core, across = flip(me_t, 1), flip(me_t, 2)
    right, left = lax.rem(me_dp + PAIR, n_dp), lax.rem(me_dp + n_dp - PAIR, n_dp)
    meet(("dp", pair), ("dp", right), ("dp", left), ("tensor", core), ("tensor", across))
    last_g = []
    if last > 1:
        src = cross_g if last == 2 else rest_g.at[last - 2].at[part(across), :]
        last_g = [lambda: remote(src, g_all.at[at(last, across), :], far, 3, "dp", right),
                  lambda: remote(part_g.at[last - 1], g_all.at[at(last, me_t), :], far, 4, "tensor", core),
                  lambda: remote(g_all.at[at(last, across), :], g_all.at[at(last, across), :], far, 5, "tensor", core)]
        last_g[0]().start()
    def ring(k):
        src = first_hbm.at[part(me_t), :] if k == 1 else first_o.at[k - 2]
        return remote(src, first_o.at[k - 1], far, 5 + k, "dp", right)
    if last > 0:
        ring(1).start()
    if late:
        late_piece().start()
    ar1 = send(back_hbm.at[half_rows(1 - low), :], in1, ar, 0, "tensor", core)
    def wait(cs):
        for c in cs:
            c.wait()
    def spread(level):
        held, other = [me_t, across][:level + 1], [across, core][level]
        return [remote(n_all.at[at(last, h), :], n_all.at[at(last, h), :], far, level + i, "tensor", other) for i, h in enumerate(held)]
    if last > 0:
        w_last.wait()
        start(spread(0))
    if last > 1:
        last_g[1]().start()

    sum2 = lambda: remote(mid, in2, ar, 1, "tensor", across)
    def pass_a(r, _):
        for k in range(groups):
            @pl.when(r == k)
            def _():
                if k == 0:
                    wait(w1)
                    wait(w2)
                    wait(w3)
                else:
                    wait(load_block(k))
                if k < last:
                    start(load_block(k + 1))
                if k == late and late:
                    late_piece().wait()
                if k == max(last - 1, 1):
                    sum2().start()
                if k == last:
                    wait(spread(0))
                    start(spread(1))
                    if last > 1:
                        last_g[0]().wait()
                        last_g[2]().start()
                    wait(spread(1))
                    if last > 1:
                        last_g[1]().wait()
                        last_g[2]().wait()
        rs = pl.ds(pl.multiple_of(r * rows, rows), rows)
        g = nt(wg[...], n_all[rs, :])
        u = nt(wu[...], n_all[rs, :])
        h = nt(wd[...], g_all[rs, :])
        a, b, d = swiglu(g, u, h)
        hid[:, rs] = a
        lowg[:, rs] = b
        lowu[:, rs] = d
        @pl.when(r == 0)
        def _():
            wait(w4)
            ar1.wait()
            mid[...] = (mine[...].astype(jnp.float32) + in1[...].astype(jnp.float32)).astype(jnp.bfloat16)
        return 0
    lax.fori_loop(0, groups, pass_a, 0)
    ar2 = sum2()
    dcols = width // n_dp
    def col_tile(low_ref, own_ref, send_ref):
        def body(q, _):
            a = pl.ds(pl.multiple_of((q * PAIR + member) * dcols, dcols), dcols)
            b = pl.ds(pl.multiple_of((q * PAIR + 1 - member) * dcols, dcols), dcols)
            send_ref[q] = nn(low_ref[...], n_all[:, b]).astype(jnp.bfloat16)
            own_ref[q] = nn(low_ref[...], n_all[:, a]).astype(jnp.bfloat16)
            return 0
        return body
    def to_pair(q):
        return remote(g_send.at[q], g_in.at[q], sy, q, "dp", pair)
    def gate_tile(q, _):
        col_tile(lowg, g_own, g_send)(q, 0)
        to_pair(q).start()
        @pl.when(q == 1)
        def _():
            if last > 1:
                ring(1).wait()
                ring(2).start()
        return 0
    lax.fori_loop(0, groups, gate_tile, 0)
    hrows = share // PAIR
    def down_tile(j, _):
        c = pl.ds(pl.multiple_of(j * 512, 512), 512)
        d_send[:, c] = nn(hid[pl.ds(pl.multiple_of((1 - member) * hrows, hrows), hrows), :], g_all[:, c]).astype(jnp.bfloat16)
        d_own[:, c] = nn(hid[pl.ds(pl.multiple_of(member * hrows, hrows), hrows), :], g_all[:, c]).astype(jnp.bfloat16)
        return 0
    lax.fori_loop(0, width // 512, down_tile, 0)
    stores = []
    def store(src, dst):
        c = pltpu.make_async_copy(src, dst, outs.at[len(stores)])
        c.start()
        stores.append(c)
    store(d_own, d_own_o)
    store(d_send, d_send_o)
    def up_tile(q, _):
        @pl.when(q == groups // 2)
        def _():
            if last > 2:
                ring(2).wait()
                ring(3).start()
        return col_tile(lowu, u_own, u_send)(q, 0)
    lax.fori_loop(0, groups, up_tile, 0)
    store(u_own, u_own_o)
    store(u_send, u_send_o)
    ar2.wait()
    sum_ref[half_rows(low), :] = (mid[...].astype(jnp.float32) + in2[...].astype(jnp.float32)).astype(jnp.bfloat16)
    ar3 = send(sum_ref.at[half_rows(low), :], sum_ref.at[half_rows(low), :], ar, 2, "tensor", core)
    for q in range(groups):
        to_pair(q).wait()
        g_sum[q] = (g_own[q].astype(jnp.float32) + g_in[q].astype(jnp.float32)).astype(jnp.bfloat16)
    store(g_sum, g_sum_o)
    ar3.wait()
    store(sum_ref, sum_o)
    if last > 0:
        ring(last).wait()
    wait(stores)

def wgrad(own_n, all_n, own_g, part_g, cross_g, rest_g, gate_t, up_t, down, back, first, n_dp, n_tensor):
    rows, width = own_n.shape
    share = gate_t.shape[0]
    groups = n_dp // PAIR
    anyspec = pl.BlockSpec(memory_space=pl.ANY)
    vm = pl.BlockSpec(memory_space=pltpu.VMEM)
    bf, f32 = jnp.bfloat16, jnp.float32
    sd = jax.ShapeDtypeStruct
    dcols = width // n_dp
    V = pltpu.VMEM
    tall = groups * rows
    return pl.pallas_call(
        functools.partial(wgrad_kernel, n_dp, n_tensor),
        out_shape=(sd((share // PAIR, width), bf), sd((share // PAIR, width), bf), sd((groups, share, dcols), bf),
                   sd((groups, share, dcols), bf), sd((groups, share, dcols), bf), sd((rows, width), bf),
                   sd((groups - 1, rows // n_tensor, width), bf)),
        in_specs=[anyspec] * 11, out_specs=(anyspec,) * 7,
        scratch_shapes=[*[V((share // PAIR, width), bf)] * 2, *[V((groups, share, dcols), bf)] * 3, V((rows, width), bf), *[V((groups, share, dcols), bf)] * 3, V((tall, width), bf), V((tall, width), bf),
                        V((share, width), bf), V((share, width), bf), V((share, width), bf),
                        V((share, tall), bf), V((share, tall), bf), V((share, tall), bf),
                        *[V((rows // 2, width), bf)] * 4,
                        pltpu.SemaphoreType.DMA((10 + (groups - 1) * (1 + n_tensor),)),
                        pltpu.SemaphoreType.DMA((2, 6 + groups)), pltpu.SemaphoreType.DMA((2, 3)), pltpu.SemaphoreType.DMA((2, groups)), pltpu.SemaphoreType.DMA((6,))],
        compiler_params=pltpu.CompilerParams(collective_id=3, has_side_effects=True, vmem_limit_bytes=62 << 20),
        cost_estimate=pl.CostEstimate(flops=12 * tall * width * share, bytes_accessed=2 * (3 * width * share + 4 * tall * width), transcendentals=tall * share),
        name="weight_gradients",
    )(own_n, all_n, own_g, part_g, cross_g, rest_g, gate_t, up_t, down, back, first)
TILE = 128
CHUNK = 128

def turn(values, cosine, sine):
    lane = lax.broadcasted_iota(jnp.int32, values.shape, 1)
    swapped = jnp.where(lane % HEAD_SIZE < HEAD_SIZE // 2,
                        pltpu.roll(values, 128 - HEAD_SIZE // 2, 1), pltpu.roll(values, HEAD_SIZE // 2, 1))
    return values * cosine + swapped * sine

def place(values, head, side):
    v = values if head == side else pltpu.roll(values, HEAD_SIZE, 1)
    lane = lax.broadcasted_iota(jnp.int32, values.shape, 1)
    return jnp.where(lane // HEAD_SIZE == side, v, jnp.zeros_like(v))

def column_of(row):
    a = lax.broadcasted_iota(jnp.int32, (128, 128), 0)
    b = lax.broadcasted_iota(jnp.int32, (128, 128), 1)
    return jnp.sum(jnp.where(a == b, row.astype(jnp.float32), 0.0), axis=1, keepdims=True)

def bias_of(ids_col, ids_row, row0, col0, shape, window):
    q = lax.broadcasted_iota(jnp.int32, shape, 0) + row0
    k = lax.broadcasted_iota(jnp.int32, shape, 1) + col0
    return jnp.where((ids_col == ids_row) & (k <= q), 0.0, -1e30)

def attention_kernel(n_dp, n_tensor, x_hbm, gain1, wq_hbm, wk_hbm, wv_hbm, wo_hbm, gain2, cos_ref, sin_ref, ids_row, g_hbm, gate_hbm, up_hbm,
                     normed_o, q_o, kv_o, idrow_o, mixed_o, res_o, normed2_o, gate_o, up_o, part_g, cross_g,
                     normed_ref, q_ref, kv_ref, idrow_ref, mixed_ref, res_ref, normed2_ref, gate_t, up_t,
                     x, wq, wk, wv, wo, raw_gate, raw_up, kvar, vvar, ids_flat, tile32, partial, out1, in1, mid, in2, total, load, outs, far, halo, ar):
    rows, width = x.shape
    groups = n_dp // PAIR
    me_dp, me_t = lax.axis_index("dp"), lax.axis_index("tensor")
    right = lax.rem(me_dp + PAIR, n_dp)
    left = lax.rem(me_dp + n_dp - PAIR, n_dp)
    after = lax.rem(me_dp + 1, n_dp)
    before = lax.rem(me_dp + n_dp - 1, n_dp)
    core, across = flip(me_t, 1), flip(me_t, 2)
    piece = rows // n_tensor
    def part(t):
        return pl.ds(pl.multiple_of(t * piece, piece), piece)
    count = [0]
    def cp(s, d):
        c = pltpu.make_async_copy(s, d, load.at[count[0]]); count[0] += 1
        c.start(); return c
    share = raw_gate.shape[1]
    stores = []
    def store(src, dst):
        c = pltpu.make_async_copy(src, dst, outs.at[len(stores)])
        c.start()
        stores.append(c)
    share = raw_gate.shape[1]
    w_x = cp(x_hbm, x); w_k = cp(wk_hbm, wk); w_v = cp(wv_hbm, wv)
    meet(("dp", after), ("dp", before), ("dp", right), ("dp", left), ("tensor", core), ("tensor", across))
    ids_go = send(ids_row, idrow_ref.at[0], halo, 0, "dp", after)
    fine = piece // 2
    def first_part(j):
        first = pl.ds(pl.multiple_of(me_t * piece + j * fine, fine), fine)
        return remote(g_hbm.at[first, :], part_g.at[0].at[pl.ds(j * fine, fine), :], far, j, "dp", right)
    def cross_first():
        return send(part_g.at[0].at[pl.ds(0, fine), :], cross_g.at[pl.ds(0, fine), :], far, groups, "tensor", across)
    def cross_second():
        second = pl.ds(pl.multiple_of(across * piece + fine, fine), fine)
        return remote(g_hbm.at[second, :], cross_g.at[pl.ds(fine, fine), :], far, groups + 1, "dp", right)
    ring0 = first_part(0)
    ring0.start()
    w_q = cp(wq_hbm, wq)
    idrow_ref[1] = ids_row[...]

    w_x.wait()
    def norm_one(i, _):
        r = pl.ds(pl.multiple_of(i * TILE, TILE), TILE)
        v = x[r, :].astype(jnp.float32)
        root = lax.rsqrt(jnp.mean(v * v, axis=1, keepdims=True) + EPS)
        normed_ref[r, :] = (v * root * gain1[...]).astype(jnp.bfloat16)
        return 0
    lax.fori_loop(0, rows // TILE, norm_one, 0)
    w_k.wait(); w_v.wait()
    own = pl.ds(rows, rows)
    kv_ref[1, :, 0:128] = turn(nn(normed_ref[...], wk[...]), cos_ref[...], sin_ref[...]).astype(jnp.bfloat16)
    kv_ref[1, :, 128:256] = nn(normed_ref[...], wv[...]).astype(jnp.bfloat16)
    w_q.wait()
    pairs = wq.shape[1] // 128
    def q_pair(p, _):
        c = pl.ds(pl.multiple_of(p * 256, 256), 256)
        raw = nn(normed_ref[...], wq[:, c])
        for s in range(2):
            d = pl.ds(pl.multiple_of(p * 256 + s * 128, 128), 128)
            q_ref[:, d] = (turn(raw[:, s * 128:(s + 1) * 128], cos_ref[...], sin_ref[...]).astype(jnp.bfloat16) * HEAD_SIZE ** -0.5).astype(jnp.bfloat16)
        return 0
    early = [pl.ds(rows // 2, rows // 2), pl.ds(0, rows // 2)]
    def kv_half(h):
        return remote(kv_ref.at[1].at[early[h], :], kv_ref.at[0].at[early[h], :], halo, 1 + h, "dp", after)
    kv_half(0).start()
    kv_half(1).start()
    w_o = cp(wo_hbm, wo)
    store(normed_ref, normed_o)
    lax.fori_loop(0, pairs // 2, q_pair, 0)
    def variants(b, r0, count):
        src = pl.ds(r0, count)
        dst = pl.ds(b * rows + r0, count)
        for g in range(2):
            for s in range(2):
                kvar[g, s, dst, :] = place(kv_ref[b, src, 0:128], g, s)
                vvar[g, s, dst, :] = place(kv_ref[b, src, 128:256], g, s)
    variants(1, 0, rows)
    ids_go.wait()
    kv_half(0).wait()
    ring0.wait()
    cross0 = cross_first()
    first_part(1).start()
    store(q_ref, q_o)
    store(idrow_ref, idrow_o)
    mine = pl.ds(pl.multiple_of(me_dp // PAIR * share, share), share)
    w_gate = cp(gate_hbm.at[:, mine], raw_gate); w_up = cp(up_hbm.at[:, mine], raw_up)
    variants(0, rows // 2, rows // 2)
    w_o.wait()
    ids_flat[:, 0:rows] = idrow_ref[0]
    ids_flat[:, rows:2 * rows] = idrow_ref[1]

    window = rows + TILE
    def attend(i):
        start = pl.multiple_of(i * TILE, TILE)
        r = pl.ds(start, TILE)
        k = pl.ds(start, window)
        ids_k = ids_flat[:, k]
        bias = bias_of(column_of(ids_flat[:, pl.ds(start + rows, TILE)]), ids_k.astype(jnp.float32), rows, 0, (TILE, window), window)
        bias = jnp.concatenate([bias, bias], axis=0)
        for g in range(2):
            q2 = jnp.concatenate([q_ref[r, (2 * g) * 128:(2 * g + 1) * 128], q_ref[r, (2 * g + 1) * 128:(2 * g + 2) * 128]], axis=0)
            mixed = None
            for s in range(2):
                score = nt(q2, kvar[g, s, k, :]) + bias
                peak = jnp.max(score, axis=1, keepdims=True)
                e = jnp.exp(score - peak)
                l = jnp.sum(e, axis=1, keepdims=True)
                prob = (e * (1.0 / l)).astype(jnp.bfloat16)
                m = nn(prob, vvar[g, s, k, :])
                mixed = m if mixed is None else mixed + m
            for b in range(2):
                mixed_ref[r, (2 * g + b) * 128:(2 * g + b + 1) * 128] = mixed[b * TILE:(b + 1) * TILE, :].astype(jnp.bfloat16)

    hrow = CHUNK // 2
    low = lax.rem(me_t, 2)
    def own_rows(c):
        return pl.ds(pl.multiple_of(c * CHUNK + low * hrow, hrow), hrow)
    def oth_rows(c):
        return pl.ds(pl.multiple_of(c * CHUNK + (1 - low) * hrow, hrow), hrow)
    def project(c):
        r = pl.ds(pl.multiple_of(c * CHUNK, CHUNK), CHUNK)
        def body(j, _):
            d = pl.ds(pl.multiple_of(j * 512, 512), 512)
            tile32[...] = nn(mixed_ref[r, :], wo[:, d])
            out1[c, :, d] = tile32[pl.ds(pl.multiple_of((1 - low) * hrow, hrow), hrow), :].astype(jnp.bfloat16)
            partial[c, :, d] = tile32[pl.ds(pl.multiple_of(low * hrow, hrow), hrow), :]
            return 0
        lax.fori_loop(0, width // 512, body, 0)
    def step1(c):
        return remote(out1.at[c], in1.at[c], ar, 3 * c, "tensor", core)
    def step2(c):
        return remote(mid.at[c], in2.at[c], ar, 3 * c + 1, "tensor", across)
    def add_core(c):
        step1(c).wait()
        mid[c] = (partial[c] + in1[c].astype(jnp.float32)).astype(jnp.bfloat16)
        step2(c).start()
    def step3(c):
        total[own_rows(c), :] = (mid[c].astype(jnp.float32) + in2[c].astype(jnp.float32)).astype(jnp.bfloat16)
        return send(total.at[own_rows(c), :], total.at[own_rows(c), :], ar, 3 * c + 2, "tensor", core)
    def finish(r):
        v = x[r, :].astype(jnp.float32) + total[r, :].astype(jnp.float32)
        res_ref[r, :] = v
        root = lax.rsqrt(jnp.mean(v * v, axis=1, keepdims=True) + EPS)
        normed2_ref[r, :] = (v * root * gain2[...]).astype(jnp.bfloat16)

    chunks = rows // CHUNK
    flights = {}
    steps = groups - 1
    def ring(s):
        return remote(part_g.at[s - 2], part_g.at[s - 1], far, s, "dp", right)
    tiles = rows // TILE
    def tile_step(j, _):
        @pl.when(j == tiles // 2)
        def _():
            kv_half(1).wait()
            variants(0, 0, rows // 2)
        i = tiles - 1 - j
        attend(i)
        @pl.when(j > 0)
        def _():
            add_core(i + 1)
        project(i)
        step1(i).start()
        @pl.when(j == 0)
        def _():
            first_part(1).wait()
            cross_second().start()
            if steps > 1:
                ring(2).start()
        return 0
    lax.fori_loop(0, tiles, tile_step, 0)
    store(mixed_ref, mixed_o)
    store(kv_ref, kv_o)
    def transpose_into(dst, raw):
        def body(j, _):
            r = pl.ds(pl.multiple_of(j * 256, 256), 256)
            dst[:, r] = raw[r, :].T
            return 0
        lax.fori_loop(0, width // 256, body, 0)
    add_core(0)
    w_gate.wait()
    transpose_into(gate_t, raw_gate)
    store(gate_t, gate_o)
    w_up.wait()
    transpose_into(up_t, raw_up)
    store(up_t, up_o)
    def out_rows(c):
        flights[3, c].wait()
        finish(oth_rows(c))
        r = pl.ds(c * CHUNK, CHUNK)
        store(res_ref.at[r, :], res_o.at[r, :])
        store(normed2_ref.at[r, :], normed2_o.at[r, :])
    for n in range(chunks):
        c = chunks - 1 - n
        if 3 <= n + 2 <= steps:
            ring(n + 1).wait()
            ring(n + 2).start()
        step2(c).wait()
        flights[3, c] = step3(c)
        finish(own_rows(c))
        if n > 0:
            out_rows(c + 1)
    out_rows(0)
    if steps > 1:
        ring(steps).wait()
    cross0.wait()
    cross_second().wait()
    for q in stores:
        q.wait()

def attend_forward(x, gain1, wq, wk, wv, wo, gain2, cosine, sine, ids, grad_output, w_gate, w_up, n_dp, n_tensor):
    rows, width = x.shape
    groups = n_dp // PAIR
    anyspec = pl.BlockSpec(memory_space=pl.ANY)
    vm = pl.BlockSpec(memory_space=pltpu.VMEM)
    bf, f32 = jnp.bfloat16, jnp.float32
    sd = jax.ShapeDtypeStruct
    V = pltpu.VMEM
    piece = rows // n_tensor
    chunks = rows // CHUNK
    qc = wq.shape[1]
    share = w_gate.shape[1] // groups
    D = pltpu.SemaphoreType.DMA
    return pl.pallas_call(
        functools.partial(attention_kernel, n_dp, n_tensor),
        out_shape=(sd((rows, width), bf), sd((rows, qc), bf), sd((2, rows, 256), bf), sd((2, 1, rows), jnp.int32),
                   sd((rows, qc), bf), sd((rows, width), f32), sd((rows, width), bf), sd((share, width), bf), sd((share, width), bf),
                   sd((groups - 1, piece, width), bf), sd((piece, width), bf)),
        in_specs=[anyspec, vm, anyspec, anyspec, anyspec, anyspec, vm, vm, vm, vm, anyspec, anyspec, anyspec],
        out_specs=(anyspec,) * 11,
        scratch_shapes=[V((rows, width), bf), V((rows, qc), bf), V((2, rows, 256), bf), V((2, 1, rows), jnp.int32), V((rows, qc), bf),
                        V((rows, width), f32), V((rows, width), bf), V((share, width), bf), V((share, width), bf),
                        V((rows, width), bf), V((width, qc), bf), V((width, 128), bf), V((width, 128), bf), V((qc, width), bf), V((width, share), bf), V((width, share), bf),
                        V((2, 2, 2 * rows, 128), bf), V((2, 2, 2 * rows, 128), bf), V((1, 2 * rows), jnp.int32), V((CHUNK, 512), f32),
                        V((chunks, CHUNK // 2, width), f32), V((chunks, CHUNK // 2, width), bf), V((chunks, CHUNK // 2, width), bf),
                        V((chunks, CHUNK // 2, width), bf), V((chunks, CHUNK // 2, width), bf), V((rows, width), bf),
                        D((7,)), D((7 + 2 * chunks,)), D((2, groups + 2)), D((2, 3)), D((2, 3 * chunks))],
        compiler_params=pltpu.CompilerParams(collective_id=1, has_side_effects=True, vmem_limit_bytes=62 << 20),
        cost_estimate=pl.CostEstimate(flops=2 * rows * width * (2 * qc + 256) + 16 * rows * rows * 5 * 128, bytes_accessed=2 * (width * (2 * qc + 256) + 6 * rows * width), transcendentals=8 * rows * rows),
        name="attention_forward",
    )(x, gain1.reshape(1, width), wq, wk, wv, wo, gain2.reshape(1, width), cosine, sine, ids.reshape(1, rows), grad_output, w_gate, w_up)

def backward_kernel(n_dp, n_tensor, gn_hbm, res_hbm, x_hbm, go_hbm, mlp_hbm, normed_hbm, wo_hbm, wq_hbm, wk_hbm, wv_hbm,
                    g_sum, u_own_hbm, u_send, d_send, mixed_hbm, q_hbm, kv_hbm, first_part, gain1, gain2, gain2_part, id_rows, ids_row, cos_ref, sin_ref,
                    out_hbm, gin_hbm, gz, uz, d_in, wz, qz, first_all, gains_ref,
                    gn, res, go, normed, wo, wq, wk, wv, mixed, q_ref, kv_ref, resid, low_res, gm, kvar, vvar, kvart, dk, dv, ids_col,
                    low, lowt, tile32, wsend, wown, win, win2, own_block, u_own, uyin, usum, lg, qsend, qown, qin,
                    amine, amid, min1, min2, ain1, ain2, hprev, hin, gacc, gs, gown, gyi, gzi, gt, gti,
                    load, sy, sz, sx, sh, sg):
    rows, width = go.shape
    groups = n_dp // PAIR
    me_dp, me_t = lax.axis_index("dp"), lax.axis_index("tensor")
    group, member = me_dp // PAIR, lax.rem(me_dp, PAIR)
    pair = flip(me_dp, 1)
    after = lax.rem(me_dp + 1, n_dp)
    before = lax.rem(me_dp + n_dp - 1, n_dp)
    core, across = flip(me_t, 1), flip(me_t, 2)
    low_t = lax.rem(me_t, 2)
    def at_group(s):
        return lax.rem(group + s, groups)
    def from_group(s):
        return lax.rem(group + groups - s, groups)
    f32, bf = jnp.float32, jnp.bfloat16
    qc = wq.shape[1]
    dcols = width // n_dp
    half = rows // 2
    def rows_of(start, size):
        return pl.ds(pl.multiple_of(start, size), size)
    def half_rows(c):
        return rows_of(c * half, half)
    def cp(s, d, i):
        c = pltpu.make_async_copy(s, d, load.at[i])
        c.start()
        return c
    w_gn = cp(gn_hbm, gn, 0); w_res = cp(res_hbm, res, 1); w_go = cp(go_hbm, go, 2)
    w_wo = cp(wo_hbm, wo, 3); w_mlp = cp(mlp_hbm.at[half_rows(low_t), :], amine, 4)
    w_g = cp(g_sum.at[group], own_block, 13)
    w_kv = cp(kv_hbm, kv_ref, 5); w_mx = cp(mixed_hbm, mixed, 6); w_qr = cp(q_hbm, q_ref, 7)
    w_own = cp(u_own_hbm, u_own, 8); w_nm = cp(normed_hbm, normed, 9)
    w_q = cp(wq_hbm, wq, 10); w_k = cp(wk_hbm, wk, 11); w_v = cp(wv_hbm, wv, 12)
    meet(("dp", pair), ("dp", after), ("dp", before), ("tensor", core), ("tensor", across),
         *[("dp", at_group(s) * PAIR + member) for s in range(1, groups)])
    def exchange(src, dst, base, distances=range(1, groups)):
        return [send(src.at[at_group(s)], dst.at[group], sz, base + s - 1, "dp", at_group(s) * PAIR + member) for s in distances]
    y_u = send(u_send, uyin, sy, 0, "dp", pair)
    z_g = exchange(g_sum, gz, 0)
    m1 = send(mlp_hbm.at[half_rows(1 - low_t), :], min1, sx, 0, "tensor", core)
    steps = groups - 1
    piece = rows // n_tensor
    def part(t):
        return rows_of(t * piece, piece)
    at_x = 3 + 3 * (rows // CHUNK)
    def first_piece(k):
        return first_part.at[k]
    def spread_x(k):
        return send(first_piece(k), first_all.at[k].at[part(me_t), :], sx, at_x + k, "tensor", across)
    def spread_core(k, t):
        src = first_piece(k) if t is me_t else first_all.at[k].at[part(t), :]
        return send(src, first_all.at[k].at[part(t), :], sx, at_x + (1 + (t is not me_t)) * steps + k, "tensor", core)
    first_x = [spread_x(0)]
    first_c = [spread_core(0, me_t)]

    w_gn.wait(); w_res.wait(); w_go.wait()
    NR = 64
    def norm_two(i, _):
        r = rows_of(i * NR, NR)
        v = res[r, :]
        root = lax.rsqrt(jnp.mean(v * v, axis=1, keepdims=True) + EPS)
        up = gn[r, :].astype(f32) * gain2[...]
        mean = jnp.mean(up * v, axis=1, keepdims=True)
        d = go[r, :].astype(f32) + root * up - v * (root * root * root * mean)
        resid[r, :] = d
        low_res[r, :] = d.astype(bf)
        return 0
    lax.fori_loop(0, rows // NR, norm_two, 0)
    w_wo.wait()
    def mix_tile(i, _):
        r = rows_of(i * half, half)
        gm[r, :] = nt(low_res[r, :], wo[...]).astype(bf)
        return 0
    lax.fori_loop(0, 2, mix_tile, 0)
    w_mlp.wait(); m1.wait()
    amid[...] = (amine[...].astype(f32) + min1[...].astype(f32)).astype(bf)
    w_kv.wait()
    for g in range(2):
        for s in range(2):
            for b in range(2):
                kvar[g, s, pl.ds(b * rows, rows), :] = place(kv_ref[b, :, 0:128], g, s)
                vvar[g, s, pl.ds(b * rows, rows), :] = place(kv_ref[b, :, 128:256], g, s)
            kvart[g, s] = kvar[g, s].T
    dk[...] = jnp.zeros_like(dk)
    dv[...] = jnp.zeros_like(dv)
    m2 = send(amid, min2, sx, 1, "tensor", across)
    for k in range(1, steps):
        first_x.append(spread_x(k))
        first_c.append(spread_core(k, me_t))
    w_g.wait()
    w_g = cp(own_block, gz.at[group], 13)
    w_mx.wait()
    lowt[0:qc, :] = mixed[...].T
    hrow = qc // n_dp
    def wout_tile(j, _):
        c = rows_of(j * 256, 256)
        tile32[...] = nn(lowt[0:qc, :], low_res[:, c])
        for z in range(groups):
            wown[z, :, c] = tile32[rows_of((z * PAIR + member) * hrow, hrow), :].astype(bf)
            wsend[z, :, c] = tile32[rows_of((z * PAIR + 1 - member) * hrow, hrow), :].astype(bf)
        return 0
    lax.fori_loop(0, width // 256, wout_tile, 0)
    w_qr.wait()
    for b in range(2):
        for j in range(rows // 128):
            ids_col[b * rows + j * 128:b * rows + (j + 1) * 128, :] = column_of(id_rows[b][:, j * 128:(j + 1) * 128])
    window = rows + TILE
    def attend(i, _):
        r = rows_of(i * TILE, TILE)
        k = pl.ds(pl.multiple_of(i * TILE, TILE), window)
        kpos = lax.broadcasted_iota(jnp.int32, (window, TILE), 0)
        qpos = lax.broadcasted_iota(jnp.int32, (window, TILE), 1) + rows
        bias = jnp.where((ids_col[k, :] == ids_row[:, r].astype(f32)) & (kpos <= qpos), 0.0, -1e30)
        bias = jnp.concatenate([bias, bias], axis=1)
        for g in range(2):
            q2 = jnp.concatenate([q_ref[r, (2 * g) * 128:(2 * g + 1) * 128], q_ref[r, (2 * g + 1) * 128:(2 * g + 2) * 128]], axis=0)
            do2 = jnp.concatenate([gm[r, (2 * g) * 128:(2 * g + 1) * 128], gm[r, (2 * g + 1) * 128:(2 * g + 2) * 128]], axis=0)
            dqt = None
            for s in range(2):
                st = nt(kvar[g, s, k, :], q2) + bias
                peak = jnp.max(st, axis=0, keepdims=True)
                e = jnp.exp(st - peak)
                pt = e * (1.0 / jnp.sum(e, axis=0, keepdims=True))
                dpt = nt(vvar[g, s, k, :], do2)
                delta = jnp.sum(pt * dpt, axis=0, keepdims=True)
                dst = (pt * (dpt - delta)).astype(bf)
                dv[g, s, k, :] += nn(pt.astype(bf), do2)
                dk[g, s, k, :] += nn(dst, q2)
                part = nn(kvart[g, s, :, k], dst)
                dqt = part if dqt is None else dqt + part
            d = dqt.T * HEAD_SIZE ** -0.5
            for b in range(2):
                low[r, (2 * g + b) * 128:(2 * g + b + 1) * 128] = turn(d[b * TILE:(b + 1) * TILE, :], cos_ref[r, :], -sin_ref[r, :]).astype(bf)
        return 0
    wpart = [pl.ds(0, groups // 2), pl.ds(groups // 2, groups // 2)]
    def pair_wout(j):
        return remote(wsend.at[wpart[j]], win.at[wpart[j]], sy, 1 + 4 * j, "dp", pair)
    def own_up():
        return pltpu.make_async_copy(usum.at[group], uz.at[group], load.at[8])
    def up_near():
        return remote(usum.at[at_group(1)], uz.at[group], sz, groups, "dp", at_group(1) * PAIR + member)
    def attend_step(i, _):
        attend(i, 0)
        @pl.when(i == rows // TILE // 2 - 1)
        def _():
            y_u.wait()
            w_own.wait()
            for z in range(groups):
                usum[z] = (u_own[z].astype(f32) + uyin[z].astype(f32)).astype(bf)
            pair_wout(0).start()
            own_up().start()
            up_near().start()
        return 0
    lax.fori_loop(0, rows // TILE, attend_step, 0)
    w_u = own_up()
    z_u = [up_near()]

    def gathered(acc, b):
        r = pl.ds(b * rows, rows)
        lane = lax.broadcasted_iota(jnp.int32, (rows, 128), 1)
        first = acc[0, 0, r, :] + pltpu.roll(acc[0, 1, r, :], HEAD_SIZE, 1)
        second = pltpu.roll(acc[1, 0, r, :], HEAD_SIZE, 1) + acc[1, 1, r, :]
        return jnp.where(lane < HEAD_SIZE, first, second)
    hprev[:, 0:128] = gathered(dk, 0).astype(bf)
    hprev[:, 128:256] = gathered(dv, 0).astype(bf)
    halo = send(hprev, hin, sh, 0, "dp", before)
    pair_wout(1).start()
    y_w = [pair_wout(0), pair_wout(1)]
    z_u = z_u + exchange(usum, uz, groups, range(2, groups))
    qs, ks = qc // groups, 128 // groups
    def to_groups(row0, count, offset, base):
        lg[0, offset:offset + count, :] = lowt[rows_of(row0 + group * count, count), :]
        return [send(lowt.at[rows_of(row0 + at_group(s) * count, count), :], lg.at[s, offset:offset + count, :], sz, base + s - 1,
                     "dp", at_group(s) * PAIR + member) for s in range(1, groups)]
    lowt[0:qc, :] = low[:, 0:qc].T
    z_low = to_groups(0, qs, 0, 3 * groups)
    m2.wait()
    def out_rows(i, _):
        r = rows_of(low_t * half + i * NR, NR)
        m = rows_of(i * NR, NR)
        summed = (amid[m, :].astype(f32) + min2[m, :].astype(f32)).astype(bf)
        go[r, :] = (res[r, :] + summed.astype(f32)).astype(bf)
        return 0
    lax.fori_loop(0, half // NR, out_rows, 0)
    w_out = cp(go.at[half_rows(low_t), :], out_hbm.at[half_rows(low_t), :], 2)
    m3 = send(go.at[half_rows(low_t), :], out_hbm.at[half_rows(low_t), :], sx, 2, "tensor", core)
    w_nm.wait()
    halo.wait()
    kraw = gathered(dk, 1) + hin[:, 0:128].astype(f32)
    low[:, qc:qc + 128] = turn(kraw, cos_ref[...], -sin_ref[...]).astype(bf)
    low[:, qc + 128:qc + 256] = (gathered(dv, 1) + hin[:, 128:256].astype(f32)).astype(bf)
    lowt[qc:qc + 256, :] = low[:, qc:qc + 256].T
    z_low = z_low + to_groups(qc, ks, qs, 4 * groups) + to_groups(qc + 128, ks, qs + ks, 5 * groups)
    for q in y_w:
        q.wait()
    quarter = d_send.shape[0] // 4
    def pair_down(first, count, slot):
        r = pl.ds(first * quarter, count * quarter)
        return send(d_send.at[r, :], d_in.at[r, :], sy, slot, "dp", pair)
    y_d = [pair_down(0, 2, 3)]
    for z in range(groups):
        wown[z] = (wown[z].astype(f32) + win[z].astype(f32)).astype(bf)
    near = flip(group, 1)
    far_group = flip(group, 2) if groups == 4 else near
    z_w = []
    if groups == 4:
        z_w = [send(wown.at[t], win2.at[i], sz, 2 * groups + i, "dp", near * PAIR + member) for i, t in enumerate((near, flip(near, 2)))]
    w_q.wait(); w_k.wait(); w_v.wait()
    def normed_part(j, _):
        c = rows_of(j * 256, 256)
        p = (nt(low[:, 0:qc], wq[c, :]) + nt(low[:, qc:qc + 128], wk[c, :]) + nt(low[:, qc + 128:qc + 256], wv[c, :]))
        res[:, c] = p
        gacc[0:1, c] = jnp.sum(p * normed[:, c].astype(f32), axis=0, keepdims=True) / gain1[0:1, c]
        gacc[1:2, c] = gain2_part[0:1, c] / gain2[0:1, c]
        return 0
    lax.fori_loop(0, width // 256, normed_part, 0)
    hchunk = CHUNK // 2
    chunks = rows // CHUNK
    def own_rows(c):
        return rows_of(c * CHUNK + low_t * hchunk, hchunk)
    def oth_rows(c):
        return rows_of(c * CHUNK + (1 - low_t) * hchunk, hchunk)
    def buf(c):
        return pl.ds(c * hchunk, hchunk)
    flights = {}
    for c in range(chunks):
        amine[buf(c), :] = res[oth_rows(c), :].astype(bf)
        flights[1, c] = send(amine.at[buf(c), :], ain1.at[buf(c), :], sx, 3 + 3 * c, "tensor", core)
    for z in range(groups):
        for m in range(PAIR):
            d0 = (z * PAIR + m) * dcols
            gs[m, z, 0:2, :] = gacc[0:2, d0:d0 + dcols]
    gown[...] = gs[member]
    y_gain = send(gs.at[1 - member], gyi, sg, 0, "dp", pair)
    for c in range(chunks):
        flights[1, c].wait()
        amid[buf(c), :] = (res[own_rows(c), :] + ain1[buf(c), :].astype(f32)).astype(bf)
        flights[2, c] = send(amid.at[buf(c), :], ain2.at[buf(c), :], sx, 4 + 3 * c, "tensor", across)
    for q in first_x:
        q.wait()
    first_c = first_c + [spread_core(k, across) for k in range(steps)]
    for q in first_c + [m3]:
        q.wait()
    w_out.wait()
    tokens = [normed, wo, low_res, go][:groups]
    w_first = []
    for k in range(steps):
        for i, t in enumerate((me_t, core, across, flip(core, 2))):
            src = first_piece(k) if i == 0 else first_all.at[k].at[part(t), :]
            w_first.append(cp(src, tokens[k + 1].at[part(t), :], 16 + k * n_tensor + i))
    y_d.append(pair_down(2, 1, 4))
    for q in z_low + w_first:
        q.wait()
    hg = groups // 2
    def share_cols(j, _):
        z = at_group(j + 1)
        for dst, m in ((qsend, 1 - member), (qown, member)):
            c = rows_of((z * PAIR + m) * dcols, dcols)
            t = nn(lg[0], tokens[0][:, c])
            for k in range(1, groups):
                t = t + nn(lg[k], tokens[k][:, c])
            dst[j] = t.astype(bf)
        @pl.when(j == hg - 1)
        def _():
            pair_q(0).start()
        return 0
    def pair_q(h):
        r = pl.ds(h * hg, hg)
        return remote(qsend.at[r], qin.at[r], sy, 2 + 4 * h, "dp", pair)
    lax.fori_loop(0, groups, share_cols, 0)
    pair_q(1).start()
    for q in z_w:
        q.wait()
    keep, give = wown[group].astype(f32), wown[far_group].astype(f32)
    if groups == 4:
        keep, give = keep + win2[0].astype(f32), give + win2[1].astype(f32)
    wsend[0] = keep.astype(bf)
    wsend[1] = give.astype(bf)
    y_gain.wait()
    gown[...] = gown[...] + gyi[...]
    z_gain = [send(gown.at[at_group(s)], gzi.at[s - 1], sg, s, "dp", at_group(s) * PAIR + member) for s in range(1, groups)]
    w_w = cp(wsend.at[0], wz.at[0], 3)
    z_w = [send(wsend.at[1], wz.at[1], sz, 2 * groups + 2, "dp", far_group * PAIR + member)]
    y_d.append(pair_down(3, 1, 7))
    w_x = cp(x_hbm, normed, 9)
    w_x.wait()
    def norm_one(r):
        v = normed[r, :].astype(f32)
        root = lax.rsqrt(jnp.mean(v * v, axis=1, keepdims=True) + EPS)
        up = gn[r, :].astype(f32) * gain1[...]
        mean = jnp.mean(up * v, axis=1, keepdims=True)
        low_res[r, :] = (resid[r, :] + root * up - v * (root * root * root * mean)).astype(bf)
    def sum_q(h):
        pair_q(h).wait()
        for j in range(h * hg, h * hg + hg):
            qown[j] = (qown[j].astype(f32) + qin[j].astype(f32)).astype(bf)
        return [send(qown.at[j], qz.at[group], sz, 6 * groups + j, "dp", at_group(j + 1) * PAIR + member) for j in range(h * hg, min(h * hg + hg, groups - 1))]
    for c in range(chunks):
        flights[2, c].wait()
        gn[own_rows(c), :] = (amid[buf(c), :].astype(f32) + ain2[buf(c), :].astype(f32)).astype(bf)
        flights[3, c] = send(gn.at[own_rows(c), :], gn.at[own_rows(c), :], sx, 5 + 3 * c, "tensor", core)
        norm_one(own_rows(c))
        flights[3, c].wait()
        norm_one(oth_rows(c))
        if c == chunks // 2 - 1:
            z_q = sum_q(0)
    w_gin = cp(low_res, gin_hbm, 1)
    z_q = z_q + sum_q(1)
    w_q2 = cp(qown.at[groups - 1], qz.at[group], 14)
    for q in z_gain:
        q.wait()
    total = gown[group]
    for s in range(1, groups):
        total = total + gzi[s - 1]
    gt[0] = total
    t1 = send(gt.at[0], gti.at[0], sg, groups, "tensor", core)
    t1.wait()
    gt[1] = gt[0] + gti[0]
    t2 = send(gt.at[1], gti.at[1], sg, groups + 1, "tensor", across)
    t2.wait()
    gains_ref[...] = gt[1] + gti[1]
    for q in z_g + z_u + z_w + z_q + y_d:
        q.wait()
    for q in [w_g, w_u, w_w, w_gin, w_q2]:
        q.wait()

def backward(gn, residual, x, grad_output, mlp_part, normed, wo, wq, wk, wv, g_sum, u_own, u_send, d_send, mixed, q, kv, first, gain1, gain2, gain2_part,
             id_rows, ids_row, cosine, sine, n_dp, n_tensor):
    rows, width = x.shape
    groups = n_dp // PAIR
    share = g_sum.shape[1]
    dcols = width // n_dp
    qc = wq.shape[1]
    cols = qc + 256
    share_q = cols // groups
    A = pl.BlockSpec(memory_space=pl.ANY)
    vm = pl.BlockSpec(memory_space=pltpu.VMEM)
    bf, f32 = jnp.bfloat16, jnp.float32
    sd = jax.ShapeDtypeStruct
    V = pltpu.VMEM
    D = pltpu.SemaphoreType.DMA
    half = rows // 2
    hrow = qc // n_dp
    act = V((rows, width), bf)
    return pl.pallas_call(
        functools.partial(backward_kernel, n_dp, n_tensor),
        out_shape=(sd((rows, width), bf), sd((rows, width), bf), sd((groups, share, dcols), bf), sd((groups, share, dcols), bf),
                   sd(d_send.shape, bf), sd((2, hrow, width), bf), sd((groups, share_q, dcols), bf),
                   sd((groups - 1, rows, width), bf), sd((8, dcols), f32)),
        in_specs=[A] * 18 + [vm] * 7,
        out_specs=(A,) * 8 + (vm,),
        scratch_shapes=[act, V((rows, width), f32), act, act, V((qc, width), bf), V((width, qc), bf), V((width, 128), bf), V((width, 128), bf),
                        V((rows, qc), bf), V((rows, qc), bf), V((2, rows, 256), bf), V((rows, width), f32), act, V((rows, qc), bf),
                        V((2, 2, 2 * rows, 128), bf), V((2, 2, 2 * rows, 128), bf), V((2, 2, 128, 2 * rows), bf),
                        V((2, 2, 2 * rows, 128), f32), V((2, 2, 2 * rows, 128), f32), V((2 * rows, 1), f32),
                        V((rows, cols), bf), V((cols, rows), bf), V((qc, 256), f32),
                        V((groups, hrow, width), bf), V((groups, hrow, width), bf), V((groups, hrow, width), bf), V((2, hrow, width), bf),
                        V((share, dcols), bf), *[V((groups, share, dcols), bf)] * 3,
                        V((groups, share_q, rows), bf), *[V((groups, share_q, dcols), bf)] * 3,
                        *[V((half, width), bf)] * 6,
                        V((rows, 256), bf), V((rows, 256), bf), V((8, width), f32), V((PAIR, groups, 8, dcols), f32), V((groups, 8, dcols), f32),
                        V((groups, 8, dcols), f32), V((groups - 1, 8, dcols), f32), V((2, 8, dcols), f32), V((2, 8, dcols), f32),
                        D((16 + groups * n_tensor,)), D((2, 8)), D((2, 8 * groups)), D((2, 3 + 3 * (rows // CHUNK) + 3 * groups)), D((2, 1)), D((2, groups + 2))],
        compiler_params=pltpu.CompilerParams(collective_id=4, has_side_effects=True, vmem_limit_bytes=67043328),
        cost_estimate=pl.CostEstimate(flops=4 * rows * width * (2 * qc + 256) + 40 * rows * rows * 5 * 128, bytes_accessed=40 * rows * width, transcendentals=8 * rows * rows),
        name="attention_backward",
    )(gn, residual, x, grad_output, mlp_part, normed, wo, wq, wk, wv, g_sum, u_own, u_send, d_send, mixed, q, kv, first,
      gain1.reshape(1, width), gain2.reshape(1, width), gain2_part, id_rows, ids_row, cosine, sine)

def finish_kernel(qc, kc, out_hbm, gin_hbm, gz_hbm, uz_hbm, d_own_hbm, d_in_hbm, wz_hbm, qz_hbm, gains,
                  gain1_o, gain2_o, out_o, gin_o, gate_o, up_o, down_o, wout_o, query_o, key_o, value_o,
                  act1, act2, gz, uz, d_own, d_in, wz, qz, gate, up, down, wout, query, key, value, ins, outs):
    f32 = jnp.float32
    groups, share, dcols = gz.shape
    gain1_o[...] = gains[0:1, :]
    gain2_o[...] = gains[1:2, :]
    loads = [pltpu.make_async_copy(s, d, ins.at[i]) for i, (s, d) in enumerate([
        (gz_hbm, gz), (uz_hbm, uz), (out_hbm, act1), (gin_hbm, act2), (d_own_hbm, d_own), (d_in_hbm, d_in), (wz_hbm, wz), (qz_hbm, qz)])]
    for c in loads:
        c.start()
    stores = []
    def store(src, dst):
        c = pltpu.make_async_copy(src, dst, outs.at[len(stores)])
        c.start()
        stores.append(c)
    for got, held, dst, i in ((gz, gate, gate_o, 0), (uz, up, up_o, 1)):
        loads[i].wait()
        for z in range(groups):
            for h in range(share // 256):
                held[:, z * share + h * 256:z * share + (h + 1) * 256] = got[z, h * 256:(h + 1) * 256, :].astype(f32).T
        store(held, dst)
    loads[2].wait()
    store(act1, out_o)
    loads[3].wait()
    store(act2, gin_o)
    loads[4].wait()
    loads[5].wait()
    down[...] = d_own[...].astype(f32) + d_in[...].astype(f32)
    store(down, down_o)
    loads[6].wait()
    wout[...] = wz[0].astype(f32) + wz[1].astype(f32)
    store(wout, wout_o)
    loads[7].wait()
    qs, ks = qc // groups, kc // groups
    for z in range(groups):
        query[:, z * qs:(z + 1) * qs] = qz[z, 0:qs, :].astype(f32).T
    key[...] = jnp.concatenate([qz[z, qs:qs + ks, :] for z in range(groups)], axis=0).astype(f32).T
    value[...] = jnp.concatenate([qz[z, qs + ks:qs + 2 * ks, :] for z in range(groups)], axis=0).astype(f32).T
    store(query, query_o)
    store(key, key_o)
    store(value, value_o)
    for c in stores:
        c.wait()

def finish_all(out, gin, gz, uz, d_own, d_in, wz, qz, gains, qc, kc):
    vm = pl.BlockSpec(memory_space=pltpu.VMEM)
    A = pl.BlockSpec(memory_space=pl.ANY)
    bf, f32 = jnp.bfloat16, jnp.float32
    sd = jax.ShapeDtypeStruct
    V = pltpu.VMEM
    groups, share, dcols = gz.shape
    shapes = [(dcols, groups * share), (dcols, groups * share), d_own.shape, wz.shape[1:], (dcols, qc), (dcols, kc), (dcols, kc)]
    return pl.pallas_call(
        functools.partial(finish_kernel, qc, kc),
        out_shape=(sd((1, dcols), f32), sd((1, dcols), f32), sd(out.shape, bf), sd(gin.shape, bf)) + tuple(sd(s, f32) for s in shapes),
        in_specs=[A] * 8 + [vm], out_specs=(vm,) * 2 + (A,) * 9,
        scratch_shapes=[V(a.shape, bf) for a in (out, gin, gz, uz, d_own, d_in, wz, qz)] + [V(s, f32) for s in shapes] + [pltpu.SemaphoreType.DMA((8,)), pltpu.SemaphoreType.DMA((9,))],
        compiler_params=pltpu.CompilerParams(vmem_limit_bytes=67043328),
        cost_estimate=pl.CostEstimate(flops=8 * out.size, bytes_accessed=24 << 20, transcendentals=0),
        name="finish",
    )(out, gin, gz, uz, d_own, d_in, wz, qz, gains)


def rope_table(half_count, copies=1):
    adjusted = []
    for index in range(half_count):
        base_value = 500000.0 ** (-index / half_count)
        wave_length = 2.0 * math.pi / base_value
        smooth = (8192.0 / wave_length - 1.0) / 3.0
        if wave_length > 8192.0:
            adjusted.append(base_value / 32.0)
        elif wave_length >= 2048.0:
            adjusted.append((1.0 - smooth) * base_value / 32.0 + smooth * base_value)
        else:
            adjusted.append(base_value)
    return jnp.asarray(adjusted * copies, dtype=jnp.float32)


def rope_angles(start_row, count_rows, half_count):
    positions = (start_row + jnp.arange(count_rows, dtype=jnp.int32)).astype(jnp.float32)
    phase_angle = positions[:, None] * rope_table(half_count)[None, :]
    return (jnp.cos(phase_angle)[:, None, :], jnp.sin(phase_angle)[:, None, :])


def rotate_halves(values, cosine_table, sine_values):
    half_size = values.shape[-1] // 2
    first_half = values[..., :half_size]
    second_half = values[..., half_size:]
    return jnp.concatenate(
        [
            first_half * cosine_table - second_half * sine_values,
            second_half * cosine_table + first_half * sine_values,
        ],
        axis=-1,
    )


def norm_rows(values, gain_row):
    inverse_root = lax.rsqrt(jnp.mean(values * values, axis=-1, keepdims=True) + NORM_EPSILON)
    return (inverse_root, values * inverse_root * gain_row)


def norm_back(values, inverse_root, gain_row, upstream):
    scaled = gain_row * upstream
    return inverse_root * scaled - values * inverse_root**3 * jnp.mean(
        scaled * values, axis=-1, keepdims=True
    )


def passed_along(block, axis, distance):
    devices = range(lax.axis_size(axis))
    route = [(i - distance, i) for i in devices if i - distance in devices]
    return lax.ppermute(block, axis, route)


def tensor_swap(block, bit):
    return lax.ppermute(block, "tensor", [(i, i ^ bit) for i in range(lax.axis_size("tensor"))])


def pair_swap(block):
    return lax.ppermute(block, "dp", [(i, i ^ 1) for i in range(lax.axis_size("dp"))])


def group_shift(block, distance):
    count = lax.axis_size("dp")
    groups = count // PAIR
    return lax.ppermute(
        block,
        "dp",
        [(i, ((i // PAIR + distance) % groups) * PAIR + i % PAIR) for i in range(count)],
    )


def tensor_sum(part):
    half = part.shape[1] // 2
    low = lax.axis_index("tensor") % 2
    first, second = part[:, :half], part[:, half:]
    mine = jnp.where(low == 0, first, second)
    other = jnp.where(low == 0, second, first).astype(jnp.bfloat16)
    mine = mine + tensor_swap(other, 1).astype(jnp.float32)
    bit = 2
    while bit < lax.axis_size("tensor"):
        rounded = mine.astype(jnp.bfloat16)
        mine = rounded.astype(jnp.float32) + tensor_swap(rounded, bit).astype(jnp.float32)
        bit *= 2
    mine = mine.astype(jnp.bfloat16)
    other = tensor_swap(mine, 1)
    return jnp.concatenate(
        [jnp.where(low == 0, mine, other), jnp.where(low == 0, other, mine)], axis=1
    ).astype(jnp.float32)


def gather_groups(block):
    half = block.shape[1] // 2
    low = lax.axis_index("tensor") % 2
    piece = lax.dynamic_slice_in_dim(block, low * half, half, axis=1)
    rows = [block]
    for _ in range(lax.axis_size("dp") // PAIR - 1):
        piece = group_shift(piece, 1)
        other = tensor_swap(piece, 1)
        rows.append(
            jnp.concatenate(
                [jnp.where(low == 0, piece, other), jnp.where(low == 0, other, piece)], axis=1
            )
        )
    return jnp.concatenate(rows, axis=0)


def pair_sum(part):
    member = lax.axis_index("dp") % PAIR
    mine = lax.dynamic_index_in_dim(part, member, 1, keepdims=False)
    other = lax.dynamic_index_in_dim(part, 1 - member, 1, keepdims=False)
    return mine + pair_swap(other.astype(jnp.bfloat16)).astype(jnp.float32)


def group_exchange(blocks):
    groups = blocks.shape[0]
    group = lax.axis_index("dp") // PAIR
    received = []
    for distance in range(groups):
        block = lax.dynamic_index_in_dim(blocks, (group + distance) % groups, 0, keepdims=False)
        received.append(block if distance == 0 else group_shift(block, distance))
    return received


def scatter_sum(part):
    summed = pair_sum(part)
    groups = summed.shape[0]
    group = lax.axis_index("dp") // PAIR
    total = lax.dynamic_index_in_dim(summed, group, 0, keepdims=False)
    rounded = summed.astype(jnp.bfloat16)
    for block in group_exchange(rounded)[1:]:
        total = total + block.astype(jnp.float32)
    return total


def block_scores(query_rows, key_rows, query_ids, key_ids, query_pos, key_pos):
    scores = jnp.einsum(
        "qgrd,kgd->grqk", query_rows, key_rows, preferred_element_type=jnp.float32
    ) * HEAD_SIZE ** (-0.5)
    allowed = (query_ids[:, None] == key_ids[None, :]) & (key_pos[None, :] <= query_pos[:, None])
    return jnp.where(allowed, scores, -1e30)


def block_forward(query_rows, key_rows, value_rows, query_ids, key_ids, query_pos, key_pos):
    scores = block_scores(query_rows, key_rows, query_ids, key_ids, query_pos, key_pos)
    row_peak = jnp.max(scores, axis=-1, keepdims=True)
    logsum = row_peak + jnp.log(jnp.sum(jnp.exp(scores - row_peak), axis=-1, keepdims=True))
    prob_low = jnp.exp(scores - logsum).astype(jnp.bfloat16)
    mixed_rows = jnp.einsum(
        "grqk,kgd->qgrd", prob_low, value_rows, preferred_element_type=jnp.float32
    )
    return (mixed_rows.astype(jnp.bfloat16), logsum)


def block_backward(
    query_rows,
    key_rows,
    value_rows,
    out_rows,
    grad_rows,
    logsum,
    query_ids,
    key_ids,
    query_pos,
    key_pos,
):
    scores = block_scores(query_rows, key_rows, query_ids, key_ids, query_pos, key_pos)
    prob_rows = jnp.exp(scores - logsum)
    grad_vals = jnp.einsum(
        "grqk,qgrd->kgd",
        prob_rows.astype(jnp.bfloat16),
        grad_rows,
        preferred_element_type=jnp.float32,
    )
    delta_rows = jnp.sum(out_rows.astype(jnp.float32) * grad_rows.astype(jnp.float32), axis=-1)
    grad_probs = jnp.einsum(
        "qgrd,kgd->grqk", grad_rows, value_rows, preferred_element_type=jnp.float32
    )
    grad_scores = (
        prob_rows * (grad_probs - jnp.transpose(delta_rows, (1, 2, 0))[..., None])
    ).astype(jnp.bfloat16)
    grad_query_rows = jnp.einsum(
        "grqk,kgd->qgrd", grad_scores, key_rows, preferred_element_type=jnp.float32
    ) * HEAD_SIZE ** (-0.5)
    grad_key_rows = jnp.einsum(
        "grqk,qgrd->kgd", grad_scores, query_rows, preferred_element_type=jnp.float32
    ) * HEAD_SIZE ** (-0.5)
    return (grad_query_rows, grad_key_rows, grad_vals)


def dot(form, left, right):
    return jnp.einsum(form, left, right, preferred_element_type=jnp.float32)


def gated(gate_value, up_value):
    return (jax.nn.silu(gate_value) * up_value).astype(jnp.bfloat16)


def gated_back(grad_hidden, gate_value, up_value):
    sigmoid_gate = jax.nn.sigmoid(gate_value)
    grad_gate_low = (
        grad_hidden * up_value * sigmoid_gate * (1.0 + gate_value * (1.0 - sigmoid_gate))
    ).astype(jnp.bfloat16)
    return grad_gate_low, (grad_hidden * jax.nn.silu(gate_value)).astype(jnp.bfloat16)


def shards_plain(
    inputs,
    norm1_gain,
    query_weight,
    key_weight,
    value_weight,
    w_out,
    norm2_gain,
    w_gate,
    w_up,
    w_down,
    doc_ids,
    grad_output,
):
    tok_rows, width = inputs.shape
    heads_here = query_weight.shape[1] // HEAD_SIZE
    kv_here = key_weight.shape[1] // HEAD_SIZE
    group_size = heads_here // kv_here
    n_dp = lax.axis_size("dp")
    groups = n_dp // PAIR
    group = lax.axis_index("dp") // PAIR
    offset = lax.axis_index("dp") * tok_rows
    grad_all = gather_groups(grad_output)

    cosine_table, sine_values = rope_angles(offset, tok_rows, HEAD_SIZE // 2)
    inputs_wide = inputs.astype(jnp.float32)
    root_one, normed = norm_rows(inputs_wide, norm1_gain)
    normed_low = normed.astype(jnp.bfloat16)
    query_raw = dot("td,dh->th", normed_low, query_weight).reshape(tok_rows, heads_here, HEAD_SIZE)
    key_raw = dot("td,dh->th", normed_low, key_weight).reshape(tok_rows, kv_here, HEAD_SIZE)
    value_low = dot("td,dh->th", normed_low, value_weight).astype(jnp.bfloat16)
    query_low = (
        rotate_halves(query_raw, cosine_table, sine_values)
        .astype(jnp.bfloat16)
        .reshape(tok_rows, kv_here, group_size, HEAD_SIZE)
    )
    key_low = (
        rotate_halves(key_raw, cosine_table, sine_values)
        .astype(jnp.bfloat16)
        .reshape(tok_rows, kv_here * HEAD_SIZE)
    )
    query_ids = doc_ids + 1
    tail = jnp.concatenate([key_low, value_low], axis=1)
    prev_tail = passed_along(tail, "dp", 1)
    prev_ids = passed_along(query_ids, "dp", 1)
    both = jnp.concatenate([prev_tail, tail], axis=0)
    keys_all = both[:, : kv_here * HEAD_SIZE].reshape(2 * DOC_MAX, kv_here, HEAD_SIZE)
    values_all = both[:, kv_here * HEAD_SIZE :].reshape(2 * DOC_MAX, kv_here, HEAD_SIZE)
    ids_all = jnp.concatenate([prev_ids, query_ids])
    pos_all = offset - DOC_MAX + jnp.arange(tok_rows + DOC_MAX, dtype=jnp.int32)
    query_pos = pos_all[DOC_MAX:]
    mixed_block, logsum_block = block_forward(
        query_low, keys_all, values_all, query_ids, ids_all, query_pos, pos_all
    )
    mixed_low = mixed_block.reshape(tok_rows, heads_here * HEAD_SIZE)
    residual = inputs_wide + tensor_sum(dot("te,ed->td", mixed_low, w_out))

    root_two, normed_two = norm_rows(residual, norm2_gain)
    normed_two_low = normed_two.astype(jnp.bfloat16)
    normed_all = gather_groups(normed_two_low)
    gate_value = dot("td,df->tf", normed_two_low, w_gate)
    up_value = dot("td,df->tf", normed_two_low, w_up)
    grad_hidden = dot("td,fd->tf", grad_output, w_down)
    hidden_low = gated(gate_value, up_value)
    grad_gate_low, grad_up_low = gated_back(grad_hidden, gate_value, up_value)
    normed_two_part = dot("tf,df->td", grad_gate_low, w_gate) + dot("tf,df->td", grad_up_low, w_up)
    grad_normed_two = tensor_sum(normed_two_part)
    gain_two_part = jnp.sum(normed_two_part * residual * root_two, axis=0)
    output = (residual + tensor_sum(dot("tf,fd->td", hidden_low, w_down))).astype(jnp.bfloat16)

    share = w_gate.shape[1] // groups
    gate_share = lax.dynamic_slice_in_dim(w_gate, group * share, share, axis=1)
    up_share = lax.dynamic_slice_in_dim(w_up, group * share, share, axis=1)
    down_share = lax.dynamic_slice_in_dim(w_down, group * share, share, axis=0)
    gate_all = dot("td,df->tf", normed_all, gate_share)
    up_all = dot("td,df->tf", normed_all, up_share)
    grad_hidden_all = dot("td,fd->tf", grad_all, down_share)
    hidden_all = gated(gate_all, up_all)
    gate_low_all, up_low_all = gated_back(grad_hidden_all, gate_all, up_all)
    down_part = dot("tf,td->fd", hidden_all, grad_all)
    grad_wdown = pair_sum(down_part.reshape(1, PAIR, share // PAIR, width))[0]
    rows_here = width // n_dp

    def column_grad(low_all):
        part = dot("td,tf->df", normed_all, low_all)
        summed = pair_sum(part.reshape(groups, PAIR, rows_here, share)).astype(jnp.bfloat16)
        full = jnp.zeros((rows_here, groups * share), jnp.float32)
        for distance, block in enumerate(group_exchange(summed)):
            full = lax.dynamic_update_slice_in_dim(
                full, block.astype(jnp.float32), ((group - distance) % groups) * share, axis=1
            )
        return full

    grad_wgate = column_grad(gate_low_all)
    grad_wup = column_grad(up_low_all)

    grad_residual = grad_output.astype(jnp.float32) + norm_back(
        residual, root_two, norm2_gain, grad_normed_two
    )
    grad_res_low = grad_residual.astype(jnp.bfloat16)
    wout_part = dot("te,td->ed", mixed_low, grad_res_low)
    grad_wout = scatter_sum(wout_part.reshape(groups, PAIR, -1, width))
    grad_mixed = (
        dot("td,ed->te", grad_res_low, w_out)
        .astype(jnp.bfloat16)
        .reshape(tok_rows, kv_here, group_size, HEAD_SIZE)
    )
    mixed_view = mixed_low.reshape(tok_rows, kv_here, group_size, HEAD_SIZE)
    grad_query_rows, grad_key_rows, grad_value_rows = block_backward(
        query_low,
        keys_all,
        values_all,
        mixed_view,
        grad_mixed,
        logsum_block,
        query_ids,
        ids_all,
        query_pos,
        pos_all,
    )
    sent = jnp.concatenate(
        [
            grad_key_rows.reshape(2 * DOC_MAX, kv_here * HEAD_SIZE),
            grad_value_rows.reshape(2 * DOC_MAX, kv_here * HEAD_SIZE),
        ],
        axis=1,
    )
    back = passed_along(sent[:DOC_MAX].astype(jnp.bfloat16), "dp", -1).astype(jnp.float32)
    own = sent[DOC_MAX:] + back
    grad_qraw = grad_query_rows.reshape(tok_rows, heads_here, HEAD_SIZE)
    query_low_gradient = (
        rotate_halves(grad_qraw, cosine_table, -sine_values)
        .astype(jnp.bfloat16)
        .reshape(tok_rows, heads_here * HEAD_SIZE)
    )
    key_low_gradient = (
        rotate_halves(
            own[:, : kv_here * HEAD_SIZE].reshape(tok_rows, kv_here, HEAD_SIZE),
            cosine_table,
            -sine_values,
        )
        .astype(jnp.bfloat16)
        .reshape(tok_rows, kv_here * HEAD_SIZE)
    )
    value_low_gradient = own[:, kv_here * HEAD_SIZE :].astype(jnp.bfloat16)
    low_gradient = jnp.concatenate(
        [query_low_gradient, key_low_gradient, value_low_gradient], axis=1
    )
    normed_one_part = (
        dot("kl,ql->kq", query_low_gradient, query_weight)
        + dot("kl,ql->kq", key_low_gradient, key_weight)
        + dot("kl,ql->kq", value_low_gradient, value_weight)
    )
    grad_normed_one = tensor_sum(normed_one_part)
    gain_one_part = jnp.sum(normed_one_part * inputs_wide * root_one, axis=0)
    qkv_part = dot("wj,wq->jq", normed_low, low_gradient)
    columns = qkv_part.shape[1]
    gains = jnp.stack(
        [gain_one_part.reshape(n_dp, rows_here), gain_two_part.reshape(n_dp, rows_here)], axis=1
    )
    gains = jnp.pad(gains, ((0, 0), (0, 14), (0, columns - rows_here)))
    qkv_part = jnp.concatenate([qkv_part.reshape(n_dp, rows_here, columns), gains], axis=1)
    qkv_sum = scatter_sum(qkv_part.reshape(groups, PAIR, rows_here + 16, columns))
    grad_qkv = qkv_sum[:rows_here]
    gain_sums = qkv_sum[rows_here : rows_here + 16, :rows_here]
    bit = 1
    while bit < lax.axis_size("tensor"):
        gain_sums = gain_sums + tensor_swap(gain_sums, bit)
        bit *= 2
    grad_input_norm = norm_back(inputs_wide, root_one, norm1_gain, grad_normed_one)
    grad_inputs = (grad_residual + grad_input_norm).astype(jnp.bfloat16)
    q_columns = query_weight.shape[1]
    k_columns = key_weight.shape[1]
    return (
        output,
        grad_inputs,
        gain_sums[0],
        grad_qkv[:, :q_columns],
        grad_qkv[:, q_columns : q_columns + k_columns],
        grad_qkv[:, q_columns + k_columns :],
        grad_wout,
        gain_sums[1],
        grad_wgate,
        grad_wup,
        grad_wdown,
    )


def shards(
    inputs,
    norm1_gain,
    query_weight,
    key_weight,
    value_weight,
    w_out,
    norm2_gain,
    w_gate,
    w_up,
    w_down,
    doc_ids,
    grad_output,
):
    tok_rows, width = inputs.shape
    heads_here = query_weight.shape[1] // HEAD_SIZE
    kv_here = key_weight.shape[1] // HEAD_SIZE
    group_size = heads_here // kv_here
    n_dp = lax.axis_size("dp")
    groups = n_dp // PAIR
    group = lax.axis_index("dp") // PAIR
    offset = lax.axis_index("dp") * tok_rows
    n_tensor = lax.axis_size("tensor")
    half = HEAD_SIZE // 2
    lanes = jnp.arange(4 * half, dtype=jnp.int32)
    positions = (offset + jnp.arange(tok_rows, dtype=jnp.int32)).astype(jnp.float32)
    angles = positions[:, None] * rope_table(half, 4)[None, :]
    cosine = jnp.cos(angles)
    sine = jnp.sin(angles) * jnp.where(lanes % HEAD_SIZE < half, -1.0, 1.0)[None, :]
    normed_low, query_scaled, kv, id_rows, mixed_low, residual, normed_two_low, gate_t, up_t, part_g, cross_g = attend_forward(
        inputs, norm1_gain, query_weight, key_weight, value_weight, w_out, norm2_gain, cosine, sine, doc_ids, grad_output,
        w_gate, w_up, n_dp, n_tensor)
    mlp_part, back_part, normed_rest, rest_g, gain_two_part = mlp(normed_two_low, grad_output, part_g, cross_g, w_gate, w_up, w_down, n_dp, n_tensor)
    d_own, d_send, g_sum, u_own, u_send, grad_normed_two, first_part = wgrad(
        normed_two_low, normed_rest, grad_output, part_g, cross_g, rest_g, gate_t, up_t, w_down, back_part, normed_low, n_dp, n_tensor)
    output, grad_inputs, gate_blocks, up_blocks, d_in, wout_blocks, qkv_blocks, _, gain_sums = backward(
        grad_normed_two, residual, inputs, grad_output, mlp_part, normed_low, w_out, query_weight, key_weight, value_weight,
        g_sum, u_own, u_send, d_send, mixed_low, query_scaled, kv, first_part, norm1_gain, norm2_gain, gain_two_part,
        id_rows, doc_ids.reshape(1, tok_rows), cosine, sine, n_dp, n_tensor)
    gain_one, gain_two, output, grad_inputs, grad_wgate, grad_wup, grad_wdown, grad_wout, grad_wquery, grad_wkey, grad_wvalue = finish_all(
        output, grad_inputs, gate_blocks, up_blocks, d_own, d_in, wout_blocks, qkv_blocks, gain_sums, query_weight.shape[1], key_weight.shape[1])
    rows_here = width // n_dp
    return (
        output,
        grad_inputs,
        gain_one.reshape(rows_here),
        grad_wquery,
        grad_wkey,
        grad_wvalue,
        grad_wout,
        gain_two.reshape(rows_here),
        grad_wgate,
        grad_wup,
        grad_wdown,
    )


def kernels_fit(mesh, *args):
    n_dp, n_tensor = mesh.shape["dp"], mesh.shape["tensor"]
    width = args[0].shape[1]
    return (
        n_dp % PAIR == 0
        and n_dp // PAIR in (2, 4)
        and n_tensor == 4
        and width // n_dp in (128, 256)
        and args[7].shape[1] // n_tensor // (n_dp // PAIR) % 256 == 0
        and args[0].shape[0] // n_dp == DOC_MAX
        and args[3].shape[1] // n_tensor == 2 * HEAD_SIZE
        and args[2].shape[1] == 4 * args[3].shape[1]
    )


def solution(mesh):
    def step(*args):
        return mapped(mesh, shards if kernels_fit(mesh, *args) else shards_plain)(*args)

    return step


def mapped(mesh, function):
    return jax.shard_map(
        function,
        mesh=mesh,
        in_specs=(
            P("dp", None),
            P(),
            P(None, "tensor"),
            P(None, "tensor"),
            P(None, "tensor"),
            P("tensor", None),
            P(),
            P(None, "tensor"),
            P(None, "tensor"),
            P("tensor", None),
            P("dp"),
            P("dp", None),
        ),
        out_specs=(
            P("dp", None),
            P("dp", None),
            P("dp"),
            P("dp", "tensor"),
            P("dp", "tensor"),
            P("dp", "tensor"),
            P(("tensor", "dp"), None),
            P("dp"),
            P("dp", "tensor"),
            P("dp", "tensor"),
            P(("tensor", "dp"), None),
        ),
        check_vma=False,
    )
```
